128 devices in a mesh: seq: 32 (over z, x, core), batch: 4 (over y).
Axes of the slice: x: 4, y: 4, z: 4, core: 2. Of those that a mesh axis runs over, the one named last changes fastest.
Arguments:
- hidden: bfloat16 [4, 4096, 1024], P('batch', 'seq'), may hold values from -6 to 6
- queries: bfloat16 [4, 4096, 2048], P('batch', 'seq'), may hold values from -0.19921875 to 0.19921875
- w_key: bfloat16 [1024, 2048], replicated, may hold values from -0.1875 to 0.1875
- w_value: bfloat16 [1024, 2048], replicated, may hold values from -0.1875 to 0.1875
- log_gate: float32 [4, 32, 4096], P('batch', None, 'seq'), may hold values from -0.1 to 0, as said below
- level_gain: float32 [32, 18], replicated, may hold values from 0.1 to 1
- segment_ids: int32 [4, 4096], P('batch', 'seq'), may hold values from 0 to 7, never falling along the last dimension, each value on 1 to 1024 neighbouring positions
- out_grad: bfloat16 [4, 4096, 2048], P('batch', 'seq'), may hold values from -0.19921875 to 0.19921875
Outputs:
- query_grad: bfloat16 [4, 4096, 2048], P('batch', 'seq')
- input_grad: bfloat16 [4, 4096, 1024], P('batch', 'seq')
- gate_grad: float32 [4, 32, 4096], P('batch', None, 'seq')
- key_weight_grad: float32 [1024, 2048], P(('seq', 'batch'))
- value_weight_grad: float32 [1024, 2048], P(('seq', 'batch'))
- gain_grad: float32 [32, 18], replicated
The draws below stay inside these ranges and needn't reach their ends.
Inputs may be any that keep to these rules, and one draw needn't show every extreme that they name: `log_gate`: entries are zero or negative. `segment_ids`: along each sequence the ids never fall, so each document is one run of tokens; the longest document has exactly a quarter of 4096 tokens in every draw.
All inputs are finite; a program needn't handle non-finite values.
Results may differ from the reference program's by a relative error of at most 0.0058.
Values sent between devices are 32-bit elements; how exact they have to be, the bound alone decides.
A program may use at most 128 MiB of HBM per device.

```python
import math
import jax
import jax.numpy as jnp
import numpy as np
from jax import lax

D = 1024
H = 32
P_SIZE = 64
LEVELS = 18
TOK_DEV = 128
DOCS = 8
SEQS = 4
LENGTH = 4096


def draw_log_gate(key, part):
    head_key, slow_key, fast_key, block_key, token_key = jax.random.split(key, 5)
    slow_share = 0.5
    is_slow = jax.random.uniform(head_key, (1, H, 1)) < slow_share
    slow_rate = jnp.exp(jax.random.uniform(slow_key, (1, H, 1), minval=math.log(0.05), maxval=0.0)) / LENGTH
    fast_rate = jnp.exp(jax.random.uniform(fast_key, (1, H, 1), minval=math.log(1.0 / 50.0), maxval=math.log(1.0 / 30.0)))
    head_rates = jnp.where(is_slow, slow_rate, fast_rate)
    blocks = jnp.exp(jax.random.uniform(block_key, (SEQS, H, LENGTH // TOK_DEV), minval=math.log(0.5), maxval=math.log(2.0)))
    per_block = jnp.repeat(blocks, TOK_DEV, axis=2)
    tokens = jnp.exp(jax.random.uniform(token_key, (SEQS, H, LENGTH), minval=math.log(0.3), maxval=math.log(1.5)))
    return (-(head_rates * per_block * tokens)).astype(jnp.float32)


def spiked(values, own_key, source, target, blocks, factor):
    def block_of(position):
        return (jnp.arange(values.shape[position]) // (values.shape[position] // blocks)).reshape((-1,) + (1,) * (values.ndim - 1 - position))

    near = jax.random.permutation(own_key, blocks)[block_of(target)]
    far = (block_of(target) + blocks // 2) % blocks
    return jnp.where((block_of(source) == near) | (block_of(source) == far), factor * values, values)


def block_scale(key, extent, pieces, least, largest):
    level = 1.0
    for position, parts in pieces:
        draws = jax.random.uniform(jax.random.fold_in(jax.random.fold_in(key, 6), position), (parts,), jnp.float32, least / len(pieces), largest / len(pieces))
        level = level * jnp.repeat(jnp.exp(draws), extent[position] // parts).reshape((-1,) + (1,) * (len(extent) - 1 - position))
    return level


def profile(amount, total, most, slope):
    weights = [(1 << 20) // math.isqrt(standing ** slope) + 1 for standing in range(2, amount + 1)]
    rest, counts = total - most - (amount - 1), [1] * (amount - 1)
    while rest > 0:
        candidates = [i for i in range(amount - 1) if counts[i] < most]
        mass, left = sum([weights[i] for i in candidates]), rest
        for i in candidates:
            extra = min(most - counts[i], max(1, left * weights[i] // mass), rest)
            counts[i] = counts[i] + extra
            rest = rest - extra
    return np.array([most] + counts)


def uneven(rng, number_of, total, most, lean):
    if number_of == 2:
        one = jax.random.randint(rng, (), max(1, total - most), min(most, total - 1) + 1)
        return jnp.stack([one, total - one])
    lengths = jnp.asarray(profile(number_of, total, most, lean), jnp.int32)
    pairs = (number_of - 1) // 2
    giver, taker = lengths[1:1 + 2 * pairs:2], lengths[2:2 + 2 * pairs:2]
    room = jnp.minimum(giver - 1, most - taker)
    passed = jax.random.randint(jax.random.fold_in(rng, 1), (pairs,), 0, 1 << 20) % (room + 1)
    lengths = lengths.at[1:1 + 2 * pairs:2].set(giver - passed).at[2:2 + 2 * pairs:2].set(taker + passed)
    return lengths[jax.random.permutation(jax.random.fold_in(rng, 2), number_of)]


def normal_values(own_key, extent, width, bound, cuts=(), kind=jnp.bfloat16):
    gain = block_scale(own_key, extent, cuts, -0.22, 0.18) if cuts else 1.0
    result = jax.random.normal(own_key, extent, jnp.float32) * width * gain
    return jnp.minimum(jnp.maximum(result, -bound), bound).astype(kind)


def noise_with(own_key, extent, scale, reach, pieces, heavy, held_as=jnp.bfloat16):
    array = scale * jax.random.normal(own_key, extent, jnp.float32)
    if pieces:
        array = array * block_scale(own_key, extent, pieces, -0.22, 0.18)
    return jnp.clip(spiked(array, jax.random.fold_in(own_key, 3), *heavy), -reach, reach).astype(held_as)


def setup_inputs(seed: int = 0) -> dict:
    streams_of = jax.random.split(jax.random.key(seed), 9)
    hidden = noise_with(streams_of[0], (SEQS, LENGTH, D), 1.0, 6.0, ((0, 4), (1, 32)), (1, 2, 32, 2.75))
    queries = normal_values(streams_of[1], (SEQS, LENGTH, H * P_SIZE), 0.03, 0.19921875, ((0, 4), (1, 32)))
    w_key = normal_values(streams_of[2], (D, H * P_SIZE), D ** -0.5, 0.1875)
    w_value = normal_values(streams_of[3], (D, H * P_SIZE), D ** -0.5, 0.1875)
    log_gate = draw_log_gate(jax.random.fold_in(streams_of[8], 71), 0)
    level_gain = jnp.clip(jnp.exp(jax.random.uniform(streams_of[5], (H, LEVELS), jnp.float32, math.log(0.1), math.log(1.0))), 0.1, 1.0)
    segment_ids = jax.vmap(lambda own: jnp.searchsorted(jnp.cumsum(uneven(own, DOCS, LENGTH, LENGTH // 4, 0)), jnp.arange(LENGTH), side="right"))(jax.random.split(streams_of[6], SEQS)).reshape((SEQS, LENGTH)).astype(jnp.int32)
    out_grad = normal_values(streams_of[7], (SEQS, LENGTH, H * P_SIZE), 0.03, 0.19921875, ((0, 4), (1, 32)))
    return dict(hidden=hidden, queries=queries, w_key=w_key, w_value=w_value, log_gate=log_gate, level_gain=level_gain, segment_ids=segment_ids, out_grad=out_grad)


HIGH = lax.Precision.HIGHEST


def bit_count(values, limit):
    total_bits = jnp.zeros_like(values)
    for bit_pos in range(limit):
        total_bits = total_bits + (values >= (1 << bit_pos)).astype(jnp.int32)
    return total_bits


def local_states(query_f, key_f, value_f, grad_f, cumulative, segment):
    block_decay = cumulative[:, -1]
    last_w = jnp.where((segment == segment[-1])[None], jnp.exp(block_decay[:, None] - cumulative), 0.0)
    fwd_state = jnp.einsum('shp,shq->hpq', key_f * last_w.T[:, :, None], value_f, precision=HIGH)
    first_w = jnp.where((segment == segment[0])[None], jnp.exp(cumulative), 0.0)
    rev_state = jnp.einsum('thp,thq->hpq', query_f * first_w.T[:, :, None], grad_f, precision=HIGH)
    return fwd_state, rev_state


def pair_terms(query_f, key_f, value_f, grad_f, cumulative, gains, level_map, allowed, log_tok):
    levels = gains.shape[1]
    scores = jnp.einsum('thp,shp->hts', query_f, key_f, precision=HIGH)
    dprobs = jnp.einsum('thp,shp->hts', grad_f, value_f, precision=HIGH)
    spread = cumulative[:, :, None] - cumulative[:, None, :]
    decays = jnp.where(allowed[None], jnp.exp(jnp.where(allowed[None], spread, 0.0)), 0.0)
    joined = decays * scores * dprobs
    level_w = jnp.zeros_like(decays)
    gain_part = jnp.zeros((gains.shape[0], levels), jnp.float32)
    for level_idx in range(log_tok + 1):
        chosen = (level_map == level_idx)[None]
        level_w = jnp.where(chosen, gains[:, level_idx][:, None, None], level_w)
        gain_part = gain_part.at[:, level_idx].set(jnp.sum(jnp.where(chosen, joined, 0.0), axis=(1, 2)))
    coeffs = level_w * decays
    weighted = coeffs * dprobs
    query_acc = jnp.einsum('hts,shp->thp', weighted, key_f, precision=HIGH)
    key_acc = jnp.einsum('hts,thp->shp', weighted, query_f, precision=HIGH)
    value_acc = jnp.einsum('hts,thp->shp', coeffs * scores, grad_f, precision=HIGH)
    grid = weighted * scores
    return query_acc, key_acc, value_acc, jnp.sum(grid, axis=2), jnp.sum(grid, axis=1), gain_part


def cross_terms(query_f, key_f, value_f, grad_f, cumulative, segment, incoming, gains, log_tok, sums):
    query_acc, key_acc, value_acc, row_sum, col_sum, gain_part = sums
    block_decay = cumulative[:, -1]
    for section_bit in range(len(incoming)):
        fwd_in, fwd_key, rev_in, rev_key = incoming[section_bit]
        level_idx = log_tok + section_bit + 1
        tier_gain = gains[:, level_idx][:, None]
        fwd_weight = jnp.where((segment == fwd_key)[None], jnp.exp(cumulative), 0.0)
        state_grad = jnp.einsum('hpq,thq->thp', fwd_in, grad_f, precision=HIGH)
        row_term = fwd_weight * jnp.sum(query_f * state_grad, axis=2).T
        gain_part = gain_part.at[:, level_idx].add(jnp.sum(row_term, axis=1))
        row_sum = row_sum + tier_gain * row_term
        query_acc = query_acc + (tier_gain * fwd_weight).T[:, :, None] * state_grad
        rev_weight = jnp.where((segment == rev_key)[None], jnp.exp(block_decay[:, None] - cumulative), 0.0)
        rev_values = jnp.einsum('hpq,shq->shp', rev_in, value_f, precision=HIGH)
        rev_keys = jnp.einsum('hpq,shp->shq', rev_in, key_f, precision=HIGH)
        col_term = rev_weight * jnp.sum(key_f * rev_values, axis=2).T
        col_sum = col_sum + tier_gain * col_term
        rev_scale = (tier_gain * rev_weight).T[:, :, None]
        key_acc = key_acc + rev_scale * rev_values
        value_acc = value_acc + rev_scale * rev_keys
    return query_acc, key_acc, value_acc, row_sum, col_sum, gain_part


def one_sequence(inputs, w_key, w_value, level_gain):
    hidden, queries, log_gate, segment, out_grad = inputs
    length = hidden.shape[0]
    block_len = TOK_DEV
    block_count = length // block_len
    head_count, levels = level_gain.shape
    head_dim = queries.shape[1] // head_count
    log_tok = block_len.bit_length() - 1
    key_rows = jnp.dot(hidden, w_key, preferred_element_type=jnp.float32).astype(jnp.bfloat16)
    value_rows = jnp.dot(hidden, w_value, preferred_element_type=jnp.float32).astype(jnp.bfloat16)

    def split_heads(rows):
        return rows.reshape(block_count, block_len, head_count, head_dim).astype(jnp.float32)

    query_blocks = split_heads(queries)
    key_blocks = split_heads(key_rows)
    value_blocks = split_heads(value_rows)
    grad_blocks = split_heads(out_grad)
    gate_blocks = log_gate.reshape(head_count, block_count, block_len).transpose(1, 0, 2)
    cumulative = jnp.cumsum(gate_blocks, axis=2)
    seg_blocks = segment.reshape(block_count, block_len)
    fstate, rstate = jax.vmap(local_states)(query_blocks, key_blocks, value_blocks, grad_blocks, cumulative, seg_blocks)
    block_total = cumulative[:, :, -1]
    last_key = seg_blocks[:, -1]
    first_key = seg_blocks[:, 0]
    before = jnp.zeros_like(block_total)
    after_sum = jnp.zeros_like(block_total)
    block_ids = np.arange(block_count)
    fwd_list, fkey_list, rev_list, rkey_list = [], [], [], []
    for section_bit in range(block_count.bit_length() - 1):
        partner = block_ids ^ (1 << section_bit)
        is_upper = jnp.asarray(((block_ids >> section_bit) & 1) == 1)
        up_four = is_upper[:, None, None, None]
        up_two = is_upper[:, None]
        peer_fwd = fstate[partner]
        peer_rev = rstate[partner]
        peer_total = block_total[partner]
        peer_last = last_key[partner]
        peer_first = first_key[partner]
        fwd_list.append(jnp.where(up_four, peer_fwd * jnp.exp(before)[:, :, None, None], 0.0))
        fkey_list.append(peer_last)
        rev_list.append(jnp.where(up_four, 0.0, peer_rev * jnp.exp(after_sum)[:, :, None, None]))
        rkey_list.append(peer_first)
        low_fwd = jnp.where(up_four, peer_fwd, fstate)
        high_fwd = jnp.where(up_four, fstate, peer_fwd)
        low_rev = jnp.where(up_four, peer_rev, rstate)
        high_rev = jnp.where(up_four, rstate, peer_rev)
        low_total = jnp.where(up_two, peer_total, block_total)
        high_total = jnp.where(up_two, block_total, peer_total)
        low_last = jnp.where(is_upper, peer_last, last_key)
        high_last = jnp.where(is_upper, last_key, peer_last)
        low_first = jnp.where(is_upper, peer_first, first_key)
        high_first = jnp.where(is_upper, first_key, peer_first)
        fwd_keep = jnp.where((low_last == high_last)[:, None], jnp.exp(high_total), 0.0)
        rev_keep = jnp.where((low_first == high_first)[:, None], jnp.exp(low_total), 0.0)
        fstate = high_fwd + fwd_keep[:, :, None, None] * low_fwd
        rstate = low_rev + rev_keep[:, :, None, None] * high_rev
        before = jnp.where(up_two, low_total + before, before)
        after_sum = jnp.where(up_two, after_sum, after_sum + high_total)
        block_total = low_total + high_total
        last_key = high_last
        first_key = low_first
    fwd_in = jnp.stack(fwd_list, axis=1)
    fwd_key = jnp.stack(fkey_list, axis=1)
    rev_in = jnp.stack(rev_list, axis=1)
    rev_key = jnp.stack(rkey_list, axis=1)
    sections = fwd_in.shape[1]
    positions = jnp.arange(block_len, dtype=jnp.int32)
    level_map = bit_count(jnp.bitwise_xor(positions[:, None], positions[None, :]), levels - 1)

    def per_block(items):
        query_f, key_f, value_f, grad_f, cumul_b, seg_b, f_in, f_key, r_in, r_key = items
        allowed = (positions[None, :] <= positions[:, None]) & (seg_b[:, None] == seg_b[None, :])
        sums = pair_terms(query_f, key_f, value_f, grad_f, cumul_b, level_gain, level_map, allowed, log_tok)
        incoming = [(f_in[idx_section], f_key[idx_section], r_in[idx_section], r_key[idx_section]) for idx_section in range(sections)]
        return cross_terms(query_f, key_f, value_f, grad_f, cumul_b, seg_b, incoming, level_gain, log_tok, sums)

    outs_all = lax.map(per_block, (query_blocks, key_blocks, value_blocks, grad_blocks, cumulative, seg_blocks, fwd_in, fwd_key, rev_in, rev_key))
    query_acc, key_acc, value_acc, row_sum, col_sum, gain_part = outs_all
    query_grad = query_acc.reshape(length, head_count * head_dim).astype(jnp.bfloat16)
    key_grad = key_acc.reshape(length, head_count * head_dim).astype(jnp.bfloat16)
    value_grad = value_acc.reshape(length, head_count * head_dim).astype(jnp.bfloat16)
    input_grad = (jnp.dot(key_grad, w_key.T, preferred_element_type=jnp.float32)
                  + jnp.dot(value_grad, w_value.T, preferred_element_type=jnp.float32)).astype(jnp.bfloat16)
    gate_diff = (row_sum - col_sum).transpose(1, 0, 2).reshape(head_count, length)
    gate_grad = jnp.cumsum(gate_diff[:, ::-1], axis=1)[:, ::-1]
    key_weight = jnp.dot(hidden.T, key_grad, preferred_element_type=jnp.float32)
    value_weight = jnp.dot(hidden.T, value_grad, preferred_element_type=jnp.float32)
    return query_grad, input_grad, gate_grad, key_weight, value_weight, jnp.sum(gain_part, axis=0)


def reference(hidden, queries, w_key, w_value, log_gate, level_gain, segment_ids, out_grad):
    def run(inputs):
        return one_sequence(inputs, w_key, w_value, level_gain)

    results = lax.map(run, (hidden, queries, log_gate, segment_ids, out_grad))
    return (results[0], results[1], results[2], jnp.sum(results[3], axis=0), jnp.sum(results[4], axis=0), jnp.sum(results[5], axis=0))
```

```python
import functools

import jax
import jax.numpy as jnp
from jax import lax
from jax.experimental import pallas as pl
from jax.experimental.pallas import tpu as pltpu
from jax.sharding import Mesh
from jax.sharding import PartitionSpec as P

SEQ = ("z", "x", "core")
SEQ_BATCH = ("z", "x", "core", "batch")
MESH = pl.DeviceIdType.MESH
HIGHEST = lax.Precision.HIGHEST
F32 = jnp.float32
BF16 = jnp.bfloat16

NT = (((1,), (1,)), ((), ()))
TN = (((0,), (0,)), ((), ()))
NN = (((1,), (0,)), ((), ()))

TOK = 128
PAIR = 128
HALF_ROWS = 1088
SROWS = 1024


def dot(a, b, dims):
    return lax.dot_general(a, b, dims, preferred_element_type=F32)


def dot_exact(a, b, dims):
    return lax.dot_general(a, b, dims, preferred_element_type=F32, precision=HIGHEST)


def split2(x):
    hi = x.astype(BF16)
    return hi, (x - hi.astype(F32)).astype(BF16)


def dot_left(a, b, dims):
    hi, lo = split2(a)
    return dot(hi, b, dims) + dot(lo, b, dims)


def dot_right(a, b, dims):
    hi, lo = split2(b)
    return dot(a, hi, dims) + dot(a, lo, dims)


def iota(shape, dim):
    return lax.broadcasted_iota(jnp.int32, shape, dim)


def pair_cumulative(cum_cols, p, low):
    return jnp.where(low, cum_cols[:, 2 * p : 2 * p + 1], cum_cols[:, 2 * p + 1 : 2 * p + 2])


def token_weights(cum_pair, seg_col):
    total = cum_pair[TOK - 1 : TOK, :]
    last = jnp.where(seg_col == seg_col[TOK - 1 : TOK, :], jnp.exp(total - cum_pair), 0.0)
    first = jnp.where(seg_col == seg_col[0:1, :], jnp.exp(cum_pair), 0.0)
    return first, last, total


def states_kernel(hid_ref, wk_ref, wv_ref, q_ref, g_ref, lg_ref, seg_ref, k_ref, v_ref, st_ref):
    step = pl.program_id(0)
    hid = hid_ref[...]
    keys = dot(hid, wk_ref[...], NN).astype(BF16)
    values = dot(hid, wv_ref[...], NN).astype(BF16)
    k_ref[...] = keys
    v_ref[...] = values
    lower = (iota((TOK, TOK), 1) <= iota((TOK, TOK), 0)).astype(F32)
    cum_cols = dot_exact(lower, lg_ref[0], NT)
    seg_col = seg_ref[...]
    seg_f = seg_col.astype(F32)
    low = iota((TOK, PAIR), 1) < 64
    low_half = iota((64, PAIR), 1) < 64
    row8 = iota((8, PAIR), 0)
    half = step // 4
    for p in range(2):
        cum_pair = pair_cumulative(cum_cols, p, low)
        first_w, last_w, total = token_weights(cum_pair, seg_col)
        cols = slice(p * PAIR, (p + 1) * PAIR)
        fwd = dot_left(keys[:, cols].astype(F32) * last_w, values[:, cols], TN)
        rev = dot_left(q_ref[:, cols].astype(F32) * first_w, g_ref[:, cols], TN)
        pp = 2 * (step % 4) + p
        st_ref[half, pl.ds(pl.multiple_of(pp * 64, 64), 64), :] = jnp.where(
            low_half, fwd[:64], fwd[64:]
        )
        st_ref[half, pl.ds(pl.multiple_of(512 + pp * 64, 64), 64), :] = jnp.where(
            low_half, rev[:64], rev[64:]
        )
        meta = jnp.where(
            row8 == 0,
            total,
            jnp.where(row8 == 1, seg_f[0:1, :], jnp.where(row8 == 2, seg_f[TOK - 1 : TOK, :], 0.0)),
        )
        st_ref[half, pl.ds(pl.multiple_of(1024 + pp * 8, 8), 8), :] = meta


def block_states(hidden, w_key, w_value, queries, out_grad, log_gate4, seg_col):
    cols = queries.shape[1]
    steps = cols // 256
    depth = hidden.shape[1]
    block = pl.BlockSpec((TOK, 256), lambda i: (0, i))
    weight = pl.BlockSpec((depth, 256), lambda i: (0, i))
    return pl.pallas_call(
        states_kernel,
        grid=(steps,),
        in_specs=[
            pl.BlockSpec((TOK, depth), lambda i: (0, 0)),
            weight,
            weight,
            block,
            block,
            pl.BlockSpec((1, 4, TOK), lambda i: (i, 0, 0)),
            pl.BlockSpec((TOK, 1), lambda i: (0, 0)),
        ],
        out_specs=[block, block, pl.BlockSpec((2, HALF_ROWS, PAIR), lambda i: (0, 0, 0))],
        out_shape=[
            jax.ShapeDtypeStruct((TOK, cols), BF16),
            jax.ShapeDtypeStruct((TOK, cols), BF16),
            jax.ShapeDtypeStruct((2, HALF_ROWS, PAIR), F32),
        ],
        compiler_params=pltpu.CompilerParams(dimension_semantics=("arbitrary",)),
        name="states",
    )(hidden, w_key, w_value, queries, out_grad, log_gate4, seg_col)


def remote(src, dst, ssem, rsem, target):
    return pltpu.make_async_remote_copy(
        src_ref=src,
        dst_ref=dst,
        send_sem=ssem,
        recv_sem=rsem,
        device_id=target,
        device_id_type=MESH,
    )


def entry_barrier(peers):
    barrier = pltpu.get_barrier_semaphore()
    for peer in peers:
        pl.semaphore_signal(barrier, inc=1, device_id=peer, device_id_type=MESH)
    pl.semaphore_wait(barrier, len(peers))


def ring(index, step):
    return lax.rem(index + step, 4)


def same(a, b):
    return jnp.where(a == b, 1.0, 0.0)


def linked(a, b, total):
    return jnp.where(a == b, jnp.exp(total), 0.0)


def exchange_kernel(
    st_ref,
    hid_ref,
    gain_ref,
    out_ref,
    gsum_ref,
    hy_out,
    hz_out,
    both,
    chip_send,
    chip_recv,
    tot_send,
    tot_recv,
    back_send,
    back_recv,
    own_blocks,
    hy,
    hz,
    s_chip,
    r_chip,
    s_x,
    r_x,
    s_z,
    r_z,
    s_back,
    r_back,
    s_fin,
    r_fin,
    s_h,
    r_h,
    s_f,
    r_f,
    s_d,
    r_d,
):
    x, y, z, c = (lax.axis_index(a) for a in ("x", "batch", "z", "core"))
    sib = {"core": 1 - c}
    peers = [sib]
    for axis, index in (("x", x), ("batch", y), ("z", z)):
        peers += [{axis: ring(index, d)} for d in (1, 2, 3)]
    entry_barrier(peers)

    swap = remote(st_ref.at[1 - c], both.at[c], s_chip, r_chip, sib)
    swap.start()

    hops = []
    for n, (axis, index, buf) in enumerate((("batch", y, hy), ("z", z, hz))):
        for m, d in enumerate((1, 3)):
            cp = remote(
                hid_ref, buf.at[index, c], s_h.at[n, m], r_h.at[n, m], {axis: ring(index, d)}
            )
            cp.start()
            hops.append(cp)
    down = []
    for n, (index, buf) in enumerate(((y, hy), (z, hz))):
        cp = remote(hid_ref, buf.at[index, c], s_d.at[n, 0], r_d.at[n, 0], sib)
        cp.start()
        down.append(cp)
    both[pl.ds(c, 1)] = st_ref[pl.ds(c, 1)]
    gsum_ref[...] = jnp.zeros_like(gsum_ref)
    swap.wait()

    row8 = iota((8, PAIR), 0)

    def meta_rows(total, first, last):
        return jnp.where(
            row8 == 0, total, jnp.where(row8 == 1, first, jnp.where(row8 == 2, last, 0.0))
        )

    for pp in range(8):
        f0 = both[0, pp * 64 : pp * 64 + 64, :]
        f1 = both[1, pp * 64 : pp * 64 + 64, :]
        r0 = both[0, 512 + pp * 64 : 576 + pp * 64, :]
        r1 = both[1, 512 + pp * 64 : 576 + pp * 64, :]
        m0 = both[0, 1024 + pp * 8 : 1032 + pp * 8, :]
        m1 = both[1, 1024 + pp * 8 : 1032 + pp * 8, :]
        t0, first0, last0 = m0[0:1], m0[1:2], m0[2:3]
        t1, first1, last1 = m1[0:1], m1[1:2], m1[2:3]
        q, p = pp // 2, pp % 2
        chip_send[q, p * 64 : p * 64 + 64, :] = f1 + linked(last0, last1, t1) * f0
        chip_send[q, 128 + p * 64 : 192 + p * 64, :] = r0 + linked(first0, first1, t0) * r1
        chip_send[q, 256 + p * 8 : 264 + p * 8, :] = meta_rows(t0 + t1, first0, last1)
        gsum_ref[pp, 0:1, :] = same(last0, first1) * jnp.sum(f0 * r1, axis=0, keepdims=True)

    xs = []
    for d in (1, 2, 3):
        to = ring(x, d)
        cp = remote(chip_send.at[to], chip_recv.at[x], s_x.at[d - 1], r_x.at[d - 1], {"x": to})
        cp.start()
        xs.append(cp)
    chip_recv[pl.ds(x, 1)] = chip_send[pl.ds(x, 1)]
    for cp in xs:
        cp.wait()

    def chip(j, p):
        return (
            chip_recv[j, p * 64 : p * 64 + 64, :],
            chip_recv[j, 128 + p * 64 : 192 + p * 64, :],
            chip_recv[j, 256 + p * 8 : 257 + p * 8, :],
            chip_recv[j, 257 + p * 8 : 258 + p * 8, :],
            chip_recv[j, 258 + p * 8 : 259 + p * 8, :],
        )

    def joined(p):
        (f0, r0, t0, a0, l0), (f1, r1, t1, a1, l1), (f2, r2, t2, a2, l2), (f3, r3, t3, a3, l3) = (
            chip(j, p) for j in range(4)
        )
        f01 = f1 + linked(l0, l1, t1) * f0
        r01 = r0 + linked(a0, a1, t0) * r1
        f23 = f3 + linked(l2, l3, t3) * f2
        r23 = r2 + linked(a2, a3, t2) * r3
        return f01, r01, f23, r23

    for p in range(2):
        f01, r01, f23, r23 = joined(p)
        t0, a0 = chip(0, p)[2:4]
        t1, l1 = chip(1, p)[2], chip(1, p)[4]
        t2, a2 = chip(2, p)[2:4]
        t3, l3 = chip(3, p)[2], chip(3, p)[4]
        tot_send[0, p * 64 : p * 64 + 64, :] = f23 + linked(l1, l3, t2 + t3) * f01
        tot_send[1, p * 64 : p * 64 + 64, :] = r01 + linked(a0, a2, t0 + t1) * r23
        tot_send[0, 128 + p * 8 : 136 + p * 8, :] = jnp.broadcast_to(l3, (8, PAIR))
        tot_send[1, 128 + p * 8 : 136 + p * 8, :] = jnp.broadcast_to(a0, (8, PAIR))
    zs = []
    for n, d in ((0, 1), (1, 3)):
        cp = remote(tot_send.at[n], tot_recv.at[n], s_z.at[n], r_z.at[n], {"z": ring(z, d)})
        cp.start()
        zs.append(cp)

    fwd = []
    for n, (axis, index, buf) in enumerate((("batch", y, hy), ("z", z, hz))):
        for m, d in enumerate((1, 3)):
            hops[2 * n + m].wait()
            came = ring(index, 4 - d)
            rows = slice(0, 512) if d == 1 else slice(512, 1024)
            cp = remote(
                buf.at[came, c, rows],
                buf.at[came, c, rows],
                s_f.at[n, m],
                r_f.at[n, m],
                {axis: ring(index, d)},
            )
            cp.start()
            fwd.append(cp)
            cp = remote(
                buf.at[came, c], buf.at[came, c], s_d.at[n, 1 + m], r_d.at[n, 1 + m], sib
            )
            cp.start()
            down.append(cp)

    for cp in zs:
        cp.wait()
    has_prev = (z > 0).astype(F32)
    has_next = (z < 3).astype(F32)
    prev_top = (z == 2).astype(F32)
    next_top = (z == 1).astype(F32)
    for p in range(2):
        (f0, r0, t0, a0, l0), (f1, r1, t1, a1, l1), (f2, r2, t2, a2, l2), (f3, r3, t3, a3, l3) = (
            chip(j, p) for j in range(4)
        )
        f01, r01, f23, r23 = joined(p)
        gains = gain_ref[pl.ds(c * 8 + 2 * x + p, 1)][0]
        g9, g10, g11, g12 = (gains[i : i + 1] for i in range(1, 5))
        zf = has_prev * tot_recv[0, p * 64 : p * 64 + 64, :]
        zl = tot_recv[0, 128 + p * 8 : 129 + p * 8, :]
        zr = has_next * tot_recv[1, p * 64 : p * 64 + 64, :]
        za = tot_recv[1, 128 + p * 8 : 129 + p * 8, :]
        gzf = g11 * (1.0 - prev_top) + g12 * prev_top
        gzr = g11 * (1.0 - next_top) + g12 * next_top
        sf = (
            gzf * same(zl, a0) * zf,
            gzf * linked(zl, a1, t0) * zf + g9 * same(l0, a1) * f0,
            gzf * linked(zl, a2, t0 + t1) * zf + g10 * same(l1, a2) * f01,
            gzf * linked(zl, a3, t0 + t1 + t2) * zf
            + g10 * linked(l1, a3, t2) * f01
            + g9 * same(l2, a3) * f2,
        )
        sr = (
            gzr * linked(za, l0, t1 + t2 + t3) * zr
            + g10 * linked(l0, a2, t1) * r23
            + g9 * same(l0, a1) * r1,
            gzr * linked(za, l1, t2 + t3) * zr + g10 * same(l1, a2) * r23,
            gzr * linked(za, l2, t3) * zr + g9 * same(l2, a3) * r3,
            gzr * same(za, l3) * zr,
        )
        for j in range(4):
            back_send[j, p * 64 : p * 64 + 64, :] = sf[j]
            back_send[j, 128 + p * 64 : 192 + p * 64, :] = sr[j]
        r_group = r01 + linked(a0, a2, t0 + t1) * r23
        d9 = same(l0, a1) * jnp.sum(f0 * r1, axis=0, keepdims=True) + same(l2, a3) * jnp.sum(
            f2 * r3, axis=0, keepdims=True
        )
        d10 = same(l1, a2) * jnp.sum(f01 * r23, axis=0, keepdims=True)
        dz = same(zl, a0) * jnp.sum(zf * r_group, axis=0, keepdims=True)
        rows = jnp.where(
            row8 == 1,
            d9,
            jnp.where(
                row8 == 2,
                d10,
                jnp.where(
                    row8 == 3, (1.0 - prev_top) * dz, jnp.where(row8 == 4, prev_top * dz, 0.0)
                ),
            ),
        )
        gsum_ref[pl.ds(2 * x + p, 1)] = gsum_ref[pl.ds(2 * x + p, 1)] + rows[None]

    bs = []
    for d in (1, 2, 3):
        to = ring(x, d)
        cp = remote(
            back_send.at[to], back_recv.at[x], s_back.at[d - 1], r_back.at[d - 1], {"x": to}
        )
        cp.start()
        bs.append(cp)
    back_recv[pl.ds(x, 1)] = back_send[pl.ds(x, 1)]
    for cp in bs:
        cp.wait()

    for pp in range(8):
        q, p = pp // 2, pp % 2
        f0 = both[0, pp * 64 : pp * 64 + 64, :]
        r1 = both[1, 512 + pp * 64 : 576 + pp * 64, :]
        m0 = both[0, 1024 + pp * 8 : 1032 + pp * 8, :]
        m1 = both[1, 1024 + pp * 8 : 1032 + pp * 8, :]
        t0, first0, last0 = m0[0:1], m0[1:2], m0[2:3]
        t1, first1, last1 = m1[0:1], m1[1:2], m1[2:3]
        g8 = gain_ref[pl.ds(c * 8 + pp, 1)][0][0:1]
        sf = back_recv[q, p * 64 : p * 64 + 64, :]
        sr = back_recv[q, 128 + p * 64 : 192 + p * 64, :]
        link = g8 * same(last0, first1)
        own_blocks[0, pp * 64 : pp * 64 + 64, :] = sf
        own_blocks[1, pp * 64 : pp * 64 + 64, :] = linked(first0, first1, t0) * sf + link * f0
        own_blocks[0, 512 + pp * 64 : 576 + pp * 64, :] = (
            linked(last0, last1, t1) * sr + link * r1
        )
        own_blocks[1, 512 + pp * 64 : 576 + pp * 64, :] = sr
    last_swap = remote(own_blocks.at[1 - c], out_ref.at[c], s_fin, r_fin, sib)
    last_swap.start()
    out_ref[pl.ds(c, 1)] = own_blocks[pl.ds(c, 1)]

    for n, (index, buf) in enumerate(((y, hy), (z, hz))):
        buf[pl.ds(index, 1), pl.ds(c, 1)] = hid_ref[...][None, None]
        fwd[2 * n].wait()
        fwd[2 * n + 1].wait()
        came = ring(index, 2)
        cp = remote(buf.at[came, c], buf.at[came, c], s_d.at[n, 3], r_d.at[n, 3], sib)
        cp.start()
        down.append(cp)
    last_swap.wait()
    for cp in down:
        cp.wait()
    for buf, out in ((hy, hy_out), (hz, hz_out)):
        for g in range(8):
            out[:, g * TOK : (g + 1) * TOK] = buf[g // 2, g % 2].astype(BF16)


def exchange(st, hidden_t, gain_rows):
    vm = pl.BlockSpec(memory_space=pltpu.VMEM)
    depth = hidden_t.shape[0]
    dma = pltpu.SemaphoreType.DMA
    return pl.pallas_call(
        exchange_kernel,
        in_specs=[vm] * 3,
        out_specs=[vm] * 4,
        out_shape=[
            jax.ShapeDtypeStruct((2, SROWS, PAIR), F32),
            jax.ShapeDtypeStruct((8, 8, PAIR), F32),
            jax.ShapeDtypeStruct((depth, 8 * TOK), BF16),
            jax.ShapeDtypeStruct((depth, 8 * TOK), BF16),
        ],
        scratch_shapes=[
            pltpu.VMEM((2, HALF_ROWS, PAIR), F32),
            pltpu.VMEM((4, 272, PAIR), F32),
            pltpu.VMEM((4, 272, PAIR), F32),
            pltpu.VMEM((2, 144, PAIR), F32),
            pltpu.VMEM((2, 144, PAIR), F32),
            pltpu.VMEM((4, 256, PAIR), F32),
            pltpu.VMEM((4, 256, PAIR), F32),
            pltpu.VMEM((2, SROWS, PAIR), F32),
            pltpu.VMEM((4, 2, depth, TOK), F32),
            pltpu.VMEM((4, 2, depth, TOK), F32),
            dma,
            dma,
            dma((3,)),
            dma((3,)),
            dma((2,)),
            dma((2,)),
            dma((3,)),
            dma((3,)),
            dma,
            dma,
            dma((2, 2)),
            dma((2, 2)),
            dma((2, 2)),
            dma((2, 2)),
            dma((2, 4)),
            dma((2, 4)),
        ],
        compiler_params=pltpu.CompilerParams(
            collective_id=0, has_side_effects=True, vmem_limit_bytes=40 * 2**20
        ),
        name="exchange",
    )(st, hidden_t, gain_rows)


def grads_kernel(
    k_ref,
    v_ref,
    q_ref,
    g_ref,
    lg_ref,
    segc_ref,
    segr_ref,
    gain_ref,
    s_ref,
    qg_ref,
    ks_ref,
    vs_ref,
    ksb_ref,
    vsb_ref,
    gate_ref,
    gsum_ref,
):
    step = pl.program_id(0)
    rows_i, cols_i = iota((TOK, TOK), 0), iota((TOK, TOK), 1)
    causal = cols_i <= rows_i
    seg_col, seg_row = segc_ref[...], segr_ref[...]
    allowed = causal & (seg_col == seg_row)
    lower = causal.astype(F32)
    strict = (rows_i < cols_i).astype(BF16)
    tail = (cols_i <= rows_i).astype(BF16)
    gap = jnp.bitwise_xor(rows_i, cols_i)
    cum_cols = dot_exact(lower, lg_ref[0], NT)
    cum_rows = dot_exact(lg_ref[0], lower, NT)
    low = iota((TOK, PAIR), 1) < 64
    low_half = iota((64, PAIR), 1) < 64
    half = step // 4
    head_pick = (iota((8, PAIR), 1) // 64 == iota((8, PAIR), 0)).astype(BF16)
    zero = jnp.zeros((TOK, PAIR), BF16)
    gate_rows, gain_rows = [], []
    for p in range(2):
        cols = slice(p * PAIR, (p + 1) * PAIR)
        k, v, q, g = (r[:, cols] for r in (k_ref, v_ref, q_ref, g_ref))
        kf, qf = k.astype(F32), q.astype(F32)
        pp = 2 * (step % 4) + p
        sf = s_ref[half, pl.ds(pl.multiple_of(pp * 64, 64), 64), :]
        sr = s_ref[half, pl.ds(pl.multiple_of(512 + pp * 64, 64), 64), :]

        def diag(s):
            return jnp.concatenate([jnp.where(low_half, s, 0.0), jnp.where(low_half, 0.0, s)], axis=0)

        first_w, last_w, _ = token_weights(pair_cumulative(cum_cols, p, low), seg_col)
        sg = first_w * dot_right(g, diag(sf), NT)
        rv = last_w * dot_right(v, diag(sr), NT)
        rk = last_w * dot_right(k, diag(sr), NN)
        diff = qf * sg - kf * rv
        hi, lo = split2(diff)
        diff_rows = dot(head_pick, hi, NT) + dot(head_pick, lo, NT)
        cross_rows = dot_left(diff_rows, tail, NN)

        weighted, scored, queries, keys, grads = [], [], [], [], []
        for h in range(2):
            head = 2 * p + h

            def own(a):
                return jnp.where(low, a, zero) if h == 0 else jnp.where(low, zero, a)

            qh, gh, kh = own(q), own(g), own(k)
            score = dot(qh, k, NT)
            dprob = dot(gh, v, NT)
            spread = cum_cols[:, head : head + 1] - cum_rows[head : head + 1, :]
            decay = jnp.where(allowed, jnp.exp(jnp.where(allowed, spread, 0.0)), 0.0)
            ds = decay * score
            joint = ds * dprob
            level = jnp.full((TOK, TOK), gain_ref[4 * step + head, 0], F32)
            gain_rows.append(jnp.sum(jnp.where(gap == 0, joint, 0.0), axis=0, keepdims=True))
            for l in range(1, 8):
                above = gap >= 2 ** (l - 1)
                level = jnp.where(above, gain_ref[4 * step + head, l], level)
                chosen = above & (gap < 2**l)
                gain_rows.append(jnp.sum(jnp.where(chosen, joint, 0.0), axis=0, keepdims=True))
            wd = level * decay * dprob
            weighted.append(wd.astype(BF16))
            scored.append((level * ds).astype(BF16))
            grid = (wd * score).astype(BF16)
            crossing = jnp.where(causal, dot(grid, strict, NN), 0.0)
            gate_rows.append(
                jnp.sum(crossing, axis=0, keepdims=True) + cross_rows[h : h + 1, :]
            )
            queries.append(qh)
            keys.append(kh)
            grads.append(gh)
        query_acc = dot(jnp.concatenate(weighted, axis=1), jnp.concatenate(keys, axis=0), NN)
        key_acc = dot(jnp.concatenate(weighted, axis=0), jnp.concatenate(queries, axis=0), TN)
        value_acc = dot(jnp.concatenate(scored, axis=0), jnp.concatenate(grads, axis=0), TN)
        qg_ref[:, cols] = (query_acc + sg).astype(BF16)
        ks = (key_acc + rv).astype(BF16)
        vs = (value_acc + rk).astype(BF16)
        ksb_ref[:, cols] = ks
        vsb_ref[:, cols] = vs
        ks_ref[0, :, cols] = ks.astype(F32)
        vs_ref[0, :, cols] = vs.astype(F32)
    gate_ref[0] = jnp.concatenate(gate_rows, axis=0)
    gsum_ref[0] = jnp.concatenate(gain_rows, axis=0)


def block_grads(keys, values, queries, out_grad, log_gate4, seg_col, seg_row, level_gain, states):
    cols = queries.shape[1]
    steps = cols // 256
    block = pl.BlockSpec((TOK, 256), lambda i: (0, i))
    slab = pl.BlockSpec((1, TOK, 256), lambda i: (i, 0, 0))
    return pl.pallas_call(
        grads_kernel,
        grid=(steps,),
        in_specs=[
            block,
            block,
            block,
            block,
            pl.BlockSpec((1, 4, TOK), lambda i: (i, 0, 0)),
            pl.BlockSpec((TOK, 1), lambda i: (0, 0)),
            pl.BlockSpec((1, TOK), lambda i: (0, 0)),
            pl.BlockSpec(memory_space=pltpu.SMEM),
            pl.BlockSpec((2, SROWS, PAIR), lambda i: (0, 0, 0)),
        ],
        out_specs=[
            block,
            slab,
            slab,
            block,
            block,
            pl.BlockSpec((1, 4, TOK), lambda i: (i, 0, 0)),
            pl.BlockSpec((1, 32, TOK), lambda i: (i, 0, 0)),
        ],
        out_shape=[
            jax.ShapeDtypeStruct((TOK, cols), BF16),
            jax.ShapeDtypeStruct((steps, TOK, 256), F32),
            jax.ShapeDtypeStruct((steps, TOK, 256), F32),
            jax.ShapeDtypeStruct((TOK, cols), BF16),
            jax.ShapeDtypeStruct((TOK, cols), BF16),
            jax.ShapeDtypeStruct((steps, 4, TOK), F32),
            jax.ShapeDtypeStruct((steps, 32, TOK), F32),
        ],
        compiler_params=pltpu.CompilerParams(dimension_semantics=("arbitrary",)),
        name="grads",
    )(keys, values, queries, out_grad, log_gate4, seg_col, seg_row, level_gain, states)


def weights_kernel(
    ks_ref,
    vs_ref,
    hy_ref,
    hz_ref,
    small_ref,
    kout_ref,
    vout_ref,
    sout_ref,
    rk,
    rv,
    pk,
    pv,
    zk,
    xv,
    zsum,
    xsum,
    xk,
    yv,
    ksum,
    vsum,
    kfin,
    vfin,
    m1,
    m1s,
    m2,
    m2s,
    m3,
    s_k,
    r_k,
    s_v,
    r_v,
    s_zk,
    r_zk,
    s_xv,
    r_xv,
    s_xk,
    r_xk,
    s_yv,
    r_yv,
    s_kf,
    r_kf,
    s_vf,
    r_vf,
    s_m1,
    r_m1,
    s_m2,
    r_m2,
    s_m3,
    r_m3,
):
    x, y, z, c = (lax.axis_index(a) for a in ("x", "batch", "z", "core"))
    offsets = [(d, e) for d in range(4) for e in (0, 1) if d or e]

    def plane(axis, index, d, e):
        to, tc = ring(index, d), lax.rem(c + e, 2)
        return {axis: to, "core": tc}, to, tc

    peers = [plane("batch", y, d, e)[0] for d, e in offsets]
    peers += [plane("z", z, d, e)[0] for d, e in offsets if d]
    peers += [{"x": ring(x, d)} for d in (1, 2, 3)]
    entry_barrier(peers)

    firsts_k, firsts_v, smalls = [], [], []
    for n, (d, e) in enumerate(offsets):
        dev, to, tc = plane("batch", y, d, e)
        cp = remote(ks_ref.at[2 * to + tc], rk.at[2 * y + c], s_k.at[n], r_k.at[n], dev)
        cp.start()
        firsts_k.append(cp)
        dev, to, tc = plane("z", z, d, e)
        cp = remote(vs_ref.at[2 * to + tc], rv.at[2 * z + c], s_v.at[n], r_v.at[n], dev)
        cp.start()
        firsts_v.append(cp)
        cp = remote(small_ref, m1.at[2 * z + c], s_m1.at[n], r_m1.at[n], dev)
        cp.start()
        smalls.append(cp)
    rk[pl.ds(2 * y + c, 1)] = ks_ref[pl.ds(2 * y + c, 1)]
    rv[pl.ds(2 * z + c, 1)] = vs_ref[pl.ds(2 * z + c, 1)]
    m1[pl.ds(2 * z + c, 1)] = small_ref[...][None]

    for cp in smalls:
        cp.wait()
    total = m1[0, 0:8, :]
    for g in range(1, 8):
        total = total + m1[g, 0:8, :]
    m1s[0:8, :] = total
    for g in range(8):
        m1s[8 + g : 9 + g, :] = m1[g, 8:9, :]
    smalls = []
    for d in (1, 2, 3):
        cp = remote(m1s, m2.at[x], s_m2.at[d - 1], r_m2.at[d - 1], {"x": ring(x, d)})
        cp.start()
        smalls.append(cp)
    m2[pl.ds(x, 1)] = m1s[...][None]

    for cp in firsts_k:
        cp.wait()
    right = rk[...].reshape(8 * TOK, 256).astype(BF16)
    for b in range(4):
        pk[b] = dot(hy_ref[b * 256 : (b + 1) * 256, :], right, NN)
    zks = []
    for d in (1, 2, 3):
        to = ring(z, d)
        cp = remote(pk.at[to], zk.at[z], s_zk.at[d - 1], r_zk.at[d - 1], {"z": to})
        cp.start()
        zks.append(cp)
    zk[pl.ds(z, 1)] = pk[pl.ds(z, 1)]

    for cp in firsts_v:
        cp.wait()
    right = rv[...].reshape(8 * TOK, 256).astype(BF16)
    for b in range(4):
        part = dot(hz_ref[b * 256 : (b + 1) * 256, :], right, NN)
        for j in range(4):
            pv[j, b] = part[j * 64 : (j + 1) * 64, :]
    xvs = []
    for d in (1, 2, 3):
        to = ring(x, d)
        cp = remote(pv.at[to], xv.at[x], s_xv.at[d - 1], r_xv.at[d - 1], {"x": to})
        cp.start()
        xvs.append(cp)
    xv[pl.ds(x, 1)] = pv[pl.ds(x, 1)]

    for cp in smalls:
        cp.wait()
    total = m2[0, 0:8, :] + m2[1, 0:8, :] + m2[2, 0:8, :] + m2[3, 0:8, :]
    m2s[...] = total
    place = z * 8 + x * 2 + c
    later = jnp.zeros((1, PAIR), F32)
    for j in range(4):
        for g in range(8):
            spot = (g // 2) * 8 + j * 2 + g % 2
            later = later + (place < spot).astype(F32) * m2[j, 8 + g : 9 + g, :]
    smalls = []
    for d in (1, 2, 3):
        cp = remote(m2s, m3.at[y], s_m3.at[d - 1], r_m3.at[d - 1], {"batch": ring(y, d)})
        cp.start()
        smalls.append(cp)
    m3[pl.ds(y, 1)] = total[None]
    sout_ref[8:16, :] = jnp.broadcast_to(later, (8, PAIR))

    for cp in zks:
        cp.wait()
    zsum[...] = (zk[0] + zk[1] + zk[2] + zk[3]).reshape(4, 64, 256)
    xks = []
    for d in (1, 2, 3):
        to = ring(x, d)
        cp = remote(zsum.at[to], xk.at[x], s_xk.at[d - 1], r_xk.at[d - 1], {"x": to})
        cp.start()
        xks.append(cp)
    xk[pl.ds(x, 1)] = zsum[pl.ds(x, 1)]

    for cp in xvs:
        cp.wait()
    part = xv[0] + xv[1] + xv[2] + xv[3]
    for zz in range(4):
        for cc in range(2):
            for yy in range(4):
                at = cc * 32 + yy * 8
                xsum[yy, 2 * zz + cc] = part[zz, at : at + 8, :]
    yvs = []
    for d in (1, 2, 3):
        to = ring(y, d)
        cp = remote(xsum.at[to], yv.at[y], s_yv.at[d - 1], r_yv.at[d - 1], {"batch": to})
        cp.start()
        yvs.append(cp)
    yv[pl.ds(y, 1)] = xsum[pl.ds(y, 1)]

    for cp in smalls:
        cp.wait()
    sout_ref[0:8, :] = m3[0] + m3[1] + m3[2] + m3[3]

    for cp in xks:
        cp.wait()
    part = xk[0] + xk[1] + xk[2] + xk[3]
    for yy in range(4):
        for cc in range(2):
            at = cc * 32 + yy * 8
            ksum[2 * yy + cc] = part[at : at + 8, :]
    fins = []
    for n, (d, e) in enumerate(offsets):
        dev, to, tc = plane("batch", y, d, e)
        cp = remote(ksum.at[2 * to + tc], kfin.at[2 * y + c], s_kf.at[n], r_kf.at[n], dev)
        cp.start()
        fins.append(cp)
    kfin[pl.ds(2 * y + c, 1)] = ksum[pl.ds(2 * y + c, 1)]

    for cp in yvs:
        cp.wait()
    vsum[...] = yv[0] + yv[1] + yv[2] + yv[3]
    for n, (d, e) in enumerate(offsets):
        dev, to, tc = plane("z", z, d, e)
        cp = remote(vsum.at[2 * to + tc], vfin.at[2 * z + c], s_vf.at[n], r_vf.at[n], dev)
        cp.start()
        fins.append(cp)
    vfin[pl.ds(2 * z + c, 1)] = vsum[pl.ds(2 * z + c, 1)]
    for cp in fins:
        cp.wait()
    for g in range(8):
        kout_ref[:, g * 256 : (g + 1) * 256] = kfin[g]
        vout_ref[:, g * 256 : (g + 1) * 256] = vfin[g]


def weight_grads(ks, vs, hy, hz, small):
    vm = pl.BlockSpec(memory_space=pltpu.VMEM)
    dma = pltpu.SemaphoreType.DMA

    def buf(*shape):
        return pltpu.VMEM(shape, F32)

    sems = []
    for n in (7, 7, 3, 3, 3, 3, 7, 7, 7, 3, 3):
        sems += [dma((n,)), dma((n,))]
    return pl.pallas_call(
        weights_kernel,
        in_specs=[vm] * 5,
        out_specs=[vm] * 3,
        out_shape=[
            jax.ShapeDtypeStruct((8, 2048), F32),
            jax.ShapeDtypeStruct((8, 2048), F32),
            jax.ShapeDtypeStruct((16, PAIR), F32),
        ],
        scratch_shapes=[
            buf(8, TOK, 256),
            buf(8, TOK, 256),
            buf(4, 256, 256),
            buf(4, 4, 64, 256),
            buf(4, 256, 256),
            buf(4, 4, 64, 256),
            buf(4, 64, 256),
            buf(4, 8, 8, 256),
            buf(4, 64, 256),
            buf(4, 8, 8, 256),
            buf(8, 8, 256),
            buf(8, 8, 256),
            buf(8, 8, 256),
            buf(8, 8, 256),
            buf(8, 16, PAIR),
            buf(16, PAIR),
            buf(4, 16, PAIR),
            buf(8, PAIR),
            buf(4, 8, PAIR),
            *sems,
        ],
        compiler_params=pltpu.CompilerParams(
            collective_id=1, has_side_effects=True, vmem_limit_bytes=40 * 2**20
        ),
        name="weights",
    )(ks, vs, hy, hz, small)


def local(hidden, queries, w_key, w_value, log_gate, level_gain, segment_ids, out_grad):
    heads, levels = level_gain.shape
    core = lax.axis_index("core")
    hidden_rows, query_rows, grad_rows = hidden[0], queries[0], out_grad[0]
    log_gate4 = log_gate[0].reshape(heads // 4, 4, TOK)
    seg_row = segment_ids
    seg_col = segment_ids.reshape(TOK, 1)
    hidden_t = hidden_rows.T.astype(F32)
    cross = jnp.pad(level_gain[:, 8:13], ((0, 0), (0, 3)))
    gain_rows = jnp.repeat(cross.reshape(16, 2, 8).transpose(0, 2, 1), 64, axis=2)
    keys, values, states = block_states(
        hidden_rows, w_key, w_value, query_rows, grad_rows, log_gate4, seg_col
    )
    incoming, cross_sums, hy, hz = exchange(states, hidden_t, gain_rows)
    query_grad, ks, vs, key_sum, value_sum, gate, gain_sums = block_grads(
        keys, values, query_rows, grad_rows, log_gate4, seg_col, seg_row, level_gain, incoming
    )
    gate = gate.reshape(heads, TOK)
    inner = jnp.sum(gain_sums, axis=2).reshape(heads, 8)
    outer = jnp.sum(cross_sums.reshape(8, 8, 2, 64), axis=3).transpose(0, 2, 1).reshape(16, 8)
    outer = jnp.where(
        (jnp.arange(heads) // 16 == core)[:, None], jnp.concatenate([outer, outer], axis=0), 0.0
    )
    gains = jnp.concatenate([inner, outer, jnp.zeros((heads, 16), F32)], axis=1)
    own_total = jnp.pad(gate[:, 0][None], ((0, 7), (0, 96)))
    small = jnp.concatenate([gains.reshape(8, 128), own_total], axis=0)
    key_weight, value_weight, summed = weight_grads(ks, vs, hy, hz, small)
    input_grad = (dot(key_sum, w_key, NT) + dot(value_sum, w_value, NT)).astype(BF16)
    gain_total = summed[:8].reshape(heads, 32)[:, :levels]
    gate_grad = gate + summed[8, :heads][:, None]
    return (
        query_grad[None],
        input_grad[None],
        gate_grad[None],
        key_weight,
        value_weight,
        gain_total,
    )


def solution(mesh):
    split = Mesh(
        mesh.devices.reshape(4, 4, 2, mesh.shape["batch"]), ("z", "x", "core", "batch")
    )
    return jax.shard_map(
        local,
        mesh=split,
        in_specs=(
            P("batch", SEQ, None),
            P("batch", SEQ, None),
            P(),
            P(),
            P("batch", None, SEQ),
            P(),
            P("batch", SEQ),
            P("batch", SEQ, None),
        ),
        out_specs=(
            P("batch", SEQ, None),
            P("batch", SEQ, None),
            P("batch", None, SEQ),
            P(SEQ_BATCH, None),
            P(SEQ_BATCH, None),
            P(),
        ),
        check_vma=False,
    )
```

```python
import functools

import jax
import jax.numpy as jnp
from jax import lax
from jax.experimental import pallas as pl
from jax.experimental.pallas import tpu as pltpu
from jax.sharding import Mesh
from jax.sharding import PartitionSpec as P

SEQ = ("z", "x", "core")
SEQ_BATCH = ("z", "x", "core", "batch")
MESH = pl.DeviceIdType.MESH
HIGHEST = lax.Precision.HIGHEST
F32 = jnp.float32
BF16 = jnp.bfloat16

NT = (((1,), (1,)), ((), ()))
TN = (((0,), (0,)), ((), ()))
NN = (((1,), (0,)), ((), ()))

TOK = 128
PAIR = 128
HALF_ROWS = 1088
SROWS = 1024


def dot(a, b, dims):
    return lax.dot_general(a, b, dims, preferred_element_type=F32)


def dot_exact(a, b, dims):
    return lax.dot_general(a, b, dims, preferred_element_type=F32, precision=HIGHEST)


def split2(x):
    hi = x.astype(BF16)
    return hi, (x - hi.astype(F32)).astype(BF16)


def dot_left(a, b, dims):
    hi, lo = split2(a)
    return dot(hi, b, dims) + dot(lo, b, dims)


def dot_right(a, b, dims):
    hi, lo = split2(b)
    return dot(a, hi, dims) + dot(a, lo, dims)


def iota(shape, dim):
    return lax.broadcasted_iota(jnp.int32, shape, dim)


def entry_signal(peers):
    barrier = pltpu.get_barrier_semaphore()
    for peer in peers:
        pl.semaphore_signal(barrier, inc=1, device_id=peer, device_id_type=MESH)
    return barrier


def ring(index, step):
    return lax.rem(index + step, 4)


def same(a, b):
    return jnp.where(a == b, 1.0, 0.0)


def linked(a, b, total):
    return jnp.where(a == b, jnp.exp(total), 0.0)


def rows_of(start, size):
    return pl.ds(pl.multiple_of(start, size), size)


SENDS = 128
LOCALS = 24


def scratch():
    def f(*shape):
        return pltpu.VMEM(shape, F32)

    def b(*shape):
        return pltpu.VMEM(shape, BF16)

    return dict(
        wk=b(1024, 2048),
        wv=b(1024, 2048),
        hid=b(TOK, 1024),
        q=b(TOK, 2048),
        g=b(TOK, 2048),
        k=b(16, TOK, PAIR),
        v=b(16, TOK, PAIR),
        hid_t=f(1024, TOK),
        cumx=f(16, TOK, PAIR),
        cumr=f(32, TOK),
        cumr3=f(16, 8, TOK),
        fw=f(16, TOK, PAIR),
        lw=f(16, TOK, PAIR),
        segc=f(TOK, TOK),
        st=f(2, HALF_ROWS, PAIR),
        both=f(2, HALF_ROWS, PAIR),
        chip_send=f(4, 272, PAIR),
        chip_recv=f(4, 272, PAIR),
        tot_send=f(2, 144, PAIR),
        tot_recv=f(2, 144, PAIR),
        back_send=f(4, 256, PAIR),
        back_recv=f(4, 256, PAIR),
        own_blocks=f(2, SROWS, PAIR),
        s_in=f(2, SROWS, PAIR),
        gcross=f(16, 8, PAIR),
        gint=f(16, 16, PAIR),
        gate=f(16, 8, TOK),
        hy=f(4, 2, 1024, TOK),
        hz=f(4, 2, 1024, TOK),
        hyb=b(1024, 8 * TOK),
        hzb=b(1024, 8 * TOK),
        qacc=f(16, TOK, PAIR),
        kacc=f(16, TOK, PAIR),
        vacc=f(16, TOK, PAIR),
        ks=f(2, 8, TOK, PAIR),
        vs=f(2, 8, TOK, PAIR),
        ksb=b(TOK, 2048),
        vsb=b(TOK, 2048),
        rk=f(2, 8, TOK, PAIR),
        rv=f(2, 8, TOK, PAIR),
        part1=f(4, 4, 256, PAIR),
        recv1=f(4, 4, 256, PAIR),
        part2=f(4, 4, 64, PAIR),
        recv2=f(4, 4, 64, PAIR),
        kown=f(8, 2, 8, PAIR),
        vown=f(8, 2, 8, PAIR),
        kfin=f(8, 2, 8, PAIR),
        vfin=f(8, 2, 8, PAIR),
        small=f(16, PAIR),
        m1=f(8, 16, PAIR),
        m1s=f(16, PAIR),
        m2=f(4, 16, PAIR),
        m2s=f(8, PAIR),
        m3=f(4, 8, PAIR),
        send_sem=pltpu.SemaphoreType.DMA((SENDS,)),
        recv_sem=pltpu.SemaphoreType.DMA((SENDS,)),
        local_sem=pltpu.SemaphoreType.DMA((LOCALS,)),
    )


def step_kernel(
    hid_hbm,
    q_hbm,
    g_hbm,
    wk_hbm,
    wv_hbm,
    lg_ref,
    segr_ref,
    gain_ref,
    qg_ref,
    ig_ref,
    gate_ref,
    kout_ref,
    vout_ref,
    sout_ref,
    *refs,
):
    s = dict(zip(scratch(), refs))
    x, y, z, c = (lax.axis_index(a) for a in ("x", "batch", "z", "core"))
    used = [0]

    def remote(src, dst, target):
        n = used[0]
        used[0] += 1
        cp = pltpu.make_async_remote_copy(
            src_ref=src,
            dst_ref=dst,
            send_sem=s["send_sem"].at[n],
            recv_sem=s["recv_sem"].at[n],
            device_id=target,
            device_id_type=MESH,
        )
        cp.start()
        return cp

    def wait(copies):
        for cp in copies:
            cp.wait()

    sib = {"core": 1 - c}
    offsets = [(d, e) for d in range(4) for e in (0, 1) if d or e]

    def plane(axis, index, d, e):
        to, tc = ring(index, d), lax.rem(c + e, 2)
        return {axis: to, "core": tc}, 2 * to + tc

    peers = [plane("batch", y, d, e)[0] for d, e in offsets]
    peers += [plane("z", z, d, e)[0] for d, e in offsets if d]
    peers += [{"x": ring(x, d)} for d in (1, 2, 3)]
    barrier = entry_signal(peers)

    local_sem = s["local_sem"]
    first_loads = [
        pltpu.make_async_copy(hid_hbm, s["hid"], local_sem.at[0]),
        pltpu.make_async_copy(q_hbm, s["q"], local_sem.at[1]),
        pltpu.make_async_copy(g_hbm, s["g"], local_sem.at[2]),
    ]

    def weight_load(hbm, name, i, base):
        cols = rows_of(i * 256, 256)
        return pltpu.make_async_copy(hbm.at[:, cols], s[name].at[:, cols], local_sem.at[base + i])

    first_loads[0].start()
    for i in range(8):
        weight_load(wk_hbm, "wk", i, 8).start()
        weight_load(wv_hbm, "wv", i, 16).start()
        if i == 0:
            first_loads[1].start()
            first_loads[2].start()

    rows_i, cols_i = iota((TOK, TOK), 0), iota((TOK, TOK), 1)
    causal = cols_i <= rows_i
    lower = causal.astype(F32)
    low = cols_i < 64
    low_half = iota((64, PAIR), 1) < 64
    row8 = iota((8, PAIR), 0)
    low_row = iota((1, PAIR), 1) < 64
    log_gate = lg_ref[...]
    cum_cols = dot_exact(lower, log_gate, NT)
    s["cumr"][...] = dot_exact(log_gate, lower, NT)
    for pair in range(16):
        s["cumx"][pair] = jnp.where(
            low, cum_cols[:, 2 * pair : 2 * pair + 1], cum_cols[:, 2 * pair + 1 : 2 * pair + 2]
        )
        s["cumr3"][pair, 0:2, :] = s["cumr"][2 * pair : 2 * pair + 2, :]
    seg_row = segr_ref[...].astype(F32)
    s["segc"][...] = jnp.broadcast_to(seg_row, (TOK, TOK)).T
    s["gcross"][...] = jnp.zeros((16, 8, PAIR), F32)

    first_loads[0].wait()
    for b in range(8):
        cols = slice(b * TOK, (b + 1) * TOK)
        s["hid_t"][cols, :] = s["hid"][:, cols].astype(F32).T
    pl.semaphore_wait(barrier, len(peers))
    gathers = (("batch", y, s["hy"]), ("z", z, s["hz"]))
    hops = []
    for axis, index, buf in gathers:
        for d in (1, 3):
            hops.append(remote(s["hid_t"], buf.at[index, c], {axis: ring(index, d)}))
    down = [remote(s["hid_t"], buf.at[index, c], sib) for _, index, buf in gathers]

    first_loads[1].wait()
    first_loads[2].wait()

    def project(step, carry):
        weight_load(wk_hbm, "wk", step, 8).wait()
        weight_load(wv_hbm, "wv", step, 16).wait()
        wide = rows_of(step * 256, 256)
        hid = s["hid"][...]
        keys = dot(hid, s["wk"][:, wide], NN).astype(BF16)
        values = dot(hid, s["wv"][:, wide], NN).astype(BF16)
        segc = s["segc"][...]
        half = step // 4
        for p in range(2):
            pair = 2 * step + p
            k, v = keys[:, p * PAIR : (p + 1) * PAIR], values[:, p * PAIR : (p + 1) * PAIR]
            s["k"][pair] = k
            s["v"][pair] = v
            cum = s["cumx"][pair]
            total = cum[TOK - 1 : TOK, :]
            last_w = jnp.where(segc == segc[TOK - 1 : TOK, :], jnp.exp(total - cum), 0.0)
            first_w = jnp.where(segc == segc[0:1, :], jnp.exp(cum), 0.0)
            s["lw"][pair] = last_w
            s["fw"][pair] = first_w
            cols = rows_of(pair * PAIR, PAIR)
            fwd = dot_left(k.astype(F32) * last_w, v, TN)
            rev = dot_left(s["q"][:, cols].astype(F32) * first_w, s["g"][:, cols], TN)
            pp = 2 * lax.rem(step, 4) + p
            s["st"][half, rows_of(pp * 64, 64), :] = jnp.where(low_half, fwd[:64], fwd[64:])
            s["st"][half, rows_of(512 + pp * 64, 64), :] = jnp.where(low_half, rev[:64], rev[64:])
            meta = jnp.where(
                row8 == 0,
                total,
                jnp.where(
                    row8 == 1, segc[0:1, :], jnp.where(row8 == 2, segc[TOK - 1 : TOK, :], 0.0)
                ),
            )
            s["st"][half, rows_of(1024 + pp * 8, 8), :] = meta
        return carry

    lax.fori_loop(0, 8, project, 0)

    def inner(pair, carry):
        cols = rows_of(pair * PAIR, PAIR)
        q, g = s["q"][:, cols], s["g"][:, cols]
        k, v = s["k"][pair], s["v"][pair]
        allowed = causal & (s["segc"][...] == seg_row)
        gap = jnp.bitwise_xor(rows_i, cols_i)
        strict = (rows_i < cols_i).astype(BF16)
        zero = jnp.zeros((TOK, PAIR), BF16)
        weighted, scored, queries, keys, grads, gate_rows, gain_rows = [], [], [], [], [], [], []
        for h in range(2):

            def own(a):
                return jnp.where(low, a, zero) if h == 0 else jnp.where(low, zero, a)

            qh, gh, kh = own(q), own(g), own(k)
            score = dot(qh, k, NT)
            dprob = dot(gh, v, NT)
            spread = s["cumx"][pair, :, 64 * h : 64 * h + 1] - s["cumr3"][pair, h : h + 1, :]
            decay = jnp.where(allowed, jnp.exp(jnp.where(allowed, spread, 0.0)), 0.0)
            ds = decay * score
            joint = ds * dprob
            head = 2 * pair + h
            level = jnp.full((TOK, TOK), gain_ref[head, 0], F32)
            gain_rows.append(jnp.sum(jnp.where(gap == 0, joint, 0.0), axis=0, keepdims=True))
            for l in range(1, 8):
                above = gap >= 2 ** (l - 1)
                level = jnp.where(above, gain_ref[head, l], level)
                chosen = above & (gap < 2**l)
                gain_rows.append(jnp.sum(jnp.where(chosen, joint, 0.0), axis=0, keepdims=True))
            wd = level * decay * dprob
            weighted.append(wd.astype(BF16))
            scored.append((level * ds).astype(BF16))
            grid = (wd * score).astype(BF16)
            crossing = jnp.where(causal, dot(grid, strict, NN), 0.0)
            gate_rows.append(jnp.sum(crossing, axis=0, keepdims=True))
            queries.append(qh)
            keys.append(kh)
            grads.append(gh)
        s["qacc"][pair] = dot(
            jnp.concatenate(weighted, axis=1), jnp.concatenate(keys, axis=0), NN
        )
        s["kacc"][pair] = dot(
            jnp.concatenate(weighted, axis=0), jnp.concatenate(queries, axis=0), TN
        )
        s["vacc"][pair] = dot(jnp.concatenate(scored, axis=0), jnp.concatenate(grads, axis=0), TN)
        s["gate"][pair] = jnp.concatenate([*gate_rows, jnp.zeros((6, TOK), F32)], axis=0)
        s["gint"][pair] = jnp.concatenate(gain_rows, axis=0)
        return carry

    both, st = s["both"], s["st"]
    swap = remote(st.at[1 - c], both.at[c], sib)
    both[pl.ds(c, 1)] = st[pl.ds(c, 1)]
    lax.fori_loop(0, 2, inner, 0)
    swap.wait()

    def meta_rows(total, first, last):
        return jnp.where(
            row8 == 0, total, jnp.where(row8 == 1, first, jnp.where(row8 == 2, last, 0.0))
        )

    chip_send, chip_recv = s["chip_send"], s["chip_recv"]
    for pp in range(8):
        f0 = both[0, pp * 64 : pp * 64 + 64, :]
        f1 = both[1, pp * 64 : pp * 64 + 64, :]
        r0 = both[0, 512 + pp * 64 : 576 + pp * 64, :]
        r1 = both[1, 512 + pp * 64 : 576 + pp * 64, :]
        m0 = both[0, 1024 + pp * 8 : 1032 + pp * 8, :]
        m1 = both[1, 1024 + pp * 8 : 1032 + pp * 8, :]
        t0, first0, last0 = m0[0:1], m0[1:2], m0[2:3]
        t1, first1, last1 = m1[0:1], m1[1:2], m1[2:3]
        n, p = pp // 2, pp % 2
        chip_send[n, p * 64 : p * 64 + 64, :] = f1 + linked(last0, last1, t1) * f0
        chip_send[n, 128 + p * 64 : 192 + p * 64, :] = r0 + linked(first0, first1, t0) * r1
        chip_send[n, 256 + p * 8 : 264 + p * 8, :] = meta_rows(t0 + t1, first0, last1)
        d8 = same(last0, first1) * jnp.sum(f0 * r1, axis=0, keepdims=True)
        s["gcross"][pl.ds(c * 8 + pp, 1)] = jnp.where(row8 == 0, d8, 0.0)[None]

    xs = []
    for d in (1, 2, 3):
        to = ring(x, d)
        xs.append(remote(chip_send.at[to], chip_recv.at[x], {"x": to}))
    chip_recv[pl.ds(x, 1)] = chip_send[pl.ds(x, 1)]

    def forward(n):
        axis, index, buf = gathers[n]
        out = []
        for m, d in enumerate((1, 3)):
            hops[2 * n + m].wait()
            came = ring(index, 4 - d)
            part = slice(0, 512) if d == 1 else slice(512, 1024)
            out.append(
                remote(buf.at[came, c, part], buf.at[came, c, part], {axis: ring(index, d)})
            )
            down.append(remote(buf.at[came, c], buf.at[came, c], sib))
        return out

    fwd_y = forward(0)
    lax.fori_loop(2, 8, inner, 0)
    wait(xs)

    def chip(j, p):
        return (
            chip_recv[j, p * 64 : p * 64 + 64, :],
            chip_recv[j, 128 + p * 64 : 192 + p * 64, :],
            chip_recv[j, 256 + p * 8 : 257 + p * 8, :],
            chip_recv[j, 257 + p * 8 : 258 + p * 8, :],
            chip_recv[j, 258 + p * 8 : 259 + p * 8, :],
        )

    def joined(p):
        (f0, r0, t0, a0, l0), (f1, r1, t1, a1, l1), (f2, r2, t2, a2, l2), (f3, r3, t3, a3, l3) = (
            chip(j, p) for j in range(4)
        )
        f01 = f1 + linked(l0, l1, t1) * f0
        r01 = r0 + linked(a0, a1, t0) * r1
        f23 = f3 + linked(l2, l3, t3) * f2
        r23 = r2 + linked(a2, a3, t2) * r3
        return f01, r01, f23, r23

    tot_send, tot_recv = s["tot_send"], s["tot_recv"]
    for p in range(2):
        f01, r01, f23, r23 = joined(p)
        t0, a0 = chip(0, p)[2:4]
        t1, l1 = chip(1, p)[2], chip(1, p)[4]
        t2, a2 = chip(2, p)[2:4]
        t3, l3 = chip(3, p)[2], chip(3, p)[4]
        tot_send[0, p * 64 : p * 64 + 64, :] = f23 + linked(l1, l3, t2 + t3) * f01
        tot_send[1, p * 64 : p * 64 + 64, :] = r01 + linked(a0, a2, t0 + t1) * r23
        tot_send[0, 128 + p * 8 : 136 + p * 8, :] = jnp.broadcast_to(l3, (8, PAIR))
        tot_send[1, 128 + p * 8 : 136 + p * 8, :] = jnp.broadcast_to(a0, (8, PAIR))
    zs = [
        remote(tot_send.at[n], tot_recv.at[n], {"z": ring(z, d)}) for n, d in ((0, 1), (1, 3))
    ]
    fwd_z = forward(1)
    lax.fori_loop(8, 10, inner, 0)
    wait(zs)

    has_prev = (z > 0).astype(F32)
    has_next = (z < 3).astype(F32)
    prev_top = (z == 2).astype(F32)
    next_top = (z == 1).astype(F32)
    back_send, back_recv = s["back_send"], s["back_recv"]

    def gain_row(pair, level):
        return jnp.where(low_row, gain_ref[2 * pair, level], gain_ref[2 * pair + 1, level])

    for p in range(2):
        (f0, r0, t0, a0, l0), (f1, r1, t1, a1, l1), (f2, r2, t2, a2, l2), (f3, r3, t3, a3, l3) = (
            chip(j, p) for j in range(4)
        )
        f01, r01, f23, r23 = joined(p)
        pair = c * 8 + 2 * x + p
        g9, g10, g11, g12 = (gain_row(pair, level) for level in range(9, 13))
        zf = has_prev * tot_recv[0, p * 64 : p * 64 + 64, :]
        zl = tot_recv[0, 128 + p * 8 : 129 + p * 8, :]
        zr = has_next * tot_recv[1, p * 64 : p * 64 + 64, :]
        za = tot_recv[1, 128 + p * 8 : 129 + p * 8, :]
        gzf = g11 * (1.0 - prev_top) + g12 * prev_top
        gzr = g11 * (1.0 - next_top) + g12 * next_top
        sf = (
            gzf * same(zl, a0) * zf,
            gzf * linked(zl, a1, t0) * zf + g9 * same(l0, a1) * f0,
            gzf * linked(zl, a2, t0 + t1) * zf + g10 * same(l1, a2) * f01,
            gzf * linked(zl, a3, t0 + t1 + t2) * zf
            + g10 * linked(l1, a3, t2) * f01
            + g9 * same(l2, a3) * f2,
        )
        sr = (
            gzr * linked(za, l0, t1 + t2 + t3) * zr
            + g10 * linked(l0, a2, t1) * r23
            + g9 * same(l0, a1) * r1,
            gzr * linked(za, l1, t2 + t3) * zr + g10 * same(l1, a2) * r23,
            gzr * linked(za, l2, t3) * zr + g9 * same(l2, a3) * r3,
            gzr * same(za, l3) * zr,
        )
        for j in range(4):
            back_send[j, p * 64 : p * 64 + 64, :] = sf[j]
            back_send[j, 128 + p * 64 : 192 + p * 64, :] = sr[j]
    bs = []
    for d in (1, 2, 3):
        to = ring(x, d)
        bs.append(remote(back_send.at[to], back_recv.at[x], {"x": to}))
    back_recv[pl.ds(x, 1)] = back_send[pl.ds(x, 1)]

    for p in range(2):
        (f0, r0, t0, a0, l0), (f1, r1, t1, a1, l1), (f2, r2, t2, a2, l2), (f3, r3, t3, a3, l3) = (
            chip(j, p) for j in range(4)
        )
        f01, r01, f23, r23 = joined(p)
        zf = has_prev * tot_recv[0, p * 64 : p * 64 + 64, :]
        zl = tot_recv[0, 128 + p * 8 : 129 + p * 8, :]
        r_group = r01 + linked(a0, a2, t0 + t1) * r23
        d9 = same(l0, a1) * jnp.sum(f0 * r1, axis=0, keepdims=True) + same(l2, a3) * jnp.sum(
            f2 * r3, axis=0, keepdims=True
        )
        d10 = same(l1, a2) * jnp.sum(f01 * r23, axis=0, keepdims=True)
        dz = same(zl, a0) * jnp.sum(zf * r_group, axis=0, keepdims=True)
        rows = jnp.where(
            row8 == 1,
            d9,
            jnp.where(
                row8 == 2,
                d10,
                jnp.where(
                    row8 == 3, (1.0 - prev_top) * dz, jnp.where(row8 == 4, prev_top * dz, 0.0)
                ),
            ),
        )
        pair = c * 8 + 2 * x + p
        s["gcross"][pl.ds(pair, 1)] = s["gcross"][pl.ds(pair, 1)] + rows[None]
    lax.fori_loop(10, 16, inner, 0)
    wait(bs)

    own_blocks, s_in = s["own_blocks"], s["s_in"]
    for pp in range(8):
        n, p = pp // 2, pp % 2
        f0 = both[0, pp * 64 : pp * 64 + 64, :]
        r1 = both[1, 512 + pp * 64 : 576 + pp * 64, :]
        m0 = both[0, 1024 + pp * 8 : 1032 + pp * 8, :]
        m1 = both[1, 1024 + pp * 8 : 1032 + pp * 8, :]
        t0, first0, last0 = m0[0:1], m0[1:2], m0[2:3]
        t1, first1, last1 = m1[0:1], m1[1:2], m1[2:3]
        sf = back_recv[n, p * 64 : p * 64 + 64, :]
        sr = back_recv[n, 128 + p * 64 : 192 + p * 64, :]
        link = gain_row(c * 8 + pp, 8) * same(last0, first1)
        own_blocks[0, pp * 64 : pp * 64 + 64, :] = sf
        own_blocks[1, pp * 64 : pp * 64 + 64, :] = linked(first0, first1, t0) * sf + link * f0
        own_blocks[0, 512 + pp * 64 : 576 + pp * 64, :] = linked(last0, last1, t1) * sr + link * r1
        own_blocks[1, 512 + pp * 64 : 576 + pp * 64, :] = sr
    swap = remote(own_blocks.at[1 - c], s_in.at[c], sib)
    s_in[pl.ds(c, 1)] = own_blocks[pl.ds(c, 1)]

    for (_, index, buf), copies in zip(gathers, (fwd_y, fwd_z)):
        buf[pl.ds(index, 1), pl.ds(c, 1)] = s["hid_t"][...][None, None]
        wait(copies)
        came = ring(index, 2)
        down.append(remote(buf.at[came, c], buf.at[came, c], sib))
    swap.wait()

    tail = causal.astype(BF16)
    head_pick = (cols_i[0:8, :] // 64 == row8).astype(BF16)

    def cross(pair, carry):
        half, pp = pair // 8, lax.rem(pair, 8)
        cols = rows_of(pair * PAIR, PAIR)
        q, g = s["q"][:, cols], s["g"][:, cols]
        k, v = s["k"][pair], s["v"][pair]
        first_w, last_w = s["fw"][pair], s["lw"][pair]
        sf = s_in[half, rows_of(pp * 64, 64), :]
        sr = s_in[half, rows_of(512 + pp * 64, 64), :]

        def diag(a):
            return jnp.concatenate([jnp.where(low_half, a, 0.0), jnp.where(low_half, 0.0, a)], axis=0)

        sg = first_w * dot_right(g, diag(sf), NT)
        rv = last_w * dot_right(v, diag(sr), NT)
        rk = last_w * dot_right(k, diag(sr), NN)
        diff = q.astype(F32) * sg - k.astype(F32) * rv
        hi, lo = split2(diff)
        diff_rows = dot(head_pick, hi, NT) + dot(head_pick, lo, NT)
        s["gate"][pair] = s["gate"][pair] + dot_left(diff_rows, tail, NN)
        qg_ref[:, cols] = (s["qacc"][pair] + sg).astype(BF16)
        key_sum = (s["kacc"][pair] + rv).astype(BF16)
        value_sum = (s["vacc"][pair] + rk).astype(BF16)
        s["ksb"][:, cols] = key_sum
        s["vsb"][:, cols] = value_sum
        s["ks"][half, pp] = key_sum.astype(F32)
        s["vs"][half, pp] = value_sum.astype(F32)
        return carry

    firsts = []
    me_y, me_z = 2 * y + c, 2 * z + c
    for n in range(2):
        lax.fori_loop(8 * n, 8 * n + 8, cross, 0)
        fk, fv = [], []
        for d, e in offsets:
            dev, to = plane("batch", y, d, e)
            fk.append(remote(s["ks"].at[n, to], s["rk"].at[n, me_y], dev))
            dev, to = plane("z", z, d, e)
            fv.append(remote(s["vs"].at[n, to], s["rv"].at[n, me_z], dev))
        s["rk"][n, pl.ds(me_y, 1)] = s["ks"][n, pl.ds(me_y, 1)]
        s["rv"][n, pl.ds(me_z, 1)] = s["vs"][n, pl.ds(me_z, 1)]
        firsts.append((fk, fv))

    ones = jnp.ones((8, PAIR), F32)
    inner_sum = dot_exact(ones, s["gint"][...].reshape(256, PAIR), NT)
    pick = (cols_i[0:8, :] // 64 == row8 - 2).astype(F32)
    outer_sum = dot_exact(pick, s["gcross"][...].reshape(128, PAIR), NT)
    start = (cols_i[0:8, :] == 0).astype(F32)
    own_total = dot_exact(start, s["gate"][...].reshape(128, TOK), NT)
    small, m1, m1s, m2, m2s, m3 = (s[n] for n in ("small", "m1", "m1s", "m2", "m2s", "m3"))
    small[0:8, :] = jnp.where(
        row8 == 0, inner_sum[:, :128], jnp.where(row8 == 1, inner_sum[:, 128:], outer_sum)
    )
    small[8:16, :] = own_total
    smalls = []
    for d, e in offsets:
        smalls.append(remote(small, m1.at[me_z], plane("z", z, d, e)[0]))
    m1[pl.ds(me_z, 1)] = small[...][None]

    wait(down)
    for name, out in (("hy", "hyb"), ("hz", "hzb")):
        for g in range(8):
            s[out][:, g * TOK : (g + 1) * TOK] = s[name][g // 2, g % 2].astype(BF16)

    def product(left, right, n):
        right = s[right][n].reshape(8 * TOK, PAIR).astype(BF16)
        for b in range(4):
            yield b, dot(s[left][b * 256 : (b + 1) * 256, :], right, NN)

    part1, recv1, part2, recv2 = s["part1"], s["recv1"], s["part2"], s["recv2"]

    def scatter(part, recv, chunk, axis, index):
        out = []
        for d in (1, 2, 3):
            to = ring(index, d)
            out.append(remote(part.at[chunk, to], recv.at[chunk, index], {axis: to}))
        recv[chunk, pl.ds(index, 1)] = part[chunk, pl.ds(index, 1)]
        return out

    wait(firsts[0][0])
    for b, block in product("hyb", "rk", 0):
        for j in range(4):
            part1[0, j, b * 64 : b * 64 + 64, :] = block[j * 64 : j * 64 + 64, :]
    k0 = scatter(part1, recv1, 0, "x", x)
    wait(firsts[0][1])
    for b, block in product("hzb", "rv", 0):
        for j in range(4):
            part1[2, j, b * 64 : b * 64 + 64, :] = block[j * 64 : j * 64 + 64, :]
    v0 = scatter(part1, recv1, 2, "x", x)

    def input_grad(n, carry):
        rows = rows_of(n * 256, 256)
        ig_ref[:, rows] = (
            dot(s["ksb"][...], s["wk"][rows, :], NT) + dot(s["vsb"][...], s["wv"][rows, :], NT)
        ).astype(BF16)
        return carry

    lax.fori_loop(0, 2, input_grad, 0)

    wait(firsts[1][0])
    for b, block in product("hyb", "rk", 1):
        part1[1, b] = block
    k1 = scatter(part1, recv1, 1, "z", z)
    wait(firsts[1][1])
    for b, block in product("hzb", "rv", 1):
        for j in range(8):
            for i in range(4):
                at = j * 32 + i * 8
                part1[3, i, b * 64 + j * 8 : b * 64 + j * 8 + 8, :] = block[at : at + 8, :]
    v1 = scatter(part1, recv1, 3, "batch", y)
    lax.fori_loop(2, 4, input_grad, 0)

    wait(smalls)
    total = m1[0, 0:8, :]
    for g in range(1, 8):
        total = total + m1[g, 0:8, :]
    m1s[0:8, :] = total
    for g in range(8):
        m1s[8 + g : 9 + g, :] = m1[g, 8:9, :]
    smalls = [remote(m1s, m2.at[x], {"x": ring(x, d)}) for d in (1, 2, 3)]
    m2[pl.ds(x, 1)] = m1s[...][None]

    def summed(recv, chunk):
        return recv[chunk, 0] + recv[chunk, 1] + recv[chunk, 2] + recv[chunk, 3]

    wait(k0)
    total = summed(recv1, 0)
    for j in range(4):
        part2[0, j] = total[j * 64 : j * 64 + 64, :]
    k0 = scatter(part2, recv2, 0, "z", z)
    wait(v0)
    total = summed(recv1, 2)
    for j in range(8):
        for i in range(4):
            at = j * 32 + i * 8
            part2[2, i, j * 8 : j * 8 + 8, :] = total[at : at + 8, :]
    v0 = scatter(part2, recv2, 2, "batch", y)
    wait(k1)
    total = summed(recv1, 1)
    for j in range(4):
        part2[1, j] = total[j * 64 : j * 64 + 64, :]
    k1 = scatter(part2, recv2, 1, "x", x)
    wait(v1)
    total = summed(recv1, 3)
    for j in range(4):
        for i in range(4):
            at = j * 64 + i * 16
            part2[3, i, j * 16 : j * 16 + 16, :] = total[at : at + 16, :]
    v1 = scatter(part2, recv2, 3, "x", x)

    wait(smalls)
    total = m2[0, 0:8, :] + m2[1, 0:8, :] + m2[2, 0:8, :] + m2[3, 0:8, :]
    m2s[...] = total
    smalls = [remote(m2s, m3.at[y], {"batch": ring(y, d)}) for d in (1, 2, 3)]
    m3[pl.ds(y, 1)] = total[None]
    place = z * 8 + x * 2 + c
    later = jnp.zeros((1, PAIR), F32)
    for j in range(4):
        for g in range(8):
            spot = (g // 2) * 8 + j * 2 + g % 2
            later = later + (place < spot).astype(F32) * m2[j, 8 + g : 9 + g, :]
    sout_ref[8:16, :] = jnp.broadcast_to(later, (8, PAIR))
    gate_ref[...] = s["gate"][...]

    fins = []
    wait(k0)
    wait(k1)
    for n in range(2):
        total = summed(recv2, n)
        for i in range(4):
            for j in range(2):
                at = j * 32 + i * 8
                s["kown"][2 * i + j, n] = total[at : at + 8, :]
    for d, e in offsets:
        dev, to = plane("batch", y, d, e)
        fins.append(remote(s["kown"].at[to], s["kfin"].at[me_y], dev))
    s["kfin"][pl.ds(me_y, 1)] = s["kown"][pl.ds(me_y, 1)]
    wait(v0)
    wait(v1)
    for n in range(2):
        total = summed(recv2, 2 + n)
        for j in range(8):
            s["vown"][j, n] = total[j * 8 : j * 8 + 8, :]
    for d, e in offsets:
        dev, to = plane("z", z, d, e)
        fins.append(remote(s["vown"].at[to], s["vfin"].at[me_z], dev))
    s["vfin"][pl.ds(me_z, 1)] = s["vown"][pl.ds(me_z, 1)]
    wait(smalls)
    sout_ref[0:8, :] = m3[0] + m3[1] + m3[2] + m3[3]
    wait(fins)
    for n in range(2):
        for g in range(8):
            cols = slice(n * 1024 + g * PAIR, n * 1024 + (g + 1) * PAIR)
            kout_ref[:, cols] = s["kfin"][g, n]
            vout_ref[:, cols] = s["vfin"][g, n]


def whole_step(hidden, queries, out_grad, w_key, w_value, log_gate, seg_row, level_gain):
    vm = pl.BlockSpec(memory_space=pltpu.VMEM)
    far = pl.BlockSpec(memory_space=pl.ANY)
    return pl.pallas_call(
        step_kernel,
        in_specs=[far] * 5 + [vm, vm, pl.BlockSpec(memory_space=pltpu.SMEM)],
        out_specs=[vm] * 6,
        out_shape=[
            jax.ShapeDtypeStruct((TOK, 2048), BF16),
            jax.ShapeDtypeStruct((TOK, 1024), BF16),
            jax.ShapeDtypeStruct((16, 8, TOK), F32),
            jax.ShapeDtypeStruct((8, 2048), F32),
            jax.ShapeDtypeStruct((8, 2048), F32),
            jax.ShapeDtypeStruct((16, PAIR), F32),
        ],
        scratch_shapes=list(scratch().values()),
        compiler_params=pltpu.CompilerParams(
            collective_id=0, has_side_effects=True, vmem_limit_bytes=63 * 2**20
        ),
        name="whole_step",
    )(hidden, queries, out_grad, w_key, w_value, log_gate, seg_row, level_gain)


def local(hidden, queries, w_key, w_value, log_gate, level_gain, segment_ids, out_grad):
    heads, levels = level_gain.shape
    query_grad, input_grad, gate, key_weight, value_weight, summed = whole_step(
        hidden[0], queries[0], out_grad[0], w_key, w_value, log_gate[0], segment_ids, level_gain
    )
    inner = summed[:2].reshape(heads, 8)
    outer = summed[2:4].reshape(2, heads // 2, 8).transpose(1, 0, 2).reshape(heads, 8)
    gain_total = jnp.concatenate([inner, outer, jnp.zeros((heads, levels - 16), F32)], axis=1)
    gate_grad = (gate + summed[8].reshape(16, 8)[:, :, None])[:, :2].reshape(heads, TOK)
    return (
        query_grad[None],
        input_grad[None],
        gate_grad[None],
        key_weight,
        value_weight,
        gain_total,
    )


def solution(mesh):
    split = Mesh(
        mesh.devices.reshape(4, 4, 2, mesh.shape["batch"]), ("z", "x", "core", "batch")
    )
    return jax.shard_map(
        local,
        mesh=split,
        in_specs=(
            P("batch", SEQ, None),
            P("batch", SEQ, None),
            P(),
            P(),
            P("batch", None, SEQ),
            P(),
            P("batch", SEQ),
            P("batch", SEQ, None),
        ),
        out_specs=(
            P("batch", SEQ, None),
            P("batch", SEQ, None),
            P("batch", None, SEQ),
            P(SEQ_BATCH, None),
            P(SEQ_BATCH, None),
            P(),
        ),
        check_vma=False,
    )
```

```python
import functools

import jax
import jax.numpy as jnp
from jax import lax
from jax.experimental import pallas as pl
from jax.experimental.pallas import tpu as pltpu
from jax.sharding import Mesh
from jax.sharding import PartitionSpec as P

SEQ = ("z", "x", "core")
SEQ_BATCH = ("z", "x", "core", "batch")
MESH = pl.DeviceIdType.MESH
HIGHEST = lax.Precision.HIGHEST
F32 = jnp.float32
BF16 = jnp.bfloat16

NT = (((1,), (1,)), ((), ()))
TN = (((0,), (0,)), ((), ()))
NN = (((1,), (0,)), ((), ()))

TOK = 128
PAIR = 128
HALF_ROWS = 1088
SROWS = 1024


def dot(a, b, dims):
    return lax.dot_general(a, b, dims, preferred_element_type=F32)


def dot_exact(a, b, dims):
    return lax.dot_general(a, b, dims, preferred_element_type=F32, precision=HIGHEST)


def split2(x):
    hi = x.astype(BF16)
    return hi, (x - hi.astype(F32)).astype(BF16)


def dot_left(a, b, dims):
    hi, lo = split2(a)
    return dot(hi, b, dims) + dot(lo, b, dims)


def dot_right(a, b, dims):
    hi, lo = split2(b)
    return dot(a, hi, dims) + dot(a, lo, dims)


def iota(shape, dim):
    return lax.broadcasted_iota(jnp.int32, shape, dim)


def entry_signal(peers):
    barrier = pltpu.get_barrier_semaphore()
    for peer in peers:
        pl.semaphore_signal(barrier, inc=1, device_id=peer, device_id_type=MESH)
    return barrier


def ring(index, step):
    return lax.rem(index + step, 4)


def same(a, b):
    return jnp.where(a == b, 1.0, 0.0)


def linked(a, b, total):
    return jnp.where(a == b, jnp.exp(total), 0.0)


def rows_of(start, size):
    return pl.ds(pl.multiple_of(start, size), size)


SENDS = 128
LOCALS = 24
VMEM_LIMIT = 56 * 2**20


def scratch():
    def f(*shape):
        return pltpu.VMEM(shape, F32)

    def b(*shape):
        return pltpu.VMEM(shape, BF16)

    return dict(
        wk=b(1024, 2048),
        wv=b(1024, 2048),
        hid=b(TOK, 1024),
        q=b(TOK, 2048),
        g=b(TOK, 2048),
        k=b(16, TOK, PAIR),
        v=b(16, TOK, PAIR),
        hid_t=f(1024, TOK),
        cumx=f(16, TOK, PAIR),
        cumr=f(32, TOK),
        cumr3=f(16, 8, TOK),
        fw=f(16, TOK, PAIR),
        lw=f(16, TOK, PAIR),
        segc=f(TOK, TOK),
        st=f(2, HALF_ROWS, PAIR),
        both=f(2, HALF_ROWS, PAIR),
        chip_send=f(4, 272, PAIR),
        chip_recv=f(4, 272, PAIR),
        tot_send=f(2, 144, PAIR),
        tot_recv=f(2, 144, PAIR),
        back_send=f(4, 256, PAIR),
        back_recv=f(4, 256, PAIR),
        own_blocks=f(2, SROWS, PAIR),
        s_in=f(2, SROWS, PAIR),
        gcross=f(16, 8, PAIR),
        gint=f(16, 16, PAIR),
        gate=f(16, 8, TOK),
        hy=f(4, 2, 1024, TOK),
        hz=f(4, 2, 1024, TOK),
        hyb=b(1024, 8 * TOK),
        hzb=b(1024, 8 * TOK),
        qacc=f(16, TOK, PAIR),
        kacc=f(16, TOK, PAIR),
        vacc=f(16, TOK, PAIR),
        ks=f(2, 8, TOK, PAIR),
        vs=f(2, 8, TOK, PAIR),
        ksb=b(TOK, 2048),
        vsb=b(TOK, 2048),
        rk=f(2, 8, TOK, PAIR),
        rv=f(2, 8, TOK, PAIR),
        part1=f(4, 4, 256, PAIR),
        recv1=f(4, 4, 256, PAIR),
        part2=f(4, 4, 64, PAIR),
        recv2=f(4, 4, 64, PAIR),
        kown=f(8, 2, 8, PAIR),
        vown=f(8, 2, 8, PAIR),
        kfin=f(8, 2, 8, PAIR),
        vfin=f(8, 2, 8, PAIR),
        small=f(16, PAIR),
        m1=f(8, 16, PAIR),
        m1s=f(16, PAIR),
        m2=f(4, 16, PAIR),
        m2s=f(8, PAIR),
        m3=f(4, 8, PAIR),
        send_sem=pltpu.SemaphoreType.DMA((SENDS,)),
        recv_sem=pltpu.SemaphoreType.DMA((SENDS,)),
        local_sem=pltpu.SemaphoreType.DMA((LOCALS,)),
    )


def step_kernel(
    hid_hbm,
    q_hbm,
    g_hbm,
    wk_hbm,
    wv_hbm,
    lg_ref,
    segr_ref,
    gain_ref,
    qg_ref,
    ig_ref,
    gate_ref,
    kout_ref,
    vout_ref,
    sout_ref,
    *refs,
):
    s = dict(zip(scratch(), refs))
    x, y, z, c = (lax.axis_index(a) for a in ("x", "batch", "z", "core"))
    used = [0]

    def remote(src, dst, target):
        n = used[0]
        used[0] += 1
        cp = pltpu.make_async_remote_copy(
            src_ref=src,
            dst_ref=dst,
            send_sem=s["send_sem"].at[n],
            recv_sem=s["recv_sem"].at[n],
            device_id=target,
            device_id_type=MESH,
        )
        cp.start()
        return cp

    def wait(copies):
        for cp in copies:
            cp.wait()

    sib = {"core": 1 - c}
    offsets = [(d, e) for d in range(4) for e in (0, 1) if d or e]

    def plane(axis, index, d, e):
        to, tc = ring(index, d), lax.rem(c + e, 2)
        return {axis: to, "core": tc}, 2 * to + tc

    peers = [plane("batch", y, d, e)[0] for d, e in offsets]
    peers += [plane("z", z, d, e)[0] for d, e in offsets if d]
    peers += [{"x": ring(x, d)} for d in (1, 2, 3)]
    barrier = entry_signal(peers)

    local_sem = s["local_sem"]
    first_loads = [
        pltpu.make_async_copy(hid_hbm, s["hid"], local_sem.at[0]),
        pltpu.make_async_copy(q_hbm, s["q"], local_sem.at[1]),
        pltpu.make_async_copy(g_hbm, s["g"], local_sem.at[2]),
    ]

    def weight_load(hbm, name, i, base):
        cols = rows_of(i * 256, 256)
        return pltpu.make_async_copy(hbm.at[:, cols], s[name].at[:, cols], local_sem.at[base + i])

    first_loads[0].start()
    for i in range(8):
        weight_load(wk_hbm, "wk", i, 8).start()
        weight_load(wv_hbm, "wv", i, 16).start()
        if i == 0:
            first_loads[1].start()
            first_loads[2].start()

    rows_i, cols_i = iota((TOK, TOK), 0), iota((TOK, TOK), 1)
    causal = cols_i <= rows_i
    lower = causal.astype(F32)
    low = cols_i < 64
    low_half = iota((64, PAIR), 1) < 64
    row8 = iota((8, PAIR), 0)
    low_row = iota((1, PAIR), 1) < 64
    log_gate = lg_ref[...]
    cum_cols = dot_exact(lower, log_gate, NT)
    s["cumr"][...] = dot_exact(log_gate, lower, NT)
    for pair in range(16):
        s["cumx"][pair] = jnp.where(
            low, cum_cols[:, 2 * pair : 2 * pair + 1], cum_cols[:, 2 * pair + 1 : 2 * pair + 2]
        )
        s["cumr3"][pair, 0:2, :] = s["cumr"][2 * pair : 2 * pair + 2, :]
    seg_row = segr_ref[...].astype(F32)
    s["segc"][...] = jnp.broadcast_to(seg_row, (TOK, TOK)).T
    s["gcross"][...] = jnp.zeros((16, 8, PAIR), F32)

    first_loads[0].wait()
    for b in range(8):
        cols = slice(b * TOK, (b + 1) * TOK)
        s["hid_t"][cols, :] = s["hid"][:, cols].astype(F32).T
    pl.semaphore_wait(barrier, len(peers))
    gathers = (("batch", y, s["hy"]), ("z", z, s["hz"]))
    hops = []
    for axis, index, buf in gathers:
        for d in (1, 3):
            hops.append(remote(s["hid_t"], buf.at[index, c], {axis: ring(index, d)}))
    down = [remote(s["hid_t"], buf.at[index, c], sib) for _, index, buf in gathers]

    first_loads[1].wait()
    first_loads[2].wait()

    def project(step, carry):
        weight_load(wk_hbm, "wk", step, 8).wait()
        weight_load(wv_hbm, "wv", step, 16).wait()
        wide = rows_of(step * 256, 256)
        hid = s["hid"][...]
        keys = dot(hid, s["wk"][:, wide], NN).astype(BF16)
        values = dot(hid, s["wv"][:, wide], NN).astype(BF16)
        segc = s["segc"][...]
        half = step // 4
        for p in range(2):
            pair = 2 * step + p
            k, v = keys[:, p * PAIR : (p + 1) * PAIR], values[:, p * PAIR : (p + 1) * PAIR]
            s["k"][pair] = k
            s["v"][pair] = v
            cum = s["cumx"][pair]
            total = cum[TOK - 1 : TOK, :]
            last_w = jnp.where(segc == segc[TOK - 1 : TOK, :], jnp.exp(total - cum), 0.0)
            first_w = jnp.where(segc == segc[0:1, :], jnp.exp(cum), 0.0)
            s["lw"][pair] = last_w
            s["fw"][pair] = first_w
            cols = rows_of(pair * PAIR, PAIR)
            fwd = dot_left(k.astype(F32) * last_w, v, TN)
            rev = dot_left(s["q"][:, cols].astype(F32) * first_w, s["g"][:, cols], TN)
            pp = 2 * lax.rem(step, 4) + p
            s["st"][half, rows_of(pp * 64, 64), :] = jnp.where(low_half, fwd[:64], fwd[64:])
            s["st"][half, rows_of(512 + pp * 64, 64), :] = jnp.where(low_half, rev[:64], rev[64:])
            meta = jnp.where(
                row8 == 0,
                total,
                jnp.where(
                    row8 == 1, segc[0:1, :], jnp.where(row8 == 2, segc[TOK - 1 : TOK, :], 0.0)
                ),
            )
            s["st"][half, rows_of(1024 + pp * 8, 8), :] = meta
        return carry

    lax.fori_loop(0, 8, project, 0)

    def inner(pair, carry):
        cols = rows_of(pair * PAIR, PAIR)
        q, g = s["q"][:, cols], s["g"][:, cols]
        k, v = s["k"][pair], s["v"][pair]
        allowed = causal & (s["segc"][...] == seg_row)
        gap = jnp.bitwise_xor(rows_i, cols_i)
        strict = (rows_i < cols_i).astype(BF16)
        zero = jnp.zeros((TOK, PAIR), BF16)
        weighted, scored, queries, keys, grads, gate_rows, gain_rows = [], [], [], [], [], [], []
        for h in range(2):

            def own(a):
                return jnp.where(low, a, zero) if h == 0 else jnp.where(low, zero, a)

            qh, gh, kh = own(q), own(g), own(k)
            score = dot(qh, k, NT)
            dprob = dot(gh, v, NT)
            spread = s["cumx"][pair, :, 64 * h : 64 * h + 1] - s["cumr3"][pair, h : h + 1, :]
            decay = jnp.where(allowed, jnp.exp(jnp.where(allowed, spread, 0.0)), 0.0)
            ds = decay * score
            joint = ds * dprob
            head = 2 * pair + h
            level = jnp.full((TOK, TOK), gain_ref[0, head], F32)
            gain_rows.append(jnp.sum(jnp.where(gap == 0, joint, 0.0), axis=0, keepdims=True))
            for l in range(1, 8):
                above = gap >= 2 ** (l - 1)
                level = jnp.where(above, gain_ref[l, head], level)
                chosen = above & (gap < 2**l)
                gain_rows.append(jnp.sum(jnp.where(chosen, joint, 0.0), axis=0, keepdims=True))
            wd = level * decay * dprob
            weighted.append(wd.astype(BF16))
            scored.append((level * ds).astype(BF16))
            grid = (wd * score).astype(BF16)
            crossing = jnp.where(causal, dot(grid, strict, NN), 0.0)
            gate_rows.append(jnp.sum(crossing, axis=0, keepdims=True))
            queries.append(qh)
            keys.append(kh)
            grads.append(gh)
        s["qacc"][pair] = dot(
            jnp.concatenate(weighted, axis=1), jnp.concatenate(keys, axis=0), NN
        )
        s["kacc"][pair] = dot(
            jnp.concatenate(weighted, axis=0), jnp.concatenate(queries, axis=0), TN
        )
        s["vacc"][pair] = dot(jnp.concatenate(scored, axis=0), jnp.concatenate(grads, axis=0), TN)
        s["gate"][pair] = jnp.concatenate([*gate_rows, jnp.zeros((6, TOK), F32)], axis=0)
        s["gint"][pair] = jnp.concatenate(gain_rows, axis=0)
        return carry

    both, st = s["both"], s["st"]
    swap = remote(st.at[1 - c], both.at[c], sib)
    both[pl.ds(c, 1)] = st[pl.ds(c, 1)]
    lax.fori_loop(0, 2, inner, 0)
    swap.wait()

    def meta_rows(total, first, last):
        return jnp.where(
            row8 == 0, total, jnp.where(row8 == 1, first, jnp.where(row8 == 2, last, 0.0))
        )

    chip_send, chip_recv = s["chip_send"], s["chip_recv"]
    for pp in range(8):
        f0 = both[0, pp * 64 : pp * 64 + 64, :]
        f1 = both[1, pp * 64 : pp * 64 + 64, :]
        r0 = both[0, 512 + pp * 64 : 576 + pp * 64, :]
        r1 = both[1, 512 + pp * 64 : 576 + pp * 64, :]
        m0 = both[0, 1024 + pp * 8 : 1032 + pp * 8, :]
        m1 = both[1, 1024 + pp * 8 : 1032 + pp * 8, :]
        t0, first0, last0 = m0[0:1], m0[1:2], m0[2:3]
        t1, first1, last1 = m1[0:1], m1[1:2], m1[2:3]
        n, p = pp // 2, pp % 2
        chip_send[n, p * 64 : p * 64 + 64, :] = f1 + linked(last0, last1, t1) * f0
        chip_send[n, 128 + p * 64 : 192 + p * 64, :] = r0 + linked(first0, first1, t0) * r1
        chip_send[n, 256 + p * 8 : 264 + p * 8, :] = meta_rows(t0 + t1, first0, last1)
        d8 = same(last0, first1) * jnp.sum(f0 * r1, axis=0, keepdims=True)
        s["gcross"][pl.ds(c * 8 + pp, 1)] = jnp.where(row8 == 0, d8, 0.0)[None]

    xs = []
    for d in (1, 2, 3):
        to = ring(x, d)
        xs.append(remote(chip_send.at[to], chip_recv.at[x], {"x": to}))
    chip_recv[pl.ds(x, 1)] = chip_send[pl.ds(x, 1)]

    def forward(n):
        axis, index, buf = gathers[n]
        out = []
        for m, d in enumerate((1, 3)):
            hops[2 * n + m].wait()
            came = ring(index, 4 - d)
            part = slice(0, 512) if d == 1 else slice(512, 1024)
            out.append(
                remote(buf.at[came, c, part], buf.at[came, c, part], {axis: ring(index, d)})
            )
            down.append(remote(buf.at[came, c], buf.at[came, c], sib))
        return out

    fwd_y = forward(0)
    lax.fori_loop(2, 8, inner, 0)
    wait(xs)

    def chip(j, p):
        return (
            chip_recv[j, p * 64 : p * 64 + 64, :],
            chip_recv[j, 128 + p * 64 : 192 + p * 64, :],
            chip_recv[j, 256 + p * 8 : 257 + p * 8, :],
            chip_recv[j, 257 + p * 8 : 258 + p * 8, :],
            chip_recv[j, 258 + p * 8 : 259 + p * 8, :],
        )

    def joined(p):
        (f0, r0, t0, a0, l0), (f1, r1, t1, a1, l1), (f2, r2, t2, a2, l2), (f3, r3, t3, a3, l3) = (
            chip(j, p) for j in range(4)
        )
        f01 = f1 + linked(l0, l1, t1) * f0
        r01 = r0 + linked(a0, a1, t0) * r1
        f23 = f3 + linked(l2, l3, t3) * f2
        r23 = r2 + linked(a2, a3, t2) * r3
        return f01, r01, f23, r23

    tot_send, tot_recv = s["tot_send"], s["tot_recv"]
    for p in range(2):
        f01, r01, f23, r23 = joined(p)
        t0, a0 = chip(0, p)[2:4]
        t1, l1 = chip(1, p)[2], chip(1, p)[4]
        t2, a2 = chip(2, p)[2:4]
        t3, l3 = chip(3, p)[2], chip(3, p)[4]
        tot_send[0, p * 64 : p * 64 + 64, :] = f23 + linked(l1, l3, t2 + t3) * f01
        tot_send[1, p * 64 : p * 64 + 64, :] = r01 + linked(a0, a2, t0 + t1) * r23
        tot_send[0, 128 + p * 8 : 136 + p * 8, :] = jnp.broadcast_to(l3, (8, PAIR))
        tot_send[1, 128 + p * 8 : 136 + p * 8, :] = jnp.broadcast_to(a0, (8, PAIR))
    zs = [
        remote(tot_send.at[n], tot_recv.at[n], {"z": ring(z, d)}) for n, d in ((0, 1), (1, 3))
    ]
    fwd_z = forward(1)
    lax.fori_loop(8, 10, inner, 0)
    wait(zs)

    has_prev = (z > 0).astype(F32)
    has_next = (z < 3).astype(F32)
    prev_top = (z == 2).astype(F32)
    next_top = (z == 1).astype(F32)
    back_send, back_recv = s["back_send"], s["back_recv"]

    def gain_row(pair, level):
        return jnp.where(low_row, gain_ref[level, 2 * pair], gain_ref[level, 2 * pair + 1])

    for p in range(2):
        (f0, r0, t0, a0, l0), (f1, r1, t1, a1, l1), (f2, r2, t2, a2, l2), (f3, r3, t3, a3, l3) = (
            chip(j, p) for j in range(4)
        )
        f01, r01, f23, r23 = joined(p)
        pair = c * 8 + 2 * x + p
        g9, g10, g11, g12 = (gain_row(pair, level) for level in range(9, 13))
        zf = has_prev * tot_recv[0, p * 64 : p * 64 + 64, :]
        zl = tot_recv[0, 128 + p * 8 : 129 + p * 8, :]
        zr = has_next * tot_recv[1, p * 64 : p * 64 + 64, :]
        za = tot_recv[1, 128 + p * 8 : 129 + p * 8, :]
        gzf = g11 * (1.0 - prev_top) + g12 * prev_top
        gzr = g11 * (1.0 - next_top) + g12 * next_top
        sf = (
            gzf * same(zl, a0) * zf,
            gzf * linked(zl, a1, t0) * zf + g9 * same(l0, a1) * f0,
            gzf * linked(zl, a2, t0 + t1) * zf + g10 * same(l1, a2) * f01,
            gzf * linked(zl, a3, t0 + t1 + t2) * zf
            + g10 * linked(l1, a3, t2) * f01
            + g9 * same(l2, a3) * f2,
        )
        sr = (
            gzr * linked(za, l0, t1 + t2 + t3) * zr
            + g10 * linked(l0, a2, t1) * r23
            + g9 * same(l0, a1) * r1,
            gzr * linked(za, l1, t2 + t3) * zr + g10 * same(l1, a2) * r23,
            gzr * linked(za, l2, t3) * zr + g9 * same(l2, a3) * r3,
            gzr * same(za, l3) * zr,
        )
        for j in range(4):
            back_send[j, p * 64 : p * 64 + 64, :] = sf[j]
            back_send[j, 128 + p * 64 : 192 + p * 64, :] = sr[j]
    bs = []
    for d in (1, 2, 3):
        to = ring(x, d)
        bs.append(remote(back_send.at[to], back_recv.at[x], {"x": to}))
    back_recv[pl.ds(x, 1)] = back_send[pl.ds(x, 1)]

    for p in range(2):
        (f0, r0, t0, a0, l0), (f1, r1, t1, a1, l1), (f2, r2, t2, a2, l2), (f3, r3, t3, a3, l3) = (
            chip(j, p) for j in range(4)
        )
        f01, r01, f23, r23 = joined(p)
        zf = has_prev * tot_recv[0, p * 64 : p * 64 + 64, :]
        zl = tot_recv[0, 128 + p * 8 : 129 + p * 8, :]
        r_group = r01 + linked(a0, a2, t0 + t1) * r23
        d9 = same(l0, a1) * jnp.sum(f0 * r1, axis=0, keepdims=True) + same(l2, a3) * jnp.sum(
            f2 * r3, axis=0, keepdims=True
        )
        d10 = same(l1, a2) * jnp.sum(f01 * r23, axis=0, keepdims=True)
        dz = same(zl, a0) * jnp.sum(zf * r_group, axis=0, keepdims=True)
        rows = jnp.where(
            row8 == 1,
            d9,
            jnp.where(
                row8 == 2,
                d10,
                jnp.where(
                    row8 == 3, (1.0 - prev_top) * dz, jnp.where(row8 == 4, prev_top * dz, 0.0)
                ),
            ),
        )
        pair = c * 8 + 2 * x + p
        s["gcross"][pl.ds(pair, 1)] = s["gcross"][pl.ds(pair, 1)] + rows[None]
    lax.fori_loop(10, 16, inner, 0)
    wait(bs)

    own_blocks, s_in = s["own_blocks"], s["s_in"]
    for pp in range(8):
        n, p = pp // 2, pp % 2
        f0 = both[0, pp * 64 : pp * 64 + 64, :]
        r1 = both[1, 512 + pp * 64 : 576 + pp * 64, :]
        m0 = both[0, 1024 + pp * 8 : 1032 + pp * 8, :]
        m1 = both[1, 1024 + pp * 8 : 1032 + pp * 8, :]
        t0, first0, last0 = m0[0:1], m0[1:2], m0[2:3]
        t1, first1, last1 = m1[0:1], m1[1:2], m1[2:3]
        sf = back_recv[n, p * 64 : p * 64 + 64, :]
        sr = back_recv[n, 128 + p * 64 : 192 + p * 64, :]
        link = gain_row(c * 8 + pp, 8) * same(last0, first1)
        own_blocks[0, pp * 64 : pp * 64 + 64, :] = sf
        own_blocks[1, pp * 64 : pp * 64 + 64, :] = linked(first0, first1, t0) * sf + link * f0
        own_blocks[0, 512 + pp * 64 : 576 + pp * 64, :] = linked(last0, last1, t1) * sr + link * r1
        own_blocks[1, 512 + pp * 64 : 576 + pp * 64, :] = sr
    swap = remote(own_blocks.at[1 - c], s_in.at[c], sib)
    s_in[pl.ds(c, 1)] = own_blocks[pl.ds(c, 1)]

    for (_, index, buf), copies in zip(gathers, (fwd_y, fwd_z)):
        buf[pl.ds(index, 1), pl.ds(c, 1)] = s["hid_t"][...][None, None]
        wait(copies)
        came = ring(index, 2)
        down.append(remote(buf.at[came, c], buf.at[came, c], sib))
    swap.wait()

    tail = causal.astype(BF16)
    head_pick = (cols_i[0:8, :] // 64 == row8).astype(BF16)

    def cross(pair, carry):
        half, pp = pair // 8, lax.rem(pair, 8)
        cols = rows_of(pair * PAIR, PAIR)
        q, g = s["q"][:, cols], s["g"][:, cols]
        k, v = s["k"][pair], s["v"][pair]
        first_w, last_w = s["fw"][pair], s["lw"][pair]
        sf = s_in[half, rows_of(pp * 64, 64), :]
        sr = s_in[half, rows_of(512 + pp * 64, 64), :]

        def diag(a):
            return jnp.concatenate([jnp.where(low_half, a, 0.0), jnp.where(low_half, 0.0, a)], axis=0)

        sg = first_w * dot_right(g, diag(sf), NT)
        rv = last_w * dot_right(v, diag(sr), NT)
        rk = last_w * dot_right(k, diag(sr), NN)
        diff = q.astype(F32) * sg - k.astype(F32) * rv
        hi, lo = split2(diff)
        diff_rows = dot(head_pick, hi, NT) + dot(head_pick, lo, NT)
        s["gate"][pair] = s["gate"][pair] + dot_left(diff_rows, tail, NN)
        qg_ref[:, cols] = (s["qacc"][pair] + sg).astype(BF16)
        key_sum = (s["kacc"][pair] + rv).astype(BF16)
        value_sum = (s["vacc"][pair] + rk).astype(BF16)
        s["ksb"][:, cols] = key_sum
        s["vsb"][:, cols] = value_sum
        s["ks"][half, pp] = key_sum.astype(F32)
        s["vs"][half, pp] = value_sum.astype(F32)
        return carry

    firsts = []
    me_y, me_z = 2 * y + c, 2 * z + c
    for n in range(2):
        lax.fori_loop(8 * n, 8 * n + 8, cross, 0)
        fk, fv = [], []
        for d, e in offsets:
            dev, to = plane("batch", y, d, e)
            fk.append(remote(s["ks"].at[n, to], s["rk"].at[n, me_y], dev))
            dev, to = plane("z", z, d, e)
            fv.append(remote(s["vs"].at[n, to], s["rv"].at[n, me_z], dev))
        s["rk"][n, pl.ds(me_y, 1)] = s["ks"][n, pl.ds(me_y, 1)]
        s["rv"][n, pl.ds(me_z, 1)] = s["vs"][n, pl.ds(me_z, 1)]
        firsts.append((fk, fv))

    ones = jnp.ones((8, PAIR), F32)
    inner_sum = dot_exact(ones, s["gint"][...].reshape(256, PAIR), NT)
    pick = (cols_i[0:8, :] // 64 == row8 - 2).astype(F32)
    outer_sum = dot_exact(pick, s["gcross"][...].reshape(128, PAIR), NT)
    start = (cols_i[0:8, :] == 0).astype(F32)
    own_total = dot_exact(start, s["gate"][...].reshape(128, TOK), NT)
    small, m1, m1s, m2, m2s, m3 = (s[n] for n in ("small", "m1", "m1s", "m2", "m2s", "m3"))
    small[0:8, :] = jnp.where(
        row8 == 0, inner_sum[:, :128], jnp.where(row8 == 1, inner_sum[:, 128:], outer_sum)
    )
    small[8:16, :] = own_total
    smalls = []
    for d, e in offsets:
        smalls.append(remote(small, m1.at[me_z], plane("z", z, d, e)[0]))
    m1[pl.ds(me_z, 1)] = small[...][None]

    wait(down)
    for name, out in (("hy", "hyb"), ("hz", "hzb")):
        for g in range(8):
            s[out][:, g * TOK : (g + 1) * TOK] = s[name][g // 2, g % 2].astype(BF16)

    def product(left, right, n):
        right = s[right][n].reshape(8 * TOK, PAIR).astype(BF16)
        for b in range(4):
            yield b, dot(s[left][b * 256 : (b + 1) * 256, :], right, NN)

    part1, recv1, part2, recv2 = s["part1"], s["recv1"], s["part2"], s["recv2"]

    def scatter(part, recv, chunk, axis, index):
        out = []
        for d in (1, 2, 3):
            to = ring(index, d)
            out.append(remote(part.at[chunk, to], recv.at[chunk, index], {axis: to}))
        recv[chunk, pl.ds(index, 1)] = part[chunk, pl.ds(index, 1)]
        return out

    wait(firsts[0][0])
    for b, block in product("hyb", "rk", 0):
        for j in range(4):
            part1[0, j, b * 64 : b * 64 + 64, :] = block[j * 64 : j * 64 + 64, :]
    k0 = scatter(part1, recv1, 0, "x", x)
    wait(firsts[0][1])
    for b, block in product("hzb", "rv", 0):
        for j in range(4):
            part1[2, j, b * 64 : b * 64 + 64, :] = block[j * 64 : j * 64 + 64, :]
    v0 = scatter(part1, recv1, 2, "x", x)

    def input_grad(n, carry):
        rows = rows_of(n * 256, 256)
        ig_ref[:, rows] = (
            dot(s["ksb"][...], s["wk"][rows, :], NT) + dot(s["vsb"][...], s["wv"][rows, :], NT)
        ).astype(BF16)
        return carry

    lax.fori_loop(0, 2, input_grad, 0)

    wait(firsts[1][0])
    for b, block in product("hyb", "rk", 1):
        part1[1, b] = block
    k1 = scatter(part1, recv1, 1, "z", z)
    wait(firsts[1][1])
    for b, block in product("hzb", "rv", 1):
        for j in range(8):
            for i in range(4):
                at = j * 32 + i * 8
                part1[3, i, b * 64 + j * 8 : b * 64 + j * 8 + 8, :] = block[at : at + 8, :]
    v1 = scatter(part1, recv1, 3, "batch", y)
    lax.fori_loop(2, 4, input_grad, 0)

    wait(smalls)
    total = m1[0, 0:8, :]
    for g in range(1, 8):
        total = total + m1[g, 0:8, :]
    m1s[0:8, :] = total
    for g in range(8):
        m1s[8 + g : 9 + g, :] = m1[g, 8:9, :]
    smalls = [remote(m1s, m2.at[x], {"x": ring(x, d)}) for d in (1, 2, 3)]
    m2[pl.ds(x, 1)] = m1s[...][None]

    def summed(recv, chunk):
        return recv[chunk, 0] + recv[chunk, 1] + recv[chunk, 2] + recv[chunk, 3]

    wait(k0)
    total = summed(recv1, 0)
    for j in range(4):
        part2[0, j] = total[j * 64 : j * 64 + 64, :]
    k0 = scatter(part2, recv2, 0, "z", z)
    wait(v0)
    total = summed(recv1, 2)
    for j in range(8):
        for i in range(4):
            at = j * 32 + i * 8
            part2[2, i, j * 8 : j * 8 + 8, :] = total[at : at + 8, :]
    v0 = scatter(part2, recv2, 2, "batch", y)
    wait(k1)
    total = summed(recv1, 1)
    for j in range(4):
        part2[1, j] = total[j * 64 : j * 64 + 64, :]
    k1 = scatter(part2, recv2, 1, "x", x)
    wait(v1)
    total = summed(recv1, 3)
    for j in range(4):
        for i in range(4):
            at = j * 64 + i * 16
            part2[3, i, j * 16 : j * 16 + 16, :] = total[at : at + 16, :]
    v1 = scatter(part2, recv2, 3, "x", x)

    wait(smalls)
    total = m2[0, 0:8, :] + m2[1, 0:8, :] + m2[2, 0:8, :] + m2[3, 0:8, :]
    m2s[...] = total
    smalls = [remote(m2s, m3.at[y], {"batch": ring(y, d)}) for d in (1, 2, 3)]
    m3[pl.ds(y, 1)] = total[None]
    place = z * 8 + x * 2 + c
    later = jnp.zeros((1, PAIR), F32)
    for j in range(4):
        for g in range(8):
            spot = (g // 2) * 8 + j * 2 + g % 2
            later = later + (place < spot).astype(F32) * m2[j, 8 + g : 9 + g, :]
    sout_ref[8:16, :] = jnp.broadcast_to(later, (8, PAIR))
    gate_ref[...] = s["gate"][...]

    fins = []
    wait(k0)
    wait(k1)
    for n in range(2):
        total = summed(recv2, n)
        for i in range(4):
            for j in range(2):
                at = j * 32 + i * 8
                s["kown"][2 * i + j, n] = total[at : at + 8, :]
    for d, e in offsets:
        dev, to = plane("batch", y, d, e)
        fins.append(remote(s["kown"].at[to], s["kfin"].at[me_y], dev))
    s["kfin"][pl.ds(me_y, 1)] = s["kown"][pl.ds(me_y, 1)]
    wait(v0)
    wait(v1)
    for n in range(2):
        total = summed(recv2, 2 + n)
        for j in range(8):
            s["vown"][j, n] = total[j * 8 : j * 8 + 8, :]
    for d, e in offsets:
        dev, to = plane("z", z, d, e)
        fins.append(remote(s["vown"].at[to], s["vfin"].at[me_z], dev))
    s["vfin"][pl.ds(me_z, 1)] = s["vown"][pl.ds(me_z, 1)]
    wait(smalls)
    sout_ref[0:8, :] = m3[0] + m3[1] + m3[2] + m3[3]
    wait(fins)
    for n in range(2):
        for g in range(8):
            cols = slice(n * 1024 + g * PAIR, n * 1024 + (g + 1) * PAIR)
            kout_ref[:, cols] = s["kfin"][g, n]
            vout_ref[:, cols] = s["vfin"][g, n]


def whole_step(hidden, queries, out_grad, w_key, w_value, log_gate, seg_row, level_gain):
    vm = pl.BlockSpec(memory_space=pltpu.VMEM)
    far = pl.BlockSpec(memory_space=pl.ANY)
    return pl.pallas_call(
        step_kernel,
        in_specs=[far] * 5 + [vm, vm, pl.BlockSpec(memory_space=pltpu.SMEM)],
        out_specs=[vm] * 6,
        out_shape=[
            jax.ShapeDtypeStruct((TOK, 2048), BF16),
            jax.ShapeDtypeStruct((TOK, 1024), BF16),
            jax.ShapeDtypeStruct((16, 8, TOK), F32),
            jax.ShapeDtypeStruct((8, 2048), F32),
            jax.ShapeDtypeStruct((8, 2048), F32),
            jax.ShapeDtypeStruct((16, PAIR), F32),
        ],
        scratch_shapes=list(scratch().values()),
        compiler_params=pltpu.CompilerParams(
            collective_id=0, has_side_effects=True, vmem_limit_bytes=VMEM_LIMIT
        ),
        name="whole_step",
    )(hidden, queries, out_grad, w_key, w_value, log_gate, seg_row, level_gain)


def finish_kernel(
    qg_ref, ig_ref, gate_ref, kw_ref, vw_ref, small_ref, qg, ig, gate, kw, vw, gains
):
    qg[...] = qg_ref[...]
    ig[...] = ig_ref[...]
    kw[...] = kw_ref[...]
    vw[...] = vw_ref[...]
    heads = gate.shape[0]
    lane = iota((heads, PAIR), 1)
    head = iota((heads, PAIR), 0)
    small = small_ref[...]
    later = jnp.broadcast_to(small[8:9, :], (TOK, TOK)).T
    rows = gate_ref[...].reshape(TOK, TOK) + later
    gate[...] = dot_exact((lane == (head // 2) * 8 + head % 2).astype(F32), rows, NN)
    levels = gains.shape[0]
    level, at = iota((levels, PAIR), 0), iota((levels, PAIR), 1) % 8
    first = (level == at).astype(F32)
    second = (level == at + 8).astype(F32)
    pick0 = jnp.where(lane // 8 == head, small[0:1, :], 0.0)
    pick1 = jnp.where(lane // 8 + 16 == head, small[1:2, :], 0.0)
    pair = jnp.where(head % 2 == 0, small[2:3, :], small[3:4, :])
    pick2 = jnp.where(lane // 8 == head // 2, pair, 0.0)
    gains[...] = dot_exact(first, pick0 + pick1, NT) + dot_exact(second, pick2, NT)


def finish(query_grad, input_grad, gate, key_weight, value_weight, small, heads, levels):
    vm = pl.BlockSpec(memory_space=pltpu.VMEM)
    outs = [
        jax.ShapeDtypeStruct(a.shape, a.dtype)
        for a in (query_grad, input_grad)
    ]
    outs.append(jax.ShapeDtypeStruct((heads, TOK), F32))
    outs += [jax.ShapeDtypeStruct(a.shape, a.dtype) for a in (key_weight, value_weight)]
    outs.append(jax.ShapeDtypeStruct((levels, heads), F32))
    return pl.pallas_call(
        finish_kernel,
        in_specs=[vm] * 6,
        out_specs=[vm] * 6,
        out_shape=outs,
        name="finish",
    )(query_grad, input_grad, gate, key_weight, value_weight, small)


def local(hidden, queries, w_key, w_value, log_gate, level_gain, segment_ids, out_grad):
    heads, levels = level_gain.shape
    parts = whole_step(
        hidden[0], queries[0], out_grad[0], w_key, w_value, log_gate[0], segment_ids, level_gain.T
    )
    query_grad, input_grad, gate_grad, key_weight, value_weight, gains = finish(
        *parts, heads, levels
    )
    return (
        query_grad[None],
        input_grad[None],
        gate_grad[None],
        key_weight,
        value_weight,
        gains.T,
    )


def solution(mesh):
    split = Mesh(
        mesh.devices.reshape(4, 4, 2, mesh.shape["batch"]), ("z", "x", "core", "batch")
    )
    return jax.shard_map(
        local,
        mesh=split,
        in_specs=(
            P("batch", SEQ, None),
            P("batch", SEQ, None),
            P(),
            P(),
            P("batch", None, SEQ),
            P(),
            P("batch", SEQ),
            P("batch", SEQ, None),
        ),
        out_specs=(
            P("batch", SEQ, None),
            P("batch", SEQ, None),
            P("batch", None, SEQ),
            P(SEQ_BATCH, None),
            P(SEQ_BATCH, None),
            P(),
        ),
        check_vma=False,
    )
```

```python
import functools

import jax
import jax.numpy as jnp
from jax import lax
from jax.experimental import pallas as pl
from jax.experimental.pallas import tpu as pltpu
from jax.sharding import Mesh
from jax.sharding import PartitionSpec as P

SEQ = ("z", "x", "core")
SEQ_BATCH = ("z", "x", "core", "batch")
MESH = pl.DeviceIdType.MESH
HIGHEST = lax.Precision.HIGHEST
F32 = jnp.float32
BF16 = jnp.bfloat16

NT = (((1,), (1,)), ((), ()))
TN = (((0,), (0,)), ((), ()))
NN = (((1,), (0,)), ((), ()))

TOK = 128
PAIR = 128
HALF_ROWS = 1088


def dot(a, b, dims):
    return lax.dot_general(a, b, dims, preferred_element_type=F32)


def dot_exact(a, b, dims):
    return lax.dot_general(a, b, dims, preferred_element_type=F32, precision=HIGHEST)


def split2(x):
    hi = x.astype(BF16)
    return hi, (x - hi.astype(F32)).astype(BF16)


def dot_left(a, b, dims):
    hi, lo = split2(a)
    return dot(hi, b, dims) + dot(lo, b, dims)


def dot_right(a, b, dims):
    hi, lo = split2(b)
    return dot(a, hi, dims) + dot(a, lo, dims)


def iota(shape, dim):
    return lax.broadcasted_iota(jnp.int32, shape, dim)


def entry_signal(peers):
    barrier = pltpu.get_barrier_semaphore()
    for peer in peers:
        pl.semaphore_signal(barrier, inc=1, device_id=peer, device_id_type=MESH)
    return barrier


def ring(index, step):
    return lax.rem(index + step, 4)


def same(a, b):
    return jnp.where(a == b, 1.0, 0.0)


def linked(a, b, total):
    return jnp.where(a == b, jnp.exp(total), 0.0)


def rows_of(start, size):
    return pl.ds(pl.multiple_of(start, size), size)


SENDS = 128
LOCALS = 24
VMEM_LIMIT = 56 * 2**20


def scratch():
    def f(*shape):
        return pltpu.VMEM(shape, F32)

    def b(*shape):
        return pltpu.VMEM(shape, BF16)

    return dict(
        wk=b(1024, 2048),
        wv=b(1024, 2048),
        hid=b(TOK, 1024),
        q=b(TOK, 2048),
        g=b(TOK, 2048),
        k=b(16, TOK, PAIR),
        v=b(16, TOK, PAIR),
        hid_t=f(1024, TOK),
        cumx=f(16, TOK, PAIR),
        cumr=f(32, TOK),
        cumr3=f(16, 8, TOK),
        fw=f(16, TOK, PAIR),
        lw=f(16, TOK, PAIR),
        segc=f(TOK, TOK),
        st=f(2, HALF_ROWS, PAIR),
        both=f(2, HALF_ROWS, PAIR),
        chip_send=f(2, 4, 136, PAIR),
        chip_recv=f(2, 4, 136, PAIR),
        tot_send=f(2, 2, 72, PAIR),
        tot_recv=f(2, 2, 72, PAIR),
        back_send=f(2, 4, 128, PAIR),
        back_recv=f(2, 4, 128, PAIR),
        own_blocks=f(2, 2, 512, PAIR),
        s_in=f(2, 2, 512, PAIR),
        gcross=f(16, 8, PAIR),
        gint=f(16, 16, PAIR),
        gate=f(16, 8, TOK),
        hy=f(4, 2, 1024, TOK),
        hz=f(4, 2, 1024, TOK),
        hyb=b(1024, 8 * TOK),
        hzb=b(1024, 8 * TOK),
        qacc=f(16, TOK, PAIR),
        kacc=f(16, TOK, PAIR),
        vacc=f(16, TOK, PAIR),
        ks=f(2, 8, TOK, PAIR),
        vs=f(2, 8, TOK, PAIR),
        ksb=b(TOK, 2048),
        vsb=b(TOK, 2048),
        rk=f(2, 8, TOK, PAIR),
        rv=f(2, 8, TOK, PAIR),
        part1=f(4, 4, 256, PAIR),
        recv1=f(4, 4, 256, PAIR),
        part2=f(4, 4, 64, PAIR),
        recv2=f(4, 4, 64, PAIR),
        kown=f(8, 2, 8, PAIR),
        vown=f(8, 2, 8, PAIR),
        kfin=f(8, 2, 8, PAIR),
        vfin=f(8, 2, 8, PAIR),
        small=f(16, PAIR),
        m1=f(8, 16, PAIR),
        m1s=f(16, PAIR),
        m2=f(4, 16, PAIR),
        m2s=f(8, PAIR),
        m3=f(4, 8, PAIR),
        send_sem=pltpu.SemaphoreType.DMA((SENDS,)),
        recv_sem=pltpu.SemaphoreType.DMA((SENDS,)),
        local_sem=pltpu.SemaphoreType.DMA((LOCALS,)),
    )


def step_kernel(
    hid_hbm,
    q_hbm,
    g_hbm,
    wk_hbm,
    wv_hbm,
    lg_ref,
    segr_ref,
    gain_ref,
    qg_ref,
    ig_ref,
    gate_ref,
    kout_ref,
    vout_ref,
    sout_ref,
    *refs,
):
    s = dict(zip(scratch(), refs))
    x, y, z, c = (lax.axis_index(a) for a in ("x", "batch", "z", "core"))
    used = [0]

    def remote(src, dst, target):
        n = used[0]
        used[0] += 1
        cp = pltpu.make_async_remote_copy(
            src_ref=src,
            dst_ref=dst,
            send_sem=s["send_sem"].at[n],
            recv_sem=s["recv_sem"].at[n],
            device_id=target,
            device_id_type=MESH,
        )
        cp.start()
        return cp

    def wait(copies):
        for cp in copies:
            cp.wait()

    sib = {"core": 1 - c}
    offsets = [(d, e) for d in range(4) for e in (0, 1) if d or e]

    def plane(axis, index, d, e):
        to, tc = ring(index, d), lax.rem(c + e, 2)
        return {axis: to, "core": tc}, 2 * to + tc

    peers = [plane("batch", y, d, e)[0] for d, e in offsets]
    peers += [plane("z", z, d, e)[0] for d, e in offsets if d]
    peers += [{"x": ring(x, d)} for d in (1, 2, 3)]
    barrier = entry_signal(peers)

    local_sem = s["local_sem"]
    first_loads = [
        pltpu.make_async_copy(hid_hbm, s["hid"], local_sem.at[0]),
        pltpu.make_async_copy(q_hbm, s["q"], local_sem.at[1]),
        pltpu.make_async_copy(g_hbm, s["g"], local_sem.at[2]),
    ]

    def weight_load(hbm, name, i, base):
        cols = rows_of(i * 256, 256)
        return pltpu.make_async_copy(hbm.at[:, cols], s[name].at[:, cols], local_sem.at[base + i])

    first_loads[0].start()
    for i in range(8):
        weight_load(wk_hbm, "wk", i, 8).start()
        weight_load(wv_hbm, "wv", i, 16).start()
        if i == 0:
            first_loads[1].start()
            first_loads[2].start()

    rows_i, cols_i = iota((TOK, TOK), 0), iota((TOK, TOK), 1)
    causal = cols_i <= rows_i
    lower = causal.astype(F32)
    low = cols_i < 64
    low_half = iota((64, PAIR), 1) < 64
    row8 = iota((8, PAIR), 0)
    low_row = iota((1, PAIR), 1) < 64
    log_gate = lg_ref[...]
    cum_cols = dot_exact(lower, log_gate, NT)
    s["cumr"][...] = dot_exact(log_gate, lower, NT)
    for pair in range(16):
        s["cumx"][pair] = jnp.where(
            low, cum_cols[:, 2 * pair : 2 * pair + 1], cum_cols[:, 2 * pair + 1 : 2 * pair + 2]
        )
        s["cumr3"][pair, 0:2, :] = s["cumr"][2 * pair : 2 * pair + 2, :]
    seg_row = segr_ref[...].astype(F32)
    s["segc"][...] = jnp.broadcast_to(seg_row, (TOK, TOK)).T
    s["gcross"][...] = jnp.zeros((16, 8, PAIR), F32)

    first_loads[0].wait()
    for b in range(8):
        cols = slice(b * TOK, (b + 1) * TOK)
        s["hid_t"][cols, :] = s["hid"][:, cols].astype(F32).T
    pl.semaphore_wait(barrier, len(peers))
    gathers = (("batch", y, s["hy"]), ("z", z, s["hz"]))
    hops = []
    for axis, index, buf in gathers:
        for d in (1, 3):
            hops.append(remote(s["hid_t"], buf.at[index, c], {axis: ring(index, d)}))
    down = [remote(s["hid_t"], buf.at[index, c], sib) for _, index, buf in gathers]

    first_loads[1].wait()
    first_loads[2].wait()

    def project(step, carry):
        weight_load(wk_hbm, "wk", step, 8).wait()
        weight_load(wv_hbm, "wv", step, 16).wait()
        wide = rows_of(step * 256, 256)
        hid = s["hid"][...]
        keys = dot(hid, s["wk"][:, wide], NN).astype(BF16)
        values = dot(hid, s["wv"][:, wide], NN).astype(BF16)
        segc = s["segc"][...]
        half = step // 4
        for p in range(2):
            pair = 2 * step + p
            k, v = keys[:, p * PAIR : (p + 1) * PAIR], values[:, p * PAIR : (p + 1) * PAIR]
            s["k"][pair] = k
            s["v"][pair] = v
            cum = s["cumx"][pair]
            total = cum[TOK - 1 : TOK, :]
            last_w = jnp.where(segc == segc[TOK - 1 : TOK, :], jnp.exp(total - cum), 0.0)
            first_w = jnp.where(segc == segc[0:1, :], jnp.exp(cum), 0.0)
            s["lw"][pair] = last_w
            s["fw"][pair] = first_w
            cols = rows_of(pair * PAIR, PAIR)
            fwd = dot_left(k.astype(F32) * last_w, v, TN)
            rev = dot_left(s["q"][:, cols].astype(F32) * first_w, s["g"][:, cols], TN)
            pp = 2 * lax.rem(step, 4) + p
            s["st"][half, rows_of(pp * 64, 64), :] = jnp.where(low_half, fwd[:64], fwd[64:])
            s["st"][half, rows_of(512 + pp * 64, 64), :] = jnp.where(low_half, rev[:64], rev[64:])
            meta = jnp.where(
                row8 == 0,
                total,
                jnp.where(
                    row8 == 1, segc[0:1, :], jnp.where(row8 == 2, segc[TOK - 1 : TOK, :], 0.0)
                ),
            )
            s["st"][half, rows_of(1024 + pp * 8, 8), :] = meta
        return carry

    lax.fori_loop(0, 8, project, 0)

    def inner(pair, carry):
        cols = rows_of(pair * PAIR, PAIR)
        q, g = s["q"][:, cols], s["g"][:, cols]
        k, v = s["k"][pair], s["v"][pair]
        allowed = causal & (s["segc"][...] == seg_row)
        gap = jnp.bitwise_xor(rows_i, cols_i)
        strict = (rows_i < cols_i).astype(BF16)
        zero = jnp.zeros((TOK, PAIR), BF16)
        weighted, scored, queries, keys, grads, gate_rows, gain_rows = [], [], [], [], [], [], []
        for h in range(2):

            def own(a):
                return jnp.where(low, a, zero) if h == 0 else jnp.where(low, zero, a)

            qh, gh, kh = own(q), own(g), own(k)
            score = dot(qh, k, NT)
            dprob = dot(gh, v, NT)
            spread = s["cumx"][pair, :, 64 * h : 64 * h + 1] - s["cumr3"][pair, h : h + 1, :]
            decay = jnp.where(allowed, jnp.exp(jnp.where(allowed, spread, 0.0)), 0.0)
            ds = decay * score
            joint = ds * dprob
            head = 2 * pair + h
            level = jnp.full((TOK, TOK), gain_ref[0, head], F32)
            gain_rows.append(jnp.sum(jnp.where(gap == 0, joint, 0.0), axis=0, keepdims=True))
            for l in range(1, 8):
                above = gap >= 2 ** (l - 1)
                level = jnp.where(above, gain_ref[l, head], level)
                chosen = above & (gap < 2**l)
                gain_rows.append(jnp.sum(jnp.where(chosen, joint, 0.0), axis=0, keepdims=True))
            wd = level * decay * dprob
            weighted.append(wd.astype(BF16))
            scored.append((level * ds).astype(BF16))
            grid = (wd * score).astype(BF16)
            crossing = jnp.where(causal, dot(grid, strict, NN), 0.0)
            gate_rows.append(jnp.sum(crossing, axis=0, keepdims=True))
            queries.append(qh)
            keys.append(kh)
            grads.append(gh)
        s["qacc"][pair] = dot(
            jnp.concatenate(weighted, axis=1), jnp.concatenate(keys, axis=0), NN
        )
        s["kacc"][pair] = dot(
            jnp.concatenate(weighted, axis=0), jnp.concatenate(queries, axis=0), TN
        )
        s["vacc"][pair] = dot(jnp.concatenate(scored, axis=0), jnp.concatenate(grads, axis=0), TN)
        s["gate"][pair] = jnp.concatenate([*gate_rows, jnp.zeros((6, TOK), F32)], axis=0)
        s["gint"][pair] = jnp.concatenate(gain_rows, axis=0)
        return carry

    both, st = s["both"], s["st"]
    swap = remote(st.at[1 - c], both.at[c], sib)
    both[pl.ds(c, 1)] = st[pl.ds(c, 1)]
    lax.fori_loop(0, 1, inner, 0)
    swap.wait()

    def meta_rows(total, first, last):
        return jnp.where(
            row8 == 0, total, jnp.where(row8 == 1, first, jnp.where(row8 == 2, last, 0.0))
        )

    chip_send, chip_recv = s["chip_send"], s["chip_recv"]

    def block_pair(pp):
        f0 = both[0, pp * 64 : pp * 64 + 64, :]
        f1 = both[1, pp * 64 : pp * 64 + 64, :]
        r0 = both[0, 512 + pp * 64 : 576 + pp * 64, :]
        r1 = both[1, 512 + pp * 64 : 576 + pp * 64, :]
        m0 = both[0, 1024 + pp * 8 : 1032 + pp * 8, :]
        m1 = both[1, 1024 + pp * 8 : 1032 + pp * 8, :]
        return f0, f1, r0, r1, m0[0:1], m0[1:2], m0[2:3], m1[0:1], m1[1:2], m1[2:3]

    xs = []
    for p in range(2):
        for n in range(4):
            f0, f1, r0, r1, t0, first0, last0, t1, first1, last1 = block_pair(2 * n + p)
            chip_send[p, n, 0:64, :] = f1 + linked(last0, last1, t1) * f0
            chip_send[p, n, 64:128, :] = r0 + linked(first0, first1, t0) * r1
            chip_send[p, n, 128:136, :] = meta_rows(t0 + t1, first0, last1)
        copies = []
        for d in (1, 2, 3):
            to = ring(x, d)
            copies.append(remote(chip_send.at[p, to], chip_recv.at[p, x], {"x": to}))
        chip_recv[p, pl.ds(x, 1)] = chip_send[p, pl.ds(x, 1)]
        xs.append(copies)
    for pp in range(8):
        f0, _, _, r1, _, _, last0, _, first1, _ = block_pair(pp)
        d8 = same(last0, first1) * jnp.sum(f0 * r1, axis=0, keepdims=True)
        s["gcross"][pl.ds(c * 8 + pp, 1)] = jnp.where(row8 == 0, d8, 0.0)[None]
    lax.fori_loop(1, 7, inner, 0)

    def chip(j, p):
        return (
            chip_recv[p, j, 0:64, :],
            chip_recv[p, j, 64:128, :],
            chip_recv[p, j, 128:129, :],
            chip_recv[p, j, 129:130, :],
            chip_recv[p, j, 130:131, :],
        )

    def joined(p):
        (f0, r0, t0, a0, l0), (f1, r1, t1, a1, l1), (f2, r2, t2, a2, l2), (f3, r3, t3, a3, l3) = (
            chip(j, p) for j in range(4)
        )
        f01 = f1 + linked(l0, l1, t1) * f0
        r01 = r0 + linked(a0, a1, t0) * r1
        f23 = f3 + linked(l2, l3, t3) * f2
        r23 = r2 + linked(a2, a3, t2) * r3
        return f01, r01, f23, r23

    tot_send, tot_recv = s["tot_send"], s["tot_recv"]
    zs = []
    for p in range(2):
        wait(xs[p])
        f01, r01, f23, r23 = joined(p)
        t0, a0 = chip(0, p)[2:4]
        t1, l1 = chip(1, p)[2], chip(1, p)[4]
        t2, a2 = chip(2, p)[2:4]
        t3, l3 = chip(3, p)[2], chip(3, p)[4]
        tot_send[p, 0, 0:64, :] = f23 + linked(l1, l3, t2 + t3) * f01
        tot_send[p, 1, 0:64, :] = r01 + linked(a0, a2, t0 + t1) * r23
        tot_send[p, 0, 64:72, :] = jnp.broadcast_to(l3, (8, PAIR))
        tot_send[p, 1, 64:72, :] = jnp.broadcast_to(a0, (8, PAIR))
        zs.append(
            [
                remote(tot_send.at[p, n], tot_recv.at[p, n], {"z": ring(z, d)})
                for n, d in ((0, 1), (1, 3))
            ]
        )
    lax.fori_loop(7, 10, inner, 0)

    has_prev = (z > 0).astype(F32)
    has_next = (z < 3).astype(F32)
    prev_top = (z == 2).astype(F32)
    next_top = (z == 1).astype(F32)
    back_send, back_recv = s["back_send"], s["back_recv"]

    def gain_row(pair, level):
        return jnp.where(low_row, gain_ref[level, 2 * pair], gain_ref[level, 2 * pair + 1])

    bs = []
    for p in range(2):
        wait(zs[p])
        (f0, r0, t0, a0, l0), (f1, r1, t1, a1, l1), (f2, r2, t2, a2, l2), (f3, r3, t3, a3, l3) = (
            chip(j, p) for j in range(4)
        )
        f01, r01, f23, r23 = joined(p)
        pair = c * 8 + 2 * x + p
        g9, g10, g11, g12 = (gain_row(pair, level) for level in range(9, 13))
        zf = has_prev * tot_recv[p, 0, 0:64, :]
        zl = tot_recv[p, 0, 64:65, :]
        zr = has_next * tot_recv[p, 1, 0:64, :]
        za = tot_recv[p, 1, 64:65, :]
        gzf = g11 * (1.0 - prev_top) + g12 * prev_top
        gzr = g11 * (1.0 - next_top) + g12 * next_top
        sf = (
            gzf * same(zl, a0) * zf,
            gzf * linked(zl, a1, t0) * zf + g9 * same(l0, a1) * f0,
            gzf * linked(zl, a2, t0 + t1) * zf + g10 * same(l1, a2) * f01,
            gzf * linked(zl, a3, t0 + t1 + t2) * zf
            + g10 * linked(l1, a3, t2) * f01
            + g9 * same(l2, a3) * f2,
        )
        sr = (
            gzr * linked(za, l0, t1 + t2 + t3) * zr
            + g10 * linked(l0, a2, t1) * r23
            + g9 * same(l0, a1) * r1,
            gzr * linked(za, l1, t2 + t3) * zr + g10 * same(l1, a2) * r23,
            gzr * linked(za, l2, t3) * zr + g9 * same(l2, a3) * r3,
            gzr * same(za, l3) * zr,
        )
        for j in range(4):
            back_send[p, j, 0:64, :] = sf[j]
            back_send[p, j, 64:128, :] = sr[j]
        copies = []
        for d in (1, 2, 3):
            to = ring(x, d)
            copies.append(remote(back_send.at[p, to], back_recv.at[p, x], {"x": to}))
        back_recv[p, pl.ds(x, 1)] = back_send[p, pl.ds(x, 1)]
        bs.append(copies)

    fwd = []
    for n, (axis, index, buf) in enumerate(gathers):
        for m, d in enumerate((1, 3)):
            hops[2 * n + m].wait()
            came = ring(index, 4 - d)
            part = slice(0, 512) if d == 1 else slice(512, 1024)
            fwd.append(
                remote(buf.at[came, c, part], buf.at[came, c, part], {axis: ring(index, d)})
            )
            down.append(remote(buf.at[came, c], buf.at[came, c], sib))

    for p in range(2):
        (f0, r0, t0, a0, l0), (f1, r1, t1, a1, l1), (f2, r2, t2, a2, l2), (f3, r3, t3, a3, l3) = (
            chip(j, p) for j in range(4)
        )
        f01, r01, f23, r23 = joined(p)
        zf = has_prev * tot_recv[p, 0, 0:64, :]
        zl = tot_recv[p, 0, 64:65, :]
        r_group = r01 + linked(a0, a2, t0 + t1) * r23
        d9 = same(l0, a1) * jnp.sum(f0 * r1, axis=0, keepdims=True) + same(l2, a3) * jnp.sum(
            f2 * r3, axis=0, keepdims=True
        )
        d10 = same(l1, a2) * jnp.sum(f01 * r23, axis=0, keepdims=True)
        dz = same(zl, a0) * jnp.sum(zf * r_group, axis=0, keepdims=True)
        rows = jnp.where(
            row8 == 1,
            d9,
            jnp.where(
                row8 == 2,
                d10,
                jnp.where(
                    row8 == 3, (1.0 - prev_top) * dz, jnp.where(row8 == 4, prev_top * dz, 0.0)
                ),
            ),
        )
        pair = c * 8 + 2 * x + p
        s["gcross"][pl.ds(pair, 1)] = s["gcross"][pl.ds(pair, 1)] + rows[None]
    lax.fori_loop(10, 16, inner, 0)

    own_blocks, s_in = s["own_blocks"], s["s_in"]
    swaps = []
    for p in range(2):
        wait(bs[p])
        for n in range(4):
            pp = 2 * n + p
            f0, _, _, r1, t0, first0, last0, t1, first1, last1 = block_pair(pp)
            sf = back_recv[p, n, 0:64, :]
            sr = back_recv[p, n, 64:128, :]
            link = gain_row(c * 8 + pp, 8) * same(last0, first1)
            at = n * 128
            own_blocks[p, 0, at : at + 64, :] = sf
            own_blocks[p, 1, at : at + 64, :] = linked(first0, first1, t0) * sf + link * f0
            own_blocks[p, 0, at + 64 : at + 128, :] = linked(last0, last1, t1) * sr + link * r1
            own_blocks[p, 1, at + 64 : at + 128, :] = sr
        swaps.append(remote(own_blocks.at[p, 1 - c], s_in.at[p, c], sib))
        s_in[p, pl.ds(c, 1)] = own_blocks[p, pl.ds(c, 1)]

    tail = causal.astype(BF16)
    head_pick = (cols_i[0:8, :] // 64 == row8).astype(BF16)

    def cross(to, p):
        pair = 2 * to + p
        half, quarter = to // 4, lax.rem(to, 4)
        cols = rows_of(pair * PAIR, PAIR)
        q, g = s["q"][:, cols], s["g"][:, cols]
        k, v = s["k"][pair], s["v"][pair]
        first_w, last_w = s["fw"][pair], s["lw"][pair]
        sf = s_in[p, half, rows_of(quarter * 128, 64), :]
        sr = s_in[p, half, rows_of(quarter * 128 + 64, 64), :]

        def diag(a):
            return jnp.concatenate([jnp.where(low_half, a, 0.0), jnp.where(low_half, 0.0, a)], axis=0)

        sg = first_w * dot_right(g, diag(sf), NT)
        rv = last_w * dot_right(v, diag(sr), NT)
        rk = last_w * dot_right(k, diag(sr), NN)
        diff = q.astype(F32) * sg - k.astype(F32) * rv
        hi, lo = split2(diff)
        diff_rows = dot(head_pick, hi, NT) + dot(head_pick, lo, NT)
        s["gate"][pair] = s["gate"][pair] + dot_left(diff_rows, tail, NN)
        qg_ref[:, cols] = (s["qacc"][pair] + sg).astype(BF16)
        key_sum = (s["kacc"][pair] + rv).astype(BF16)
        value_sum = (s["vacc"][pair] + rk).astype(BF16)
        s["ksb"][:, cols] = key_sum
        s["vsb"][:, cols] = value_sum
        s["ks"][p, to] = key_sum.astype(F32)
        s["vs"][p, to] = value_sum.astype(F32)

    firsts = []
    me_y, me_z = 2 * y + c, 2 * z + c
    for n in range(2):
        swaps[n].wait()
        lax.fori_loop(0, 8, lambda to, carry: cross(to, n), None)
        fk, fv = [], []
        for d, e in offsets:
            dev, to = plane("batch", y, d, e)
            fk.append(remote(s["ks"].at[n, to], s["rk"].at[n, me_y], dev))
            dev, to = plane("z", z, d, e)
            fv.append(remote(s["vs"].at[n, to], s["rv"].at[n, me_z], dev))
        s["rk"][n, pl.ds(me_y, 1)] = s["ks"][n, pl.ds(me_y, 1)]
        s["rv"][n, pl.ds(me_z, 1)] = s["vs"][n, pl.ds(me_z, 1)]
        firsts.append((fk, fv))

    ones = jnp.ones((8, PAIR), F32)
    inner_sum = dot_exact(ones, s["gint"][...].reshape(256, PAIR), NT)
    pick = (cols_i[0:8, :] // 64 == row8 - 2).astype(F32)
    outer_sum = dot_exact(pick, s["gcross"][...].reshape(128, PAIR), NT)
    start = (cols_i[0:8, :] == 0).astype(F32)
    own_total = dot_exact(start, s["gate"][...].reshape(128, TOK), NT)
    small, m1, m1s, m2, m2s, m3 = (s[n] for n in ("small", "m1", "m1s", "m2", "m2s", "m3"))
    small[0:8, :] = jnp.where(
        row8 == 0, inner_sum[:, :128], jnp.where(row8 == 1, inner_sum[:, 128:], outer_sum)
    )
    small[8:16, :] = own_total
    smalls = []
    for d, e in offsets:
        smalls.append(remote(small, m1.at[me_z], plane("z", z, d, e)[0]))
    m1[pl.ds(me_z, 1)] = small[...][None]

    for n, (_, index, buf) in enumerate(gathers):
        buf[pl.ds(index, 1), pl.ds(c, 1)] = s["hid_t"][...][None, None]
        wait(fwd[2 * n : 2 * n + 2])
        came = ring(index, 2)
        down.append(remote(buf.at[came, c], buf.at[came, c], sib))
    wait(down)
    for name, out in (("hy", "hyb"), ("hz", "hzb")):
        for g in range(8):
            s[out][:, g * TOK : (g + 1) * TOK] = s[name][g // 2, g % 2].astype(BF16)

    def product(left, right, n):
        right = s[right][n].reshape(8 * TOK, PAIR).astype(BF16)
        for b in range(4):
            yield b, dot(s[left][b * 256 : (b + 1) * 256, :], right, NN)

    part1, recv1, part2, recv2 = s["part1"], s["recv1"], s["part2"], s["recv2"]

    def scatter(part, recv, chunk, axis, index):
        out = []
        for d in (1, 2, 3):
            to = ring(index, d)
            out.append(remote(part.at[chunk, to], recv.at[chunk, index], {axis: to}))
        recv[chunk, pl.ds(index, 1)] = part[chunk, pl.ds(index, 1)]
        return out

    wait(firsts[0][0])
    for b, block in product("hyb", "rk", 0):
        for j in range(4):
            part1[0, j, b * 64 : b * 64 + 64, :] = block[j * 64 : j * 64 + 64, :]
    k0 = scatter(part1, recv1, 0, "x", x)
    wait(firsts[0][1])
    for b, block in product("hzb", "rv", 0):
        for j in range(4):
            part1[2, j, b * 64 : b * 64 + 64, :] = block[j * 64 : j * 64 + 64, :]
    v0 = scatter(part1, recv1, 2, "x", x)

    def input_grad(n, carry):
        rows = rows_of(n * 256, 256)
        ig_ref[:, rows] = (
            dot(s["ksb"][...], s["wk"][rows, :], NT) + dot(s["vsb"][...], s["wv"][rows, :], NT)
        ).astype(BF16)
        return carry

    lax.fori_loop(0, 2, input_grad, 0)

    wait(firsts[1][0])
    for b, block in product("hyb", "rk", 1):
        part1[1, b] = block
    k1 = scatter(part1, recv1, 1, "z", z)
    wait(firsts[1][1])
    for b, block in product("hzb", "rv", 1):
        for j in range(8):
            for i in range(4):
                at = j * 32 + i * 8
                part1[3, i, b * 64 + j * 8 : b * 64 + j * 8 + 8, :] = block[at : at + 8, :]
    v1 = scatter(part1, recv1, 3, "batch", y)
    lax.fori_loop(2, 4, input_grad, 0)

    wait(smalls)
    total = m1[0, 0:8, :]
    for g in range(1, 8):
        total = total + m1[g, 0:8, :]
    m1s[0:8, :] = total
    for g in range(8):
        m1s[8 + g : 9 + g, :] = m1[g, 8:9, :]
    smalls = [remote(m1s, m2.at[x], {"x": ring(x, d)}) for d in (1, 2, 3)]
    m2[pl.ds(x, 1)] = m1s[...][None]

    def summed(recv, chunk):
        return recv[chunk, 0] + recv[chunk, 1] + recv[chunk, 2] + recv[chunk, 3]

    wait(k0)
    total = summed(recv1, 0)
    for j in range(4):
        part2[0, j] = total[j * 64 : j * 64 + 64, :]
    k0 = scatter(part2, recv2, 0, "z", z)
    wait(v0)
    total = summed(recv1, 2)
    for j in range(8):
        for i in range(4):
            at = j * 32 + i * 8
            part2[2, i, j * 8 : j * 8 + 8, :] = total[at : at + 8, :]
    v0 = scatter(part2, recv2, 2, "batch", y)
    wait(k1)
    total = summed(recv1, 1)
    for j in range(4):
        part2[1, j] = total[j * 64 : j * 64 + 64, :]
    k1 = scatter(part2, recv2, 1, "x", x)
    wait(v1)
    total = summed(recv1, 3)
    for j in range(4):
        for i in range(4):
            at = j * 64 + i * 16
            part2[3, i, j * 16 : j * 16 + 16, :] = total[at : at + 16, :]
    v1 = scatter(part2, recv2, 3, "x", x)

    wait(smalls)
    total = m2[0, 0:8, :] + m2[1, 0:8, :] + m2[2, 0:8, :] + m2[3, 0:8, :]
    m2s[...] = total
    smalls = [remote(m2s, m3.at[y], {"batch": ring(y, d)}) for d in (1, 2, 3)]
    m3[pl.ds(y, 1)] = total[None]
    place = z * 8 + x * 2 + c
    later = jnp.zeros((1, PAIR), F32)
    for j in range(4):
        for g in range(8):
            spot = (g // 2) * 8 + j * 2 + g % 2
            later = later + (place < spot).astype(F32) * m2[j, 8 + g : 9 + g, :]
    sout_ref[8:16, :] = jnp.broadcast_to(later, (8, PAIR))
    gate_ref[...] = s["gate"][...]

    fins = []
    wait(k0)
    wait(k1)
    for n in range(2):
        total = summed(recv2, n)
        for i in range(4):
            for j in range(2):
                at = j * 32 + i * 8
                s["kown"][2 * i + j, n] = total[at : at + 8, :]
    for d, e in offsets:
        dev, to = plane("batch", y, d, e)
        fins.append(remote(s["kown"].at[to], s["kfin"].at[me_y], dev))
    s["kfin"][pl.ds(me_y, 1)] = s["kown"][pl.ds(me_y, 1)]
    wait(v0)
    wait(v1)
    for n in range(2):
        total = summed(recv2, 2 + n)
        for j in range(8):
            s["vown"][j, n] = total[j * 8 : j * 8 + 8, :]
    for d, e in offsets:
        dev, to = plane("z", z, d, e)
        fins.append(remote(s["vown"].at[to], s["vfin"].at[me_z], dev))
    s["vfin"][pl.ds(me_z, 1)] = s["vown"][pl.ds(me_z, 1)]
    wait(smalls)
    sout_ref[0:8, :] = m3[0] + m3[1] + m3[2] + m3[3]
    wait(fins)
    for n in range(2):
        for g in range(8):
            cols = slice((2 * g + n) * PAIR, (2 * g + n + 1) * PAIR)
            kout_ref[:, cols] = s["kfin"][g, n]
            vout_ref[:, cols] = s["vfin"][g, n]


def whole_step(hidden, queries, out_grad, w_key, w_value, log_gate, seg_row, level_gain):
    vm = pl.BlockSpec(memory_space=pltpu.VMEM)
    far = pl.BlockSpec(memory_space=pl.ANY)
    return pl.pallas_call(
        step_kernel,
        in_specs=[far] * 5 + [vm, vm, pl.BlockSpec(memory_space=pltpu.SMEM)],
        out_specs=[vm] * 6,
        out_shape=[
            jax.ShapeDtypeStruct((TOK, 2048), BF16),
            jax.ShapeDtypeStruct((TOK, 1024), BF16),
            jax.ShapeDtypeStruct((16, 8, TOK), F32),
            jax.ShapeDtypeStruct((8, 2048), F32),
            jax.ShapeDtypeStruct((8, 2048), F32),
            jax.ShapeDtypeStruct((16, PAIR), F32),
        ],
        scratch_shapes=list(scratch().values()),
        compiler_params=pltpu.CompilerParams(
            collective_id=0, has_side_effects=True, vmem_limit_bytes=VMEM_LIMIT
        ),
        name="whole_step",
    )(hidden, queries, out_grad, w_key, w_value, log_gate, seg_row, level_gain)


def finish_kernel(
    qg_ref, ig_ref, gate_ref, kw_ref, vw_ref, small_ref, qg, ig, gate, kw, vw, gains
):
    qg[...] = qg_ref[...]
    ig[...] = ig_ref[...]
    kw[...] = kw_ref[...]
    vw[...] = vw_ref[...]
    heads = gate.shape[0]
    lane = iota((heads, PAIR), 1)
    head = iota((heads, PAIR), 0)
    small = small_ref[...]
    later = jnp.broadcast_to(small[8:9, :], (TOK, TOK)).T
    rows = gate_ref[...].reshape(TOK, TOK) + later
    gate[...] = dot_exact((lane == (head // 2) * 8 + head % 2).astype(F32), rows, NN)
    levels = gains.shape[0]
    level, at = iota((levels, PAIR), 0), iota((levels, PAIR), 1) % 8
    first = (level == at).astype(F32)
    second = (level == at + 8).astype(F32)
    pick0 = jnp.where(lane // 8 == head, small[0:1, :], 0.0)
    pick1 = jnp.where(lane // 8 + 16 == head, small[1:2, :], 0.0)
    pair = jnp.where(head % 2 == 0, small[2:3, :], small[3:4, :])
    pick2 = jnp.where(lane // 8 == head // 2, pair, 0.0)
    gains[...] = dot_exact(first, pick0 + pick1, NT) + dot_exact(second, pick2, NT)


def finish(query_grad, input_grad, gate, key_weight, value_weight, small, heads, levels):
    vm = pl.BlockSpec(memory_space=pltpu.VMEM)
    outs = [
        jax.ShapeDtypeStruct(a.shape, a.dtype)
        for a in (query_grad, input_grad)
    ]
    outs.append(jax.ShapeDtypeStruct((heads, TOK), F32))
    outs += [jax.ShapeDtypeStruct(a.shape, a.dtype) for a in (key_weight, value_weight)]
    outs.append(jax.ShapeDtypeStruct((levels, heads), F32))
    return pl.pallas_call(
        finish_kernel,
        in_specs=[vm] * 6,
        out_specs=[vm] * 6,
        out_shape=outs,
        name="finish",
    )(query_grad, input_grad, gate, key_weight, value_weight, small)


def local(hidden, queries, w_key, w_value, log_gate, level_gain, segment_ids, out_grad):
    heads, levels = level_gain.shape
    parts = whole_step(
        hidden[0], queries[0], out_grad[0], w_key, w_value, log_gate[0], segment_ids, level_gain.T
    )
    query_grad, input_grad, gate_grad, key_weight, value_weight, gains = finish(
        *parts, heads, levels
    )
    return (
        query_grad[None],
        input_grad[None],
        gate_grad[None],
        key_weight,
        value_weight,
        gains.T,
    )


def solution(mesh):
    split = Mesh(
        mesh.devices.reshape(4, 4, 2, mesh.shape["batch"]), ("z", "x", "core", "batch")
    )
    return jax.shard_map(
        local,
        mesh=split,
        in_specs=(
            P("batch", SEQ, None),
            P("batch", SEQ, None),
            P(),
            P(),
            P("batch", None, SEQ),
            P(),
            P("batch", SEQ),
            P("batch", SEQ, None),
        ),
        out_specs=(
            P("batch", SEQ, None),
            P("batch", SEQ, None),
            P("batch", None, SEQ),
            P(SEQ_BATCH, None),
            P(SEQ_BATCH, None),
            P(),
        ),
        check_vma=False,
    )
```

```python
import functools

import jax
import jax.numpy as jnp
from jax import lax
from jax.experimental import pallas as pl
from jax.experimental.pallas import tpu as pltpu
from jax.sharding import Mesh
from jax.sharding import PartitionSpec as P

SEQ = ("z", "x", "core")
SEQ_BATCH = ("z", "x", "core", "batch")
MESH = pl.DeviceIdType.MESH
HIGHEST = lax.Precision.HIGHEST
F32 = jnp.float32
BF16 = jnp.bfloat16

NT = (((1,), (1,)), ((), ()))
TN = (((0,), (0,)), ((), ()))
NN = (((1,), (0,)), ((), ()))

TOK = 128
PAIR = 128
HALF_ROWS = 1088


def dot(a, b, dims):
    return lax.dot_general(a, b, dims, preferred_element_type=F32)


def dot_exact(a, b, dims):
    return lax.dot_general(a, b, dims, preferred_element_type=F32, precision=HIGHEST)


def split2(x):
    hi = x.astype(BF16)
    return hi, (x - hi.astype(F32)).astype(BF16)


def dot_left(a, b, dims):
    hi, lo = split2(a)
    return dot(hi, b, dims) + dot(lo, b, dims)


def dot_right(a, b, dims):
    hi, lo = split2(b)
    return dot(a, hi, dims) + dot(a, lo, dims)


def iota(shape, dim):
    return lax.broadcasted_iota(jnp.int32, shape, dim)


def entry_signal(peers):
    barrier = pltpu.get_barrier_semaphore()
    for peer in peers:
        pl.semaphore_signal(barrier, inc=1, device_id=peer, device_id_type=MESH)
    return barrier


def ring(index, step):
    return lax.rem(index + step, 4)


def same(a, b):
    return jnp.where(a == b, 1.0, 0.0)


def linked(a, b, total):
    return jnp.where(a == b, jnp.exp(total), 0.0)


def rows_of(start, size):
    return pl.ds(pl.multiple_of(start, size), size)


SENDS = 128
LOCALS = 32
VMEM_LIMIT = 56 * 2**20


def scratch():
    def f(*shape):
        return pltpu.VMEM(shape, F32)

    def b(*shape):
        return pltpu.VMEM(shape, BF16)

    return dict(
        wk=b(1024, 2048),
        wv=b(1024, 2048),
        hid=b(TOK, 1024),
        q=b(TOK, 2048),
        g=b(TOK, 2048),
        k=b(16, TOK, PAIR),
        v=b(16, TOK, PAIR),
        hid_t=f(1024, TOK),
        cumx=f(16, TOK, PAIR),
        cumr=f(32, TOK),
        cumr3=f(16, 8, TOK),
        fw=f(16, TOK, PAIR),
        lw=f(16, TOK, PAIR),
        segc=f(TOK, TOK),
        st=f(HALF_ROWS, PAIR),
        both=f(2, HALF_ROWS, PAIR),
        chip_send=f(2, 4, 136, PAIR),
        chip_recv=f(2, 4, 136, PAIR),
        tot_send=f(2, 2, 72, PAIR),
        tot_recv=f(2, 2, 72, PAIR),
        back_send=f(2, 4, 128, PAIR),
        back_recv=f(2, 4, 128, PAIR),
        own_blocks=f(2, 2, 512, PAIR),
        s_in=f(2, 2, 512, PAIR),
        gcross=f(16, 8, PAIR),
        gint=f(16, 16, PAIR),
        gate=f(16, 8, TOK),
        hy=f(4, 2, 1024, TOK),
        hz=f(4, 2, 1024, TOK),
        hyb=b(1024, 8 * TOK),
        hzb=b(1024, 8 * TOK),
        qacc=f(16, TOK, PAIR),
        kacc=f(16, TOK, PAIR),
        vacc=f(16, TOK, PAIR),
        ks=f(2, 8, TOK, PAIR),
        vs=f(2, 8, TOK, PAIR),
        ksb=b(TOK, 2048),
        vsb=b(TOK, 2048),
        rk=f(2, 8, TOK, PAIR),
        rv=f(2, 8, TOK, PAIR),
        part1=f(4, 4, 256, PAIR),
        recv1=f(4, 4, 256, PAIR),
        part2=f(4, 4, 64, PAIR),
        recv2=f(4, 4, 64, PAIR),
        kown=f(8, 2, 8, PAIR),
        vown=f(8, 2, 8, PAIR),
        kfin=f(8, 2, 8, PAIR),
        vfin=f(8, 2, 8, PAIR),
        small=f(16, PAIR),
        m1=f(8, 16, PAIR),
        m1s=f(16, PAIR),
        m2=f(4, 16, PAIR),
        m2s=f(8, PAIR),
        m3=f(4, 8, PAIR),
        lg=f(32, TOK),
        segr=pltpu.VMEM((1, TOK), jnp.int32),
        gain=pltpu.SMEM((18, 32), F32),
        qg=b(TOK, 2048),
        ig=b(TOK, 1024),
        kout=f(8, 2048),
        vout=f(8, 2048),
        sout=f(16, PAIR),
        send_sem=pltpu.SemaphoreType.DMA((SENDS,)),
        recv_sem=pltpu.SemaphoreType.DMA((SENDS,)),
        local_sem=pltpu.SemaphoreType.DMA((LOCALS,)),
    )


def step_kernel(
    hid_hbm,
    q_hbm,
    g_hbm,
    wk_hbm,
    wv_hbm,
    lg_hbm,
    segr_hbm,
    gain_hbm,
    qg_hbm,
    ig_hbm,
    gate_hbm,
    kout_hbm,
    vout_hbm,
    sout_hbm,
    *refs,
):
    s = dict(zip(scratch(), refs))
    gain_ref, qg_ref, ig_ref = s["gain"], s["qg"], s["ig"]
    kout_ref, vout_ref, sout_ref = s["kout"], s["vout"], s["sout"]
    x, y, z, c = (lax.axis_index(a) for a in ("x", "batch", "z", "core"))
    used = [0]

    def remote(src, dst, target):
        n = used[0]
        used[0] += 1
        cp = pltpu.make_async_remote_copy(
            src_ref=src,
            dst_ref=dst,
            send_sem=s["send_sem"].at[n],
            recv_sem=s["recv_sem"].at[n],
            device_id=target,
            device_id_type=MESH,
        )
        cp.start()
        return cp

    def wait(copies):
        for cp in copies:
            cp.wait()

    sib = {"core": 1 - c}
    offsets = [(d, e) for d in range(4) for e in (0, 1) if d or e]

    def plane(axis, index, d, e):
        to, tc = ring(index, d), lax.rem(c + e, 2)
        return {axis: to, "core": tc}, 2 * to + tc

    peers = [plane("batch", y, d, e)[0] for d, e in offsets]
    peers += [plane("z", z, d, e)[0] for d, e in offsets if d]
    peers += [{"x": ring(x, d)} for d in (1, 2, 3)]
    barrier = entry_signal(peers)

    local_sem = s["local_sem"]
    first_loads = [
        pltpu.make_async_copy(hid_hbm, s["hid"], local_sem.at[0]),
        pltpu.make_async_copy(q_hbm, s["q"], local_sem.at[1]),
        pltpu.make_async_copy(g_hbm, s["g"], local_sem.at[2]),
        pltpu.make_async_copy(lg_hbm, s["lg"], local_sem.at[3]),
        pltpu.make_async_copy(segr_hbm, s["segr"], local_sem.at[4]),
        pltpu.make_async_copy(gain_hbm, s["gain"], local_sem.at[5]),
    ]

    def step_at(i):
        return lax.rem(i + 4 - 4 * c, 8)

    def weight_load(hbm, name, i, base):
        cols = rows_of(step_at(i) * 256, 256)
        return pltpu.make_async_copy(hbm.at[:, cols], s[name].at[:, cols], local_sem.at[base + i])

    first_loads[0].start()
    for n in (3, 4, 5):
        first_loads[n].start()
    for i in range(8):
        weight_load(wk_hbm, "wk", i, 8).start()
        weight_load(wv_hbm, "wv", i, 16).start()
        if i == 0:
            first_loads[1].start()
            first_loads[2].start()

    rows_i, cols_i = iota((TOK, TOK), 0), iota((TOK, TOK), 1)
    causal = cols_i <= rows_i
    lower = causal.astype(F32)
    low = cols_i < 64
    low_half = iota((64, PAIR), 1) < 64
    row8 = iota((8, PAIR), 0)
    low_row = iota((1, PAIR), 1) < 64
    for n in (3, 4, 5):
        first_loads[n].wait()
    log_gate = s["lg"][...]
    cum_cols = dot_exact(lower, log_gate, NT)
    s["cumr"][...] = dot_exact(log_gate, lower, NT)
    for pair in range(16):
        s["cumx"][pair] = jnp.where(
            low, cum_cols[:, 2 * pair : 2 * pair + 1], cum_cols[:, 2 * pair + 1 : 2 * pair + 2]
        )
        s["cumr3"][pair, 0:2, :] = s["cumr"][2 * pair : 2 * pair + 2, :]
    seg_row = s["segr"][...].astype(F32)
    s["segc"][...] = jnp.broadcast_to(seg_row, (TOK, TOK)).T
    s["gcross"][...] = jnp.zeros((16, 8, PAIR), F32)

    first_loads[0].wait()
    for b in range(8):
        cols = slice(b * TOK, (b + 1) * TOK)
        s["hid_t"][cols, :] = s["hid"][:, cols].astype(F32).T

    first_loads[1].wait()
    first_loads[2].wait()

    def project(i, st):
        step = step_at(i)
        weight_load(wk_hbm, "wk", i, 8).wait()
        weight_load(wv_hbm, "wv", i, 16).wait()
        wide = rows_of(step * 256, 256)
        hid = s["hid"][...]
        keys = dot(hid, s["wk"][:, wide], NN).astype(BF16)
        values = dot(hid, s["wv"][:, wide], NN).astype(BF16)
        segc = s["segc"][...]
        for p in range(2):
            pair = 2 * step + p
            k, v = keys[:, p * PAIR : (p + 1) * PAIR], values[:, p * PAIR : (p + 1) * PAIR]
            s["k"][pair] = k
            s["v"][pair] = v
            cum = s["cumx"][pair]
            total = cum[TOK - 1 : TOK, :]
            last_w = jnp.where(segc == segc[TOK - 1 : TOK, :], jnp.exp(total - cum), 0.0)
            first_w = jnp.where(segc == segc[0:1, :], jnp.exp(cum), 0.0)
            s["lw"][pair] = last_w
            s["fw"][pair] = first_w
            cols = rows_of(pair * PAIR, PAIR)
            fwd = dot_left(k.astype(F32) * last_w, v, TN)
            rev = dot_left(s["q"][:, cols].astype(F32) * first_w, s["g"][:, cols], TN)
            pp = 2 * lax.rem(step, 4) + p
            st[rows_of(pp * 64, 64), :] = jnp.where(low_half, fwd[:64], fwd[64:])
            st[rows_of(512 + pp * 64, 64), :] = jnp.where(low_half, rev[:64], rev[64:])
            meta = jnp.where(
                row8 == 0,
                total,
                jnp.where(
                    row8 == 1, segc[0:1, :], jnp.where(row8 == 2, segc[TOK - 1 : TOK, :], 0.0)
                ),
            )
            st[rows_of(1024 + pp * 8, 8), :] = meta

    both = s["both"]
    lax.fori_loop(0, 4, lambda i, carry: project(i, s["st"]), None)
    pl.semaphore_wait(barrier, len(peers))
    swap = remote(s["st"], both.at[c], sib)

    gathers = (("batch", y, s["hy"]), ("z", z, s["hz"]))
    hops = []
    for axis, index, buf in gathers:
        for d in (1, 3):
            hops.append(remote(s["hid_t"], buf.at[index, c], {axis: ring(index, d)}))
    down = [remote(s["hid_t"], buf.at[index, c], sib) for _, index, buf in gathers]
    lax.fori_loop(4, 8, lambda i, carry: project(i, both.at[c]), None)

    def inner(pair, carry):
        cols = rows_of(pair * PAIR, PAIR)
        q, g = s["q"][:, cols], s["g"][:, cols]
        k, v = s["k"][pair], s["v"][pair]
        allowed = causal & (s["segc"][...] == seg_row)
        gap = jnp.bitwise_xor(rows_i, cols_i)
        strict = (rows_i < cols_i).astype(BF16)
        zero = jnp.zeros((TOK, PAIR), BF16)
        weighted, scored, queries, keys, grads, gate_rows, gain_rows = [], [], [], [], [], [], []
        for h in range(2):

            def own(a):
                return jnp.where(low, a, zero) if h == 0 else jnp.where(low, zero, a)

            qh, gh, kh = own(q), own(g), own(k)
            score = dot(qh, k, NT)
            dprob = dot(gh, v, NT)
            spread = s["cumx"][pair, :, 64 * h : 64 * h + 1] - s["cumr3"][pair, h : h + 1, :]
            decay = jnp.where(allowed, jnp.exp(jnp.where(allowed, spread, 0.0)), 0.0)
            ds = decay * score
            joint = ds * dprob
            head = 2 * pair + h
            level = jnp.full((TOK, TOK), gain_ref[0, head], F32)
            gain_rows.append(jnp.sum(jnp.where(gap == 0, joint, 0.0), axis=0, keepdims=True))
            for l in range(1, 8):
                above = gap >= 2 ** (l - 1)
                level = jnp.where(above, gain_ref[l, head], level)
                chosen = above & (gap < 2**l)
                gain_rows.append(jnp.sum(jnp.where(chosen, joint, 0.0), axis=0, keepdims=True))
            wd = level * decay * dprob
            weighted.append(wd.astype(BF16))
            scored.append((level * ds).astype(BF16))
            grid = (wd * score).astype(BF16)
            crossing = jnp.where(causal, dot(grid, strict, NN), 0.0)
            gate_rows.append(jnp.sum(crossing, axis=0, keepdims=True))
            queries.append(qh)
            keys.append(kh)
            grads.append(gh)
        s["qacc"][pair] = dot(
            jnp.concatenate(weighted, axis=1), jnp.concatenate(keys, axis=0), NN
        )
        s["kacc"][pair] = dot(
            jnp.concatenate(weighted, axis=0), jnp.concatenate(queries, axis=0), TN
        )
        s["vacc"][pair] = dot(jnp.concatenate(scored, axis=0), jnp.concatenate(grads, axis=0), TN)
        s["gate"][pair] = jnp.concatenate([*gate_rows, jnp.zeros((6, TOK), F32)], axis=0)
        s["gint"][pair] = jnp.concatenate(gain_rows, axis=0)
        return carry

    swap.wait()

    def meta_rows(total, first, last):
        return jnp.where(
            row8 == 0, total, jnp.where(row8 == 1, first, jnp.where(row8 == 2, last, 0.0))
        )

    chip_send, chip_recv = s["chip_send"], s["chip_recv"]

    def block_pair(pp):
        f0 = both[0, pp * 64 : pp * 64 + 64, :]
        f1 = both[1, pp * 64 : pp * 64 + 64, :]
        r0 = both[0, 512 + pp * 64 : 576 + pp * 64, :]
        r1 = both[1, 512 + pp * 64 : 576 + pp * 64, :]
        m0 = both[0, 1024 + pp * 8 : 1032 + pp * 8, :]
        m1 = both[1, 1024 + pp * 8 : 1032 + pp * 8, :]
        return f0, f1, r0, r1, m0[0:1], m0[1:2], m0[2:3], m1[0:1], m1[1:2], m1[2:3]

    xs = []
    for p in range(2):
        for n in range(4):
            f0, f1, r0, r1, t0, first0, last0, t1, first1, last1 = block_pair(2 * n + p)
            chip_send[p, n, 0:64, :] = f1 + linked(last0, last1, t1) * f0
            chip_send[p, n, 64:128, :] = r0 + linked(first0, first1, t0) * r1
            chip_send[p, n, 128:136, :] = meta_rows(t0 + t1, first0, last1)
        copies = []
        for d in (1, 2, 3):
            to = ring(x, d)
            copies.append(remote(chip_send.at[p, to], chip_recv.at[p, x], {"x": to}))
        chip_recv[p, pl.ds(x, 1)] = chip_send[p, pl.ds(x, 1)]
        xs.append(copies)
    for pp in range(8):
        f0, _, _, r1, _, _, last0, _, first1, _ = block_pair(pp)
        d8 = same(last0, first1) * jnp.sum(f0 * r1, axis=0, keepdims=True)
        s["gcross"][pl.ds(c * 8 + pp, 1)] = jnp.where(row8 == 0, d8, 0.0)[None]
    lax.fori_loop(0, 7, inner, 0)

    def chip(j, p):
        return (
            chip_recv[p, j, 0:64, :],
            chip_recv[p, j, 64:128, :],
            chip_recv[p, j, 128:129, :],
            chip_recv[p, j, 129:130, :],
            chip_recv[p, j, 130:131, :],
        )

    def joined(p):
        (f0, r0, t0, a0, l0), (f1, r1, t1, a1, l1), (f2, r2, t2, a2, l2), (f3, r3, t3, a3, l3) = (
            chip(j, p) for j in range(4)
        )
        f01 = f1 + linked(l0, l1, t1) * f0
        r01 = r0 + linked(a0, a1, t0) * r1
        f23 = f3 + linked(l2, l3, t3) * f2
        r23 = r2 + linked(a2, a3, t2) * r3
        return f01, r01, f23, r23

    tot_send, tot_recv = s["tot_send"], s["tot_recv"]
    zs = []
    for p in range(2):
        wait(xs[p])
        f01, r01, f23, r23 = joined(p)
        t0, a0 = chip(0, p)[2:4]
        t1, l1 = chip(1, p)[2], chip(1, p)[4]
        t2, a2 = chip(2, p)[2:4]
        t3, l3 = chip(3, p)[2], chip(3, p)[4]
        tot_send[p, 0, 0:64, :] = f23 + linked(l1, l3, t2 + t3) * f01
        tot_send[p, 1, 0:64, :] = r01 + linked(a0, a2, t0 + t1) * r23
        tot_send[p, 0, 64:72, :] = jnp.broadcast_to(l3, (8, PAIR))
        tot_send[p, 1, 64:72, :] = jnp.broadcast_to(a0, (8, PAIR))
        zs.append(
            [
                remote(tot_send.at[p, n], tot_recv.at[p, n], {"z": ring(z, d)})
                for n, d in ((0, 1), (1, 3))
            ]
        )
    lax.fori_loop(7, 10, inner, 0)

    has_prev = (z > 0).astype(F32)
    has_next = (z < 3).astype(F32)
    prev_top = (z == 2).astype(F32)
    next_top = (z == 1).astype(F32)
    back_send, back_recv = s["back_send"], s["back_recv"]

    def gain_row(pair, level):
        return jnp.where(low_row, gain_ref[level, 2 * pair], gain_ref[level, 2 * pair + 1])

    bs = []
    for p in range(2):
        wait(zs[p])
        (f0, r0, t0, a0, l0), (f1, r1, t1, a1, l1), (f2, r2, t2, a2, l2), (f3, r3, t3, a3, l3) = (
            chip(j, p) for j in range(4)
        )
        f01, r01, f23, r23 = joined(p)
        pair = c * 8 + 2 * x + p
        g9, g10, g11, g12 = (gain_row(pair, level) for level in range(9, 13))
        zf = has_prev * tot_recv[p, 0, 0:64, :]
        zl = tot_recv[p, 0, 64:65, :]
        zr = has_next * tot_recv[p, 1, 0:64, :]
        za = tot_recv[p, 1, 64:65, :]
        gzf = g11 * (1.0 - prev_top) + g12 * prev_top
        gzr = g11 * (1.0 - next_top) + g12 * next_top
        sf = (
            gzf * same(zl, a0) * zf,
            gzf * linked(zl, a1, t0) * zf + g9 * same(l0, a1) * f0,
            gzf * linked(zl, a2, t0 + t1) * zf + g10 * same(l1, a2) * f01,
            gzf * linked(zl, a3, t0 + t1 + t2) * zf
            + g10 * linked(l1, a3, t2) * f01
            + g9 * same(l2, a3) * f2,
        )
        sr = (
            gzr * linked(za, l0, t1 + t2 + t3) * zr
            + g10 * linked(l0, a2, t1) * r23
            + g9 * same(l0, a1) * r1,
            gzr * linked(za, l1, t2 + t3) * zr + g10 * same(l1, a2) * r23,
            gzr * linked(za, l2, t3) * zr + g9 * same(l2, a3) * r3,
            gzr * same(za, l3) * zr,
        )
        for j in range(4):
            back_send[p, j, 0:64, :] = sf[j]
            back_send[p, j, 64:128, :] = sr[j]
        copies = []
        for d in (1, 2, 3):
            to = ring(x, d)
            copies.append(remote(back_send.at[p, to], back_recv.at[p, x], {"x": to}))
        back_recv[p, pl.ds(x, 1)] = back_send[p, pl.ds(x, 1)]
        bs.append(copies)

    fwd = []
    for n, (axis, index, buf) in enumerate(gathers):
        for m, d in enumerate((1, 3)):
            hops[2 * n + m].wait()
            came = ring(index, 4 - d)
            part = slice(0, 512) if d == 1 else slice(512, 1024)
            fwd.append(
                remote(buf.at[came, c, part], buf.at[came, c, part], {axis: ring(index, d)})
            )
            down.append(remote(buf.at[came, c], buf.at[came, c], sib))

    for p in range(2):
        (f0, r0, t0, a0, l0), (f1, r1, t1, a1, l1), (f2, r2, t2, a2, l2), (f3, r3, t3, a3, l3) = (
            chip(j, p) for j in range(4)
        )
        f01, r01, f23, r23 = joined(p)
        zf = has_prev * tot_recv[p, 0, 0:64, :]
        zl = tot_recv[p, 0, 64:65, :]
        r_group = r01 + linked(a0, a2, t0 + t1) * r23
        d9 = same(l0, a1) * jnp.sum(f0 * r1, axis=0, keepdims=True) + same(l2, a3) * jnp.sum(
            f2 * r3, axis=0, keepdims=True
        )
        d10 = same(l1, a2) * jnp.sum(f01 * r23, axis=0, keepdims=True)
        dz = same(zl, a0) * jnp.sum(zf * r_group, axis=0, keepdims=True)
        rows = jnp.where(
            row8 == 1,
            d9,
            jnp.where(
                row8 == 2,
                d10,
                jnp.where(
                    row8 == 3, (1.0 - prev_top) * dz, jnp.where(row8 == 4, prev_top * dz, 0.0)
                ),
            ),
        )
        pair = c * 8 + 2 * x + p
        s["gcross"][pl.ds(pair, 1)] = s["gcross"][pl.ds(pair, 1)] + rows[None]
    lax.fori_loop(10, 16, inner, 0)

    own_blocks, s_in = s["own_blocks"], s["s_in"]
    swaps = []
    for p in range(2):
        wait(bs[p])
        for n in range(4):
            pp = 2 * n + p
            f0, _, _, r1, t0, first0, last0, t1, first1, last1 = block_pair(pp)
            sf = back_recv[p, n, 0:64, :]
            sr = back_recv[p, n, 64:128, :]
            link = gain_row(c * 8 + pp, 8) * same(last0, first1)
            at = n * 128
            own_blocks[p, 0, at : at + 64, :] = sf
            own_blocks[p, 1, at : at + 64, :] = linked(first0, first1, t0) * sf + link * f0
            own_blocks[p, 0, at + 64 : at + 128, :] = linked(last0, last1, t1) * sr + link * r1
            own_blocks[p, 1, at + 64 : at + 128, :] = sr
        swaps.append(remote(own_blocks.at[p, 1 - c], s_in.at[p, c], sib))
        s_in[p, pl.ds(c, 1)] = own_blocks[p, pl.ds(c, 1)]

    tail = causal.astype(BF16)
    head_pick = (cols_i[0:8, :] // 64 == row8).astype(BF16)

    def diag(a):
        return jnp.concatenate([jnp.where(low_half, a, 0.0), jnp.where(low_half, 0.0, a)], axis=0)

    def incoming(to, p, part):
        at = lax.rem(to, 4) * 128 + part * 64
        return diag(s_in[p, to // 4, rows_of(at, 64), :])

    def key_part(to, p):
        pair = 2 * to + p
        rv = s["lw"][pair] * dot_right(s["v"][pair], incoming(to, p, 1), NT)
        key_sum = (s["kacc"][pair] + rv).astype(BF16)
        s["kacc"][pair] = s["k"][pair].astype(F32) * rv
        s["ksb"][:, rows_of(pair * PAIR, PAIR)] = key_sum
        s["ks"][p, to] = key_sum.astype(F32)

    def value_part(to, p):
        pair = 2 * to + p
        rk = s["lw"][pair] * dot_right(s["k"][pair], incoming(to, p, 1), NN)
        value_sum = (s["vacc"][pair] + rk).astype(BF16)
        s["vsb"][:, rows_of(pair * PAIR, PAIR)] = value_sum
        s["vs"][p, to] = value_sum.astype(F32)

    def query_part(to, p):
        pair = 2 * to + p
        cols = rows_of(pair * PAIR, PAIR)
        sg = s["fw"][pair] * dot_right(s["g"][:, cols], incoming(to, p, 0), NT)
        qg_ref[:, cols] = (s["qacc"][pair] + sg).astype(BF16)
        diff = s["q"][:, cols].astype(F32) * sg - s["kacc"][pair]
        hi, lo = split2(diff)
        diff_rows = dot(head_pick, hi, NT) + dot(head_pick, lo, NT)
        s["gate"][pair] = s["gate"][pair] + dot_left(diff_rows, tail, NN)

    firsts = []
    me_y, me_z = 2 * y + c, 2 * z + c
    far_first = [(2, 0), (2, 1), (1, 0), (3, 0), (1, 1), (3, 1), (0, 1)]
    for n in range(2):
        swaps[n].wait()
        fk, fv = [], []
        for d, e in far_first:
            dev, to = plane("batch", y, d, e)
            key_part(to, n)
            fk.append(remote(s["ks"].at[n, to], s["rk"].at[n, me_y], dev))
            dev, to = plane("z", z, d, e)
            value_part(to, n)
            fv.append(remote(s["vs"].at[n, to], s["rv"].at[n, me_z], dev))
        key_part(me_y, n)
        value_part(me_z, n)
        s["rk"][n, pl.ds(me_y, 1)] = s["ks"][n, pl.ds(me_y, 1)]
        s["rv"][n, pl.ds(me_z, 1)] = s["vs"][n, pl.ds(me_z, 1)]
        firsts.append((fk, fv))
    for n in range(2):
        lax.fori_loop(0, 8, lambda to, carry: query_part(to, n), None)
    stores = []

    def store(ref, hbm):
        cp = pltpu.make_async_copy(ref, hbm, local_sem.at[24 + len(stores)])
        cp.start()
        stores.append(cp)

    store(qg_ref, qg_hbm)
    store(s["gate"], gate_hbm)

    ones = jnp.ones((8, PAIR), F32)
    inner_sum = dot_exact(ones, s["gint"][...].reshape(256, PAIR), NT)
    pick = (cols_i[0:8, :] // 64 == row8 - 2).astype(F32)
    outer_sum = dot_exact(pick, s["gcross"][...].reshape(128, PAIR), NT)
    start = (cols_i[0:8, :] == 0).astype(F32)
    own_total = dot_exact(start, s["gate"][...].reshape(128, TOK), NT)
    small, m1, m1s, m2, m2s, m3 = (s[n] for n in ("small", "m1", "m1s", "m2", "m2s", "m3"))
    small[0:8, :] = jnp.where(
        row8 == 0, inner_sum[:, :128], jnp.where(row8 == 1, inner_sum[:, 128:], outer_sum)
    )
    small[8:16, :] = own_total
    smalls = []
    for d, e in offsets:
        smalls.append(remote(small, m1.at[me_z], plane("z", z, d, e)[0]))
    m1[pl.ds(me_z, 1)] = small[...][None]

    for n, (_, index, buf) in enumerate(gathers):
        buf[pl.ds(index, 1), pl.ds(c, 1)] = s["hid_t"][...][None, None]
        wait(fwd[2 * n : 2 * n + 2])
        came = ring(index, 2)
        down.append(remote(buf.at[came, c], buf.at[came, c], sib))
    wait(down)
    for name, out in (("hy", "hyb"), ("hz", "hzb")):
        for g in range(8):
            s[out][:, g * TOK : (g + 1) * TOK] = s[name][g // 2, g % 2].astype(BF16)

    def product(left, right, n):
        right = s[right][n].reshape(8 * TOK, PAIR).astype(BF16)
        for b in range(4):
            yield b, dot(s[left][b * 256 : (b + 1) * 256, :], right, NN)

    part1, recv1, part2, recv2 = s["part1"], s["recv1"], s["part2"], s["recv2"]

    def scatter(part, recv, chunk, axis, index):
        out = []
        for d in (1, 2, 3):
            to = ring(index, d)
            out.append(remote(part.at[chunk, to], recv.at[chunk, index], {axis: to}))
        recv[chunk, pl.ds(index, 1)] = part[chunk, pl.ds(index, 1)]
        return out

    wait(firsts[0][0])
    for b, block in product("hyb", "rk", 0):
        for j in range(4):
            part1[0, j, b * 64 : b * 64 + 64, :] = block[j * 64 : j * 64 + 64, :]
    k0 = scatter(part1, recv1, 0, "x", x)
    wait(firsts[0][1])
    for b, block in product("hzb", "rv", 0):
        for j in range(4):
            part1[2, j, b * 64 : b * 64 + 64, :] = block[j * 64 : j * 64 + 64, :]
    v0 = scatter(part1, recv1, 2, "x", x)

    def input_grad(n, carry):
        rows = rows_of(n * 256, 256)
        ig_ref[:, rows] = (
            dot(s["ksb"][...], s["wk"][rows, :], NT) + dot(s["vsb"][...], s["wv"][rows, :], NT)
        ).astype(BF16)
        return carry

    lax.fori_loop(0, 2, input_grad, 0)

    wait(firsts[1][0])
    for b, block in product("hyb", "rk", 1):
        part1[1, b] = block
    k1 = scatter(part1, recv1, 1, "z", z)
    wait(firsts[1][1])
    for b, block in product("hzb", "rv", 1):
        for j in range(8):
            for i in range(4):
                at = j * 32 + i * 8
                part1[3, i, b * 64 + j * 8 : b * 64 + j * 8 + 8, :] = block[at : at + 8, :]
    v1 = scatter(part1, recv1, 3, "batch", y)
    lax.fori_loop(2, 4, input_grad, 0)
    store(ig_ref, ig_hbm)

    wait(smalls)
    total = m1[0, 0:8, :]
    for g in range(1, 8):
        total = total + m1[g, 0:8, :]
    m1s[0:8, :] = total
    for g in range(8):
        m1s[8 + g : 9 + g, :] = m1[g, 8:9, :]
    smalls = [remote(m1s, m2.at[x], {"x": ring(x, d)}) for d in (1, 2, 3)]
    m2[pl.ds(x, 1)] = m1s[...][None]

    def summed(recv, chunk):
        return recv[chunk, 0] + recv[chunk, 1] + recv[chunk, 2] + recv[chunk, 3]

    wait(k0)
    total = summed(recv1, 0)
    for j in range(4):
        part2[0, j] = total[j * 64 : j * 64 + 64, :]
    k0 = scatter(part2, recv2, 0, "z", z)
    wait(v0)
    total = summed(recv1, 2)
    for j in range(8):
        for i in range(4):
            at = j * 32 + i * 8
            part2[2, i, j * 8 : j * 8 + 8, :] = total[at : at + 8, :]
    v0 = scatter(part2, recv2, 2, "batch", y)
    wait(k1)
    total = summed(recv1, 1)
    for j in range(4):
        part2[1, j] = total[j * 64 : j * 64 + 64, :]
    k1 = scatter(part2, recv2, 1, "x", x)
    wait(v1)
    total = summed(recv1, 3)
    for j in range(4):
        for i in range(4):
            at = j * 64 + i * 16
            part2[3, i, j * 16 : j * 16 + 16, :] = total[at : at + 16, :]
    v1 = scatter(part2, recv2, 3, "x", x)

    wait(smalls)
    total = m2[0, 0:8, :] + m2[1, 0:8, :] + m2[2, 0:8, :] + m2[3, 0:8, :]
    m2s[...] = total
    smalls = [remote(m2s, m3.at[y], {"batch": ring(y, d)}) for d in (1, 2, 3)]
    m3[pl.ds(y, 1)] = total[None]
    place = z * 8 + x * 2 + c
    later = jnp.zeros((1, PAIR), F32)
    for j in range(4):
        for g in range(8):
            spot = (g // 2) * 8 + j * 2 + g % 2
            later = later + (place < spot).astype(F32) * m2[j, 8 + g : 9 + g, :]
    sout_ref[8:16, :] = jnp.broadcast_to(later, (8, PAIR))

    fins = []
    wait(k0)
    wait(k1)
    for n in range(2):
        total = summed(recv2, n)
        for i in range(4):
            for j in range(2):
                at = j * 32 + i * 8
                s["kown"][2 * i + j, n] = total[at : at + 8, :]
    for d, e in offsets:
        dev, to = plane("batch", y, d, e)
        fins.append(remote(s["kown"].at[to], s["kfin"].at[me_y], dev))
    s["kfin"][pl.ds(me_y, 1)] = s["kown"][pl.ds(me_y, 1)]
    wait(v0)
    wait(v1)
    for n in range(2):
        total = summed(recv2, 2 + n)
        for j in range(8):
            s["vown"][j, n] = total[j * 8 : j * 8 + 8, :]
    for d, e in offsets:
        dev, to = plane("z", z, d, e)
        fins.append(remote(s["vown"].at[to], s["vfin"].at[me_z], dev))
    s["vfin"][pl.ds(me_z, 1)] = s["vown"][pl.ds(me_z, 1)]
    wait(smalls)
    sout_ref[0:8, :] = m3[0] + m3[1] + m3[2] + m3[3]
    store(sout_ref, sout_hbm)
    wait(fins)
    for n in range(2):
        for g in range(8):
            cols = slice((2 * g + n) * PAIR, (2 * g + n + 1) * PAIR)
            kout_ref[:, cols] = s["kfin"][g, n]
            vout_ref[:, cols] = s["vfin"][g, n]
    store(kout_ref, kout_hbm)
    store(vout_ref, vout_hbm)
    wait(stores)


def whole_step(hidden, queries, out_grad, w_key, w_value, log_gate, seg_row, level_gain):
    far = pl.BlockSpec(memory_space=pltpu.HBM)
    return pl.pallas_call(
        step_kernel,
        in_specs=[far] * 8,
        out_specs=[far] * 6,
        out_shape=[
            jax.ShapeDtypeStruct((TOK, 2048), BF16),
            jax.ShapeDtypeStruct((TOK, 1024), BF16),
            jax.ShapeDtypeStruct((16, 8, TOK), F32),
            jax.ShapeDtypeStruct((8, 2048), F32),
            jax.ShapeDtypeStruct((8, 2048), F32),
            jax.ShapeDtypeStruct((16, PAIR), F32),
        ],
        scratch_shapes=list(scratch().values()),
        compiler_params=pltpu.CompilerParams(
            collective_id=0, has_side_effects=True, vmem_limit_bytes=VMEM_LIMIT
        ),
        name="whole_step",
    )(hidden, queries, out_grad, w_key, w_value, log_gate, seg_row, level_gain)


def finish_kernel(
    qg_in, ig_in, gate_in, kw_in, vw_in, small_in, qg_out, ig_out, gate_out, kw_out, vw_out, gains_out,
    qg, ig, gate_ref, kw, vw, small_ref, gate, gains, load_sem, store_sem
):
    loads = [
        pltpu.make_async_copy(a, b, load_sem.at[n])
        for n, (a, b) in enumerate(
            ((gate_in, gate_ref), (small_in, small_ref), (qg_in, qg), (ig_in, ig), (kw_in, kw), (vw_in, vw))
        )
    ]
    for cp in loads:
        cp.start()
    stores = []

    def store(ref, out):
        cp = pltpu.make_async_copy(ref, out, store_sem.at[len(stores)])
        cp.start()
        stores.append(cp)

    loads[0].wait()
    loads[1].wait()
    heads = gate.shape[0]
    lane = iota((heads, PAIR), 1)
    head = iota((heads, PAIR), 0)
    small = small_ref[...]
    later = jnp.broadcast_to(small[8:9, :], (TOK, TOK)).T
    rows = gate_ref[...].reshape(TOK, TOK) + later
    gate[...] = dot_exact((lane == (head // 2) * 8 + head % 2).astype(F32), rows, NN)
    levels = gains.shape[0]
    level, at = iota((levels, PAIR), 0), iota((levels, PAIR), 1) % 8
    first = (level == at).astype(F32)
    second = (level == at + 8).astype(F32)
    pick0 = jnp.where(lane // 8 == head, small[0:1, :], 0.0)
    pick1 = jnp.where(lane // 8 + 16 == head, small[1:2, :], 0.0)
    pair = jnp.where(head % 2 == 0, small[2:3, :], small[3:4, :])
    pick2 = jnp.where(lane // 8 == head // 2, pair, 0.0)
    gains[...] = dot_exact(first, pick0 + pick1, NT) + dot_exact(second, pick2, NT)
    for cp, ref, out in zip(
        loads[2:], (qg, ig, kw, vw), (qg_out, ig_out, kw_out, vw_out)
    ):
        cp.wait()
        store(ref, out)
    store(gate, gate_out)
    store(gains, gains_out)
    for cp in stores:
        cp.wait()


def finish(query_grad, input_grad, gate, key_weight, value_weight, small, heads, levels):
    far = pl.BlockSpec(memory_space=pltpu.HBM)
    parts = (query_grad, input_grad, gate, key_weight, value_weight, small)
    outs = [jax.ShapeDtypeStruct(a.shape, a.dtype) for a in parts]
    outs[2] = jax.ShapeDtypeStruct((heads, TOK), F32)
    outs[5] = jax.ShapeDtypeStruct((levels, heads), F32)
    return pl.pallas_call(
        finish_kernel,
        in_specs=[far] * 6,
        out_specs=[far] * 6,
        out_shape=outs,
        scratch_shapes=[pltpu.VMEM(a.shape, a.dtype) for a in (*parts, outs[2], outs[5])]
        + [pltpu.SemaphoreType.DMA((6,)), pltpu.SemaphoreType.DMA((6,))],
        name="finish",
    )(*parts)


def local(hidden, queries, w_key, w_value, log_gate, level_gain, segment_ids, out_grad):
    heads, levels = level_gain.shape
    parts = whole_step(
        hidden[0], queries[0], out_grad[0], w_key, w_value, log_gate[0], segment_ids, level_gain.T
    )
    query_grad, input_grad, gate_grad, key_weight, value_weight, gains = finish(
        *parts, heads, levels
    )
    return (
        query_grad[None],
        input_grad[None],
        gate_grad[None],
        key_weight,
        value_weight,
        gains.T,
    )


def solution(mesh):
    split = Mesh(
        mesh.devices.reshape(4, 4, 2, mesh.shape["batch"]), ("z", "x", "core", "batch")
    )
    return jax.shard_map(
        local,
        mesh=split,
        in_specs=(
            P("batch", SEQ, None),
            P("batch", SEQ, None),
            P(),
            P(),
            P("batch", None, SEQ),
            P(),
            P("batch", SEQ),
            P("batch", SEQ, None),
        ),
        out_specs=(
            P("batch", SEQ, None),
            P("batch", SEQ, None),
            P("batch", None, SEQ),
            P(SEQ_BATCH, None),
            P(SEQ_BATCH, None),
            P(),
        ),
        check_vma=False,
    )
```

```python
import functools

import jax
import jax.numpy as jnp
from jax import lax
from jax.experimental import pallas as pl
from jax.experimental.pallas import tpu as pltpu
from jax.sharding import Mesh
from jax.sharding import PartitionSpec as P

SEQ = ("z", "x", "core")
SEQ_BATCH = ("z", "x", "core", "batch")
MESH = pl.DeviceIdType.MESH
HIGHEST = lax.Precision.HIGHEST
F32 = jnp.float32
BF16 = jnp.bfloat16

NT = (((1,), (1,)), ((), ()))
TN = (((0,), (0,)), ((), ()))
NN = (((1,), (0,)), ((), ()))

TOK = 128
PAIR = 128
HALF_ROWS = 1088


def dot(a, b, dims):
    return lax.dot_general(a, b, dims, preferred_element_type=F32)


def dot_exact(a, b, dims):
    return lax.dot_general(a, b, dims, preferred_element_type=F32, precision=HIGHEST)


def split2(x):
    hi = x.astype(BF16)
    return hi, (x - hi.astype(F32)).astype(BF16)


def dot_left(a, b, dims):
    hi, lo = split2(a)
    return dot(hi, b, dims) + dot(lo, b, dims)


def dot_right(a, b, dims):
    hi, lo = split2(b)
    return dot(a, hi, dims) + dot(a, lo, dims)


def iota(shape, dim):
    return lax.broadcasted_iota(jnp.int32, shape, dim)


def entry_signal(peers):
    barrier = pltpu.get_barrier_semaphore()
    for peer in peers:
        pl.semaphore_signal(barrier, inc=1, device_id=peer, device_id_type=MESH)
    return barrier


def ring(index, step):
    return lax.rem(index + step, 4)


def same(a, b):
    return jnp.where(a == b, 1.0, 0.0)


def linked(a, b, total):
    return jnp.where(a == b, jnp.exp(total), 0.0)


def rows_of(start, size):
    return pl.ds(pl.multiple_of(start, size), size)


SENDS = 128
LOCALS = 32
VMEM_LIMIT = 56 * 2**20


def scratch():
    def f(*shape):
        return pltpu.VMEM(shape, F32)

    def b(*shape):
        return pltpu.VMEM(shape, BF16)

    return dict(
        wk=b(1024, 2048),
        wv=b(1024, 2048),
        hid=b(TOK, 1024),
        q=b(TOK, 2048),
        g=b(TOK, 2048),
        k=b(16, TOK, PAIR),
        v=b(16, TOK, PAIR),
        hid_t=f(1024, TOK),
        cumx=f(16, TOK, PAIR),
        cumr=f(32, TOK),
        cumr3=f(16, 8, TOK),
        fw=f(16, TOK, PAIR),
        lw=f(16, TOK, PAIR),
        segc=f(TOK, TOK),
        st=f(HALF_ROWS, PAIR),
        both=f(2, HALF_ROWS, PAIR),
        chip_send=f(2, 4, 136, PAIR),
        chip_recv=f(2, 4, 136, PAIR),
        tot_send=f(2, 2, 72, PAIR),
        tot_recv=f(2, 2, 72, PAIR),
        back_send=f(2, 4, 128, PAIR),
        back_recv=f(2, 4, 128, PAIR),
        own_blocks=f(2, 2, 512, PAIR),
        s_in=f(2, 2, 512, PAIR),
        gcross=f(16, 8, PAIR),
        gint=f(16, 16, PAIR),
        gate=f(16, 8, TOK),
        hy=f(4, 2, 1024, TOK),
        hz=f(4, 2, 1024, TOK),
        hyb=b(1024, 8 * TOK),
        hzb=b(1024, 8 * TOK),
        qacc=f(16, TOK, PAIR),
        kacc=f(16, TOK, PAIR),
        vacc=f(16, TOK, PAIR),
        ks=f(2, 8, TOK, PAIR),
        vs=f(2, 8, TOK, PAIR),
        ksb=b(TOK, 2048),
        vsb=b(TOK, 2048),
        rk=f(2, 8, TOK, PAIR),
        rv=f(2, 8, TOK, PAIR),
        part1=f(4, 4, 256, PAIR),
        recv1=f(4, 4, 256, PAIR),
        part2=f(4, 4, 64, PAIR),
        recv2=f(4, 4, 64, PAIR),
        kown=f(8, 2, 8, PAIR),
        vown=f(8, 2, 8, PAIR),
        kfin=f(8, 2, 8, PAIR),
        vfin=f(8, 2, 8, PAIR),
        small=f(16, PAIR),
        m1=f(8, 16, PAIR),
        m1s=f(16, PAIR),
        m2=f(4, 16, PAIR),
        m2s=f(8, PAIR),
        m3=f(4, 8, PAIR),
        lg=f(32, TOK),
        segr=pltpu.VMEM((1, TOK), jnp.int32),
        gain=pltpu.SMEM((18, 32), F32),
        qg=b(TOK, 2048),
        ig=b(TOK, 1024),
        kout=f(8, 2048),
        vout=f(8, 2048),
        sout=f(16, PAIR),
        send_sem=pltpu.SemaphoreType.DMA((SENDS,)),
        recv_sem=pltpu.SemaphoreType.DMA((SENDS,)),
        local_sem=pltpu.SemaphoreType.DMA((LOCALS,)),
    )


def step_kernel(
    hid_hbm,
    q_hbm,
    g_hbm,
    wk_hbm,
    wv_hbm,
    lg_hbm,
    segr_hbm,
    gain_hbm,
    qg_hbm,
    ig_hbm,
    gate_hbm,
    kout_hbm,
    vout_hbm,
    sout_hbm,
    *refs,
):
    s = dict(zip(scratch(), refs))
    gain_ref, qg_ref, ig_ref = s["gain"], s["qg"], s["ig"]
    kout_ref, vout_ref, sout_ref = s["kout"], s["vout"], s["sout"]
    x, y, z, c = (lax.axis_index(a) for a in ("x", "batch", "z", "core"))
    used = [0]

    def remote(src, dst, target):
        n = used[0]
        used[0] += 1
        cp = pltpu.make_async_remote_copy(
            src_ref=src,
            dst_ref=dst,
            send_sem=s["send_sem"].at[n],
            recv_sem=s["recv_sem"].at[n],
            device_id=target,
            device_id_type=MESH,
        )
        cp.start()
        return cp

    def wait(copies):
        for cp in copies:
            cp.wait()

    def wait_recv(copies):
        for cp in copies:
            cp.wait_recv()

    sib = {"core": 1 - c}
    offsets = [(d, e) for d in range(4) for e in (0, 1) if d or e]

    def plane(axis, index, d, e):
        to, tc = ring(index, d), lax.rem(c + e, 2)
        return {axis: to, "core": tc}, 2 * to + tc

    peers = [plane("batch", y, d, e)[0] for d, e in offsets]
    peers += [plane("z", z, d, e)[0] for d, e in offsets if d]
    peers += [{"x": ring(x, d)} for d in (1, 2, 3)]
    barrier = entry_signal(peers)

    local_sem = s["local_sem"]
    first_loads = [
        pltpu.make_async_copy(hid_hbm, s["hid"], local_sem.at[0]),
        pltpu.make_async_copy(q_hbm, s["q"], local_sem.at[1]),
        pltpu.make_async_copy(g_hbm, s["g"], local_sem.at[2]),
        pltpu.make_async_copy(lg_hbm, s["lg"], local_sem.at[3]),
        pltpu.make_async_copy(segr_hbm, s["segr"], local_sem.at[4]),
        pltpu.make_async_copy(gain_hbm, s["gain"], local_sem.at[5]),
    ]

    def step_at(i):
        return lax.rem(i + 4 - 4 * c, 8)

    def weight_load(hbm, name, i, base):
        cols = rows_of(step_at(i) * 256, 256)
        return pltpu.make_async_copy(hbm.at[:, cols], s[name].at[:, cols], local_sem.at[base + i])

    first_loads[0].start()
    for n in (3, 4, 5):
        first_loads[n].start()
    for i in range(8):
        weight_load(wk_hbm, "wk", i, 8).start()
        weight_load(wv_hbm, "wv", i, 16).start()
        if i == 0:
            first_loads[1].start()
            first_loads[2].start()

    rows_i, cols_i = iota((TOK, TOK), 0), iota((TOK, TOK), 1)
    causal = cols_i <= rows_i
    lower = causal.astype(F32)
    low = cols_i < 64
    low_half = iota((64, PAIR), 1) < 64
    row8 = iota((8, PAIR), 0)
    low_row = iota((1, PAIR), 1) < 64
    for n in (3, 4, 5):
        first_loads[n].wait()
    log_gate = s["lg"][...]
    cum_cols = dot_exact(lower, log_gate, NT)
    s["cumr"][...] = dot_exact(log_gate, lower, NT)
    for pair in range(16):
        s["cumx"][pair] = jnp.where(
            low, cum_cols[:, 2 * pair : 2 * pair + 1], cum_cols[:, 2 * pair + 1 : 2 * pair + 2]
        )
        s["cumr3"][pair, 0:2, :] = s["cumr"][2 * pair : 2 * pair + 2, :]
    seg_row = s["segr"][...].astype(F32)
    s["segc"][...] = jnp.broadcast_to(seg_row, (TOK, TOK)).T
    s["gcross"][...] = jnp.zeros((16, 8, PAIR), F32)

    first_loads[0].wait()
    for b in range(8):
        cols = slice(b * TOK, (b + 1) * TOK)
        s["hid_t"][cols, :] = s["hid"][:, cols].astype(F32).T

    first_loads[1].wait()
    first_loads[2].wait()

    def project(i, st):
        step = step_at(i)
        weight_load(wk_hbm, "wk", i, 8).wait()
        weight_load(wv_hbm, "wv", i, 16).wait()
        wide = rows_of(step * 256, 256)
        hid = s["hid"][...]
        keys = dot(hid, s["wk"][:, wide], NN).astype(BF16)
        values = dot(hid, s["wv"][:, wide], NN).astype(BF16)
        segc = s["segc"][...]
        for p in range(2):
            pair = 2 * step + p
            k, v = keys[:, p * PAIR : (p + 1) * PAIR], values[:, p * PAIR : (p + 1) * PAIR]
            s["k"][pair] = k
            s["v"][pair] = v
            cum = s["cumx"][pair]
            total = cum[TOK - 1 : TOK, :]
            last_w = jnp.where(segc == segc[TOK - 1 : TOK, :], jnp.exp(total - cum), 0.0)
            first_w = jnp.where(segc == segc[0:1, :], jnp.exp(cum), 0.0)
            s["lw"][pair] = last_w
            s["fw"][pair] = first_w
            cols = rows_of(pair * PAIR, PAIR)
            fwd = dot_left(k.astype(F32) * last_w, v, TN)
            rev = dot_left(s["q"][:, cols].astype(F32) * first_w, s["g"][:, cols], TN)
            pp = 2 * lax.rem(step, 4) + p
            st[rows_of(pp * 64, 64), :] = jnp.where(low_half, fwd[:64], fwd[64:])
            st[rows_of(512 + pp * 64, 64), :] = jnp.where(low_half, rev[:64], rev[64:])
            meta = jnp.where(
                row8 == 0,
                total,
                jnp.where(
                    row8 == 1, segc[0:1, :], jnp.where(row8 == 2, segc[TOK - 1 : TOK, :], 0.0)
                ),
            )
            st[rows_of(1024 + pp * 8, 8), :] = meta

    both = s["both"]
    project(0, s["st"])
    pl.semaphore_wait(barrier, len(peers))

    gathers = (("batch", y, s["hy"]), ("z", z, s["hz"]))
    hops = []
    for axis, index, buf in gathers:
        for d in (1, 3):
            hops.append(remote(s["hid_t"], buf.at[index, c], {axis: ring(index, d)}))
    lax.fori_loop(1, 4, lambda i, carry: project(i, s["st"]), None)
    swap = remote(s["st"], both.at[c], sib)
    down = [remote(s["hid_t"], buf.at[index, c], sib) for _, index, buf in gathers]
    lax.fori_loop(4, 8, lambda i, carry: project(i, both.at[c]), None)

    def inner(pair, carry):
        cols = rows_of(pair * PAIR, PAIR)
        q, g = s["q"][:, cols], s["g"][:, cols]
        k, v = s["k"][pair], s["v"][pair]
        allowed = causal & (s["segc"][...] == seg_row)
        gap = jnp.bitwise_xor(rows_i, cols_i)
        strict = (rows_i < cols_i).astype(BF16)
        zero = jnp.zeros((TOK, PAIR), BF16)
        weighted, scored, queries, keys, grads, gate_rows, gain_rows = [], [], [], [], [], [], []
        for h in range(2):

            def own(a):
                return jnp.where(low, a, zero) if h == 0 else jnp.where(low, zero, a)

            qh, gh, kh = own(q), own(g), own(k)
            score = dot(qh, k, NT)
            dprob = dot(gh, v, NT)
            spread = s["cumx"][pair, :, 64 * h : 64 * h + 1] - s["cumr3"][pair, h : h + 1, :]
            decay = jnp.where(allowed, jnp.exp(jnp.where(allowed, spread, 0.0)), 0.0)
            ds = decay * score
            joint = ds * dprob
            head = 2 * pair + h
            level = jnp.full((TOK, TOK), gain_ref[0, head], F32)
            gain_rows.append(jnp.sum(jnp.where(gap == 0, joint, 0.0), axis=0, keepdims=True))
            for l in range(1, 8):
                above = gap >= 2 ** (l - 1)
                level = jnp.where(above, gain_ref[l, head], level)
                chosen = above & (gap < 2**l)
                gain_rows.append(jnp.sum(jnp.where(chosen, joint, 0.0), axis=0, keepdims=True))
            wd = level * decay * dprob
            weighted.append(wd.astype(BF16))
            scored.append((level * ds).astype(BF16))
            grid = (wd * score).astype(BF16)
            crossing = jnp.where(causal, dot(grid, strict, NN), 0.0)
            gate_rows.append(jnp.sum(crossing, axis=0, keepdims=True))
            queries.append(qh)
            keys.append(kh)
            grads.append(gh)
        s["qacc"][pair] = dot(
            jnp.concatenate(weighted, axis=1), jnp.concatenate(keys, axis=0), NN
        )
        s["kacc"][pair] = dot(
            jnp.concatenate(weighted, axis=0), jnp.concatenate(queries, axis=0), TN
        )
        s["vacc"][pair] = dot(jnp.concatenate(scored, axis=0), jnp.concatenate(grads, axis=0), TN)
        s["gate"][pair] = jnp.concatenate([*gate_rows, jnp.zeros((6, TOK), F32)], axis=0)
        s["gint"][pair] = jnp.concatenate(gain_rows, axis=0)
        return carry

    swap.wait()

    def meta_rows(total, first, last):
        return jnp.where(
            row8 == 0, total, jnp.where(row8 == 1, first, jnp.where(row8 == 2, last, 0.0))
        )

    chip_send, chip_recv = s["chip_send"], s["chip_recv"]

    def block_pair(pp):
        f0 = both[0, pp * 64 : pp * 64 + 64, :]
        f1 = both[1, pp * 64 : pp * 64 + 64, :]
        r0 = both[0, 512 + pp * 64 : 576 + pp * 64, :]
        r1 = both[1, 512 + pp * 64 : 576 + pp * 64, :]
        m0 = both[0, 1024 + pp * 8 : 1032 + pp * 8, :]
        m1 = both[1, 1024 + pp * 8 : 1032 + pp * 8, :]
        return f0, f1, r0, r1, m0[0:1], m0[1:2], m0[2:3], m1[0:1], m1[1:2], m1[2:3]

    def chip_sums(p):
        for n in range(4):
            f0, f1, r0, r1, t0, first0, last0, t1, first1, last1 = block_pair(2 * n + p)
            chip_send[p, n, 0:64, :] = f1 + linked(last0, last1, t1) * f0
            chip_send[p, n, 64:128, :] = r0 + linked(first0, first1, t0) * r1
            chip_send[p, n, 128:136, :] = meta_rows(t0 + t1, first0, last1)

    def chip_sends(p):
        copies = []
        for d in (2, 1, 3):
            to = ring(x, d)
            copies.append(remote(chip_send.at[p, to], chip_recv.at[p, x], {"x": to}))
        chip_recv[p, pl.ds(x, 1)] = chip_send[p, pl.ds(x, 1)]
        return copies

    chip_sums(0)
    xs = [chip_sends(0)]
    chip_sums(1)
    for pp in range(8):
        f0, _, _, r1, _, _, last0, _, first1, _ = block_pair(pp)
        d8 = same(last0, first1) * jnp.sum(f0 * r1, axis=0, keepdims=True)
        s["gcross"][pl.ds(c * 8 + pp, 1)] = jnp.where(row8 == 0, d8, 0.0)[None]
    lax.fori_loop(0, 4, inner, 0)
    for cp in xs[0]:
        cp.wait_send()
    xs.append(chip_sends(1))
    lax.fori_loop(4, 7, inner, 0)

    def chip(j, p):
        return (
            chip_recv[p, j, 0:64, :],
            chip_recv[p, j, 64:128, :],
            chip_recv[p, j, 128:129, :],
            chip_recv[p, j, 129:130, :],
            chip_recv[p, j, 130:131, :],
        )

    def joined(p):
        (f0, r0, t0, a0, l0), (f1, r1, t1, a1, l1), (f2, r2, t2, a2, l2), (f3, r3, t3, a3, l3) = (
            chip(j, p) for j in range(4)
        )
        f01 = f1 + linked(l0, l1, t1) * f0
        r01 = r0 + linked(a0, a1, t0) * r1
        f23 = f3 + linked(l2, l3, t3) * f2
        r23 = r2 + linked(a2, a3, t2) * r3
        return f01, r01, f23, r23

    tot_send, tot_recv = s["tot_send"], s["tot_recv"]
    zs = []
    for p in range(2):
        for cp in xs[p]:
            if p == 0:
                cp.wait_recv()
            else:
                cp.wait()
        f01, r01, f23, r23 = joined(p)
        t0, a0 = chip(0, p)[2:4]
        t1, l1 = chip(1, p)[2], chip(1, p)[4]
        t2, a2 = chip(2, p)[2:4]
        t3, l3 = chip(3, p)[2], chip(3, p)[4]
        tot_send[p, 0, 0:64, :] = f23 + linked(l1, l3, t2 + t3) * f01
        tot_send[p, 1, 0:64, :] = r01 + linked(a0, a2, t0 + t1) * r23
        tot_send[p, 0, 64:72, :] = jnp.broadcast_to(l3, (8, PAIR))
        tot_send[p, 1, 64:72, :] = jnp.broadcast_to(a0, (8, PAIR))
        zs.append(
            [
                remote(tot_send.at[p, n], tot_recv.at[p, n], {"z": ring(z, d)})
                for n, d in ((0, 1), (1, 3))
            ]
        )

    fwd = []
    for n, (axis, index, buf) in enumerate(gathers):
        for m, d in enumerate((1, 3)):
            hops[2 * n + m].wait()
            came = ring(index, 4 - d)
            part = slice(0, 512) if d == 1 else slice(512, 1024)
            fwd.append(
                remote(buf.at[came, c, part], buf.at[came, c, part], {axis: ring(index, d)})
            )
            down.append(remote(buf.at[came, c], buf.at[came, c], sib))

    lax.fori_loop(7, 9, inner, 0)

    has_prev = (z > 0).astype(F32)
    has_next = (z < 3).astype(F32)
    prev_top = (z == 2).astype(F32)
    next_top = (z == 1).astype(F32)
    back_send, back_recv = s["back_send"], s["back_recv"]

    def gain_row(pair, level):
        return jnp.where(low_row, gain_ref[level, 2 * pair], gain_ref[level, 2 * pair + 1])

    bs = []
    for p in range(2):
        wait(zs[p])
        (f0, r0, t0, a0, l0), (f1, r1, t1, a1, l1), (f2, r2, t2, a2, l2), (f3, r3, t3, a3, l3) = (
            chip(j, p) for j in range(4)
        )
        f01, r01, f23, r23 = joined(p)
        pair = c * 8 + 2 * x + p
        g9, g10, g11, g12 = (gain_row(pair, level) for level in range(9, 13))
        zf = has_prev * tot_recv[p, 0, 0:64, :]
        zl = tot_recv[p, 0, 64:65, :]
        zr = has_next * tot_recv[p, 1, 0:64, :]
        za = tot_recv[p, 1, 64:65, :]
        gzf = g11 * (1.0 - prev_top) + g12 * prev_top
        gzr = g11 * (1.0 - next_top) + g12 * next_top
        sf = (
            gzf * same(zl, a0) * zf,
            gzf * linked(zl, a1, t0) * zf + g9 * same(l0, a1) * f0,
            gzf * linked(zl, a2, t0 + t1) * zf + g10 * same(l1, a2) * f01,
            gzf * linked(zl, a3, t0 + t1 + t2) * zf
            + g10 * linked(l1, a3, t2) * f01
            + g9 * same(l2, a3) * f2,
        )
        sr = (
            gzr * linked(za, l0, t1 + t2 + t3) * zr
            + g10 * linked(l0, a2, t1) * r23
            + g9 * same(l0, a1) * r1,
            gzr * linked(za, l1, t2 + t3) * zr + g10 * same(l1, a2) * r23,
            gzr * linked(za, l2, t3) * zr + g9 * same(l2, a3) * r3,
            gzr * same(za, l3) * zr,
        )
        for j in range(4):
            back_send[p, j, 0:64, :] = sf[j]
            back_send[p, j, 64:128, :] = sr[j]
        copies = []
        for d in (1, 2, 3):
            to = ring(x, d)
            copies.append(remote(back_send.at[p, to], back_recv.at[p, x], {"x": to}))
        back_recv[p, pl.ds(x, 1)] = back_send[p, pl.ds(x, 1)]
        bs.append(copies)

    for p in range(2):
        (f0, r0, t0, a0, l0), (f1, r1, t1, a1, l1), (f2, r2, t2, a2, l2), (f3, r3, t3, a3, l3) = (
            chip(j, p) for j in range(4)
        )
        f01, r01, f23, r23 = joined(p)
        zf = has_prev * tot_recv[p, 0, 0:64, :]
        zl = tot_recv[p, 0, 64:65, :]
        r_group = r01 + linked(a0, a2, t0 + t1) * r23
        d9 = same(l0, a1) * jnp.sum(f0 * r1, axis=0, keepdims=True) + same(l2, a3) * jnp.sum(
            f2 * r3, axis=0, keepdims=True
        )
        d10 = same(l1, a2) * jnp.sum(f01 * r23, axis=0, keepdims=True)
        dz = same(zl, a0) * jnp.sum(zf * r_group, axis=0, keepdims=True)
        rows = jnp.where(
            row8 == 1,
            d9,
            jnp.where(
                row8 == 2,
                d10,
                jnp.where(
                    row8 == 3, (1.0 - prev_top) * dz, jnp.where(row8 == 4, prev_top * dz, 0.0)
                ),
            ),
        )
        pair = c * 8 + 2 * x + p
        s["gcross"][pl.ds(pair, 1)] = s["gcross"][pl.ds(pair, 1)] + rows[None]
    lax.fori_loop(9, 16, inner, 0)

    own_blocks, s_in = s["own_blocks"], s["s_in"]
    swaps = []
    for p in range(2):
        wait(bs[p])
        for n in range(4):
            pp = 2 * n + p
            f0, _, _, r1, t0, first0, last0, t1, first1, last1 = block_pair(pp)
            sf = back_recv[p, n, 0:64, :]
            sr = back_recv[p, n, 64:128, :]
            link = gain_row(c * 8 + pp, 8) * same(last0, first1)
            at = n * 128
            own_blocks[p, 0, at : at + 64, :] = sf
            own_blocks[p, 1, at : at + 64, :] = linked(first0, first1, t0) * sf + link * f0
            own_blocks[p, 0, at + 64 : at + 128, :] = linked(last0, last1, t1) * sr + link * r1
            own_blocks[p, 1, at + 64 : at + 128, :] = sr
        swaps.append(remote(own_blocks.at[p, 1 - c], s_in.at[p, c], sib))
        s_in[p, pl.ds(c, 1)] = own_blocks[p, pl.ds(c, 1)]

    tail = causal.astype(BF16)
    head_pick = (cols_i[0:8, :] // 64 == row8).astype(BF16)

    def diag(a):
        return jnp.concatenate([jnp.where(low_half, a, 0.0), jnp.where(low_half, 0.0, a)], axis=0)

    def incoming(to, p, part):
        at = lax.rem(to, 4) * 128 + part * 64
        return diag(s_in[p, to // 4, rows_of(at, 64), :])

    def key_part(to, p):
        pair = 2 * to + p
        rv = s["lw"][pair] * dot_right(s["v"][pair], incoming(to, p, 1), NT)
        key_sum = (s["kacc"][pair] + rv).astype(BF16)
        s["kacc"][pair] = s["k"][pair].astype(F32) * rv
        s["ksb"][:, rows_of(pair * PAIR, PAIR)] = key_sum
        s["ks"][p, to] = key_sum.astype(F32)

    def value_part(to, p):
        pair = 2 * to + p
        rk = s["lw"][pair] * dot_right(s["k"][pair], incoming(to, p, 1), NN)
        value_sum = (s["vacc"][pair] + rk).astype(BF16)
        s["vsb"][:, rows_of(pair * PAIR, PAIR)] = value_sum
        s["vs"][p, to] = value_sum.astype(F32)

    def query_part(to, p):
        pair = 2 * to + p
        cols = rows_of(pair * PAIR, PAIR)
        sg = s["fw"][pair] * dot_right(s["g"][:, cols], incoming(to, p, 0), NT)
        qg_ref[:, cols] = (s["qacc"][pair] + sg).astype(BF16)
        diff = s["q"][:, cols].astype(F32) * sg - s["kacc"][pair]
        hi, lo = split2(diff)
        diff_rows = dot(head_pick, hi, NT) + dot(head_pick, lo, NT)
        s["gate"][pair] = s["gate"][pair] + dot_left(diff_rows, tail, NN)

    firsts = []
    me_y, me_z = 2 * y + c, 2 * z + c
    far_first = [(2, 0), (2, 1), (1, 0), (3, 0), (1, 1), (3, 1), (0, 1)]
    swaps[0].wait()
    fk, fv = [], []
    for d, e in far_first:
        dev, to = plane("batch", y, d, e)
        key_part(to, 0)
        fk.append(remote(s["ks"].at[0, to], s["rk"].at[0, me_y], dev))
        dev, to = plane("z", z, d, e)
        value_part(to, 0)
        fv.append(remote(s["vs"].at[0, to], s["rv"].at[0, me_z], dev))
    key_part(me_y, 0)
    value_part(me_z, 0)
    firsts.append((fk, fv))
    swaps[1].wait()

    def both_parts(to, carry):
        key_part(to, 1)
        value_part(to, 1)
        return carry

    lax.fori_loop(0, 8, both_parts, 0)
    lax.fori_loop(0, 8, lambda to, carry: query_part(to, 0), None)
    for cp in fk + fv:
        cp.wait_send()
    fk, fv = [], []
    for d, e in far_first:
        dev, to = plane("batch", y, d, e)
        fk.append(remote(s["ks"].at[1, to], s["rk"].at[1, me_y], dev))
        dev, to = plane("z", z, d, e)
        fv.append(remote(s["vs"].at[1, to], s["rv"].at[1, me_z], dev))
    firsts.append((fk, fv))
    for n in range(2):
        s["rk"][n, pl.ds(me_y, 1)] = s["ks"][n, pl.ds(me_y, 1)]
        s["rv"][n, pl.ds(me_z, 1)] = s["vs"][n, pl.ds(me_z, 1)]
    lax.fori_loop(0, 8, lambda to, carry: query_part(to, 1), None)
    stores = []

    def store(ref, hbm):
        cp = pltpu.make_async_copy(ref, hbm, local_sem.at[24 + len(stores)])
        cp.start()
        stores.append(cp)

    store(qg_ref, qg_hbm)
    store(s["gate"], gate_hbm)

    ones = jnp.ones((8, PAIR), F32)
    inner_sum = dot_exact(ones, s["gint"][...].reshape(256, PAIR), NT)
    pick = (cols_i[0:8, :] // 64 == row8 - 2).astype(F32)
    outer_sum = dot_exact(pick, s["gcross"][...].reshape(128, PAIR), NT)
    start = (cols_i[0:8, :] == 0).astype(F32)
    own_total = dot_exact(start, s["gate"][...].reshape(128, TOK), NT)
    small, m1, m1s, m2, m2s, m3 = (s[n] for n in ("small", "m1", "m1s", "m2", "m2s", "m3"))
    small[0:8, :] = jnp.where(
        row8 == 0, inner_sum[:, :128], jnp.where(row8 == 1, inner_sum[:, 128:], outer_sum)
    )
    small[8:16, :] = own_total
    smalls = []
    for d, e in offsets:
        smalls.append(remote(small, m1.at[me_z], plane("z", z, d, e)[0]))
    m1[pl.ds(me_z, 1)] = small[...][None]

    for n, (_, index, buf) in enumerate(gathers):
        buf[pl.ds(index, 1), pl.ds(c, 1)] = s["hid_t"][...][None, None]
        wait(fwd[2 * n : 2 * n + 2])
        came = ring(index, 2)
        down.append(remote(buf.at[came, c], buf.at[came, c], sib))
    wait(down)
    for name, out in (("hy", "hyb"), ("hz", "hzb")):
        for g in range(8):
            s[out][:, g * TOK : (g + 1) * TOK] = s[name][g // 2, g % 2].astype(BF16)

    def product(left, right, n):
        right = s[right][n].reshape(8 * TOK, PAIR).astype(BF16)
        for b in range(4):
            yield b, dot(s[left][b * 256 : (b + 1) * 256, :], right, NN)

    part1, recv1, part2, recv2 = s["part1"], s["recv1"], s["part2"], s["recv2"]

    def scatter(part, recv, chunk, axis, index):
        out = []
        for d in (1, 2, 3):
            to = ring(index, d)
            out.append(remote(part.at[chunk, to], recv.at[chunk, index], {axis: to}))
        recv[chunk, pl.ds(index, 1)] = part[chunk, pl.ds(index, 1)]
        return out

    wait_recv(firsts[0][0])
    for b, block in product("hyb", "rk", 0):
        for j in range(4):
            part1[0, j, b * 64 : b * 64 + 64, :] = block[j * 64 : j * 64 + 64, :]
    k0 = scatter(part1, recv1, 0, "x", x)
    wait_recv(firsts[0][1])
    for b, block in product("hzb", "rv", 0):
        for j in range(4):
            part1[2, j, b * 64 : b * 64 + 64, :] = block[j * 64 : j * 64 + 64, :]
    v0 = scatter(part1, recv1, 2, "x", x)

    def input_grad(n, carry):
        rows = rows_of(n * 256, 256)
        ig_ref[:, rows] = (
            dot(s["ksb"][...], s["wk"][rows, :], NT) + dot(s["vsb"][...], s["wv"][rows, :], NT)
        ).astype(BF16)
        return carry

    lax.fori_loop(0, 2, input_grad, 0)

    wait(firsts[1][0])
    for b, block in product("hyb", "rk", 1):
        part1[1, b] = block
    k1 = scatter(part1, recv1, 1, "z", z)
    wait(firsts[1][1])
    for b, block in product("hzb", "rv", 1):
        for j in range(8):
            for i in range(4):
                at = j * 32 + i * 8
                part1[3, i, b * 64 + j * 8 : b * 64 + j * 8 + 8, :] = block[at : at + 8, :]
    v1 = scatter(part1, recv1, 3, "batch", y)
    lax.fori_loop(2, 4, input_grad, 0)
    store(ig_ref, ig_hbm)

    wait(smalls)
    total = m1[0, 0:8, :]
    for g in range(1, 8):
        total = total + m1[g, 0:8, :]
    m1s[0:8, :] = total
    for g in range(8):
        m1s[8 + g : 9 + g, :] = m1[g, 8:9, :]
    smalls = [remote(m1s, m2.at[x], {"x": ring(x, d)}) for d in (1, 2, 3)]
    m2[pl.ds(x, 1)] = m1s[...][None]

    def summed(recv, chunk):
        return recv[chunk, 0] + recv[chunk, 1] + recv[chunk, 2] + recv[chunk, 3]

    wait(k0)
    total = summed(recv1, 0)
    for j in range(4):
        part2[0, j] = total[j * 64 : j * 64 + 64, :]
    k0 = scatter(part2, recv2, 0, "z", z)
    wait(v0)
    total = summed(recv1, 2)
    for j in range(8):
        for i in range(4):
            at = j * 32 + i * 8
            part2[2, i, j * 8 : j * 8 + 8, :] = total[at : at + 8, :]
    v0 = scatter(part2, recv2, 2, "batch", y)
    wait(k1)
    total = summed(recv1, 1)
    for j in range(4):
        part2[1, j] = total[j * 64 : j * 64 + 64, :]
    k1 = scatter(part2, recv2, 1, "x", x)
    wait(v1)
    total = summed(recv1, 3)
    for j in range(4):
        for i in range(4):
            at = j * 64 + i * 16
            part2[3, i, j * 16 : j * 16 + 16, :] = total[at : at + 16, :]
    v1 = scatter(part2, recv2, 3, "x", x)

    wait(smalls)
    total = m2[0, 0:8, :] + m2[1, 0:8, :] + m2[2, 0:8, :] + m2[3, 0:8, :]
    m2s[...] = total
    smalls = [remote(m2s, m3.at[y], {"batch": ring(y, d)}) for d in (1, 2, 3)]
    m3[pl.ds(y, 1)] = total[None]
    place = z * 8 + x * 2 + c
    later = jnp.zeros((1, PAIR), F32)
    for j in range(4):
        for g in range(8):
            spot = (g // 2) * 8 + j * 2 + g % 2
            later = later + (place < spot).astype(F32) * m2[j, 8 + g : 9 + g, :]
    sout_ref[8:16, :] = jnp.broadcast_to(later, (8, PAIR))

    fins = []
    wait(k0)
    wait(k1)
    for n in range(2):
        total = summed(recv2, n)
        for i in range(4):
            for j in range(2):
                at = j * 32 + i * 8
                s["kown"][2 * i + j, n] = total[at : at + 8, :]
    for d, e in offsets:
        dev, to = plane("batch", y, d, e)
        fins.append(remote(s["kown"].at[to], s["kfin"].at[me_y], dev))
    s["kfin"][pl.ds(me_y, 1)] = s["kown"][pl.ds(me_y, 1)]
    wait(v0)
    wait(v1)
    for n in range(2):
        total = summed(recv2, 2 + n)
        for j in range(8):
            s["vown"][j, n] = total[j * 8 : j * 8 + 8, :]
    for d, e in offsets:
        dev, to = plane("z", z, d, e)
        fins.append(remote(s["vown"].at[to], s["vfin"].at[me_z], dev))
    s["vfin"][pl.ds(me_z, 1)] = s["vown"][pl.ds(me_z, 1)]
    wait(smalls)
    sout_ref[0:8, :] = m3[0] + m3[1] + m3[2] + m3[3]
    store(sout_ref, sout_hbm)
    wait(fins)
    for n in range(2):
        for g in range(8):
            cols = slice((2 * g + n) * PAIR, (2 * g + n + 1) * PAIR)
            kout_ref[:, cols] = s["kfin"][g, n]
            vout_ref[:, cols] = s["vfin"][g, n]
    store(kout_ref, kout_hbm)
    store(vout_ref, vout_hbm)
    wait(stores)


def whole_step(hidden, queries, out_grad, w_key, w_value, log_gate, seg_row, level_gain):
    far = pl.BlockSpec(memory_space=pltpu.HBM)
    return pl.pallas_call(
        step_kernel,
        in_specs=[far] * 8,
        out_specs=[far] * 6,
        out_shape=[
            jax.ShapeDtypeStruct((TOK, 2048), BF16),
            jax.ShapeDtypeStruct((TOK, 1024), BF16),
            jax.ShapeDtypeStruct((16, 8, TOK), F32),
            jax.ShapeDtypeStruct((8, 2048), F32),
            jax.ShapeDtypeStruct((8, 2048), F32),
            jax.ShapeDtypeStruct((16, PAIR), F32),
        ],
        scratch_shapes=list(scratch().values()),
        compiler_params=pltpu.CompilerParams(
            collective_id=0, has_side_effects=True, vmem_limit_bytes=VMEM_LIMIT
        ),
        name="whole_step",
    )(hidden, queries, out_grad, w_key, w_value, log_gate, seg_row, level_gain)


def finish_kernel(
    qg_in, ig_in, gate_in, kw_in, vw_in, small_in, qg_out, ig_out, gate_out, kw_out, vw_out, gains_out,
    qg, ig, gate_ref, kw, vw, small_ref, gate, gains, load_sem, store_sem
):
    loads = [
        pltpu.make_async_copy(a, b, load_sem.at[n])
        for n, (a, b) in enumerate(
            ((gate_in, gate_ref), (small_in, small_ref), (qg_in, qg), (ig_in, ig), (kw_in, kw), (vw_in, vw))
        )
    ]
    for cp in loads:
        cp.start()
    stores = []

    def store(ref, out):
        cp = pltpu.make_async_copy(ref, out, store_sem.at[len(stores)])
        cp.start()
        stores.append(cp)

    loads[0].wait()
    loads[1].wait()
    heads = gate.shape[0]
    lane = iota((heads, PAIR), 1)
    head = iota((heads, PAIR), 0)
    small = small_ref[...]
    later = jnp.broadcast_to(small[8:9, :], (TOK, TOK)).T
    rows = gate_ref[...].reshape(TOK, TOK) + later
    gate[...] = dot_exact((lane == (head // 2) * 8 + head % 2).astype(F32), rows, NN)
    levels = gains.shape[0]
    level, at = iota((levels, PAIR), 0), iota((levels, PAIR), 1) % 8
    first = (level == at).astype(F32)
    second = (level == at + 8).astype(F32)
    pick0 = jnp.where(lane // 8 == head, small[0:1, :], 0.0)
    pick1 = jnp.where(lane // 8 + 16 == head, small[1:2, :], 0.0)
    pair = jnp.where(head % 2 == 0, small[2:3, :], small[3:4, :])
    pick2 = jnp.where(lane // 8 == head // 2, pair, 0.0)
    gains[...] = dot_exact(first, pick0 + pick1, NT) + dot_exact(second, pick2, NT)
    for cp, ref, out in zip(
        loads[2:], (qg, ig, kw, vw), (qg_out, ig_out, kw_out, vw_out)
    ):
        cp.wait()
        store(ref, out)
    store(gate, gate_out)
    store(gains, gains_out)
    for cp in stores:
        cp.wait()


def finish(query_grad, input_grad, gate, key_weight, value_weight, small, heads, levels):
    far = pl.BlockSpec(memory_space=pltpu.HBM)
    parts = (query_grad, input_grad, gate, key_weight, value_weight, small)
    outs = [jax.ShapeDtypeStruct(a.shape, a.dtype) for a in parts]
    outs[2] = jax.ShapeDtypeStruct((heads, TOK), F32)
    outs[5] = jax.ShapeDtypeStruct((levels, heads), F32)
    return pl.pallas_call(
        finish_kernel,
        in_specs=[far] * 6,
        out_specs=[far] * 6,
        out_shape=outs,
        scratch_shapes=[pltpu.VMEM(a.shape, a.dtype) for a in (*parts, outs[2], outs[5])]
        + [pltpu.SemaphoreType.DMA((6,)), pltpu.SemaphoreType.DMA((6,))],
        name="finish",
    )(*parts)


def local(hidden, queries, w_key, w_value, log_gate, level_gain, segment_ids, out_grad):
    heads, levels = level_gain.shape
    parts = whole_step(
        hidden[0], queries[0], out_grad[0], w_key, w_value, log_gate[0], segment_ids, level_gain.T
    )
    query_grad, input_grad, gate_grad, key_weight, value_weight, gains = finish(
        *parts, heads, levels
    )
    return (
        query_grad[None],
        input_grad[None],
        gate_grad[None],
        key_weight,
        value_weight,
        gains.T,
    )


def solution(mesh):
    split = Mesh(
        mesh.devices.reshape(4, 4, 2, mesh.shape["batch"]), ("z", "x", "core", "batch")
    )
    return jax.shard_map(
        local,
        mesh=split,
        in_specs=(
            P("batch", SEQ, None),
            P("batch", SEQ, None),
            P(),
            P(),
            P("batch", None, SEQ),
            P(),
            P("batch", SEQ),
            P("batch", SEQ, None),
        ),
        out_specs=(
            P("batch", SEQ, None),
            P("batch", SEQ, None),
            P("batch", None, SEQ),
            P(SEQ_BATCH, None),
            P(SEQ_BATCH, None),
            P(),
        ),
        check_vma=False,
    )
```

```python
import functools

import jax
import jax.numpy as jnp
from jax import lax
from jax.experimental import pallas as pl
from jax.experimental.pallas import tpu as pltpu
from jax.sharding import Mesh
from jax.sharding import PartitionSpec as P

SEQ = ("z", "x", "core")
SEQ_BATCH = ("z", "x", "core", "batch")
MESH = pl.DeviceIdType.MESH
HIGHEST = lax.Precision.HIGHEST
F32 = jnp.float32
BF16 = jnp.bfloat16

NT = (((1,), (1,)), ((), ()))
TN = (((0,), (0,)), ((), ()))
NN = (((1,), (0,)), ((), ()))

TOK = 128
PAIR = 128
HALF_ROWS = 1088


def dot(a, b, dims):
    return lax.dot_general(a, b, dims, preferred_element_type=F32)


def dot_exact(a, b, dims):
    return lax.dot_general(a, b, dims, preferred_element_type=F32, precision=HIGHEST)


def split2(x):
    hi = x.astype(BF16)
    return hi, (x - hi.astype(F32)).astype(BF16)


def dot_left(a, b, dims):
    hi, lo = split2(a)
    return dot(hi, b, dims) + dot(lo, b, dims)


def dot_right(a, b, dims):
    hi, lo = split2(b)
    return dot(a, hi, dims) + dot(a, lo, dims)


def iota(shape, dim):
    return lax.broadcasted_iota(jnp.int32, shape, dim)


def entry_signal(peers):
    barrier = pltpu.get_barrier_semaphore()
    for peer in peers:
        pl.semaphore_signal(barrier, inc=1, device_id=peer, device_id_type=MESH)
    return barrier


def ring(index, step):
    return lax.rem(index + step, 4)


def same(a, b):
    return jnp.where(a == b, 1.0, 0.0)


def linked(a, b, total):
    return jnp.where(a == b, jnp.exp(total), 0.0)


def rows_of(start, size):
    return pl.ds(pl.multiple_of(start, size), size)


SENDS = 128
LOCALS = 32
VMEM_LIMIT = 56 * 2**20


def scratch():
    def f(*shape):
        return pltpu.VMEM(shape, F32)

    def b(*shape):
        return pltpu.VMEM(shape, BF16)

    return dict(
        wk=b(1024, 2048),
        wv=b(1024, 2048),
        hid=b(TOK, 1024),
        q=b(TOK, 2048),
        g=b(TOK, 2048),
        k=b(16, TOK, PAIR),
        v=b(16, TOK, PAIR),
        hid_t=f(1024, TOK),
        cumx=f(16, TOK, PAIR),
        cumr=f(32, TOK),
        cumr3=f(16, 8, TOK),
        fw=f(16, TOK, PAIR),
        lw=f(16, TOK, PAIR),
        segc=f(TOK, TOK),
        st=f(HALF_ROWS, PAIR),
        both=f(2, HALF_ROWS, PAIR),
        chip_send=f(2, 4, 136, PAIR),
        chip_recv=f(2, 4, 136, PAIR),
        tot_send=f(2, 2, 72, PAIR),
        tot_recv=f(2, 2, 72, PAIR),
        back_send=f(2, 4, 128, PAIR),
        back_recv=f(2, 4, 128, PAIR),
        own_blocks=f(2, 2, 512, PAIR),
        s_in=f(2, 2, 512, PAIR),
        gcross=f(16, 8, PAIR),
        gint=f(16, 16, PAIR),
        gate=f(16, 8, TOK),
        hy=f(4, 2, 1024, TOK),
        hz=f(4, 2, 1024, TOK),
        hyb=b(1024, 8 * TOK),
        hzb=b(1024, 8 * TOK),
        qacc=f(16, TOK, PAIR),
        kacc=f(16, TOK, PAIR),
        vacc=f(16, TOK, PAIR),
        ks=f(2, 8, TOK, PAIR),
        vs=f(2, 8, TOK, PAIR),
        ksb=b(TOK, 2048),
        vsb=b(TOK, 2048),
        rk=f(2, 8, TOK, PAIR),
        rv=f(2, 8, TOK, PAIR),
        part1=f(4, 4, 256, PAIR),
        recv1=f(4, 4, 256, PAIR),
        part2=f(4, 4, 64, PAIR),
        recv2=f(4, 4, 64, PAIR),
        kown=f(8, 2, 8, PAIR),
        vown=f(8, 2, 8, PAIR),
        kfin=f(8, 2, 8, PAIR),
        vfin=f(8, 2, 8, PAIR),
        small=f(16, PAIR),
        m1=f(8, 16, PAIR),
        m1s=f(16, PAIR),
        m2=f(4, 16, PAIR),
        m2s=f(8, PAIR),
        m3=f(4, 8, PAIR),
        lg=f(32, TOK),
        segr=pltpu.VMEM((1, TOK), jnp.int32),
        gain=pltpu.SMEM((18, 32), F32),
        qg=b(TOK, 2048),
        ig=b(TOK, 1024),
        kout=f(8, 2048),
        vout=f(8, 2048),
        sout=f(16, PAIR),
        send_sem=pltpu.SemaphoreType.DMA((SENDS,)),
        recv_sem=pltpu.SemaphoreType.DMA((SENDS,)),
        local_sem=pltpu.SemaphoreType.DMA((LOCALS,)),
    )


def step_kernel(
    hid_hbm,
    q_hbm,
    g_hbm,
    wk_hbm,
    wv_hbm,
    lg_hbm,
    segr_hbm,
    gain_hbm,
    qg_hbm,
    ig_hbm,
    gate_hbm,
    kout_hbm,
    vout_hbm,
    sout_hbm,
    *refs,
):
    s = dict(zip(scratch(), refs))
    gain_ref, qg_ref, ig_ref = s["gain"], s["qg"], s["ig"]
    kout_ref, vout_ref, sout_ref = s["kout"], s["vout"], s["sout"]
    x, y, z, c = (lax.axis_index(a) for a in ("x", "batch", "z", "core"))
    used = [0]

    def remote(src, dst, target):
        n = used[0]
        used[0] += 1
        cp = pltpu.make_async_remote_copy(
            src_ref=src,
            dst_ref=dst,
            send_sem=s["send_sem"].at[n],
            recv_sem=s["recv_sem"].at[n],
            device_id=target,
            device_id_type=MESH,
        )
        cp.start()
        return cp

    def wait(copies):
        for cp in copies:
            cp.wait()

    sib = {"core": 1 - c}
    offsets = [(d, e) for d in range(4) for e in (0, 1) if d or e]

    def plane(axis, index, d, e):
        to, tc = ring(index, d), lax.rem(c + e, 2)
        return {axis: to, "core": tc}, 2 * to + tc

    peers = [plane("batch", y, d, e)[0] for d, e in offsets]
    peers += [plane("z", z, d, e)[0] for d, e in offsets if d]
    peers += [{"x": ring(x, d)} for d in (1, 2, 3)]
    barrier = entry_signal(peers)

    local_sem = s["local_sem"]
    first_loads = [
        pltpu.make_async_copy(hid_hbm, s["hid"], local_sem.at[0]),
        pltpu.make_async_copy(q_hbm, s["q"], local_sem.at[1]),
        pltpu.make_async_copy(g_hbm, s["g"], local_sem.at[2]),
        pltpu.make_async_copy(lg_hbm, s["lg"], local_sem.at[3]),
        pltpu.make_async_copy(segr_hbm, s["segr"], local_sem.at[4]),
        pltpu.make_async_copy(gain_hbm, s["gain"], local_sem.at[5]),
    ]

    def step_at(i):
        return lax.rem(i + 4 - 4 * c, 8)

    def weight_load(hbm, name, i, base):
        cols = rows_of(step_at(i) * 256, 256)
        return pltpu.make_async_copy(hbm.at[:, cols], s[name].at[:, cols], local_sem.at[base + i])

    first_loads[0].start()
    for n in (3, 4, 5):
        first_loads[n].start()
    for i in range(8):
        weight_load(wk_hbm, "wk", i, 8).start()
        weight_load(wv_hbm, "wv", i, 16).start()
        if i == 0:
            first_loads[1].start()
            first_loads[2].start()

    rows_i, cols_i = iota((TOK, TOK), 0), iota((TOK, TOK), 1)
    causal = cols_i <= rows_i
    lower = causal.astype(F32)
    low = cols_i < 64
    low_half = iota((64, PAIR), 1) < 64
    row8 = iota((8, PAIR), 0)
    low_row = iota((1, PAIR), 1) < 64
    for n in (3, 4, 5):
        first_loads[n].wait()
    log_gate = s["lg"][...]
    cum_cols = dot_exact(lower, log_gate, NT)
    s["cumr"][...] = dot_exact(log_gate, lower, NT)
    for pair in range(16):
        s["cumx"][pair] = jnp.where(
            low, cum_cols[:, 2 * pair : 2 * pair + 1], cum_cols[:, 2 * pair + 1 : 2 * pair + 2]
        )
        s["cumr3"][pair, 0:2, :] = s["cumr"][2 * pair : 2 * pair + 2, :]
    seg_row = s["segr"][...].astype(F32)
    s["segc"][...] = jnp.broadcast_to(seg_row, (TOK, TOK)).T
    s["gcross"][...] = jnp.zeros((16, 8, PAIR), F32)

    first_loads[0].wait()
    for b in range(8):
        cols = slice(b * TOK, (b + 1) * TOK)
        s["hid_t"][cols, :] = s["hid"][:, cols].astype(F32).T

    first_loads[1].wait()
    first_loads[2].wait()

    def project(i, st):
        step = step_at(i)
        weight_load(wk_hbm, "wk", i, 8).wait()
        weight_load(wv_hbm, "wv", i, 16).wait()
        wide = rows_of(step * 256, 256)
        hid = s["hid"][...]
        keys = dot(hid, s["wk"][:, wide], NN).astype(BF16)
        values = dot(hid, s["wv"][:, wide], NN).astype(BF16)
        segc = s["segc"][...]
        for p in range(2):
            pair = 2 * step + p
            k, v = keys[:, p * PAIR : (p + 1) * PAIR], values[:, p * PAIR : (p + 1) * PAIR]
            s["k"][pair] = k
            s["v"][pair] = v
            cum = s["cumx"][pair]
            total = cum[TOK - 1 : TOK, :]
            last_w = jnp.where(segc == segc[TOK - 1 : TOK, :], jnp.exp(total - cum), 0.0)
            first_w = jnp.where(segc == segc[0:1, :], jnp.exp(cum), 0.0)
            s["lw"][pair] = last_w
            s["fw"][pair] = first_w
            cols = rows_of(pair * PAIR, PAIR)
            fwd = dot_left(k.astype(F32) * last_w, v, TN)
            rev = dot_left(s["q"][:, cols].astype(F32) * first_w, s["g"][:, cols], TN)
            pp = 2 * lax.rem(step, 4) + p
            st[rows_of(pp * 64, 64), :] = jnp.where(low_half, fwd[:64], fwd[64:])
            st[rows_of(512 + pp * 64, 64), :] = jnp.where(low_half, rev[:64], rev[64:])
            meta = jnp.where(
                row8 == 0,
                total,
                jnp.where(
                    row8 == 1, segc[0:1, :], jnp.where(row8 == 2, segc[TOK - 1 : TOK, :], 0.0)
                ),
            )
            st[rows_of(1024 + pp * 8, 8), :] = meta

    both = s["both"]
    project(0, s["st"])
    pl.semaphore_wait(barrier, len(peers))

    gathers = (("batch", y, s["hy"]), ("z", z, s["hz"]))
    hops = []
    for axis, index, buf in gathers:
        for d in (1, 3):
            hops.append(remote(s["hid_t"], buf.at[index, c], {axis: ring(index, d)}))
    lax.fori_loop(1, 4, lambda i, carry: project(i, s["st"]), None)
    swap = remote(s["st"], both.at[c], sib)
    down = [remote(s["hid_t"], buf.at[index, c], sib) for _, index, buf in gathers]
    lax.fori_loop(4, 8, lambda i, carry: project(i, both.at[c]), None)

    def inner(pair, carry):
        cols = rows_of(pair * PAIR, PAIR)
        q, g = s["q"][:, cols], s["g"][:, cols]
        k, v = s["k"][pair], s["v"][pair]
        allowed = causal & (s["segc"][...] == seg_row)
        gap = jnp.bitwise_xor(rows_i, cols_i)
        strict = (rows_i < cols_i).astype(BF16)
        zero = jnp.zeros((TOK, PAIR), BF16)
        weighted, scored, queries, keys, grads, gate_rows, gain_rows = [], [], [], [], [], [], []
        for h in range(2):

            def own(a):
                return jnp.where(low, a, zero) if h == 0 else jnp.where(low, zero, a)

            qh, gh, kh = own(q), own(g), own(k)
            score = dot(qh, k, NT)
            dprob = dot(gh, v, NT)
            spread = s["cumx"][pair, :, 64 * h : 64 * h + 1] - s["cumr3"][pair, h : h + 1, :]
            decay = jnp.where(allowed, jnp.exp(jnp.where(allowed, spread, 0.0)), 0.0)
            ds = decay * score
            joint = ds * dprob
            head = 2 * pair + h
            level = jnp.full((TOK, TOK), gain_ref[0, head], F32)
            gain_rows.append(jnp.sum(jnp.where(gap == 0, joint, 0.0), axis=0, keepdims=True))
            for l in range(1, 8):
                above = gap >= 2 ** (l - 1)
                level = jnp.where(above, gain_ref[l, head], level)
                chosen = above & (gap < 2**l)
                gain_rows.append(jnp.sum(jnp.where(chosen, joint, 0.0), axis=0, keepdims=True))
            wd = level * decay * dprob
            weighted.append(wd.astype(BF16))
            scored.append((level * ds).astype(BF16))
            grid = (wd * score).astype(BF16)
            crossing = jnp.where(causal, dot(grid, strict, NN), 0.0)
            gate_rows.append(jnp.sum(crossing, axis=0, keepdims=True))
            queries.append(qh)
            keys.append(kh)
            grads.append(gh)
        s["qacc"][pair] = dot(
            jnp.concatenate(weighted, axis=1), jnp.concatenate(keys, axis=0), NN
        )
        s["kacc"][pair] = dot(
            jnp.concatenate(weighted, axis=0), jnp.concatenate(queries, axis=0), TN
        )
        s["vacc"][pair] = dot(jnp.concatenate(scored, axis=0), jnp.concatenate(grads, axis=0), TN)
        s["gate"][pair] = jnp.concatenate([*gate_rows, jnp.zeros((6, TOK), F32)], axis=0)
        s["gint"][pair] = jnp.concatenate(gain_rows, axis=0)
        return carry

    swap.wait()

    def meta_rows(total, first, last):
        return jnp.where(
            row8 == 0, total, jnp.where(row8 == 1, first, jnp.where(row8 == 2, last, 0.0))
        )

    chip_send, chip_recv = s["chip_send"], s["chip_recv"]

    def block_pair(pp):
        f0 = both[0, pp * 64 : pp * 64 + 64, :]
        f1 = both[1, pp * 64 : pp * 64 + 64, :]
        r0 = both[0, 512 + pp * 64 : 576 + pp * 64, :]
        r1 = both[1, 512 + pp * 64 : 576 + pp * 64, :]
        m0 = both[0, 1024 + pp * 8 : 1032 + pp * 8, :]
        m1 = both[1, 1024 + pp * 8 : 1032 + pp * 8, :]
        return f0, f1, r0, r1, m0[0:1], m0[1:2], m0[2:3], m1[0:1], m1[1:2], m1[2:3]

    def chip_sums(p):
        for n in range(4):
            f0, f1, r0, r1, t0, first0, last0, t1, first1, last1 = block_pair(2 * n + p)
            chip_send[p, n, 0:64, :] = f1 + linked(last0, last1, t1) * f0
            chip_send[p, n, 64:128, :] = r0 + linked(first0, first1, t0) * r1
            chip_send[p, n, 128:136, :] = meta_rows(t0 + t1, first0, last1)

    def chip_sends(p):
        copies = []
        for d in (2, 1, 3):
            to = ring(x, d)
            copies.append(remote(chip_send.at[p, to], chip_recv.at[p, x], {"x": to}))
        chip_recv[p, pl.ds(x, 1)] = chip_send[p, pl.ds(x, 1)]
        return copies

    xs = []
    for p in range(2):
        chip_sums(p)
        xs.append(chip_sends(p))
    for pp in range(8):
        f0, _, _, r1, _, _, last0, _, first1, _ = block_pair(pp)
        d8 = same(last0, first1) * jnp.sum(f0 * r1, axis=0, keepdims=True)
        s["gcross"][pl.ds(c * 8 + pp, 1)] = jnp.where(row8 == 0, d8, 0.0)[None]
    lax.fori_loop(0, 7, inner, 0)

    def chip(j, p):
        return (
            chip_recv[p, j, 0:64, :],
            chip_recv[p, j, 64:128, :],
            chip_recv[p, j, 128:129, :],
            chip_recv[p, j, 129:130, :],
            chip_recv[p, j, 130:131, :],
        )

    def joined(p):
        (f0, r0, t0, a0, l0), (f1, r1, t1, a1, l1), (f2, r2, t2, a2, l2), (f3, r3, t3, a3, l3) = (
            chip(j, p) for j in range(4)
        )
        f01 = f1 + linked(l0, l1, t1) * f0
        r01 = r0 + linked(a0, a1, t0) * r1
        f23 = f3 + linked(l2, l3, t3) * f2
        r23 = r2 + linked(a2, a3, t2) * r3
        return f01, r01, f23, r23

    tot_send, tot_recv = s["tot_send"], s["tot_recv"]
    zs = []
    for p in range(2):
        wait(xs[p])
        f01, r01, f23, r23 = joined(p)
        t0, a0 = chip(0, p)[2:4]
        t1, l1 = chip(1, p)[2], chip(1, p)[4]
        t2, a2 = chip(2, p)[2:4]
        t3, l3 = chip(3, p)[2], chip(3, p)[4]
        tot_send[p, 0, 0:64, :] = f23 + linked(l1, l3, t2 + t3) * f01
        tot_send[p, 1, 0:64, :] = r01 + linked(a0, a2, t0 + t1) * r23
        tot_send[p, 0, 64:72, :] = jnp.broadcast_to(l3, (8, PAIR))
        tot_send[p, 1, 64:72, :] = jnp.broadcast_to(a0, (8, PAIR))
        zs.append(
            [
                remote(tot_send.at[p, n], tot_recv.at[p, n], {"z": ring(z, d)})
                for n, d in ((0, 1), (1, 3))
            ]
        )

    fwd = []
    for n, (axis, index, buf) in enumerate(gathers):
        for m, d in enumerate((1, 3)):
            hops[2 * n + m].wait()
            came = ring(index, 4 - d)
            part = slice(0, 512) if d == 1 else slice(512, 1024)
            fwd.append(
                remote(buf.at[came, c, part], buf.at[came, c, part], {axis: ring(index, d)})
            )
            down.append(remote(buf.at[came, c], buf.at[came, c], sib))

    lax.fori_loop(7, 9, inner, 0)

    has_prev = (z > 0).astype(F32)
    has_next = (z < 3).astype(F32)
    prev_top = (z == 2).astype(F32)
    next_top = (z == 1).astype(F32)
    back_send, back_recv = s["back_send"], s["back_recv"]

    def gain_row(pair, level):
        return jnp.where(low_row, gain_ref[level, 2 * pair], gain_ref[level, 2 * pair + 1])

    bs = []
    for p in range(2):
        wait(zs[p])
        (f0, r0, t0, a0, l0), (f1, r1, t1, a1, l1), (f2, r2, t2, a2, l2), (f3, r3, t3, a3, l3) = (
            chip(j, p) for j in range(4)
        )
        f01, r01, f23, r23 = joined(p)
        pair = c * 8 + 2 * x + p
        g9, g10, g11, g12 = (gain_row(pair, level) for level in range(9, 13))
        zf = has_prev * tot_recv[p, 0, 0:64, :]
        zl = tot_recv[p, 0, 64:65, :]
        zr = has_next * tot_recv[p, 1, 0:64, :]
        za = tot_recv[p, 1, 64:65, :]
        gzf = g11 * (1.0 - prev_top) + g12 * prev_top
        gzr = g11 * (1.0 - next_top) + g12 * next_top
        sf = (
            gzf * same(zl, a0) * zf,
            gzf * linked(zl, a1, t0) * zf + g9 * same(l0, a1) * f0,
            gzf * linked(zl, a2, t0 + t1) * zf + g10 * same(l1, a2) * f01,
            gzf * linked(zl, a3, t0 + t1 + t2) * zf
            + g10 * linked(l1, a3, t2) * f01
            + g9 * same(l2, a3) * f2,
        )
        sr = (
            gzr * linked(za, l0, t1 + t2 + t3) * zr
            + g10 * linked(l0, a2, t1) * r23
            + g9 * same(l0, a1) * r1,
            gzr * linked(za, l1, t2 + t3) * zr + g10 * same(l1, a2) * r23,
            gzr * linked(za, l2, t3) * zr + g9 * same(l2, a3) * r3,
            gzr * same(za, l3) * zr,
        )
        for j in range(4):
            back_send[p, j, 0:64, :] = sf[j]
            back_send[p, j, 64:128, :] = sr[j]
        copies = []
        for d in (1, 2, 3):
            to = ring(x, d)
            copies.append(remote(back_send.at[p, to], back_recv.at[p, x], {"x": to}))
        back_recv[p, pl.ds(x, 1)] = back_send[p, pl.ds(x, 1)]
        bs.append(copies)

    for p in range(2):
        (f0, r0, t0, a0, l0), (f1, r1, t1, a1, l1), (f2, r2, t2, a2, l2), (f3, r3, t3, a3, l3) = (
            chip(j, p) for j in range(4)
        )
        f01, r01, f23, r23 = joined(p)
        zf = has_prev * tot_recv[p, 0, 0:64, :]
        zl = tot_recv[p, 0, 64:65, :]
        r_group = r01 + linked(a0, a2, t0 + t1) * r23
        d9 = same(l0, a1) * jnp.sum(f0 * r1, axis=0, keepdims=True) + same(l2, a3) * jnp.sum(
            f2 * r3, axis=0, keepdims=True
        )
        d10 = same(l1, a2) * jnp.sum(f01 * r23, axis=0, keepdims=True)
        dz = same(zl, a0) * jnp.sum(zf * r_group, axis=0, keepdims=True)
        rows = jnp.where(
            row8 == 1,
            d9,
            jnp.where(
                row8 == 2,
                d10,
                jnp.where(
                    row8 == 3, (1.0 - prev_top) * dz, jnp.where(row8 == 4, prev_top * dz, 0.0)
                ),
            ),
        )
        pair = c * 8 + 2 * x + p
        s["gcross"][pl.ds(pair, 1)] = s["gcross"][pl.ds(pair, 1)] + rows[None]
    lax.fori_loop(9, 16, inner, 0)
    for n, (_, index, buf) in enumerate(gathers):
        buf[pl.ds(index, 1), pl.ds(c, 1)] = s["hid_t"][...][None, None]
        wait(fwd[2 * n : 2 * n + 2])
        came = ring(index, 2)
        down.append(remote(buf.at[came, c], buf.at[came, c], sib))

    own_blocks, s_in = s["own_blocks"], s["s_in"]
    swaps = []
    for p in range(2):
        wait(bs[p])
        for n in range(4):
            pp = 2 * n + p
            f0, _, _, r1, t0, first0, last0, t1, first1, last1 = block_pair(pp)
            sf = back_recv[p, n, 0:64, :]
            sr = back_recv[p, n, 64:128, :]
            link = gain_row(c * 8 + pp, 8) * same(last0, first1)
            at = n * 128
            own_blocks[p, 0, at : at + 64, :] = sf
            own_blocks[p, 1, at : at + 64, :] = linked(first0, first1, t0) * sf + link * f0
            own_blocks[p, 0, at + 64 : at + 128, :] = linked(last0, last1, t1) * sr + link * r1
            own_blocks[p, 1, at + 64 : at + 128, :] = sr
        swaps.append(remote(own_blocks.at[p, 1 - c], s_in.at[p, c], sib))
        s_in[p, pl.ds(c, 1)] = own_blocks[p, pl.ds(c, 1)]

    tail = causal.astype(BF16)
    head_pick = (cols_i[0:8, :] // 64 == row8).astype(BF16)

    def diag(a):
        return jnp.concatenate([jnp.where(low_half, a, 0.0), jnp.where(low_half, 0.0, a)], axis=0)

    def incoming(to, p, part):
        at = lax.rem(to, 4) * 128 + part * 64
        return diag(s_in[p, to // 4, rows_of(at, 64), :])

    def key_part(to, p):
        pair = 2 * to + p
        rv = s["lw"][pair] * dot_right(s["v"][pair], incoming(to, p, 1), NT)
        key_sum = (s["kacc"][pair] + rv).astype(BF16)
        s["kacc"][pair] = s["k"][pair].astype(F32) * rv
        s["ksb"][:, rows_of(pair * PAIR, PAIR)] = key_sum
        s["ks"][p, to] = key_sum.astype(F32)

    def value_part(to, p):
        pair = 2 * to + p
        rk = s["lw"][pair] * dot_right(s["k"][pair], incoming(to, p, 1), NN)
        value_sum = (s["vacc"][pair] + rk).astype(BF16)
        s["vsb"][:, rows_of(pair * PAIR, PAIR)] = value_sum
        s["vs"][p, to] = value_sum.astype(F32)

    def query_part(to, p):
        pair = 2 * to + p
        cols = rows_of(pair * PAIR, PAIR)
        sg = s["fw"][pair] * dot_right(s["g"][:, cols], incoming(to, p, 0), NT)
        qg_ref[:, cols] = (s["qacc"][pair] + sg).astype(BF16)
        diff = s["q"][:, cols].astype(F32) * sg - s["kacc"][pair]
        hi, lo = split2(diff)
        diff_rows = dot(head_pick, hi, NT) + dot(head_pick, lo, NT)
        s["gate"][pair] = s["gate"][pair] + dot_left(diff_rows, tail, NN)

    firsts = []
    me_y, me_z = 2 * y + c, 2 * z + c
    far_first = [(2, 0), (2, 1), (1, 0), (3, 0), (1, 1), (3, 1), (0, 1)]
    for n in range(2):
        swaps[n].wait()
        fk, fv = [], []
        for d, e in far_first:
            dev, to = plane("batch", y, d, e)
            key_part(to, n)
            fk.append(remote(s["ks"].at[n, to], s["rk"].at[n, me_y], dev))
            dev, to = plane("z", z, d, e)
            value_part(to, n)
            fv.append(remote(s["vs"].at[n, to], s["rv"].at[n, me_z], dev))
        key_part(me_y, n)
        value_part(me_z, n)
        firsts.append((fk, fv))
    for n in range(2):
        s["rk"][n, pl.ds(me_y, 1)] = s["ks"][n, pl.ds(me_y, 1)]
        s["rv"][n, pl.ds(me_z, 1)] = s["vs"][n, pl.ds(me_z, 1)]

    wait(down)
    for name, out in (("hy", "hyb"), ("hz", "hzb")):
        for g in range(8):
            s[out][:, g * TOK : (g + 1) * TOK] = s[name][g // 2, g % 2].astype(BF16)

    for n in range(2):
        lax.fori_loop(0, 8, lambda to, carry: query_part(to, n), None)
    stores = []

    def store(ref, hbm):
        cp = pltpu.make_async_copy(ref, hbm, local_sem.at[24 + len(stores)])
        cp.start()
        stores.append(cp)

    store(qg_ref, qg_hbm)
    store(s["gate"], gate_hbm)

    def product(left, right, n):
        right = s[right][n].reshape(8 * TOK, PAIR).astype(BF16)
        for b in range(4):
            yield b, dot(s[left][b * 256 : (b + 1) * 256, :], right, NN)

    part1, recv1, part2, recv2 = s["part1"], s["recv1"], s["part2"], s["recv2"]

    def scatter(part, recv, chunk, axis, index):
        out = []
        for d in (1, 2, 3):
            to = ring(index, d)
            out.append(remote(part.at[chunk, to], recv.at[chunk, index], {axis: to}))
        recv[chunk, pl.ds(index, 1)] = part[chunk, pl.ds(index, 1)]
        return out

    wait(firsts[0][0])
    for b, block in product("hyb", "rk", 0):
        for j in range(4):
            part1[0, j, b * 64 : b * 64 + 64, :] = block[j * 64 : j * 64 + 64, :]
    k0 = scatter(part1, recv1, 0, "x", x)
    wait(firsts[0][1])
    for b, block in product("hzb", "rv", 0):
        for j in range(4):
            part1[2, j, b * 64 : b * 64 + 64, :] = block[j * 64 : j * 64 + 64, :]
    v0 = scatter(part1, recv1, 2, "x", x)

    ones = jnp.ones((8, PAIR), F32)
    inner_sum = dot_exact(ones, s["gint"][...].reshape(256, PAIR), NT)
    pick = (cols_i[0:8, :] // 64 == row8 - 2).astype(F32)
    outer_sum = dot_exact(pick, s["gcross"][...].reshape(128, PAIR), NT)
    start = (cols_i[0:8, :] == 0).astype(F32)
    own_total = dot_exact(start, s["gate"][...].reshape(128, TOK), NT)
    small, m1, m1s, m2, m2s, m3 = (s[n] for n in ("small", "m1", "m1s", "m2", "m2s", "m3"))
    small[0:8, :] = jnp.where(
        row8 == 0, inner_sum[:, :128], jnp.where(row8 == 1, inner_sum[:, 128:], outer_sum)
    )
    small[8:16, :] = own_total
    smalls = []
    for d, e in offsets:
        smalls.append(remote(small, m1.at[me_z], plane("z", z, d, e)[0]))
    m1[pl.ds(me_z, 1)] = small[...][None]

    def input_grad(n, carry):
        rows = rows_of(n * 256, 256)
        ig_ref[:, rows] = (
            dot(s["ksb"][...], s["wk"][rows, :], NT) + dot(s["vsb"][...], s["wv"][rows, :], NT)
        ).astype(BF16)
        return carry

    lax.fori_loop(0, 2, input_grad, 0)

    wait(firsts[1][0])
    for b, block in product("hyb", "rk", 1):
        part1[1, b] = block
    k1 = scatter(part1, recv1, 1, "z", z)
    wait(firsts[1][1])
    for b, block in product("hzb", "rv", 1):
        for j in range(8):
            for i in range(4):
                at = j * 32 + i * 8
                part1[3, i, b * 64 + j * 8 : b * 64 + j * 8 + 8, :] = block[at : at + 8, :]
    v1 = scatter(part1, recv1, 3, "batch", y)
    lax.fori_loop(2, 4, input_grad, 0)
    store(ig_ref, ig_hbm)

    wait(smalls)
    total = m1[0, 0:8, :]
    for g in range(1, 8):
        total = total + m1[g, 0:8, :]
    m1s[0:8, :] = total
    for g in range(8):
        m1s[8 + g : 9 + g, :] = m1[g, 8:9, :]
    smalls = [remote(m1s, m2.at[x], {"x": ring(x, d)}) for d in (1, 2, 3)]
    m2[pl.ds(x, 1)] = m1s[...][None]

    def summed(recv, chunk):
        return recv[chunk, 0] + recv[chunk, 1] + recv[chunk, 2] + recv[chunk, 3]

    wait(k0)
    total = summed(recv1, 0)
    for j in range(4):
        part2[0, j] = total[j * 64 : j * 64 + 64, :]
    k0 = scatter(part2, recv2, 0, "z", z)
    wait(v0)
    total = summed(recv1, 2)
    for j in range(8):
        for i in range(4):
            at = j * 32 + i * 8
            part2[2, i, j * 8 : j * 8 + 8, :] = total[at : at + 8, :]
    v0 = scatter(part2, recv2, 2, "batch", y)
    wait(k1)
    total = summed(recv1, 1)
    for j in range(4):
        part2[1, j] = total[j * 64 : j * 64 + 64, :]
    k1 = scatter(part2, recv2, 1, "x", x)
    wait(v1)
    total = summed(recv1, 3)
    for j in range(4):
        for i in range(4):
            at = j * 64 + i * 16
            part2[3, i, j * 16 : j * 16 + 16, :] = total[at : at + 16, :]
    v1 = scatter(part2, recv2, 3, "x", x)

    wait(smalls)
    total = m2[0, 0:8, :] + m2[1, 0:8, :] + m2[2, 0:8, :] + m2[3, 0:8, :]
    m2s[...] = total
    smalls = [remote(m2s, m3.at[y], {"batch": ring(y, d)}) for d in (1, 2, 3)]
    m3[pl.ds(y, 1)] = total[None]
    place = z * 8 + x * 2 + c
    later = jnp.zeros((1, PAIR), F32)
    for j in range(4):
        for g in range(8):
            spot = (g // 2) * 8 + j * 2 + g % 2
            later = later + (place < spot).astype(F32) * m2[j, 8 + g : 9 + g, :]
    sout_ref[8:16, :] = jnp.broadcast_to(later, (8, PAIR))

    fins = []
    wait(k0)
    wait(k1)
    for n in range(2):
        total = summed(recv2, n)
        for i in range(4):
            for j in range(2):
                at = j * 32 + i * 8
                s["kown"][2 * i + j, n] = total[at : at + 8, :]
    for d, e in offsets:
        dev, to = plane("batch", y, d, e)
        fins.append(remote(s["kown"].at[to], s["kfin"].at[me_y], dev))
    s["kfin"][pl.ds(me_y, 1)] = s["kown"][pl.ds(me_y, 1)]
    wait(v0)
    wait(v1)
    for n in range(2):
        total = summed(recv2, 2 + n)
        for j in range(8):
            s["vown"][j, n] = total[j * 8 : j * 8 + 8, :]
    for d, e in offsets:
        dev, to = plane("z", z, d, e)
        fins.append(remote(s["vown"].at[to], s["vfin"].at[me_z], dev))
    s["vfin"][pl.ds(me_z, 1)] = s["vown"][pl.ds(me_z, 1)]
    wait(smalls)
    sout_ref[0:8, :] = m3[0] + m3[1] + m3[2] + m3[3]
    store(sout_ref, sout_hbm)
    wait(fins)
    for n in range(2):
        for g in range(8):
            cols = slice((2 * g + n) * PAIR, (2 * g + n + 1) * PAIR)
            kout_ref[:, cols] = s["kfin"][g, n]
            vout_ref[:, cols] = s["vfin"][g, n]
    store(kout_ref, kout_hbm)
    store(vout_ref, vout_hbm)
    wait(stores)


def whole_step(hidden, queries, out_grad, w_key, w_value, log_gate, seg_row, level_gain):
    far = pl.BlockSpec(memory_space=pltpu.HBM)
    return pl.pallas_call(
        step_kernel,
        in_specs=[far] * 8,
        out_specs=[far] * 6,
        out_shape=[
            jax.ShapeDtypeStruct((TOK, 2048), BF16),
            jax.ShapeDtypeStruct((TOK, 1024), BF16),
            jax.ShapeDtypeStruct((16, 8, TOK), F32),
            jax.ShapeDtypeStruct((8, 2048), F32),
            jax.ShapeDtypeStruct((8, 2048), F32),
            jax.ShapeDtypeStruct((16, PAIR), F32),
        ],
        scratch_shapes=list(scratch().values()),
        compiler_params=pltpu.CompilerParams(
            collective_id=0, has_side_effects=True, vmem_limit_bytes=VMEM_LIMIT
        ),
        name="whole_step",
    )(hidden, queries, out_grad, w_key, w_value, log_gate, seg_row, level_gain)


def finish_kernel(
    qg_in, ig_in, gate_in, kw_in, vw_in, small_in, qg_out, ig_out, gate_out, kw_out, vw_out, gains_out,
    qg, ig, gate_ref, kw, vw, small_ref, gate, gains, load_sem, store_sem
):
    loads = [
        pltpu.make_async_copy(a, b, load_sem.at[n])
        for n, (a, b) in enumerate(
            ((gate_in, gate_ref), (small_in, small_ref), (qg_in, qg), (ig_in, ig), (kw_in, kw), (vw_in, vw))
        )
    ]
    for cp in loads:
        cp.start()
    stores = []

    def store(ref, out):
        cp = pltpu.make_async_copy(ref, out, store_sem.at[len(stores)])
        cp.start()
        stores.append(cp)

    loads[0].wait()
    loads[1].wait()
    heads = gate.shape[0]
    lane = iota((heads, PAIR), 1)
    head = iota((heads, PAIR), 0)
    small = small_ref[...]
    later = jnp.broadcast_to(small[8:9, :], (TOK, TOK)).T
    rows = gate_ref[...].reshape(TOK, TOK) + later
    gate[...] = dot_exact((lane == (head // 2) * 8 + head % 2).astype(F32), rows, NN)
    levels = gains.shape[0]
    level, at = iota((levels, PAIR), 0), iota((levels, PAIR), 1) % 8
    first = (level == at).astype(F32)
    second = (level == at + 8).astype(F32)
    pick0 = jnp.where(lane // 8 == head, small[0:1, :], 0.0)
    pick1 = jnp.where(lane // 8 + 16 == head, small[1:2, :], 0.0)
    pair = jnp.where(head % 2 == 0, small[2:3, :], small[3:4, :])
    pick2 = jnp.where(lane // 8 == head // 2, pair, 0.0)
    gains[...] = dot_exact(first, pick0 + pick1, NT) + dot_exact(second, pick2, NT)
    for cp, ref, out in zip(
        loads[2:], (qg, ig, kw, vw), (qg_out, ig_out, kw_out, vw_out)
    ):
        cp.wait()
        store(ref, out)
    store(gate, gate_out)
    store(gains, gains_out)
    for cp in stores:
        cp.wait()


def finish(query_grad, input_grad, gate, key_weight, value_weight, small, heads, levels):
    far = pl.BlockSpec(memory_space=pltpu.HBM)
    parts = (query_grad, input_grad, gate, key_weight, value_weight, small)
    outs = [jax.ShapeDtypeStruct(a.shape, a.dtype) for a in parts]
    outs[2] = jax.ShapeDtypeStruct((heads, TOK), F32)
    outs[5] = jax.ShapeDtypeStruct((levels, heads), F32)
    return pl.pallas_call(
        finish_kernel,
        in_specs=[far] * 6,
        out_specs=[far] * 6,
        out_shape=outs,
        scratch_shapes=[pltpu.VMEM(a.shape, a.dtype) for a in (*parts, outs[2], outs[5])]
        + [pltpu.SemaphoreType.DMA((6,)), pltpu.SemaphoreType.DMA((6,))],
        name="finish",
    )(*parts)


def local(hidden, queries, w_key, w_value, log_gate, level_gain, segment_ids, out_grad):
    heads, levels = level_gain.shape
    parts = whole_step(
        hidden[0], queries[0], out_grad[0], w_key, w_value, log_gate[0], segment_ids, level_gain.T
    )
    query_grad, input_grad, gate_grad, key_weight, value_weight, gains = finish(
        *parts, heads, levels
    )
    return (
        query_grad[None],
        input_grad[None],
        gate_grad[None],
        key_weight,
        value_weight,
        gains.T,
    )


def solution(mesh):
    split = Mesh(
        mesh.devices.reshape(4, 4, 2, mesh.shape["batch"]), ("z", "x", "core", "batch")
    )
    return jax.shard_map(
        local,
        mesh=split,
        in_specs=(
            P("batch", SEQ, None),
            P("batch", SEQ, None),
            P(),
            P(),
            P("batch", None, SEQ),
            P(),
            P("batch", SEQ),
            P("batch", SEQ, None),
        ),
        out_specs=(
            P("batch", SEQ, None),
            P("batch", SEQ, None),
            P("batch", None, SEQ),
            P(SEQ_BATCH, None),
            P(SEQ_BATCH, None),
            P(),
        ),
        check_vma=False,
    )
```

```python
import functools

import jax
import jax.numpy as jnp
from jax import lax
from jax.experimental import pallas as pl
from jax.experimental.pallas import tpu as pltpu
from jax.sharding import Mesh
from jax.sharding import PartitionSpec as P

SEQ = ("z", "x", "core")
SEQ_BATCH = ("z", "x", "core", "batch")
MESH = pl.DeviceIdType.MESH
HIGHEST = lax.Precision.HIGHEST
F32 = jnp.float32
BF16 = jnp.bfloat16

NT = (((1,), (1,)), ((), ()))
TN = (((0,), (0,)), ((), ()))
NN = (((1,), (0,)), ((), ()))

TOK = 128
PAIR = 128
HALF_ROWS = 1088


def dot(a, b, dims):
    return lax.dot_general(a, b, dims, preferred_element_type=F32)


def dot_exact(a, b, dims):
    return lax.dot_general(a, b, dims, preferred_element_type=F32, precision=HIGHEST)


def split2(x):
    hi = x.astype(BF16)
    return hi, (x - hi.astype(F32)).astype(BF16)


def dot_left(a, b, dims):
    hi, lo = split2(a)
    return dot(hi, b, dims) + dot(lo, b, dims)


def dot_right(a, b, dims):
    hi, lo = split2(b)
    return dot(a, hi, dims) + dot(a, lo, dims)


def iota(shape, dim):
    return lax.broadcasted_iota(jnp.int32, shape, dim)


def entry_signal(peers):
    barrier = pltpu.get_barrier_semaphore()
    for peer in peers:
        pl.semaphore_signal(barrier, inc=1, device_id=peer, device_id_type=MESH)
    return barrier


def ring(index, step):
    return lax.rem(index + step, 4)


def same(a, b):
    return jnp.where(a == b, 1.0, 0.0)


def linked(a, b, total):
    return jnp.where(a == b, jnp.exp(total), 0.0)


def rows_of(start, size):
    return pl.ds(pl.multiple_of(start, size), size)


SENDS = 128
LOCALS = 32
VMEM_LIMIT = 56 * 2**20


def scratch():
    def f(*shape):
        return pltpu.VMEM(shape, F32)

    def b(*shape):
        return pltpu.VMEM(shape, BF16)

    return dict(
        wk=b(1024, 2048),
        wv=b(1024, 2048),
        hid=b(TOK, 1024),
        q=b(TOK, 2048),
        g=b(TOK, 2048),
        k=b(16, TOK, PAIR),
        v=b(16, TOK, PAIR),
        hid_t=f(1024, TOK),
        cumx=f(16, TOK, PAIR),
        cumr=f(32, TOK),
        cumr3=f(16, 8, TOK),
        fw=f(16, TOK, PAIR),
        lw=f(16, TOK, PAIR),
        segc=f(TOK, TOK),
        st=f(HALF_ROWS, PAIR),
        both=f(2, HALF_ROWS, PAIR),
        chip_send=f(2, 4, 136, PAIR),
        chip_recv=f(2, 4, 136, PAIR),
        tot_send=f(2, 2, 72, PAIR),
        tot_recv=f(2, 2, 72, PAIR),
        back_send=f(2, 4, 128, PAIR),
        back_recv=f(2, 4, 128, PAIR),
        own_blocks=f(2, 2, 512, PAIR),
        s_in=f(2, 2, 512, PAIR),
        gcross=f(16, 8, PAIR),
        gint=f(16, 16, PAIR),
        gate=f(16, 8, TOK),
        hy=f(4, 2, 1024, TOK),
        hz=f(4, 2, 1024, TOK),
        hyb=b(1024, 8 * TOK),
        hzb=b(1024, 8 * TOK),
        qacc=f(16, TOK, PAIR),
        kacc=f(16, TOK, PAIR),
        vacc=f(16, TOK, PAIR),
        ks=f(2, 8, TOK, PAIR),
        vs=f(2, 8, TOK, PAIR),
        ksb=b(TOK, 2048),
        vsb=b(TOK, 2048),
        rk=f(2, 8, TOK, PAIR),
        rv=f(2, 8, TOK, PAIR),
        part1=f(4, 4, 256, PAIR),
        recv1=f(4, 4, 256, PAIR),
        part2=f(4, 4, 64, PAIR),
        recv2=f(4, 4, 64, PAIR),
        kown=f(8, 2, 8, PAIR),
        vown=f(8, 2, 8, PAIR),
        kfin=f(8, 2, 8, PAIR),
        vfin=f(8, 2, 8, PAIR),
        small=f(16, PAIR),
        m1=f(8, 16, PAIR),
        m1s=f(16, PAIR),
        m2=f(4, 16, PAIR),
        m2s=f(8, PAIR),
        m3=f(4, 8, PAIR),
        lg=f(32, TOK),
        segr=pltpu.VMEM((1, TOK), jnp.int32),
        gain=pltpu.SMEM((18, 32), F32),
        qg=b(TOK, 2048),
        ig=b(TOK, 1024),
        kout=f(8, 2048),
        vout=f(8, 2048),
        sout=f(16, PAIR),
        send_sem=pltpu.SemaphoreType.DMA((SENDS,)),
        recv_sem=pltpu.SemaphoreType.DMA((SENDS,)),
        local_sem=pltpu.SemaphoreType.DMA((LOCALS,)),
    )


def step_kernel(
    hid_hbm,
    q_hbm,
    g_hbm,
    wk_hbm,
    wv_hbm,
    lg_hbm,
    segr_hbm,
    gain_hbm,
    qg_hbm,
    ig_hbm,
    gate_hbm,
    kout_hbm,
    vout_hbm,
    sout_hbm,
    *refs,
):
    s = dict(zip(scratch(), refs))
    gain_ref, qg_ref, ig_ref = s["gain"], s["qg"], s["ig"]
    kout_ref, vout_ref, sout_ref = s["kout"], s["vout"], s["sout"]
    x, y, z, c = (lax.axis_index(a) for a in ("x", "batch", "z", "core"))
    used = [0]

    def remote(src, dst, target):
        n = used[0]
        used[0] += 1
        cp = pltpu.make_async_remote_copy(
            src_ref=src,
            dst_ref=dst,
            send_sem=s["send_sem"].at[n],
            recv_sem=s["recv_sem"].at[n],
            device_id=target,
            device_id_type=MESH,
        )
        cp.start()
        return cp

    def wait(copies):
        for cp in copies:
            cp.wait()

    sib = {"core": 1 - c}
    offsets = [(d, e) for d in range(4) for e in (0, 1) if d or e]

    def plane(axis, index, d, e):
        to, tc = ring(index, d), lax.rem(c + e, 2)
        return {axis: to, "core": tc}, 2 * to + tc

    peers = [plane("batch", y, d, e)[0] for d, e in offsets]
    peers += [plane("z", z, d, e)[0] for d, e in offsets if d]
    peers += [{"x": ring(x, d)} for d in (1, 2, 3)]
    barrier = entry_signal(peers)

    local_sem = s["local_sem"]
    first_loads = [
        pltpu.make_async_copy(hid_hbm, s["hid"], local_sem.at[0]),
        pltpu.make_async_copy(q_hbm, s["q"], local_sem.at[1]),
        pltpu.make_async_copy(g_hbm, s["g"], local_sem.at[2]),
        pltpu.make_async_copy(lg_hbm, s["lg"], local_sem.at[3]),
        pltpu.make_async_copy(segr_hbm, s["segr"], local_sem.at[4]),
        pltpu.make_async_copy(gain_hbm, s["gain"], local_sem.at[5]),
    ]

    def step_at(i):
        return lax.rem(i + 4 - 4 * c, 8)

    def weight_load(hbm, name, i, base):
        cols = rows_of(step_at(i) * 256, 256)
        return pltpu.make_async_copy(hbm.at[:, cols], s[name].at[:, cols], local_sem.at[base + i])

    first_loads[0].start()
    for n in (3, 4, 5):
        first_loads[n].start()
    for i in range(8):
        weight_load(wk_hbm, "wk", i, 8).start()
        weight_load(wv_hbm, "wv", i, 16).start()
        if i == 0:
            first_loads[1].start()
            first_loads[2].start()

    rows_i, cols_i = iota((TOK, TOK), 0), iota((TOK, TOK), 1)
    causal = cols_i <= rows_i
    lower = causal.astype(F32)
    low = cols_i < 64
    low_half = iota((64, PAIR), 1) < 64
    row8 = iota((8, PAIR), 0)
    low_row = iota((1, PAIR), 1) < 64
    for n in (3, 4, 5):
        first_loads[n].wait()
    log_gate = s["lg"][...]
    cum_cols = dot_exact(lower, log_gate, NT)
    s["cumr"][...] = dot_exact(log_gate, lower, NT)
    for pair in range(16):
        s["cumx"][pair] = jnp.where(
            low, cum_cols[:, 2 * pair : 2 * pair + 1], cum_cols[:, 2 * pair + 1 : 2 * pair + 2]
        )
        s["cumr3"][pair, 0:2, :] = s["cumr"][2 * pair : 2 * pair + 2, :]
    seg_row = s["segr"][...].astype(F32)
    s["segc"][...] = jnp.broadcast_to(seg_row, (TOK, TOK)).T
    s["gcross"][...] = jnp.zeros((16, 8, PAIR), F32)

    first_loads[0].wait()
    for b in range(8):
        cols = slice(b * TOK, (b + 1) * TOK)
        s["hid_t"][cols, :] = s["hid"][:, cols].astype(F32).T

    first_loads[1].wait()
    first_loads[2].wait()

    def project(i, st):
        step = step_at(i)
        weight_load(wk_hbm, "wk", i, 8).wait()
        weight_load(wv_hbm, "wv", i, 16).wait()
        wide = rows_of(step * 256, 256)
        hid = s["hid"][...]
        keys = dot(hid, s["wk"][:, wide], NN).astype(BF16)
        values = dot(hid, s["wv"][:, wide], NN).astype(BF16)
        segc = s["segc"][...]
        for p in range(2):
            pair = 2 * step + p
            k, v = keys[:, p * PAIR : (p + 1) * PAIR], values[:, p * PAIR : (p + 1) * PAIR]
            s["k"][pair] = k
            s["v"][pair] = v
            cum = s["cumx"][pair]
            total = cum[TOK - 1 : TOK, :]
            last_w = jnp.where(segc == segc[TOK - 1 : TOK, :], jnp.exp(total - cum), 0.0)
            first_w = jnp.where(segc == segc[0:1, :], jnp.exp(cum), 0.0)
            s["lw"][pair] = last_w
            s["fw"][pair] = first_w
            cols = rows_of(pair * PAIR, PAIR)
            fwd = dot_left(k.astype(F32) * last_w, v, TN)
            rev = dot_left(s["q"][:, cols].astype(F32) * first_w, s["g"][:, cols], TN)
            pp = 2 * lax.rem(step, 4) + p
            st[rows_of(pp * 64, 64), :] = jnp.where(low_half, fwd[:64], fwd[64:])
            st[rows_of(512 + pp * 64, 64), :] = jnp.where(low_half, rev[:64], rev[64:])
            meta = jnp.where(
                row8 == 0,
                total,
                jnp.where(
                    row8 == 1, segc[0:1, :], jnp.where(row8 == 2, segc[TOK - 1 : TOK, :], 0.0)
                ),
            )
            st[rows_of(1024 + pp * 8, 8), :] = meta

    both = s["both"]
    project(0, s["st"])
    pl.semaphore_wait(barrier, len(peers))

    gathers = (("batch", y, s["hy"]), ("z", z, s["hz"]))
    hops = []
    for axis, index, buf in gathers:
        for d in (1, 3):
            hops.append(remote(s["hid_t"], buf.at[index, c], {axis: ring(index, d)}))
    lax.fori_loop(1, 4, lambda i, carry: project(i, s["st"]), None)
    swap = remote(s["st"], both.at[c], sib)
    down = [remote(s["hid_t"], buf.at[index, c], sib) for _, index, buf in gathers]
    lax.fori_loop(4, 8, lambda i, carry: project(i, both.at[c]), None)

    def inner(pair, carry):
        cols = rows_of(pair * PAIR, PAIR)
        q, g = s["q"][:, cols], s["g"][:, cols]
        k, v = s["k"][pair], s["v"][pair]
        allowed = causal & (s["segc"][...] == seg_row)
        gap = jnp.bitwise_xor(rows_i, cols_i)
        strict = (rows_i < cols_i).astype(BF16)
        zero = jnp.zeros((TOK, PAIR), BF16)
        weighted, scored, queries, keys, grads, gate_rows, gain_rows = [], [], [], [], [], [], []
        for h in range(2):

            def own(a):
                return jnp.where(low, a, zero) if h == 0 else jnp.where(low, zero, a)

            qh, gh, kh = own(q), own(g), own(k)
            score = dot(qh, k, NT)
            dprob = dot(gh, v, NT)
            spread = s["cumx"][pair, :, 64 * h : 64 * h + 1] - s["cumr3"][pair, h : h + 1, :]
            decay = jnp.where(allowed, jnp.exp(jnp.where(allowed, spread, 0.0)), 0.0)
            ds = decay * score
            joint = ds * dprob
            head = 2 * pair + h
            level = jnp.full((TOK, TOK), gain_ref[0, head], F32)
            gain_rows.append(jnp.sum(jnp.where(gap == 0, joint, 0.0), axis=0, keepdims=True))
            for l in range(1, 8):
                above = gap >= 2 ** (l - 1)
                level = jnp.where(above, gain_ref[l, head], level)
                chosen = above & (gap < 2**l)
                gain_rows.append(jnp.sum(jnp.where(chosen, joint, 0.0), axis=0, keepdims=True))
            wd = level * decay * dprob
            weighted.append(wd.astype(BF16))
            scored.append((level * ds).astype(BF16))
            grid = (wd * score).astype(BF16)
            crossing = jnp.where(causal, dot(grid, strict, NN), 0.0)
            gate_rows.append(jnp.sum(crossing, axis=0, keepdims=True))
            queries.append(qh)
            keys.append(kh)
            grads.append(gh)
        s["qacc"][pair] = dot(
            jnp.concatenate(weighted, axis=1), jnp.concatenate(keys, axis=0), NN
        )
        s["kacc"][pair] = dot(
            jnp.concatenate(weighted, axis=0), jnp.concatenate(queries, axis=0), TN
        )
        s["vacc"][pair] = dot(jnp.concatenate(scored, axis=0), jnp.concatenate(grads, axis=0), TN)
        s["gate"][pair] = jnp.concatenate([*gate_rows, jnp.zeros((6, TOK), F32)], axis=0)
        s["gint"][pair] = jnp.concatenate(gain_rows, axis=0)
        return carry

    swap.wait()

    def meta_rows(total, first, last):
        return jnp.where(
            row8 == 0, total, jnp.where(row8 == 1, first, jnp.where(row8 == 2, last, 0.0))
        )

    chip_send, chip_recv = s["chip_send"], s["chip_recv"]

    def block_pair(pp):
        f0 = both[0, pp * 64 : pp * 64 + 64, :]
        f1 = both[1, pp * 64 : pp * 64 + 64, :]
        r0 = both[0, 512 + pp * 64 : 576 + pp * 64, :]
        r1 = both[1, 512 + pp * 64 : 576 + pp * 64, :]
        m0 = both[0, 1024 + pp * 8 : 1032 + pp * 8, :]
        m1 = both[1, 1024 + pp * 8 : 1032 + pp * 8, :]
        return f0, f1, r0, r1, m0[0:1], m0[1:2], m0[2:3], m1[0:1], m1[1:2], m1[2:3]

    def chip_sums(p):
        for n in range(4):
            f0, f1, r0, r1, t0, first0, last0, t1, first1, last1 = block_pair(2 * n + p)
            chip_send[p, n, 0:64, :] = f1 + linked(last0, last1, t1) * f0
            chip_send[p, n, 64:128, :] = r0 + linked(first0, first1, t0) * r1
            chip_send[p, n, 128:136, :] = meta_rows(t0 + t1, first0, last1)

    def chip_sends(p):
        copies = []
        for d in (2, 1, 3):
            to = ring(x, d)
            copies.append(remote(chip_send.at[p, to], chip_recv.at[p, x], {"x": to}))
        chip_recv[p, pl.ds(x, 1)] = chip_send[p, pl.ds(x, 1)]
        return copies

    xs = []
    for p in range(2):
        chip_sums(p)
        xs.append(chip_sends(p))
    for pp in range(8):
        f0, _, _, r1, _, _, last0, _, first1, _ = block_pair(pp)
        d8 = same(last0, first1) * jnp.sum(f0 * r1, axis=0, keepdims=True)
        s["gcross"][pl.ds(c * 8 + pp, 1)] = jnp.where(row8 == 0, d8, 0.0)[None]
    lax.fori_loop(0, 7, inner, 0)

    def chip(j, p):
        return (
            chip_recv[p, j, 0:64, :],
            chip_recv[p, j, 64:128, :],
            chip_recv[p, j, 128:129, :],
            chip_recv[p, j, 129:130, :],
            chip_recv[p, j, 130:131, :],
        )

    def joined(p):
        (f0, r0, t0, a0, l0), (f1, r1, t1, a1, l1), (f2, r2, t2, a2, l2), (f3, r3, t3, a3, l3) = (
            chip(j, p) for j in range(4)
        )
        f01 = f1 + linked(l0, l1, t1) * f0
        r01 = r0 + linked(a0, a1, t0) * r1
        f23 = f3 + linked(l2, l3, t3) * f2
        r23 = r2 + linked(a2, a3, t2) * r3
        return f01, r01, f23, r23

    tot_send, tot_recv = s["tot_send"], s["tot_recv"]
    zs = []
    for p in range(2):
        wait(xs[p])
        f01, r01, f23, r23 = joined(p)
        t0, a0 = chip(0, p)[2:4]
        t1, l1 = chip(1, p)[2], chip(1, p)[4]
        t2, a2 = chip(2, p)[2:4]
        t3, l3 = chip(3, p)[2], chip(3, p)[4]
        tot_send[p, 0, 0:64, :] = f23 + linked(l1, l3, t2 + t3) * f01
        tot_send[p, 1, 0:64, :] = r01 + linked(a0, a2, t0 + t1) * r23
        tot_send[p, 0, 64:72, :] = jnp.broadcast_to(l3, (8, PAIR))
        tot_send[p, 1, 64:72, :] = jnp.broadcast_to(a0, (8, PAIR))
        zs.append(
            [
                remote(tot_send.at[p, n], tot_recv.at[p, n], {"z": ring(z, d)})
                for n, d in ((0, 1), (1, 3))
            ]
        )

    fwd = []
    for n, (axis, index, buf) in enumerate(gathers):
        for m, d in enumerate((1, 3)):
            hops[2 * n + m].wait()
            came = ring(index, 4 - d)
            part = slice(0, 512) if d == 1 else slice(512, 1024)
            fwd.append(
                remote(buf.at[came, c, part], buf.at[came, c, part], {axis: ring(index, d)})
            )
            down.append(remote(buf.at[came, c], buf.at[came, c], sib))

    lax.fori_loop(7, 9, inner, 0)

    has_prev = (z > 0).astype(F32)
    has_next = (z < 3).astype(F32)
    prev_top = (z == 2).astype(F32)
    next_top = (z == 1).astype(F32)
    back_send, back_recv = s["back_send"], s["back_recv"]

    def gain_row(pair, level):
        return jnp.where(low_row, gain_ref[level, 2 * pair], gain_ref[level, 2 * pair + 1])

    bs = []
    for p in range(2):
        wait(zs[p])
        (f0, r0, t0, a0, l0), (f1, r1, t1, a1, l1), (f2, r2, t2, a2, l2), (f3, r3, t3, a3, l3) = (
            chip(j, p) for j in range(4)
        )
        f01, r01, f23, r23 = joined(p)
        pair = c * 8 + 2 * x + p
        g9, g10, g11, g12 = (gain_row(pair, level) for level in range(9, 13))
        zf = has_prev * tot_recv[p, 0, 0:64, :]
        zl = tot_recv[p, 0, 64:65, :]
        zr = has_next * tot_recv[p, 1, 0:64, :]
        za = tot_recv[p, 1, 64:65, :]
        gzf = g11 * (1.0 - prev_top) + g12 * prev_top
        gzr = g11 * (1.0 - next_top) + g12 * next_top
        sf = (
            gzf * same(zl, a0) * zf,
            gzf * linked(zl, a1, t0) * zf + g9 * same(l0, a1) * f0,
            gzf * linked(zl, a2, t0 + t1) * zf + g10 * same(l1, a2) * f01,
            gzf * linked(zl, a3, t0 + t1 + t2) * zf
            + g10 * linked(l1, a3, t2) * f01
            + g9 * same(l2, a3) * f2,
        )
        sr = (
            gzr * linked(za, l0, t1 + t2 + t3) * zr
            + g10 * linked(l0, a2, t1) * r23
            + g9 * same(l0, a1) * r1,
            gzr * linked(za, l1, t2 + t3) * zr + g10 * same(l1, a2) * r23,
            gzr * linked(za, l2, t3) * zr + g9 * same(l2, a3) * r3,
            gzr * same(za, l3) * zr,
        )
        for j in range(4):
            back_send[p, j, 0:64, :] = sf[j]
            back_send[p, j, 64:128, :] = sr[j]
        copies = []
        for d in (1, 2, 3):
            to = ring(x, d)
            copies.append(remote(back_send.at[p, to], back_recv.at[p, x], {"x": to}))
        back_recv[p, pl.ds(x, 1)] = back_send[p, pl.ds(x, 1)]
        bs.append(copies)

    for p in range(2):
        (f0, r0, t0, a0, l0), (f1, r1, t1, a1, l1), (f2, r2, t2, a2, l2), (f3, r3, t3, a3, l3) = (
            chip(j, p) for j in range(4)
        )
        f01, r01, f23, r23 = joined(p)
        zf = has_prev * tot_recv[p, 0, 0:64, :]
        zl = tot_recv[p, 0, 64:65, :]
        r_group = r01 + linked(a0, a2, t0 + t1) * r23
        d9 = same(l0, a1) * jnp.sum(f0 * r1, axis=0, keepdims=True) + same(l2, a3) * jnp.sum(
            f2 * r3, axis=0, keepdims=True
        )
        d10 = same(l1, a2) * jnp.sum(f01 * r23, axis=0, keepdims=True)
        dz = same(zl, a0) * jnp.sum(zf * r_group, axis=0, keepdims=True)
        rows = jnp.where(
            row8 == 1,
            d9,
            jnp.where(
                row8 == 2,
                d10,
                jnp.where(
                    row8 == 3, (1.0 - prev_top) * dz, jnp.where(row8 == 4, prev_top * dz, 0.0)
                ),
            ),
        )
        pair = c * 8 + 2 * x + p
        s["gcross"][pl.ds(pair, 1)] = s["gcross"][pl.ds(pair, 1)] + rows[None]
    lax.fori_loop(9, 16, inner, 0)
    def rounded(n, block, core):
        buf, out = gathers[n][2], s[("hyb", "hzb")[n]]
        out[:, rows_of((2 * block + core) * TOK, TOK)] = buf[block, core].astype(BF16)

    for n, (_, index, buf) in enumerate(gathers):
        s[("hyb", "hzb")[n]][:, rows_of((2 * index + c) * TOK, TOK)] = s["hid_t"][...].astype(BF16)
        down[n].wait()
        rounded(n, index, 1 - c)
        for m, d in enumerate((1, 3)):
            came = ring(index, 4 - d)
            rounded(n, came, c)
            down[2 + 2 * n + m].wait()
            rounded(n, came, 1 - c)
    for n, (_, index, buf) in enumerate(gathers):
        wait(fwd[2 * n : 2 * n + 2])
        came = ring(index, 2)
        down.append(remote(buf.at[came, c], buf.at[came, c], sib))

    own_blocks, s_in = s["own_blocks"], s["s_in"]
    swaps = []
    for p in range(2):
        wait(bs[p])
        for n in range(4):
            pp = 2 * n + p
            f0, _, _, r1, t0, first0, last0, t1, first1, last1 = block_pair(pp)
            sf = back_recv[p, n, 0:64, :]
            sr = back_recv[p, n, 64:128, :]
            link = gain_row(c * 8 + pp, 8) * same(last0, first1)
            at = n * 128
            own_blocks[p, 0, at : at + 64, :] = sf
            own_blocks[p, 1, at : at + 64, :] = linked(first0, first1, t0) * sf + link * f0
            own_blocks[p, 0, at + 64 : at + 128, :] = linked(last0, last1, t1) * sr + link * r1
            own_blocks[p, 1, at + 64 : at + 128, :] = sr
        swaps.append(remote(own_blocks.at[p, 1 - c], s_in.at[p, c], sib))
        s_in[p, pl.ds(c, 1)] = own_blocks[p, pl.ds(c, 1)]

    tail = causal.astype(BF16)
    head_pick = (cols_i[0:8, :] // 64 == row8).astype(BF16)

    def diag(a):
        return jnp.concatenate([jnp.where(low_half, a, 0.0), jnp.where(low_half, 0.0, a)], axis=0)

    def incoming(to, p, part):
        at = lax.rem(to, 4) * 128 + part * 64
        return diag(s_in[p, to // 4, rows_of(at, 64), :])

    def key_part(to, p):
        pair = 2 * to + p
        rv = s["lw"][pair] * dot_right(s["v"][pair], incoming(to, p, 1), NT)
        key_sum = (s["kacc"][pair] + rv).astype(BF16)
        s["kacc"][pair] = s["k"][pair].astype(F32) * rv
        s["ksb"][:, rows_of(pair * PAIR, PAIR)] = key_sum
        s["ks"][p, to] = key_sum.astype(F32)

    def value_part(to, p):
        pair = 2 * to + p
        rk = s["lw"][pair] * dot_right(s["k"][pair], incoming(to, p, 1), NN)
        value_sum = (s["vacc"][pair] + rk).astype(BF16)
        s["vsb"][:, rows_of(pair * PAIR, PAIR)] = value_sum
        s["vs"][p, to] = value_sum.astype(F32)

    def query_part(to, p):
        pair = 2 * to + p
        cols = rows_of(pair * PAIR, PAIR)
        sg = s["fw"][pair] * dot_right(s["g"][:, cols], incoming(to, p, 0), NT)
        qg_ref[:, cols] = (s["qacc"][pair] + sg).astype(BF16)
        diff = s["q"][:, cols].astype(F32) * sg - s["kacc"][pair]
        hi, lo = split2(diff)
        diff_rows = dot(head_pick, hi, NT) + dot(head_pick, lo, NT)
        s["gate"][pair] = s["gate"][pair] + dot_left(diff_rows, tail, NN)

    firsts = []
    me_y, me_z = 2 * y + c, 2 * z + c
    far_first = [(2, 0), (2, 1), (1, 0), (3, 0), (1, 1), (3, 1), (0, 1)]
    for n in range(2):
        swaps[n].wait()
        fk, fv = [], []
        for d, e in far_first:
            dev, to = plane("batch", y, d, e)
            key_part(to, n)
            fk.append(remote(s["ks"].at[n, to], s["rk"].at[n, me_y], dev))
            dev, to = plane("z", z, d, e)
            value_part(to, n)
            fv.append(remote(s["vs"].at[n, to], s["rv"].at[n, me_z], dev))
        key_part(me_y, n)
        value_part(me_z, n)
        firsts.append((fk, fv))
    for n in range(2):
        s["rk"][n, pl.ds(me_y, 1)] = s["ks"][n, pl.ds(me_y, 1)]
        s["rv"][n, pl.ds(me_z, 1)] = s["vs"][n, pl.ds(me_z, 1)]

    for n, (_, index, buf) in enumerate(gathers):
        came = ring(index, 2)
        rounded(n, came, c)
        down[6 + n].wait()
        rounded(n, came, 1 - c)

    def product(left, right, n):
        right = s[right][n].reshape(8 * TOK, PAIR).astype(BF16)
        for b in range(4):
            yield b, dot(s[left][b * 256 : (b + 1) * 256, :], right, NN)

    part1, recv1, part2, recv2 = s["part1"], s["recv1"], s["part2"], s["recv2"]

    def scatter(part, recv, chunk, axis, index):
        out = []
        for d in (1, 2, 3):
            to = ring(index, d)
            out.append(remote(part.at[chunk, to], recv.at[chunk, index], {axis: to}))
        recv[chunk, pl.ds(index, 1)] = part[chunk, pl.ds(index, 1)]
        return out

    wait(firsts[0][0])
    for b, block in product("hyb", "rk", 0):
        for j in range(4):
            part1[0, j, b * 64 : b * 64 + 64, :] = block[j * 64 : j * 64 + 64, :]
    k0 = scatter(part1, recv1, 0, "x", x)
    wait(firsts[0][1])
    for b, block in product("hzb", "rv", 0):
        for j in range(4):
            part1[2, j, b * 64 : b * 64 + 64, :] = block[j * 64 : j * 64 + 64, :]
    v0 = scatter(part1, recv1, 2, "x", x)

    for n in range(2):
        lax.fori_loop(0, 8, lambda to, carry: query_part(to, n), None)
    stores = []

    def store(ref, hbm):
        cp = pltpu.make_async_copy(ref, hbm, local_sem.at[24 + len(stores)])
        cp.start()
        stores.append(cp)

    store(qg_ref, qg_hbm)
    store(s["gate"], gate_hbm)

    ones = jnp.ones((8, PAIR), F32)
    inner_sum = dot_exact(ones, s["gint"][...].reshape(256, PAIR), NT)
    pick = (cols_i[0:8, :] // 64 == row8 - 2).astype(F32)
    outer_sum = dot_exact(pick, s["gcross"][...].reshape(128, PAIR), NT)
    start = (cols_i[0:8, :] == 0).astype(F32)
    own_total = dot_exact(start, s["gate"][...].reshape(128, TOK), NT)
    small, m1, m1s, m2, m2s, m3 = (s[n] for n in ("small", "m1", "m1s", "m2", "m2s", "m3"))
    small[0:8, :] = jnp.where(
        row8 == 0, inner_sum[:, :128], jnp.where(row8 == 1, inner_sum[:, 128:], outer_sum)
    )
    small[8:16, :] = own_total
    smalls = []
    for d, e in offsets:
        smalls.append(remote(small, m1.at[me_z], plane("z", z, d, e)[0]))
    m1[pl.ds(me_z, 1)] = small[...][None]

    def input_grad(n, carry):
        rows = rows_of(n * 256, 256)
        ig_ref[:, rows] = (
            dot(s["ksb"][...], s["wk"][rows, :], NT) + dot(s["vsb"][...], s["wv"][rows, :], NT)
        ).astype(BF16)
        return carry

    lax.fori_loop(0, 2, input_grad, 0)

    wait(firsts[1][0])
    for b, block in product("hyb", "rk", 1):
        part1[1, b] = block
    k1 = scatter(part1, recv1, 1, "z", z)
    wait(firsts[1][1])
    for b, block in product("hzb", "rv", 1):
        for j in range(8):
            for i in range(4):
                at = j * 32 + i * 8
                part1[3, i, b * 64 + j * 8 : b * 64 + j * 8 + 8, :] = block[at : at + 8, :]
    v1 = scatter(part1, recv1, 3, "batch", y)
    lax.fori_loop(2, 4, input_grad, 0)
    store(ig_ref, ig_hbm)

    wait(smalls)
    total = m1[0, 0:8, :]
    for g in range(1, 8):
        total = total + m1[g, 0:8, :]
    m1s[0:8, :] = total
    for g in range(8):
        m1s[8 + g : 9 + g, :] = m1[g, 8:9, :]
    smalls = [remote(m1s, m2.at[x], {"x": ring(x, d)}) for d in (1, 2, 3)]
    m2[pl.ds(x, 1)] = m1s[...][None]

    def summed(recv, chunk):
        return recv[chunk, 0] + recv[chunk, 1] + recv[chunk, 2] + recv[chunk, 3]

    wait(k0)
    total = summed(recv1, 0)
    for j in range(4):
        part2[0, j] = total[j * 64 : j * 64 + 64, :]
    k0 = scatter(part2, recv2, 0, "z", z)
    wait(v0)
    total = summed(recv1, 2)
    for j in range(8):
        for i in range(4):
            at = j * 32 + i * 8
            part2[2, i, j * 8 : j * 8 + 8, :] = total[at : at + 8, :]
    v0 = scatter(part2, recv2, 2, "batch", y)
    wait(k1)
    total = summed(recv1, 1)
    for j in range(4):
        part2[1, j] = total[j * 64 : j * 64 + 64, :]
    k1 = scatter(part2, recv2, 1, "x", x)
    wait(v1)
    total = summed(recv1, 3)
    for j in range(4):
        for i in range(4):
            at = j * 64 + i * 16
            part2[3, i, j * 16 : j * 16 + 16, :] = total[at : at + 16, :]
    v1 = scatter(part2, recv2, 3, "x", x)

    wait(smalls)
    total = m2[0, 0:8, :] + m2[1, 0:8, :] + m2[2, 0:8, :] + m2[3, 0:8, :]
    m2s[...] = total
    smalls = [remote(m2s, m3.at[y], {"batch": ring(y, d)}) for d in (1, 2, 3)]
    m3[pl.ds(y, 1)] = total[None]
    place = z * 8 + x * 2 + c
    later = jnp.zeros((1, PAIR), F32)
    for j in range(4):
        for g in range(8):
            spot = (g // 2) * 8 + j * 2 + g % 2
            later = later + (place < spot).astype(F32) * m2[j, 8 + g : 9 + g, :]
    sout_ref[8:16, :] = jnp.broadcast_to(later, (8, PAIR))

    fins = []
    wait(k0)
    wait(k1)
    for n in range(2):
        total = summed(recv2, n)
        for i in range(4):
            for j in range(2):
                at = j * 32 + i * 8
                s["kown"][2 * i + j, n] = total[at : at + 8, :]
    for d, e in offsets:
        dev, to = plane("batch", y, d, e)
        fins.append(remote(s["kown"].at[to], s["kfin"].at[me_y], dev))
    s["kfin"][pl.ds(me_y, 1)] = s["kown"][pl.ds(me_y, 1)]
    wait(v0)
    wait(v1)
    for n in range(2):
        total = summed(recv2, 2 + n)
        for j in range(8):
            s["vown"][j, n] = total[j * 8 : j * 8 + 8, :]
    for d, e in offsets:
        dev, to = plane("z", z, d, e)
        fins.append(remote(s["vown"].at[to], s["vfin"].at[me_z], dev))
    s["vfin"][pl.ds(me_z, 1)] = s["vown"][pl.ds(me_z, 1)]
    wait(smalls)
    sout_ref[0:8, :] = m3[0] + m3[1] + m3[2] + m3[3]
    store(sout_ref, sout_hbm)
    wait(fins)
    for n in range(2):
        for g in range(8):
            cols = slice((2 * g + n) * PAIR, (2 * g + n + 1) * PAIR)
            kout_ref[:, cols] = s["kfin"][g, n]
            vout_ref[:, cols] = s["vfin"][g, n]
    store(kout_ref, kout_hbm)
    store(vout_ref, vout_hbm)
    wait(stores)


def whole_step(hidden, queries, out_grad, w_key, w_value, log_gate, seg_row, level_gain):
    far = pl.BlockSpec(memory_space=pltpu.HBM)
    return pl.pallas_call(
        step_kernel,
        in_specs=[far] * 8,
        out_specs=[far] * 6,
        out_shape=[
            jax.ShapeDtypeStruct((TOK, 2048), BF16),
            jax.ShapeDtypeStruct((TOK, 1024), BF16),
            jax.ShapeDtypeStruct((16, 8, TOK), F32),
            jax.ShapeDtypeStruct((8, 2048), F32),
            jax.ShapeDtypeStruct((8, 2048), F32),
            jax.ShapeDtypeStruct((16, PAIR), F32),
        ],
        scratch_shapes=list(scratch().values()),
        compiler_params=pltpu.CompilerParams(
            collective_id=0, has_side_effects=True, vmem_limit_bytes=VMEM_LIMIT
        ),
        name="whole_step",
    )(hidden, queries, out_grad, w_key, w_value, log_gate, seg_row, level_gain)


def finish_kernel(
    qg_in, ig_in, gate_in, kw_in, vw_in, small_in, qg_out, ig_out, gate_out, kw_out, vw_out, gains_out,
    qg, ig, gate_ref, kw, vw, small_ref, gate, gains, load_sem, store_sem
):
    loads = [
        pltpu.make_async_copy(a, b, load_sem.at[n])
        for n, (a, b) in enumerate(
            ((gate_in, gate_ref), (small_in, small_ref), (qg_in, qg), (ig_in, ig), (kw_in, kw), (vw_in, vw))
        )
    ]
    for cp in loads:
        cp.start()
    stores = []

    def store(ref, out):
        cp = pltpu.make_async_copy(ref, out, store_sem.at[len(stores)])
        cp.start()
        stores.append(cp)

    loads[0].wait()
    loads[1].wait()
    heads = gate.shape[0]
    lane = iota((heads, PAIR), 1)
    head = iota((heads, PAIR), 0)
    small = small_ref[...]
    later = jnp.broadcast_to(small[8:9, :], (TOK, TOK)).T
    rows = gate_ref[...].reshape(TOK, TOK) + later
    gate[...] = dot_exact((lane == (head // 2) * 8 + head % 2).astype(F32), rows, NN)
    levels = gains.shape[0]
    level, at = iota((levels, PAIR), 0), iota((levels, PAIR), 1) % 8
    first = (level == at).astype(F32)
    second = (level == at + 8).astype(F32)
    pick0 = jnp.where(lane // 8 == head, small[0:1, :], 0.0)
    pick1 = jnp.where(lane // 8 + 16 == head, small[1:2, :], 0.0)
    pair = jnp.where(head % 2 == 0, small[2:3, :], small[3:4, :])
    pick2 = jnp.where(lane // 8 == head // 2, pair, 0.0)
    gains[...] = dot_exact(first, pick0 + pick1, NT) + dot_exact(second, pick2, NT)
    for cp, ref, out in zip(
        loads[2:], (qg, ig, kw, vw), (qg_out, ig_out, kw_out, vw_out)
    ):
        cp.wait()
        store(ref, out)
    store(gate, gate_out)
    store(gains, gains_out)
    for cp in stores:
        cp.wait()


def finish(query_grad, input_grad, gate, key_weight, value_weight, small, heads, levels):
    far = pl.BlockSpec(memory_space=pltpu.HBM)
    parts = (query_grad, input_grad, gate, key_weight, value_weight, small)
    outs = [jax.ShapeDtypeStruct(a.shape, a.dtype) for a in parts]
    outs[2] = jax.ShapeDtypeStruct((heads, TOK), F32)
    outs[5] = jax.ShapeDtypeStruct((levels, heads), F32)
    return pl.pallas_call(
        finish_kernel,
        in_specs=[far] * 6,
        out_specs=[far] * 6,
        out_shape=outs,
        scratch_shapes=[pltpu.VMEM(a.shape, a.dtype) for a in (*parts, outs[2], outs[5])]
        + [pltpu.SemaphoreType.DMA((6,)), pltpu.SemaphoreType.DMA((6,))],
        name="finish",
    )(*parts)


def local(hidden, queries, w_key, w_value, log_gate, level_gain, segment_ids, out_grad):
    heads, levels = level_gain.shape
    parts = whole_step(
        hidden[0], queries[0], out_grad[0], w_key, w_value, log_gate[0], segment_ids, level_gain.T
    )
    query_grad, input_grad, gate_grad, key_weight, value_weight, gains = finish(
        *parts, heads, levels
    )
    return (
        query_grad[None],
        input_grad[None],
        gate_grad[None],
        key_weight,
        value_weight,
        gains.T,
    )


def solution(mesh):
    split = Mesh(
        mesh.devices.reshape(4, 4, 2, mesh.shape["batch"]), ("z", "x", "core", "batch")
    )
    return jax.shard_map(
        local,
        mesh=split,
        in_specs=(
            P("batch", SEQ, None),
            P("batch", SEQ, None),
            P(),
            P(),
            P("batch", None, SEQ),
            P(),
            P("batch", SEQ),
            P("batch", SEQ, None),
        ),
        out_specs=(
            P("batch", SEQ, None),
            P("batch", SEQ, None),
            P("batch", None, SEQ),
            P(SEQ_BATCH, None),
            P(SEQ_BATCH, None),
            P(),
        ),
        check_vma=False,
    )
```

```python
import functools

import jax
import jax.numpy as jnp
from jax import lax
from jax.experimental import pallas as pl
from jax.experimental.pallas import tpu as pltpu
from jax.sharding import Mesh
from jax.sharding import PartitionSpec as P

SEQ = ("z", "x", "core")
SEQ_BATCH = ("z", "x", "core", "batch")
MESH = pl.DeviceIdType.MESH
HIGHEST = lax.Precision.HIGHEST
F32 = jnp.float32
BF16 = jnp.bfloat16

NT = (((1,), (1,)), ((), ()))
TN = (((0,), (0,)), ((), ()))
NN = (((1,), (0,)), ((), ()))

TOK = 128
PAIR = 128
HALF_ROWS = 1088


def dot(a, b, dims):
    return lax.dot_general(a, b, dims, preferred_element_type=F32)


def dot_exact(a, b, dims):
    return lax.dot_general(a, b, dims, preferred_element_type=F32, precision=HIGHEST)


def split2(x):
    hi = x.astype(BF16)
    return hi, (x - hi.astype(F32)).astype(BF16)


def dot_left(a, b, dims):
    hi, lo = split2(a)
    return dot(hi, b, dims) + dot(lo, b, dims)


def dot_right(a, b, dims):
    hi, lo = split2(b)
    return dot(a, hi, dims) + dot(a, lo, dims)


def iota(shape, dim):
    return lax.broadcasted_iota(jnp.int32, shape, dim)


def entry_signal(peers):
    barrier = pltpu.get_barrier_semaphore()
    for peer in peers:
        pl.semaphore_signal(barrier, inc=1, device_id=peer, device_id_type=MESH)
    return barrier


def ring(index, step):
    return lax.rem(index + step, 4)


def same(a, b):
    return jnp.where(a == b, 1.0, 0.0)


def linked(a, b, total):
    return jnp.where(a == b, jnp.exp(total), 0.0)


def rows_of(start, size):
    return pl.ds(pl.multiple_of(start, size), size)


SENDS = 128
LOCALS = 32
VMEM_LIMIT = 56 * 2**20


def scratch():
    def f(*shape):
        return pltpu.VMEM(shape, F32)

    def b(*shape):
        return pltpu.VMEM(shape, BF16)

    return dict(
        wk=b(1024, 2048),
        wv=b(1024, 2048),
        hid=b(TOK, 1024),
        q=b(TOK, 2048),
        g=b(TOK, 2048),
        k=b(16, TOK, PAIR),
        v=b(16, TOK, PAIR),
        hid_t=f(1024, TOK),
        cumx=f(16, TOK, PAIR),
        cumr=f(32, TOK),
        cumr3=f(16, 8, TOK),
        fw=f(16, TOK, PAIR),
        lw=f(16, TOK, PAIR),
        segc=f(TOK, TOK),
        st=f(HALF_ROWS, PAIR),
        both=f(2, HALF_ROWS, PAIR),
        chip_send=f(2, 4, 136, PAIR),
        chip_recv=f(2, 4, 136, PAIR),
        tot_send=f(2, 2, 72, PAIR),
        tot_recv=f(2, 2, 72, PAIR),
        back_send=f(2, 4, 128, PAIR),
        back_recv=f(2, 4, 128, PAIR),
        own_blocks=f(2, 2, 512, PAIR),
        s_in=f(2, 2, 512, PAIR),
        gcross=f(16, 8, PAIR),
        gint=f(16, 16, PAIR),
        gate=f(16, 8, TOK),
        hy=f(4, 2, 1024, TOK),
        hz=f(4, 2, 1024, TOK),
        hyb=b(1024, 8 * TOK),
        hzb=b(1024, 8 * TOK),
        qacc=f(16, TOK, PAIR),
        kacc=f(16, TOK, PAIR),
        vacc=f(16, TOK, PAIR),
        ks=f(2, 8, TOK, PAIR),
        vs=f(2, 8, TOK, PAIR),
        ksb=b(TOK, 2048),
        vsb=b(TOK, 2048),
        rk=f(2, 8, TOK, PAIR),
        rv=f(2, 8, TOK, PAIR),
        part1=f(4, 4, 256, PAIR),
        recv1=f(4, 4, 256, PAIR),
        part2=f(4, 4, 64, PAIR),
        recv2=f(4, 4, 64, PAIR),
        kown=f(8, 2, 8, PAIR),
        vown=f(8, 2, 8, PAIR),
        kfin=f(8, 2, 8, PAIR),
        vfin=f(8, 2, 8, PAIR),
        small=f(16, PAIR),
        m1=f(8, 16, PAIR),
        m1s=f(16, PAIR),
        m2=f(4, 16, PAIR),
        m2s=f(8, PAIR),
        m3=f(4, 8, PAIR),
        lg=f(32, TOK),
        segr=pltpu.VMEM((1, TOK), jnp.int32),
        gain=pltpu.SMEM((18, 32), F32),
        qg=b(TOK, 2048),
        ig=b(TOK, 1024),
        kout=f(8, 2048),
        vout=f(8, 2048),
        sout=f(16, PAIR),
        send_sem=pltpu.SemaphoreType.DMA((SENDS,)),
        recv_sem=pltpu.SemaphoreType.DMA((SENDS,)),
        local_sem=pltpu.SemaphoreType.DMA((LOCALS,)),
    )


def step_kernel(
    hid_hbm,
    q_hbm,
    g_hbm,
    wk_hbm,
    wv_hbm,
    lg_hbm,
    segr_hbm,
    gain_hbm,
    qg_hbm,
    ig_hbm,
    gate_hbm,
    kout_hbm,
    vout_hbm,
    sout_hbm,
    *refs,
):
    s = dict(zip(scratch(), refs))
    gain_ref, qg_ref, ig_ref = s["gain"], s["qg"], s["ig"]
    kout_ref, vout_ref, sout_ref = s["kout"], s["vout"], s["sout"]
    x, y, z, c = (lax.axis_index(a) for a in ("x", "batch", "z", "core"))
    used = [0]

    def remote(src, dst, target):
        n = used[0]
        used[0] += 1
        cp = pltpu.make_async_remote_copy(
            src_ref=src,
            dst_ref=dst,
            send_sem=s["send_sem"].at[n],
            recv_sem=s["recv_sem"].at[n],
            device_id=target,
            device_id_type=MESH,
        )
        cp.start()
        return cp

    def wait(copies):
        for cp in copies:
            cp.wait()

    sib = {"core": 1 - c}
    offsets = [(d, e) for d in range(4) for e in (0, 1) if d or e]

    def plane(axis, index, d, e):
        to, tc = ring(index, d), lax.rem(c + e, 2)
        return {axis: to, "core": tc}, 2 * to + tc

    peers = [plane("batch", y, d, e)[0] for d, e in offsets]
    peers += [plane("z", z, d, e)[0] for d, e in offsets if d]
    peers += [{"x": ring(x, d)} for d in (1, 2, 3)]
    barrier = entry_signal(peers)

    local_sem = s["local_sem"]
    first_loads = [
        pltpu.make_async_copy(hid_hbm, s["hid"], local_sem.at[0]),
        pltpu.make_async_copy(q_hbm, s["q"], local_sem.at[1]),
        pltpu.make_async_copy(g_hbm, s["g"], local_sem.at[2]),
        pltpu.make_async_copy(lg_hbm, s["lg"], local_sem.at[3]),
        pltpu.make_async_copy(segr_hbm, s["segr"], local_sem.at[4]),
        pltpu.make_async_copy(gain_hbm, s["gain"], local_sem.at[5]),
    ]

    def step_at(i):
        return lax.rem(i + 4 - 4 * c, 8)

    def weight_load(hbm, name, i, base):
        cols = rows_of(step_at(i) * 256, 256)
        return pltpu.make_async_copy(hbm.at[:, cols], s[name].at[:, cols], local_sem.at[base + i])

    first_loads[0].start()
    for n in (3, 4, 5):
        first_loads[n].start()
    for i in range(8):
        weight_load(wk_hbm, "wk", i, 8).start()
        weight_load(wv_hbm, "wv", i, 16).start()
        if i == 0:
            first_loads[1].start()
            first_loads[2].start()

    rows_i, cols_i = iota((TOK, TOK), 0), iota((TOK, TOK), 1)
    causal = cols_i <= rows_i
    lower = causal.astype(F32)
    low = cols_i < 64
    low_half = iota((64, PAIR), 1) < 64
    row8 = iota((8, PAIR), 0)
    low_row = iota((1, PAIR), 1) < 64
    for n in (3, 4, 5):
        first_loads[n].wait()
    log_gate = s["lg"][...]
    cum_cols = dot_exact(lower, log_gate, NT)
    s["cumr"][...] = dot_exact(log_gate, lower, NT)
    for pair in range(16):
        s["cumx"][pair] = jnp.where(
            low, cum_cols[:, 2 * pair : 2 * pair + 1], cum_cols[:, 2 * pair + 1 : 2 * pair + 2]
        )
        s["cumr3"][pair, 0:2, :] = s["cumr"][2 * pair : 2 * pair + 2, :]
    seg_row = s["segr"][...].astype(F32)
    s["segc"][...] = jnp.broadcast_to(seg_row, (TOK, TOK)).T
    s["gcross"][...] = jnp.zeros((16, 8, PAIR), F32)

    first_loads[0].wait()
    for b in range(8):
        cols = slice(b * TOK, (b + 1) * TOK)
        s["hid_t"][cols, :] = s["hid"][:, cols].astype(F32).T

    first_loads[1].wait()
    first_loads[2].wait()

    def project(i, st):
        step = step_at(i)
        weight_load(wk_hbm, "wk", i, 8).wait()
        weight_load(wv_hbm, "wv", i, 16).wait()
        wide = rows_of(step * 256, 256)
        hid = s["hid"][...]
        keys = dot(hid, s["wk"][:, wide], NN).astype(BF16)
        values = dot(hid, s["wv"][:, wide], NN).astype(BF16)
        segc = s["segc"][...]
        for p in range(2):
            pair = 2 * step + p
            k, v = keys[:, p * PAIR : (p + 1) * PAIR], values[:, p * PAIR : (p + 1) * PAIR]
            s["k"][pair] = k
            s["v"][pair] = v
            cum = s["cumx"][pair]
            total = cum[TOK - 1 : TOK, :]
            last_w = jnp.where(segc == segc[TOK - 1 : TOK, :], jnp.exp(total - cum), 0.0)
            first_w = jnp.where(segc == segc[0:1, :], jnp.exp(cum), 0.0)
            s["lw"][pair] = last_w
            s["fw"][pair] = first_w
            cols = rows_of(pair * PAIR, PAIR)
            fwd = dot_left(k.astype(F32) * last_w, v, TN)
            rev = dot_left(s["q"][:, cols].astype(F32) * first_w, s["g"][:, cols], TN)
            pp = 2 * lax.rem(step, 4) + p
            st[rows_of(pp * 64, 64), :] = jnp.where(low_half, fwd[:64], fwd[64:])
            st[rows_of(512 + pp * 64, 64), :] = jnp.where(low_half, rev[:64], rev[64:])
            meta = jnp.where(
                row8 == 0,
                total,
                jnp.where(
                    row8 == 1, segc[0:1, :], jnp.where(row8 == 2, segc[TOK - 1 : TOK, :], 0.0)
                ),
            )
            st[rows_of(1024 + pp * 8, 8), :] = meta

    both = s["both"]
    project(0, s["st"])
    pl.semaphore_wait(barrier, len(peers))

    gathers = (("batch", y, s["hy"]), ("z", z, s["hz"]))
    hops = []
    for axis, index, buf in gathers:
        for d in (1, 3):
            hops.append(remote(s["hid_t"], buf.at[index, c], {axis: ring(index, d)}))
    lax.fori_loop(1, 4, lambda i, carry: project(i, s["st"]), None)
    swap = remote(s["st"], both.at[c], sib)
    down = [remote(s["hid_t"], buf.at[index, c], sib) for _, index, buf in gathers]
    lax.fori_loop(4, 8, lambda i, carry: project(i, both.at[c]), None)

    def inner(pair, carry):
        cols = rows_of(pair * PAIR, PAIR)
        q, g = s["q"][:, cols], s["g"][:, cols]
        k, v = s["k"][pair], s["v"][pair]
        allowed = causal & (s["segc"][...] == seg_row)
        gap = jnp.bitwise_xor(rows_i, cols_i)
        strict = (rows_i < cols_i).astype(BF16)
        zero = jnp.zeros((TOK, PAIR), BF16)
        weighted, scored, queries, keys, grads, gate_rows, gain_rows = [], [], [], [], [], [], []
        for h in range(2):

            def own(a):
                return jnp.where(low, a, zero) if h == 0 else jnp.where(low, zero, a)

            qh, gh, kh = own(q), own(g), own(k)
            score = dot(qh, k, NT)
            dprob = dot(gh, v, NT)
            spread = s["cumx"][pair, :, 64 * h : 64 * h + 1] - s["cumr3"][pair, h : h + 1, :]
            decay = jnp.where(allowed, jnp.exp(jnp.where(allowed, spread, 0.0)), 0.0)
            ds = decay * score
            joint = ds * dprob
            head = 2 * pair + h
            level = jnp.full((TOK, TOK), gain_ref[0, head], F32)
            gain_rows.append(jnp.sum(jnp.where(gap == 0, joint, 0.0), axis=0, keepdims=True))
            for l in range(1, 8):
                above = gap >= 2 ** (l - 1)
                level = jnp.where(above, gain_ref[l, head], level)
                chosen = above & (gap < 2**l)
                gain_rows.append(jnp.sum(jnp.where(chosen, joint, 0.0), axis=0, keepdims=True))
            wd = level * decay * dprob
            weighted.append(wd.astype(BF16))
            scored.append((level * ds).astype(BF16))
            grid = (wd * score).astype(BF16)
            crossing = jnp.where(causal, dot(grid, strict, NN), 0.0)
            gate_rows.append(jnp.sum(crossing, axis=0, keepdims=True))
            queries.append(qh)
            keys.append(kh)
            grads.append(gh)
        s["qacc"][pair] = dot(
            jnp.concatenate(weighted, axis=1), jnp.concatenate(keys, axis=0), NN
        )
        s["kacc"][pair] = dot(
            jnp.concatenate(weighted, axis=0), jnp.concatenate(queries, axis=0), TN
        )
        s["vacc"][pair] = dot(jnp.concatenate(scored, axis=0), jnp.concatenate(grads, axis=0), TN)
        s["gate"][pair] = jnp.concatenate([*gate_rows, jnp.zeros((6, TOK), F32)], axis=0)
        s["gint"][pair] = jnp.concatenate(gain_rows, axis=0)
        return carry

    swap.wait()

    def meta_rows(total, first, last):
        return jnp.where(
            row8 == 0, total, jnp.where(row8 == 1, first, jnp.where(row8 == 2, last, 0.0))
        )

    chip_send, chip_recv = s["chip_send"], s["chip_recv"]

    def block_pair(pp):
        f0 = both[0, pp * 64 : pp * 64 + 64, :]
        f1 = both[1, pp * 64 : pp * 64 + 64, :]
        r0 = both[0, 512 + pp * 64 : 576 + pp * 64, :]
        r1 = both[1, 512 + pp * 64 : 576 + pp * 64, :]
        m0 = both[0, 1024 + pp * 8 : 1032 + pp * 8, :]
        m1 = both[1, 1024 + pp * 8 : 1032 + pp * 8, :]
        return f0, f1, r0, r1, m0[0:1], m0[1:2], m0[2:3], m1[0:1], m1[1:2], m1[2:3]

    def chip_sums(p):
        for n in range(4):
            f0, f1, r0, r1, t0, first0, last0, t1, first1, last1 = block_pair(2 * n + p)
            chip_send[p, n, 0:64, :] = f1 + linked(last0, last1, t1) * f0
            chip_send[p, n, 64:128, :] = r0 + linked(first0, first1, t0) * r1
            chip_send[p, n, 128:136, :] = meta_rows(t0 + t1, first0, last1)

    def chip_sends(p):
        copies = []
        for d in (2, 1, 3):
            to = ring(x, d)
            copies.append(remote(chip_send.at[p, to], chip_recv.at[p, x], {"x": to}))
        chip_recv[p, pl.ds(x, 1)] = chip_send[p, pl.ds(x, 1)]
        return copies

    xs = []
    for p in range(2):
        chip_sums(p)
        xs.append(chip_sends(p))
    for pp in range(8):
        f0, _, _, r1, _, _, last0, _, first1, _ = block_pair(pp)
        d8 = same(last0, first1) * jnp.sum(f0 * r1, axis=0, keepdims=True)
        s["gcross"][pl.ds(c * 8 + pp, 1)] = jnp.where(row8 == 0, d8, 0.0)[None]
    lax.fori_loop(0, 7, inner, 0)

    def chip(j, p):
        return (
            chip_recv[p, j, 0:64, :],
            chip_recv[p, j, 64:128, :],
            chip_recv[p, j, 128:129, :],
            chip_recv[p, j, 129:130, :],
            chip_recv[p, j, 130:131, :],
        )

    def joined(p):
        (f0, r0, t0, a0, l0), (f1, r1, t1, a1, l1), (f2, r2, t2, a2, l2), (f3, r3, t3, a3, l3) = (
            chip(j, p) for j in range(4)
        )
        f01 = f1 + linked(l0, l1, t1) * f0
        r01 = r0 + linked(a0, a1, t0) * r1
        f23 = f3 + linked(l2, l3, t3) * f2
        r23 = r2 + linked(a2, a3, t2) * r3
        return f01, r01, f23, r23

    tot_send, tot_recv = s["tot_send"], s["tot_recv"]
    zs = []
    for p in range(2):
        wait(xs[p])
        f01, r01, f23, r23 = joined(p)
        t0, a0 = chip(0, p)[2:4]
        t1, l1 = chip(1, p)[2], chip(1, p)[4]
        t2, a2 = chip(2, p)[2:4]
        t3, l3 = chip(3, p)[2], chip(3, p)[4]
        tot_send[p, 0, 0:64, :] = f23 + linked(l1, l3, t2 + t3) * f01
        tot_send[p, 1, 0:64, :] = r01 + linked(a0, a2, t0 + t1) * r23
        tot_send[p, 0, 64:72, :] = jnp.broadcast_to(l3, (8, PAIR))
        tot_send[p, 1, 64:72, :] = jnp.broadcast_to(a0, (8, PAIR))
        zs.append(
            [
                remote(tot_send.at[p, n], tot_recv.at[p, n], {"z": ring(z, d)})
                for n, d in ((0, 1), (1, 3))
            ]
        )

    fwd = []
    for n, (axis, index, buf) in enumerate(gathers):
        for m, d in enumerate((1, 3)):
            hops[2 * n + m].wait()
            came = ring(index, 4 - d)
            part = slice(0, 512) if d == 1 else slice(512, 1024)
            fwd.append(
                remote(buf.at[came, c, part], buf.at[came, c, part], {axis: ring(index, d)})
            )
            down.append(remote(buf.at[came, c], buf.at[came, c], sib))

    lax.fori_loop(7, 9, inner, 0)

    has_prev = (z > 0).astype(F32)
    has_next = (z < 3).astype(F32)
    prev_top = (z == 2).astype(F32)
    next_top = (z == 1).astype(F32)
    back_send, back_recv = s["back_send"], s["back_recv"]

    def gain_row(pair, level):
        return jnp.where(low_row, gain_ref[level, 2 * pair], gain_ref[level, 2 * pair + 1])

    bs = []
    for p in range(2):
        wait(zs[p])
        (f0, r0, t0, a0, l0), (f1, r1, t1, a1, l1), (f2, r2, t2, a2, l2), (f3, r3, t3, a3, l3) = (
            chip(j, p) for j in range(4)
        )
        f01, r01, f23, r23 = joined(p)
        pair = c * 8 + 2 * x + p
        g9, g10, g11, g12 = (gain_row(pair, level) for level in range(9, 13))
        zf = has_prev * tot_recv[p, 0, 0:64, :]
        zl = tot_recv[p, 0, 64:65, :]
        zr = has_next * tot_recv[p, 1, 0:64, :]
        za = tot_recv[p, 1, 64:65, :]
        gzf = g11 * (1.0 - prev_top) + g12 * prev_top
        gzr = g11 * (1.0 - next_top) + g12 * next_top
        sf = (
            gzf * same(zl, a0) * zf,
            gzf * linked(zl, a1, t0) * zf + g9 * same(l0, a1) * f0,
            gzf * linked(zl, a2, t0 + t1) * zf + g10 * same(l1, a2) * f01,
            gzf * linked(zl, a3, t0 + t1 + t2) * zf
            + g10 * linked(l1, a3, t2) * f01
            + g9 * same(l2, a3) * f2,
        )
        sr = (
            gzr * linked(za, l0, t1 + t2 + t3) * zr
            + g10 * linked(l0, a2, t1) * r23
            + g9 * same(l0, a1) * r1,
            gzr * linked(za, l1, t2 + t3) * zr + g10 * same(l1, a2) * r23,
            gzr * linked(za, l2, t3) * zr + g9 * same(l2, a3) * r3,
            gzr * same(za, l3) * zr,
        )
        for j in range(4):
            back_send[p, j, 0:64, :] = sf[j]
            back_send[p, j, 64:128, :] = sr[j]
        copies = []
        for d in (1, 2, 3):
            to = ring(x, d)
            copies.append(remote(back_send.at[p, to], back_recv.at[p, x], {"x": to}))
        back_recv[p, pl.ds(x, 1)] = back_send[p, pl.ds(x, 1)]
        bs.append(copies)

    for p in range(2):
        (f0, r0, t0, a0, l0), (f1, r1, t1, a1, l1), (f2, r2, t2, a2, l2), (f3, r3, t3, a3, l3) = (
            chip(j, p) for j in range(4)
        )
        f01, r01, f23, r23 = joined(p)
        zf = has_prev * tot_recv[p, 0, 0:64, :]
        zl = tot_recv[p, 0, 64:65, :]
        r_group = r01 + linked(a0, a2, t0 + t1) * r23
        d9 = same(l0, a1) * jnp.sum(f0 * r1, axis=0, keepdims=True) + same(l2, a3) * jnp.sum(
            f2 * r3, axis=0, keepdims=True
        )
        d10 = same(l1, a2) * jnp.sum(f01 * r23, axis=0, keepdims=True)
        dz = same(zl, a0) * jnp.sum(zf * r_group, axis=0, keepdims=True)
        rows = jnp.where(
            row8 == 1,
            d9,
            jnp.where(
                row8 == 2,
                d10,
                jnp.where(
                    row8 == 3, (1.0 - prev_top) * dz, jnp.where(row8 == 4, prev_top * dz, 0.0)
                ),
            ),
        )
        pair = c * 8 + 2 * x + p
        s["gcross"][pl.ds(pair, 1)] = s["gcross"][pl.ds(pair, 1)] + rows[None]
    lax.fori_loop(9, 16, inner, 0)
    def rounded(n, block, core):
        buf, out = gathers[n][2], s[("hyb", "hzb")[n]]
        out[:, rows_of((2 * block + core) * TOK, TOK)] = buf[block, core].astype(BF16)

    for n, (_, index, buf) in enumerate(gathers):
        s[("hyb", "hzb")[n]][:, rows_of((2 * index + c) * TOK, TOK)] = s["hid_t"][...].astype(BF16)
        down[n].wait()
        rounded(n, index, 1 - c)
        for m, d in enumerate((1, 3)):
            came = ring(index, 4 - d)
            rounded(n, came, c)
            down[2 + 2 * n + m].wait()
            rounded(n, came, 1 - c)
    for n, (_, index, buf) in enumerate(gathers):
        wait(fwd[2 * n : 2 * n + 2])
        came = ring(index, 2)
        down.append(remote(buf.at[came, c], buf.at[came, c], sib))

    own_blocks, s_in = s["own_blocks"], s["s_in"]
    swaps = []
    for p in range(2):
        wait(bs[p])
        for n in range(4):
            pp = 2 * n + p
            f0, _, _, r1, t0, first0, last0, t1, first1, last1 = block_pair(pp)
            sf = back_recv[p, n, 0:64, :]
            sr = back_recv[p, n, 64:128, :]
            link = gain_row(c * 8 + pp, 8) * same(last0, first1)
            at = n * 128
            own_blocks[p, 0, at : at + 64, :] = sf
            own_blocks[p, 1, at : at + 64, :] = linked(first0, first1, t0) * sf + link * f0
            own_blocks[p, 0, at + 64 : at + 128, :] = linked(last0, last1, t1) * sr + link * r1
            own_blocks[p, 1, at + 64 : at + 128, :] = sr
        swaps.append(remote(own_blocks.at[p, 1 - c], s_in.at[p, c], sib))
        s_in[p, pl.ds(c, 1)] = own_blocks[p, pl.ds(c, 1)]

    tail = causal.astype(BF16)
    head_pick = (cols_i[0:8, :] // 64 == row8).astype(BF16)

    def diag(a):
        return jnp.concatenate([jnp.where(low_half, a, 0.0), jnp.where(low_half, 0.0, a)], axis=0)

    def incoming(to, p, part):
        if isinstance(to, int):
            at = to % 4 * 128 + part * 64
            return diag(s_in[p, to // 4, at : at + 64, :])
        at = lax.rem(to, 4) * 128 + part * 64
        return diag(s_in[p, to // 4, rows_of(at, 64), :])

    def key_part(to, p):
        pair = 2 * to + p
        rv = s["lw"][pair] * dot_right(s["v"][pair], incoming(to, p, 1), NT)
        key_sum = (s["kacc"][pair] + rv).astype(BF16)
        s["kacc"][pair] = s["k"][pair].astype(F32) * rv
        s["ksb"][:, rows_of(pair * PAIR, PAIR)] = key_sum
        s["ks"][p, to] = key_sum.astype(F32)

    def value_part(to, p):
        pair = 2 * to + p
        rk = s["lw"][pair] * dot_right(s["k"][pair], incoming(to, p, 1), NN)
        value_sum = (s["vacc"][pair] + rk).astype(BF16)
        s["vsb"][:, rows_of(pair * PAIR, PAIR)] = value_sum
        s["vs"][p, to] = value_sum.astype(F32)

    def query_part(to, p):
        pair = 2 * to + p
        cols = slice(pair * PAIR, (pair + 1) * PAIR)
        sg = s["fw"][pair] * dot_right(s["g"][:, cols], incoming(to, p, 0), NT)
        qg_ref[:, cols] = (s["qacc"][pair] + sg).astype(BF16)
        diff = s["q"][:, cols].astype(F32) * sg - s["kacc"][pair]
        hi, lo = split2(diff)
        diff_rows = dot(head_pick, hi, NT) + dot(head_pick, lo, NT)
        s["gate"][pair] = s["gate"][pair] + dot_left(diff_rows, tail, NN)

    firsts = []
    me_y, me_z = 2 * y + c, 2 * z + c
    far_first = [(2, 0), (2, 1), (1, 0), (3, 0), (1, 1), (3, 1), (0, 1)]
    for n in range(2):
        swaps[n].wait()
        fk, fv = [], []
        for d, e in far_first:
            dev, to = plane("batch", y, d, e)
            key_part(to, n)
            fk.append(remote(s["ks"].at[n, to], s["rk"].at[n, me_y], dev))
            dev, to = plane("z", z, d, e)
            value_part(to, n)
            fv.append(remote(s["vs"].at[n, to], s["rv"].at[n, me_z], dev))
        key_part(me_y, n)
        value_part(me_z, n)
        firsts.append((fk, fv))
    for n in range(2):
        s["rk"][n, pl.ds(me_y, 1)] = s["ks"][n, pl.ds(me_y, 1)]
        s["rv"][n, pl.ds(me_z, 1)] = s["vs"][n, pl.ds(me_z, 1)]

    for n, (_, index, buf) in enumerate(gathers):
        came = ring(index, 2)
        rounded(n, came, c)
        down[6 + n].wait()
        rounded(n, came, 1 - c)

    def product(left, right, n):
        right = s[right][n].reshape(8 * TOK, PAIR).astype(BF16)
        for b in range(4):
            yield b, dot(s[left][b * 256 : (b + 1) * 256, :], right, NN)

    part1, recv1, part2, recv2 = s["part1"], s["recv1"], s["part2"], s["recv2"]

    def scatter(part, recv, chunk, axis, index):
        out = []
        for d in (1, 2, 3):
            to = ring(index, d)
            out.append(remote(part.at[chunk, to], recv.at[chunk, index], {axis: to}))
        recv[chunk, pl.ds(index, 1)] = part[chunk, pl.ds(index, 1)]
        return out

    wait(firsts[0][0])
    for b, block in product("hyb", "rk", 0):
        for j in range(4):
            part1[0, j, b * 64 : b * 64 + 64, :] = block[j * 64 : j * 64 + 64, :]
    k0 = scatter(part1, recv1, 0, "x", x)
    wait(firsts[0][1])
    for b, block in product("hzb", "rv", 0):
        for j in range(4):
            part1[2, j, b * 64 : b * 64 + 64, :] = block[j * 64 : j * 64 + 64, :]
    v0 = scatter(part1, recv1, 2, "x", x)

    for n in range(2):
        for to in range(8):
            query_part(to, n)
    stores = []

    def store(ref, hbm):
        cp = pltpu.make_async_copy(ref, hbm, local_sem.at[24 + len(stores)])
        cp.start()
        stores.append(cp)

    store(qg_ref, qg_hbm)
    store(s["gate"], gate_hbm)

    ones = jnp.ones((8, PAIR), F32)
    inner_sum = dot_exact(ones, s["gint"][...].reshape(256, PAIR), NT)
    pick = (cols_i[0:8, :] // 64 == row8 - 2).astype(F32)
    outer_sum = dot_exact(pick, s["gcross"][...].reshape(128, PAIR), NT)
    start = (cols_i[0:8, :] == 0).astype(F32)
    own_total = dot_exact(start, s["gate"][...].reshape(128, TOK), NT)
    small, m1, m1s, m2, m2s, m3 = (s[n] for n in ("small", "m1", "m1s", "m2", "m2s", "m3"))
    small[0:8, :] = jnp.where(
        row8 == 0, inner_sum[:, :128], jnp.where(row8 == 1, inner_sum[:, 128:], outer_sum)
    )
    small[8:16, :] = own_total
    smalls = []
    for d, e in offsets:
        smalls.append(remote(small, m1.at[me_z], plane("z", z, d, e)[0]))
    m1[pl.ds(me_z, 1)] = small[...][None]

    def input_grad(n, carry):
        rows = rows_of(n * 256, 256)
        ig_ref[:, rows] = (
            dot(s["ksb"][...], s["wk"][rows, :], NT) + dot(s["vsb"][...], s["wv"][rows, :], NT)
        ).astype(BF16)
        return carry


    wait(firsts[1][0])
    for b, block in product("hyb", "rk", 1):
        part1[1, b] = block
    k1 = scatter(part1, recv1, 1, "z", z)
    wait(firsts[1][1])
    for b, block in product("hzb", "rv", 1):
        for j in range(8):
            for i in range(4):
                at = j * 32 + i * 8
                part1[3, i, b * 64 + j * 8 : b * 64 + j * 8 + 8, :] = block[at : at + 8, :]
    v1 = scatter(part1, recv1, 3, "batch", y)
    lax.fori_loop(0, 4, input_grad, 0)
    store(ig_ref, ig_hbm)

    wait(smalls)
    total = m1[0, 0:8, :]
    for g in range(1, 8):
        total = total + m1[g, 0:8, :]
    m1s[0:8, :] = total
    for g in range(8):
        m1s[8 + g : 9 + g, :] = m1[g, 8:9, :]
    smalls = [remote(m1s, m2.at[x], {"x": ring(x, d)}) for d in (1, 2, 3)]
    m2[pl.ds(x, 1)] = m1s[...][None]

    def summed(recv, chunk):
        return recv[chunk, 0] + recv[chunk, 1] + recv[chunk, 2] + recv[chunk, 3]

    wait(k0)
    total = summed(recv1, 0)
    for j in range(4):
        part2[0, j] = total[j * 64 : j * 64 + 64, :]
    k0 = scatter(part2, recv2, 0, "z", z)
    wait(v0)
    total = summed(recv1, 2)
    for j in range(8):
        for i in range(4):
            at = j * 32 + i * 8
            part2[2, i, j * 8 : j * 8 + 8, :] = total[at : at + 8, :]
    v0 = scatter(part2, recv2, 2, "batch", y)
    wait(k1)
    total = summed(recv1, 1)
    for j in range(4):
        part2[1, j] = total[j * 64 : j * 64 + 64, :]
    k1 = scatter(part2, recv2, 1, "x", x)
    wait(v1)
    total = summed(recv1, 3)
    for j in range(4):
        for i in range(4):
            at = j * 64 + i * 16
            part2[3, i, j * 16 : j * 16 + 16, :] = total[at : at + 16, :]
    v1 = scatter(part2, recv2, 3, "x", x)

    wait(smalls)
    total = m2[0, 0:8, :] + m2[1, 0:8, :] + m2[2, 0:8, :] + m2[3, 0:8, :]
    m2s[...] = total
    smalls = [remote(m2s, m3.at[y], {"batch": ring(y, d)}) for d in (1, 2, 3)]
    m3[pl.ds(y, 1)] = total[None]
    place = z * 8 + x * 2 + c
    later = jnp.zeros((1, PAIR), F32)
    for j in range(4):
        for g in range(8):
            spot = (g // 2) * 8 + j * 2 + g % 2
            later = later + (place < spot).astype(F32) * m2[j, 8 + g : 9 + g, :]
    sout_ref[8:16, :] = jnp.broadcast_to(later, (8, PAIR))

    fins = []
    wait(k0)
    wait(k1)
    for n in range(2):
        total = summed(recv2, n)
        for i in range(4):
            for j in range(2):
                at = j * 32 + i * 8
                s["kown"][2 * i + j, n] = total[at : at + 8, :]
    for d, e in offsets:
        dev, to = plane("batch", y, d, e)
        fins.append(remote(s["kown"].at[to], s["kfin"].at[me_y], dev))
    s["kfin"][pl.ds(me_y, 1)] = s["kown"][pl.ds(me_y, 1)]
    wait(v0)
    wait(v1)
    for n in range(2):
        total = summed(recv2, 2 + n)
        for j in range(8):
            s["vown"][j, n] = total[j * 8 : j * 8 + 8, :]
    for d, e in offsets:
        dev, to = plane("z", z, d, e)
        fins.append(remote(s["vown"].at[to], s["vfin"].at[me_z], dev))
    s["vfin"][pl.ds(me_z, 1)] = s["vown"][pl.ds(me_z, 1)]
    wait(smalls)
    sout_ref[0:8, :] = m3[0] + m3[1] + m3[2] + m3[3]
    store(sout_ref, sout_hbm)
    wait(fins)
    for n in range(2):
        for g in range(8):
            cols = slice((2 * g + n) * PAIR, (2 * g + n + 1) * PAIR)
            kout_ref[:, cols] = s["kfin"][g, n]
            vout_ref[:, cols] = s["vfin"][g, n]
    store(kout_ref, kout_hbm)
    store(vout_ref, vout_hbm)
    wait(stores)


def whole_step(hidden, queries, out_grad, w_key, w_value, log_gate, seg_row, level_gain):
    far = pl.BlockSpec(memory_space=pltpu.HBM)
    return pl.pallas_call(
        step_kernel,
        in_specs=[far] * 8,
        out_specs=[far] * 6,
        out_shape=[
            jax.ShapeDtypeStruct((TOK, 2048), BF16),
            jax.ShapeDtypeStruct((TOK, 1024), BF16),
            jax.ShapeDtypeStruct((16, 8, TOK), F32),
            jax.ShapeDtypeStruct((8, 2048), F32),
            jax.ShapeDtypeStruct((8, 2048), F32),
            jax.ShapeDtypeStruct((16, PAIR), F32),
        ],
        scratch_shapes=list(scratch().values()),
        compiler_params=pltpu.CompilerParams(
            collective_id=0, has_side_effects=True, vmem_limit_bytes=VMEM_LIMIT
        ),
        name="whole_step",
    )(hidden, queries, out_grad, w_key, w_value, log_gate, seg_row, level_gain)


def finish_kernel(
    qg_in, ig_in, gate_in, kw_in, vw_in, small_in, qg_out, ig_out, gate_out, kw_out, vw_out, gains_out,
    qg, ig, gate_ref, kw, vw, small_ref, gate, gains, load_sem, store_sem
):
    loads = [
        pltpu.make_async_copy(a, b, load_sem.at[n])
        for n, (a, b) in enumerate(
            ((gate_in, gate_ref), (small_in, small_ref), (qg_in, qg), (ig_in, ig), (kw_in, kw), (vw_in, vw))
        )
    ]
    for cp in loads:
        cp.start()
    stores = []

    def store(ref, out):
        cp = pltpu.make_async_copy(ref, out, store_sem.at[len(stores)])
        cp.start()
        stores.append(cp)

    loads[0].wait()
    loads[1].wait()
    heads = gate.shape[0]
    lane = iota((heads, PAIR), 1)
    head = iota((heads, PAIR), 0)
    small = small_ref[...]
    later = jnp.broadcast_to(small[8:9, :], (TOK, TOK)).T
    rows = gate_ref[...].reshape(TOK, TOK) + later
    gate[...] = dot_exact((lane == (head // 2) * 8 + head % 2).astype(F32), rows, NN)
    levels = gains.shape[0]
    level, at = iota((levels, PAIR), 0), iota((levels, PAIR), 1) % 8
    first = (level == at).astype(F32)
    second = (level == at + 8).astype(F32)
    pick0 = jnp.where(lane // 8 == head, small[0:1, :], 0.0)
    pick1 = jnp.where(lane // 8 + 16 == head, small[1:2, :], 0.0)
    pair = jnp.where(head % 2 == 0, small[2:3, :], small[3:4, :])
    pick2 = jnp.where(lane // 8 == head // 2, pair, 0.0)
    gains[...] = dot_exact(first, pick0 + pick1, NT) + dot_exact(second, pick2, NT)
    for cp, ref, out in zip(
        loads[2:], (qg, ig, kw, vw), (qg_out, ig_out, kw_out, vw_out)
    ):
        cp.wait()
        store(ref, out)
    store(gate, gate_out)
    store(gains, gains_out)
    for cp in stores:
        cp.wait()


def finish(query_grad, input_grad, gate, key_weight, value_weight, small, heads, levels):
    far = pl.BlockSpec(memory_space=pltpu.HBM)
    parts = (query_grad, input_grad, gate, key_weight, value_weight, small)
    outs = [jax.ShapeDtypeStruct(a.shape, a.dtype) for a in parts]
    outs[2] = jax.ShapeDtypeStruct((heads, TOK), F32)
    outs[5] = jax.ShapeDtypeStruct((levels, heads), F32)
    return pl.pallas_call(
        finish_kernel,
        in_specs=[far] * 6,
        out_specs=[far] * 6,
        out_shape=outs,
        scratch_shapes=[pltpu.VMEM(a.shape, a.dtype) for a in (*parts, outs[2], outs[5])]
        + [pltpu.SemaphoreType.DMA((6,)), pltpu.SemaphoreType.DMA((6,))],
        name="finish",
    )(*parts)


def local(hidden, queries, w_key, w_value, log_gate, level_gain, segment_ids, out_grad):
    heads, levels = level_gain.shape
    parts = whole_step(
        hidden[0], queries[0], out_grad[0], w_key, w_value, log_gate[0], segment_ids, level_gain.T
    )
    query_grad, input_grad, gate_grad, key_weight, value_weight, gains = finish(
        *parts, heads, levels
    )
    return (
        query_grad[None],
        input_grad[None],
        gate_grad[None],
        key_weight,
        value_weight,
        gains.T,
    )


def solution(mesh):
    split = Mesh(
        mesh.devices.reshape(4, 4, 2, mesh.shape["batch"]), ("z", "x", "core", "batch")
    )
    return jax.shard_map(
        local,
        mesh=split,
        in_specs=(
            P("batch", SEQ, None),
            P("batch", SEQ, None),
            P(),
            P(),
            P("batch", None, SEQ),
            P(),
            P("batch", SEQ),
            P("batch", SEQ, None),
        ),
        out_specs=(
            P("batch", SEQ, None),
            P("batch", SEQ, None),
            P("batch", None, SEQ),
            P(SEQ_BATCH, None),
            P(SEQ_BATCH, None),
            P(),
        ),
        check_vma=False,
    )
```

```python
import functools

import jax
import jax.numpy as jnp
from jax import lax
from jax.experimental import pallas as pl
from jax.experimental.pallas import tpu as pltpu
from jax.sharding import Mesh
from jax.sharding import PartitionSpec as P

SEQ = ("z", "x", "core")
SEQ_BATCH = ("z", "x", "core", "batch")
MESH = pl.DeviceIdType.MESH
HIGHEST = lax.Precision.HIGHEST
F32 = jnp.float32
BF16 = jnp.bfloat16

NT = (((1,), (1,)), ((), ()))
TN = (((0,), (0,)), ((), ()))
NN = (((1,), (0,)), ((), ()))

TOK = 128
PAIR = 128
HALF_ROWS = 1088


def dot(a, b, dims):
    return lax.dot_general(a, b, dims, preferred_element_type=F32)


def dot_exact(a, b, dims):
    return lax.dot_general(a, b, dims, preferred_element_type=F32, precision=HIGHEST)


def split2(x):
    hi = x.astype(BF16)
    return hi, (x - hi.astype(F32)).astype(BF16)


def dot_left(a, b, dims):
    hi, lo = split2(a)
    return dot(hi, b, dims) + dot(lo, b, dims)


def dot_right(a, b, dims):
    hi, lo = split2(b)
    return dot(a, hi, dims) + dot(a, lo, dims)


def iota(shape, dim):
    return lax.broadcasted_iota(jnp.int32, shape, dim)


def entry_signal(peers):
    barrier = pltpu.get_barrier_semaphore()
    for peer in peers:
        pl.semaphore_signal(barrier, inc=1, device_id=peer, device_id_type=MESH)
    return barrier


def ring(index, step):
    return lax.rem(index + step, 4)


def same(a, b):
    return jnp.where(a == b, 1.0, 0.0)


def linked(a, b, total):
    return jnp.where(a == b, jnp.exp(total), 0.0)


def rows_of(start, size):
    return pl.ds(pl.multiple_of(start, size), size)


SENDS = 128
LOCALS = 32
VMEM_LIMIT = 56 * 2**20


def scratch():
    def f(*shape):
        return pltpu.VMEM(shape, F32)

    def b(*shape):
        return pltpu.VMEM(shape, BF16)

    return dict(
        wk=b(1024, 2048),
        wv=b(1024, 2048),
        hid=b(TOK, 1024),
        q=b(TOK, 2048),
        g=b(TOK, 2048),
        k=b(16, TOK, PAIR),
        v=b(16, TOK, PAIR),
        hid_t=f(1024, TOK),
        cumx=f(16, TOK, PAIR),
        cumr=f(32, TOK),
        cumr3=f(16, 8, TOK),
        fw=f(16, TOK, PAIR),
        lw=f(16, TOK, PAIR),
        segc=f(TOK, TOK),
        st=f(HALF_ROWS, PAIR),
        both=f(2, HALF_ROWS, PAIR),
        chip_send=f(2, 4, 136, PAIR),
        chip_recv=f(2, 4, 136, PAIR),
        tot_send=f(2, 2, 72, PAIR),
        tot_recv=f(2, 2, 72, PAIR),
        back_send=f(2, 4, 128, PAIR),
        back_recv=f(2, 4, 128, PAIR),
        own_blocks=f(2, 2, 512, PAIR),
        s_in=f(2, 2, 512, PAIR),
        gcross=f(16, 8, PAIR),
        gint=f(16, 16, PAIR),
        gate=f(16, 8, TOK),
        hy=f(4, 2, 1024, TOK),
        hz=f(4, 2, 1024, TOK),
        hyb=b(1024, 8 * TOK),
        hzb=b(1024, 8 * TOK),
        qacc=f(16, TOK, PAIR),
        kacc=f(16, TOK, PAIR),
        vacc=f(16, TOK, PAIR),
        ks=f(2, 8, TOK, PAIR),
        vs=f(2, 8, TOK, PAIR),
        ksb=b(TOK, 2048),
        vsb=b(TOK, 2048),
        rk=f(2, 8, TOK, PAIR),
        rv=f(2, 8, TOK, PAIR),
        part1=f(4, 4, 256, PAIR),
        recv1=f(4, 4, 256, PAIR),
        part2=f(4, 4, 64, PAIR),
        recv2=f(4, 4, 64, PAIR),
        kown=f(8, 2, 8, PAIR),
        vown=f(8, 2, 8, PAIR),
        kfin=f(8, 2, 8, PAIR),
        vfin=f(8, 2, 8, PAIR),
        small=f(16, PAIR),
        m1=f(8, 16, PAIR),
        m1s=f(16, PAIR),
        m2=f(4, 16, PAIR),
        m2s=f(8, PAIR),
        m3=f(4, 8, PAIR),
        lg=f(32, TOK),
        segr=pltpu.VMEM((1, TOK), jnp.int32),
        gain=pltpu.SMEM((18, 32), F32),
        qg=b(TOK, 2048),
        ig=b(TOK, 1024),
        kout=f(8, 2048),
        vout=f(8, 2048),
        sout=f(16, PAIR),
        send_sem=pltpu.SemaphoreType.DMA((SENDS,)),
        recv_sem=pltpu.SemaphoreType.DMA((SENDS,)),
        local_sem=pltpu.SemaphoreType.DMA((LOCALS,)),
    )


def step_kernel(
    hid_hbm,
    q_hbm,
    g_hbm,
    wk_hbm,
    wv_hbm,
    lg_hbm,
    segr_hbm,
    gain_hbm,
    qg_hbm,
    ig_hbm,
    gate_hbm,
    kout_hbm,
    vout_hbm,
    sout_hbm,
    *refs,
):
    s = dict(zip(scratch(), refs))
    gain_ref, qg_ref, ig_ref = s["gain"], s["qg"], s["ig"]
    kout_ref, vout_ref, sout_ref = s["kout"], s["vout"], s["sout"]
    x, y, z, c = (lax.axis_index(a) for a in ("x", "batch", "z", "core"))
    used = [0]

    def remote(src, dst, target):
        n = used[0]
        used[0] += 1
        cp = pltpu.make_async_remote_copy(
            src_ref=src,
            dst_ref=dst,
            send_sem=s["send_sem"].at[n],
            recv_sem=s["recv_sem"].at[n],
            device_id=target,
            device_id_type=MESH,
        )
        cp.start()
        return cp

    def wait(copies):
        for cp in copies:
            cp.wait()

    sib = {"core": 1 - c}
    offsets = [(d, e) for d in range(4) for e in (0, 1) if d or e]

    def plane(axis, index, d, e):
        to, tc = ring(index, d), lax.rem(c + e, 2)
        return {axis: to, "core": tc}, 2 * to + tc

    peers = [plane("batch", y, d, e)[0] for d, e in offsets]
    peers += [plane("z", z, d, e)[0] for d, e in offsets if d]
    peers += [{"x": ring(x, d)} for d in (1, 2, 3)]
    barrier = entry_signal(peers)

    local_sem = s["local_sem"]
    first_loads = [
        pltpu.make_async_copy(hid_hbm, s["hid"], local_sem.at[0]),
        pltpu.make_async_copy(q_hbm, s["q"], local_sem.at[1]),
        pltpu.make_async_copy(g_hbm, s["g"], local_sem.at[2]),
        pltpu.make_async_copy(lg_hbm, s["lg"], local_sem.at[3]),
        pltpu.make_async_copy(segr_hbm, s["segr"], local_sem.at[4]),
        pltpu.make_async_copy(gain_hbm, s["gain"], local_sem.at[5]),
    ]

    def step_at(i):
        return lax.rem(i + 4 - 4 * c, 8)

    def weight_load(hbm, name, i, base):
        cols = rows_of(step_at(i) * 256, 256)
        return pltpu.make_async_copy(hbm.at[:, cols], s[name].at[:, cols], local_sem.at[base + i])

    first_loads[0].start()
    for n in (3, 4, 5):
        first_loads[n].start()
    for i in range(8):
        weight_load(wk_hbm, "wk", i, 8).start()
        weight_load(wv_hbm, "wv", i, 16).start()
        if i == 0:
            first_loads[1].start()
            first_loads[2].start()

    first_loads[0].wait()
    for b in range(8):
        cols = slice(b * TOK, (b + 1) * TOK)
        s["hid_t"][cols, :] = s["hid"][:, cols].astype(F32).T
    pl.semaphore_wait(barrier, len(peers))
    gathers = (("batch", y, s["hy"]), ("z", z, s["hz"]))
    hops = []
    for axis, index, buf in gathers:
        for d in (1, 3):
            hops.append(remote(s["hid_t"], buf.at[index, c], {axis: ring(index, d)}))

    rows_i, cols_i = iota((TOK, TOK), 0), iota((TOK, TOK), 1)
    causal = cols_i <= rows_i
    lower = causal.astype(F32)
    low = cols_i < 64
    low_half = iota((64, PAIR), 1) < 64
    row8 = iota((8, PAIR), 0)
    low_row = iota((1, PAIR), 1) < 64
    for n in (3, 4, 5):
        first_loads[n].wait()
    log_gate = s["lg"][...]
    cum_cols = dot_exact(lower, log_gate, NT)
    s["cumr"][...] = dot_exact(log_gate, lower, NT)
    for pair in range(16):
        s["cumx"][pair] = jnp.where(
            low, cum_cols[:, 2 * pair : 2 * pair + 1], cum_cols[:, 2 * pair + 1 : 2 * pair + 2]
        )
        s["cumr3"][pair, 0:2, :] = s["cumr"][2 * pair : 2 * pair + 2, :]
    seg_row = s["segr"][...].astype(F32)
    s["segc"][...] = jnp.broadcast_to(seg_row, (TOK, TOK)).T
    s["gcross"][...] = jnp.zeros((16, 8, PAIR), F32)

    first_loads[1].wait()
    first_loads[2].wait()

    def project(i, st):
        step = step_at(i)
        weight_load(wk_hbm, "wk", i, 8).wait()
        weight_load(wv_hbm, "wv", i, 16).wait()
        wide = rows_of(step * 256, 256)
        hid = s["hid"][...]
        keys = dot(hid, s["wk"][:, wide], NN).astype(BF16)
        values = dot(hid, s["wv"][:, wide], NN).astype(BF16)
        segc = s["segc"][...]
        for p in range(2):
            pair = 2 * step + p
            k, v = keys[:, p * PAIR : (p + 1) * PAIR], values[:, p * PAIR : (p + 1) * PAIR]
            s["k"][pair] = k
            s["v"][pair] = v
            cum = s["cumx"][pair]
            total = cum[TOK - 1 : TOK, :]
            last_w = jnp.where(segc == segc[TOK - 1 : TOK, :], jnp.exp(total - cum), 0.0)
            first_w = jnp.where(segc == segc[0:1, :], jnp.exp(cum), 0.0)
            s["lw"][pair] = last_w
            s["fw"][pair] = first_w
            cols = rows_of(pair * PAIR, PAIR)
            fwd = dot_left(k.astype(F32) * last_w, v, TN)
            rev = dot_left(s["q"][:, cols].astype(F32) * first_w, s["g"][:, cols], TN)
            pp = 2 * lax.rem(step, 4) + p
            st[rows_of(pp * 64, 64), :] = jnp.where(low_half, fwd[:64], fwd[64:])
            st[rows_of(512 + pp * 64, 64), :] = jnp.where(low_half, rev[:64], rev[64:])
            meta = jnp.where(
                row8 == 0,
                total,
                jnp.where(
                    row8 == 1, segc[0:1, :], jnp.where(row8 == 2, segc[TOK - 1 : TOK, :], 0.0)
                ),
            )
            st[rows_of(1024 + pp * 8, 8), :] = meta

    both = s["both"]
    lax.fori_loop(0, 4, lambda i, carry: project(i, s["st"]), None)
    swap = remote(s["st"], both.at[c], sib)
    down = [remote(s["hid_t"], buf.at[index, c], sib) for _, index, buf in gathers]
    lax.fori_loop(4, 8, lambda i, carry: project(i, both.at[c]), None)

    def inner(pair, carry):
        cols = rows_of(pair * PAIR, PAIR)
        q, g = s["q"][:, cols], s["g"][:, cols]
        k, v = s["k"][pair], s["v"][pair]
        allowed = causal & (s["segc"][...] == seg_row)
        gap = jnp.bitwise_xor(rows_i, cols_i)
        strict = (rows_i < cols_i).astype(BF16)
        zero = jnp.zeros((TOK, PAIR), BF16)
        weighted, scored, queries, keys, grads, gate_rows, gain_rows = [], [], [], [], [], [], []
        for h in range(2):

            def own(a):
                return jnp.where(low, a, zero) if h == 0 else jnp.where(low, zero, a)

            qh, gh, kh = own(q), own(g), own(k)
            score = dot(qh, k, NT)
            dprob = dot(gh, v, NT)
            spread = s["cumx"][pair, :, 64 * h : 64 * h + 1] - s["cumr3"][pair, h : h + 1, :]
            decay = jnp.where(allowed, jnp.exp(jnp.where(allowed, spread, 0.0)), 0.0)
            ds = decay * score
            joint = ds * dprob
            head = 2 * pair + h
            level = jnp.full((TOK, TOK), gain_ref[0, head], F32)
            gain_rows.append(jnp.sum(jnp.where(gap == 0, joint, 0.0), axis=0, keepdims=True))
            for l in range(1, 8):
                above = gap >= 2 ** (l - 1)
                level = jnp.where(above, gain_ref[l, head], level)
                chosen = above & (gap < 2**l)
                gain_rows.append(jnp.sum(jnp.where(chosen, joint, 0.0), axis=0, keepdims=True))
            wd = level * decay * dprob
            weighted.append(wd.astype(BF16))
            scored.append((level * ds).astype(BF16))
            grid = (wd * score).astype(BF16)
            crossing = jnp.where(causal, dot(grid, strict, NN), 0.0)
            gate_rows.append(jnp.sum(crossing, axis=0, keepdims=True))
            queries.append(qh)
            keys.append(kh)
            grads.append(gh)
        s["qacc"][pair] = dot(
            jnp.concatenate(weighted, axis=1), jnp.concatenate(keys, axis=0), NN
        )
        s["kacc"][pair] = dot(
            jnp.concatenate(weighted, axis=0), jnp.concatenate(queries, axis=0), TN
        )
        s["vacc"][pair] = dot(jnp.concatenate(scored, axis=0), jnp.concatenate(grads, axis=0), TN)
        s["gate"][pair] = jnp.concatenate([*gate_rows, jnp.zeros((6, TOK), F32)], axis=0)
        s["gint"][pair] = jnp.concatenate(gain_rows, axis=0)
        return carry

    swap.wait()

    def meta_rows(total, first, last):
        return jnp.where(
            row8 == 0, total, jnp.where(row8 == 1, first, jnp.where(row8 == 2, last, 0.0))
        )

    chip_send, chip_recv = s["chip_send"], s["chip_recv"]

    def block_pair(pp):
        f0 = both[0, pp * 64 : pp * 64 + 64, :]
        f1 = both[1, pp * 64 : pp * 64 + 64, :]
        r0 = both[0, 512 + pp * 64 : 576 + pp * 64, :]
        r1 = both[1, 512 + pp * 64 : 576 + pp * 64, :]
        m0 = both[0, 1024 + pp * 8 : 1032 + pp * 8, :]
        m1 = both[1, 1024 + pp * 8 : 1032 + pp * 8, :]
        return f0, f1, r0, r1, m0[0:1], m0[1:2], m0[2:3], m1[0:1], m1[1:2], m1[2:3]

    def chip_sums(p):
        for n in range(4):
            f0, f1, r0, r1, t0, first0, last0, t1, first1, last1 = block_pair(2 * n + p)
            chip_send[p, n, 0:64, :] = f1 + linked(last0, last1, t1) * f0
            chip_send[p, n, 64:128, :] = r0 + linked(first0, first1, t0) * r1
            chip_send[p, n, 128:136, :] = meta_rows(t0 + t1, first0, last1)

    def chip_sends(p):
        copies = []
        for d in (2, 1, 3):
            to = ring(x, d)
            copies.append(remote(chip_send.at[p, to], chip_recv.at[p, x], {"x": to}))
        chip_recv[p, pl.ds(x, 1)] = chip_send[p, pl.ds(x, 1)]
        return copies

    xs = []
    for p in range(2):
        chip_sums(p)
        xs.append(chip_sends(p))
    for pp in range(8):
        f0, _, _, r1, _, _, last0, _, first1, _ = block_pair(pp)
        d8 = same(last0, first1) * jnp.sum(f0 * r1, axis=0, keepdims=True)
        s["gcross"][pl.ds(c * 8 + pp, 1)] = jnp.where(row8 == 0, d8, 0.0)[None]
    lax.fori_loop(0, 7, inner, 0)

    def chip(j, p):
        return (
            chip_recv[p, j, 0:64, :],
            chip_recv[p, j, 64:128, :],
            chip_recv[p, j, 128:129, :],
            chip_recv[p, j, 129:130, :],
            chip_recv[p, j, 130:131, :],
        )

    def joined(p):
        (f0, r0, t0, a0, l0), (f1, r1, t1, a1, l1), (f2, r2, t2, a2, l2), (f3, r3, t3, a3, l3) = (
            chip(j, p) for j in range(4)
        )
        f01 = f1 + linked(l0, l1, t1) * f0
        r01 = r0 + linked(a0, a1, t0) * r1
        f23 = f3 + linked(l2, l3, t3) * f2
        r23 = r2 + linked(a2, a3, t2) * r3
        return f01, r01, f23, r23

    tot_send, tot_recv = s["tot_send"], s["tot_recv"]
    zs = []
    for p in range(2):
        wait(xs[p])
        f01, r01, f23, r23 = joined(p)
        t0, a0 = chip(0, p)[2:4]
        t1, l1 = chip(1, p)[2], chip(1, p)[4]
        t2, a2 = chip(2, p)[2:4]
        t3, l3 = chip(3, p)[2], chip(3, p)[4]
        tot_send[p, 0, 0:64, :] = f23 + linked(l1, l3, t2 + t3) * f01
        tot_send[p, 1, 0:64, :] = r01 + linked(a0, a2, t0 + t1) * r23
        tot_send[p, 0, 64:72, :] = jnp.broadcast_to(l3, (8, PAIR))
        tot_send[p, 1, 64:72, :] = jnp.broadcast_to(a0, (8, PAIR))
        zs.append(
            [
                remote(tot_send.at[p, n], tot_recv.at[p, n], {"z": ring(z, d)})
                for n, d in ((0, 1), (1, 3))
            ]
        )

    fwd = []
    for n, (axis, index, buf) in enumerate(gathers):
        for m, d in enumerate((1, 3)):
            hops[2 * n + m].wait()
            came = ring(index, 4 - d)
            part = slice(0, 512) if d == 1 else slice(512, 1024)
            fwd.append(
                remote(buf.at[came, c, part], buf.at[came, c, part], {axis: ring(index, d)})
            )
            down.append(remote(buf.at[came, c], buf.at[came, c], sib))

    lax.fori_loop(7, 9, inner, 0)

    has_prev = (z > 0).astype(F32)
    has_next = (z < 3).astype(F32)
    prev_top = (z == 2).astype(F32)
    next_top = (z == 1).astype(F32)
    back_send, back_recv = s["back_send"], s["back_recv"]

    def gain_row(pair, level):
        return jnp.where(low_row, gain_ref[level, 2 * pair], gain_ref[level, 2 * pair + 1])

    bs = []
    for p in range(2):
        wait(zs[p])
        (f0, r0, t0, a0, l0), (f1, r1, t1, a1, l1), (f2, r2, t2, a2, l2), (f3, r3, t3, a3, l3) = (
            chip(j, p) for j in range(4)
        )
        f01, r01, f23, r23 = joined(p)
        pair = c * 8 + 2 * x + p
        g9, g10, g11, g12 = (gain_row(pair, level) for level in range(9, 13))
        zf = has_prev * tot_recv[p, 0, 0:64, :]
        zl = tot_recv[p, 0, 64:65, :]
        zr = has_next * tot_recv[p, 1, 0:64, :]
        za = tot_recv[p, 1, 64:65, :]
        gzf = g11 * (1.0 - prev_top) + g12 * prev_top
        gzr = g11 * (1.0 - next_top) + g12 * next_top
        sf = (
            gzf * same(zl, a0) * zf,
            gzf * linked(zl, a1, t0) * zf + g9 * same(l0, a1) * f0,
            gzf * linked(zl, a2, t0 + t1) * zf + g10 * same(l1, a2) * f01,
            gzf * linked(zl, a3, t0 + t1 + t2) * zf
            + g10 * linked(l1, a3, t2) * f01
            + g9 * same(l2, a3) * f2,
        )
        sr = (
            gzr * linked(za, l0, t1 + t2 + t3) * zr
            + g10 * linked(l0, a2, t1) * r23
            + g9 * same(l0, a1) * r1,
            gzr * linked(za, l1, t2 + t3) * zr + g10 * same(l1, a2) * r23,
            gzr * linked(za, l2, t3) * zr + g9 * same(l2, a3) * r3,
            gzr * same(za, l3) * zr,
        )
        for j in range(4):
            back_send[p, j, 0:64, :] = sf[j]
            back_send[p, j, 64:128, :] = sr[j]
        copies = []
        for d in (1, 2, 3):
            to = ring(x, d)
            copies.append(remote(back_send.at[p, to], back_recv.at[p, x], {"x": to}))
        back_recv[p, pl.ds(x, 1)] = back_send[p, pl.ds(x, 1)]
        bs.append(copies)

    for p in range(2):
        (f0, r0, t0, a0, l0), (f1, r1, t1, a1, l1), (f2, r2, t2, a2, l2), (f3, r3, t3, a3, l3) = (
            chip(j, p) for j in range(4)
        )
        f01, r01, f23, r23 = joined(p)
        zf = has_prev * tot_recv[p, 0, 0:64, :]
        zl = tot_recv[p, 0, 64:65, :]
        r_group = r01 + linked(a0, a2, t0 + t1) * r23
        d9 = same(l0, a1) * jnp.sum(f0 * r1, axis=0, keepdims=True) + same(l2, a3) * jnp.sum(
            f2 * r3, axis=0, keepdims=True
        )
        d10 = same(l1, a2) * jnp.sum(f01 * r23, axis=0, keepdims=True)
        dz = same(zl, a0) * jnp.sum(zf * r_group, axis=0, keepdims=True)
        rows = jnp.where(
            row8 == 1,
            d9,
            jnp.where(
                row8 == 2,
                d10,
                jnp.where(
                    row8 == 3, (1.0 - prev_top) * dz, jnp.where(row8 == 4, prev_top * dz, 0.0)
                ),
            ),
        )
        pair = c * 8 + 2 * x + p
        s["gcross"][pl.ds(pair, 1)] = s["gcross"][pl.ds(pair, 1)] + rows[None]
    lax.fori_loop(9, 16, inner, 0)
    def rounded(n, block, core):
        buf, out = gathers[n][2], s[("hyb", "hzb")[n]]
        out[:, rows_of((2 * block + core) * TOK, TOK)] = buf[block, core].astype(BF16)

    for n, (_, index, buf) in enumerate(gathers):
        s[("hyb", "hzb")[n]][:, rows_of((2 * index + c) * TOK, TOK)] = s["hid_t"][...].astype(BF16)
        down[n].wait()
        rounded(n, index, 1 - c)
        for m, d in enumerate((1, 3)):
            came = ring(index, 4 - d)
            rounded(n, came, c)
            down[2 + 2 * n + m].wait()
            rounded(n, came, 1 - c)

    own_blocks, s_in = s["own_blocks"], s["s_in"]
    swaps = []
    for p in range(2):
        wait(bs[p])
        for n in range(4):
            pp = 2 * n + p
            f0, _, _, r1, t0, first0, last0, t1, first1, last1 = block_pair(pp)
            sf = back_recv[p, n, 0:64, :]
            sr = back_recv[p, n, 64:128, :]
            link = gain_row(c * 8 + pp, 8) * same(last0, first1)
            at = n * 128
            own_blocks[p, 0, at : at + 64, :] = sf
            own_blocks[p, 1, at : at + 64, :] = linked(first0, first1, t0) * sf + link * f0
            own_blocks[p, 0, at + 64 : at + 128, :] = linked(last0, last1, t1) * sr + link * r1
            own_blocks[p, 1, at + 64 : at + 128, :] = sr
        swaps.append(remote(own_blocks.at[p, 1 - c], s_in.at[p, c], sib))
        s_in[p, pl.ds(c, 1)] = own_blocks[p, pl.ds(c, 1)]

    tail = causal.astype(BF16)
    head_pick = (cols_i[0:8, :] // 64 == row8).astype(BF16)

    def diag(a):
        return jnp.concatenate([jnp.where(low_half, a, 0.0), jnp.where(low_half, 0.0, a)], axis=0)

    def incoming(to, p, part):
        if isinstance(to, int):
            at = to % 4 * 128 + part * 64
            return diag(s_in[p, to // 4, at : at + 64, :])
        at = lax.rem(to, 4) * 128 + part * 64
        return diag(s_in[p, to // 4, rows_of(at, 64), :])

    def key_part(to, p):
        pair = 2 * to + p
        rv = s["lw"][pair] * dot_right(s["v"][pair], incoming(to, p, 1), NT)
        key_sum = (s["kacc"][pair] + rv).astype(BF16)
        s["kacc"][pair] = s["k"][pair].astype(F32) * rv
        s["ksb"][:, rows_of(pair * PAIR, PAIR)] = key_sum
        s["ks"][p, to] = key_sum.astype(F32)

    def value_part(to, p):
        pair = 2 * to + p
        rk = s["lw"][pair] * dot_right(s["k"][pair], incoming(to, p, 1), NN)
        value_sum = (s["vacc"][pair] + rk).astype(BF16)
        s["vsb"][:, rows_of(pair * PAIR, PAIR)] = value_sum
        s["vs"][p, to] = value_sum.astype(F32)

    def query_part(to, p):
        pair = 2 * to + p
        cols = slice(pair * PAIR, (pair + 1) * PAIR)
        sg = s["fw"][pair] * dot_right(s["g"][:, cols], incoming(to, p, 0), NT)
        qg_ref[:, cols] = (s["qacc"][pair] + sg).astype(BF16)
        diff = s["q"][:, cols].astype(F32) * sg - s["kacc"][pair]
        hi, lo = split2(diff)
        diff_rows = dot(head_pick, hi, NT) + dot(head_pick, lo, NT)
        s["gate"][pair] = s["gate"][pair] + dot_left(diff_rows, tail, NN)

    firsts = []
    me_y, me_z = 2 * y + c, 2 * z + c
    far_first = [(2, 0), (2, 1), (1, 0), (3, 0), (1, 1), (3, 1), (0, 1)]
    for n in range(2):
        swaps[n].wait()
        fk, fv = [], []
        for d, e in far_first:
            dev, to = plane("batch", y, d, e)
            key_part(to, n)
            fk.append(remote(s["ks"].at[n, to], s["rk"].at[n, me_y], dev))
            dev, to = plane("z", z, d, e)
            value_part(to, n)
            fv.append(remote(s["vs"].at[n, to], s["rv"].at[n, me_z], dev))
        key_part(me_y, n)
        value_part(me_z, n)
        firsts.append((fk, fv))
    for n, (_, index, buf) in enumerate(gathers):
        wait(fwd[2 * n : 2 * n + 2])
        came = ring(index, 2)
        down.append(remote(buf.at[came, c], buf.at[came, c], sib))
    for n in range(2):
        s["rk"][n, pl.ds(me_y, 1)] = s["ks"][n, pl.ds(me_y, 1)]
        s["rv"][n, pl.ds(me_z, 1)] = s["vs"][n, pl.ds(me_z, 1)]

    for n, (_, index, buf) in enumerate(gathers):
        came = ring(index, 2)
        rounded(n, came, c)
        down[6 + n].wait()
        rounded(n, came, 1 - c)

    def product(left, right, n):
        right = s[right][n].reshape(8 * TOK, PAIR).astype(BF16)
        for b in range(4):
            yield b, dot(s[left][b * 256 : (b + 1) * 256, :], right, NN)

    part1, recv1, part2, recv2 = s["part1"], s["recv1"], s["part2"], s["recv2"]

    def scatter(part, recv, chunk, axis, index):
        out = []
        for d in (1, 2, 3):
            to = ring(index, d)
            out.append(remote(part.at[chunk, to], recv.at[chunk, index], {axis: to}))
        recv[chunk, pl.ds(index, 1)] = part[chunk, pl.ds(index, 1)]
        return out

    wait(firsts[0][0])
    for b, block in product("hyb", "rk", 0):
        for j in range(4):
            part1[0, j, b * 64 : b * 64 + 64, :] = block[j * 64 : j * 64 + 64, :]
    k0 = scatter(part1, recv1, 0, "x", x)
    wait(firsts[0][1])
    for b, block in product("hzb", "rv", 0):
        for j in range(4):
            part1[2, j, b * 64 : b * 64 + 64, :] = block[j * 64 : j * 64 + 64, :]
    v0 = scatter(part1, recv1, 2, "x", x)

    for n in range(2):
        for to in range(8):
            query_part(to, n)
    stores = []

    def store(ref, hbm):
        cp = pltpu.make_async_copy(ref, hbm, local_sem.at[24 + len(stores)])
        cp.start()
        stores.append(cp)

    store(qg_ref, qg_hbm)
    store(s["gate"], gate_hbm)

    ones = jnp.ones((8, PAIR), F32)
    inner_sum = dot_exact(ones, s["gint"][...].reshape(256, PAIR), NT)
    pick = (cols_i[0:8, :] // 64 == row8 - 2).astype(F32)
    outer_sum = dot_exact(pick, s["gcross"][...].reshape(128, PAIR), NT)
    start = (cols_i[0:8, :] == 0).astype(F32)
    own_total = dot_exact(start, s["gate"][...].reshape(128, TOK), NT)
    small, m1, m1s, m2, m2s, m3 = (s[n] for n in ("small", "m1", "m1s", "m2", "m2s", "m3"))
    small[0:8, :] = jnp.where(
        row8 == 0, inner_sum[:, :128], jnp.where(row8 == 1, inner_sum[:, 128:], outer_sum)
    )
    small[8:16, :] = own_total
    smalls = []
    for d, e in offsets:
        smalls.append(remote(small, m1.at[me_z], plane("z", z, d, e)[0]))
    m1[pl.ds(me_z, 1)] = small[...][None]

    def input_grad(n, carry):
        rows = rows_of(n * 256, 256)
        ig_ref[:, rows] = (
            dot(s["ksb"][...], s["wk"][rows, :], NT) + dot(s["vsb"][...], s["wv"][rows, :], NT)
        ).astype(BF16)
        return carry


    wait(firsts[1][0])
    for b, block in product("hyb", "rk", 1):
        part1[1, b] = block
    k1 = scatter(part1, recv1, 1, "z", z)
    wait(firsts[1][1])
    for b, block in product("hzb", "rv", 1):
        for j in range(8):
            for i in range(4):
                at = j * 32 + i * 8
                part1[3, i, b * 64 + j * 8 : b * 64 + j * 8 + 8, :] = block[at : at + 8, :]
    v1 = scatter(part1, recv1, 3, "batch", y)
    lax.fori_loop(0, 4, input_grad, 0)
    store(ig_ref, ig_hbm)

    wait(smalls)
    total = m1[0, 0:8, :]
    for g in range(1, 8):
        total = total + m1[g, 0:8, :]
    m1s[0:8, :] = total
    for g in range(8):
        m1s[8 + g : 9 + g, :] = m1[g, 8:9, :]
    smalls = [remote(m1s, m2.at[x], {"x": ring(x, d)}) for d in (1, 2, 3)]
    m2[pl.ds(x, 1)] = m1s[...][None]

    def summed(recv, chunk):
        return recv[chunk, 0] + recv[chunk, 1] + recv[chunk, 2] + recv[chunk, 3]

    wait(k0)
    total = summed(recv1, 0)
    for j in range(4):
        part2[0, j] = total[j * 64 : j * 64 + 64, :]
    k0 = scatter(part2, recv2, 0, "z", z)
    wait(v0)
    total = summed(recv1, 2)
    for j in range(8):
        for i in range(4):
            at = j * 32 + i * 8
            part2[2, i, j * 8 : j * 8 + 8, :] = total[at : at + 8, :]
    v0 = scatter(part2, recv2, 2, "batch", y)
    wait(k1)
    total = summed(recv1, 1)
    for j in range(4):
        part2[1, j] = total[j * 64 : j * 64 + 64, :]
    k1 = scatter(part2, recv2, 1, "x", x)
    wait(v1)
    total = summed(recv1, 3)
    for j in range(4):
        for i in range(4):
            at = j * 64 + i * 16
            part2[3, i, j * 16 : j * 16 + 16, :] = total[at : at + 16, :]
    v1 = scatter(part2, recv2, 3, "x", x)

    wait(smalls)
    total = m2[0, 0:8, :] + m2[1, 0:8, :] + m2[2, 0:8, :] + m2[3, 0:8, :]
    m2s[...] = total
    smalls = [remote(m2s, m3.at[y], {"batch": ring(y, d)}) for d in (1, 2, 3)]
    m3[pl.ds(y, 1)] = total[None]
    place = z * 8 + x * 2 + c
    later = jnp.zeros((1, PAIR), F32)
    for j in range(4):
        for g in range(8):
            spot = (g // 2) * 8 + j * 2 + g % 2
            later = later + (place < spot).astype(F32) * m2[j, 8 + g : 9 + g, :]
    sout_ref[8:16, :] = jnp.broadcast_to(later, (8, PAIR))

    fins = []
    wait(k0)
    wait(k1)
    for n in range(2):
        total = summed(recv2, n)
        for i in range(4):
            for j in range(2):
                at = j * 32 + i * 8
                s["kown"][2 * i + j, n] = total[at : at + 8, :]
    for d, e in offsets:
        dev, to = plane("batch", y, d, e)
        fins.append(remote(s["kown"].at[to], s["kfin"].at[me_y], dev))
    s["kfin"][pl.ds(me_y, 1)] = s["kown"][pl.ds(me_y, 1)]
    wait(v0)
    wait(v1)
    for n in range(2):
        total = summed(recv2, 2 + n)
        for j in range(8):
            s["vown"][j, n] = total[j * 8 : j * 8 + 8, :]
    for d, e in offsets:
        dev, to = plane("z", z, d, e)
        fins.append(remote(s["vown"].at[to], s["vfin"].at[me_z], dev))
    s["vfin"][pl.ds(me_z, 1)] = s["vown"][pl.ds(me_z, 1)]
    wait(smalls)
    sout_ref[0:8, :] = m3[0] + m3[1] + m3[2] + m3[3]
    store(sout_ref, sout_hbm)
    wait(fins)
    for n in range(2):
        for g in range(8):
            cols = slice((2 * g + n) * PAIR, (2 * g + n + 1) * PAIR)
            kout_ref[:, cols] = s["kfin"][g, n]
            vout_ref[:, cols] = s["vfin"][g, n]
    store(kout_ref, kout_hbm)
    store(vout_ref, vout_hbm)
    wait(stores)


def whole_step(hidden, queries, out_grad, w_key, w_value, log_gate, seg_row, level_gain):
    far = pl.BlockSpec(memory_space=pltpu.HBM)
    return pl.pallas_call(
        step_kernel,
        in_specs=[far] * 8,
        out_specs=[far] * 6,
        out_shape=[
            jax.ShapeDtypeStruct((TOK, 2048), BF16),
            jax.ShapeDtypeStruct((TOK, 1024), BF16),
            jax.ShapeDtypeStruct((16, 8, TOK), F32),
            jax.ShapeDtypeStruct((8, 2048), F32),
            jax.ShapeDtypeStruct((8, 2048), F32),
            jax.ShapeDtypeStruct((16, PAIR), F32),
        ],
        scratch_shapes=list(scratch().values()),
        compiler_params=pltpu.CompilerParams(
            collective_id=0, has_side_effects=True, vmem_limit_bytes=VMEM_LIMIT
        ),
        name="whole_step",
    )(hidden, queries, out_grad, w_key, w_value, log_gate, seg_row, level_gain)


def finish_kernel(
    qg_in, ig_in, gate_in, kw_in, vw_in, small_in, qg_out, ig_out, gate_out, kw_out, vw_out, gains_out,
    qg, ig, gate_ref, kw, vw, small_ref, gate, gains, load_sem, store_sem
):
    loads = [
        pltpu.make_async_copy(a, b, load_sem.at[n])
        for n, (a, b) in enumerate(
            ((gate_in, gate_ref), (small_in, small_ref), (qg_in, qg), (ig_in, ig), (kw_in, kw), (vw_in, vw))
        )
    ]
    for cp in loads:
        cp.start()
    stores = []

    def store(ref, out):
        cp = pltpu.make_async_copy(ref, out, store_sem.at[len(stores)])
        cp.start()
        stores.append(cp)

    loads[0].wait()
    loads[1].wait()
    heads = gate.shape[0]
    lane = iota((heads, PAIR), 1)
    head = iota((heads, PAIR), 0)
    small = small_ref[...]
    later = jnp.broadcast_to(small[8:9, :], (TOK, TOK)).T
    rows = gate_ref[...].reshape(TOK, TOK) + later
    gate[...] = dot_exact((lane == (head // 2) * 8 + head % 2).astype(F32), rows, NN)
    levels = gains.shape[0]
    level, at = iota((levels, PAIR), 0), iota((levels, PAIR), 1) % 8
    first = (level == at).astype(F32)
    second = (level == at + 8).astype(F32)
    pick0 = jnp.where(lane // 8 == head, small[0:1, :], 0.0)
    pick1 = jnp.where(lane // 8 + 16 == head, small[1:2, :], 0.0)
    pair = jnp.where(head % 2 == 0, small[2:3, :], small[3:4, :])
    pick2 = jnp.where(lane // 8 == head // 2, pair, 0.0)
    gains[...] = dot_exact(first, pick0 + pick1, NT) + dot_exact(second, pick2, NT)
    for cp, ref, out in zip(
        loads[2:], (qg, ig, kw, vw), (qg_out, ig_out, kw_out, vw_out)
    ):
        cp.wait()
        store(ref, out)
    store(gate, gate_out)
    store(gains, gains_out)
    for cp in stores:
        cp.wait()


def finish(query_grad, input_grad, gate, key_weight, value_weight, small, heads, levels):
    far = pl.BlockSpec(memory_space=pltpu.HBM)
    parts = (query_grad, input_grad, gate, key_weight, value_weight, small)
    outs = [jax.ShapeDtypeStruct(a.shape, a.dtype) for a in parts]
    outs[2] = jax.ShapeDtypeStruct((heads, TOK), F32)
    outs[5] = jax.ShapeDtypeStruct((levels, heads), F32)
    return pl.pallas_call(
        finish_kernel,
        in_specs=[far] * 6,
        out_specs=[far] * 6,
        out_shape=outs,
        scratch_shapes=[pltpu.VMEM(a.shape, a.dtype) for a in (*parts, outs[2], outs[5])]
        + [pltpu.SemaphoreType.DMA((6,)), pltpu.SemaphoreType.DMA((6,))],
        name="finish",
    )(*parts)


def local(hidden, queries, w_key, w_value, log_gate, level_gain, segment_ids, out_grad):
    heads, levels = level_gain.shape
    parts = whole_step(
        hidden[0], queries[0], out_grad[0], w_key, w_value, log_gate[0], segment_ids, level_gain.T
    )
    query_grad, input_grad, gate_grad, key_weight, value_weight, gains = finish(
        *parts, heads, levels
    )
    return (
        query_grad[None],
        input_grad[None],
        gate_grad[None],
        key_weight,
        value_weight,
        gains.T,
    )


def solution(mesh):
    split = Mesh(
        mesh.devices.reshape(4, 4, 2, mesh.shape["batch"]), ("z", "x", "core", "batch")
    )
    return jax.shard_map(
        local,
        mesh=split,
        in_specs=(
            P("batch", SEQ, None),
            P("batch", SEQ, None),
            P(),
            P(),
            P("batch", None, SEQ),
            P(),
            P("batch", SEQ),
            P("batch", SEQ, None),
        ),
        out_specs=(
            P("batch", SEQ, None),
            P("batch", SEQ, None),
            P("batch", None, SEQ),
            P(SEQ_BATCH, None),
            P(SEQ_BATCH, None),
            P(),
        ),
        check_vma=False,
    )
```

```python
import functools

import jax
import jax.numpy as jnp
from jax import lax
from jax.experimental import pallas as pl
from jax.experimental.pallas import tpu as pltpu
from jax.sharding import Mesh
from jax.sharding import PartitionSpec as P

SEQ = ("z", "x", "core")
SEQ_BATCH = ("z", "x", "core", "batch")
MESH = pl.DeviceIdType.MESH
HIGHEST = lax.Precision.HIGHEST
F32 = jnp.float32
BF16 = jnp.bfloat16

NT = (((1,), (1,)), ((), ()))
TN = (((0,), (0,)), ((), ()))
NN = (((1,), (0,)), ((), ()))

TOK = 128
PAIR = 128
HALF_ROWS = 1088


def dot(a, b, dims):
    return lax.dot_general(a, b, dims, preferred_element_type=F32)


def dot_exact(a, b, dims):
    return lax.dot_general(a, b, dims, preferred_element_type=F32, precision=HIGHEST)


def split2(x):
    hi = x.astype(BF16)
    return hi, (x - hi.astype(F32)).astype(BF16)


def dot_left(a, b, dims):
    hi, lo = split2(a)
    return dot(hi, b, dims) + dot(lo, b, dims)


def dot_right(a, b, dims):
    hi, lo = split2(b)
    return dot(a, hi, dims) + dot(a, lo, dims)


def iota(shape, dim):
    return lax.broadcasted_iota(jnp.int32, shape, dim)


def entry_signal(peers):
    barrier = pltpu.get_barrier_semaphore()
    for peer in peers:
        pl.semaphore_signal(barrier, inc=1, device_id=peer, device_id_type=MESH)
    return barrier


def ring(index, step):
    return lax.rem(index + step, 4)


def same(a, b):
    return jnp.where(a == b, 1.0, 0.0)


def linked(a, b, total):
    return jnp.where(a == b, jnp.exp(total), 0.0)


def rows_of(start, size):
    return pl.ds(pl.multiple_of(start, size), size)


SENDS = 128
LOCALS = 32
VMEM_LIMIT = 56 * 2**20


def scratch():
    def f(*shape):
        return pltpu.VMEM(shape, F32)

    def b(*shape):
        return pltpu.VMEM(shape, BF16)

    return dict(
        wk=b(1024, 2048),
        wv=b(1024, 2048),
        hid=b(TOK, 1024),
        q=b(TOK, 2048),
        g=b(TOK, 2048),
        k=b(16, TOK, PAIR),
        v=b(16, TOK, PAIR),
        hid_t=f(1024, TOK),
        cumx=f(16, TOK, PAIR),
        cumr=f(32, TOK),
        cumr3=f(16, 8, TOK),
        fw=f(16, TOK, PAIR),
        lw=f(16, TOK, PAIR),
        segc=f(TOK, TOK),
        st=f(HALF_ROWS, PAIR),
        both=f(2, HALF_ROWS, PAIR),
        chip_send=f(2, 4, 136, PAIR),
        chip_recv=f(2, 4, 136, PAIR),
        tot_send=f(2, 2, 72, PAIR),
        tot_recv=f(2, 2, 72, PAIR),
        back_send=f(2, 4, 128, PAIR),
        back_recv=f(2, 4, 128, PAIR),
        own_blocks=f(2, 2, 512, PAIR),
        s_in=f(2, 2, 512, PAIR),
        gcross=f(16, 8, PAIR),
        gint=f(16, 16, PAIR),
        gate=f(16, 8, TOK),
        hy=f(4, 2, 1024, TOK),
        hz=f(4, 2, 1024, TOK),
        hyb=b(1024, 8 * TOK),
        hzb=b(1024, 8 * TOK),
        qacc=f(16, TOK, PAIR),
        kacc=f(16, TOK, PAIR),
        vacc=f(16, TOK, PAIR),
        ks=f(2, 8, TOK, PAIR),
        vs=f(2, 8, TOK, PAIR),
        ksb=b(TOK, 2048),
        vsb=b(TOK, 2048),
        rk=f(2, 8, TOK, PAIR),
        rv=f(2, 8, TOK, PAIR),
        part1=f(4, 4, 256, PAIR),
        recv1=f(4, 4, 256, PAIR),
        part2=f(4, 4, 64, PAIR),
        recv2=f(4, 4, 64, PAIR),
        kown=f(8, 2, 8, PAIR),
        vown=f(8, 2, 8, PAIR),
        kfin=f(8, 2, 8, PAIR),
        vfin=f(8, 2, 8, PAIR),
        small=f(16, PAIR),
        m1=f(8, 16, PAIR),
        m1s=f(16, PAIR),
        m2=f(4, 16, PAIR),
        m2s=f(8, PAIR),
        m3=f(4, 8, PAIR),
        lg=f(32, TOK),
        segr=pltpu.VMEM((1, TOK), jnp.int32),
        gain=pltpu.SMEM((18, 32), F32),
        qg=b(TOK, 2048),
        ig=b(TOK, 1024),
        kout=f(8, 2048),
        vout=f(8, 2048),
        sout=f(16, PAIR),
        send_sem=pltpu.SemaphoreType.DMA((SENDS,)),
        recv_sem=pltpu.SemaphoreType.DMA((SENDS,)),
        local_sem=pltpu.SemaphoreType.DMA((LOCALS,)),
    )


def step_kernel(
    hid_hbm,
    q_hbm,
    g_hbm,
    wk_hbm,
    wv_hbm,
    lg_hbm,
    segr_hbm,
    gain_hbm,
    qg_hbm,
    ig_hbm,
    gate_hbm,
    kout_hbm,
    vout_hbm,
    sout_hbm,
    *refs,
):
    s = dict(zip(scratch(), refs))
    gain_ref, qg_ref, ig_ref = s["gain"], s["qg"], s["ig"]
    kout_ref, vout_ref, sout_ref = s["kout"], s["vout"], s["sout"]
    x, y, z, c = (lax.axis_index(a) for a in ("x", "batch", "z", "core"))
    used = [0]

    def remote(src, dst, target):
        n = used[0]
        used[0] += 1
        cp = pltpu.make_async_remote_copy(
            src_ref=src,
            dst_ref=dst,
            send_sem=s["send_sem"].at[n],
            recv_sem=s["recv_sem"].at[n],
            device_id=target,
            device_id_type=MESH,
        )
        cp.start()
        return cp

    def wait(copies):
        for cp in copies:
            cp.wait()

    sib = {"core": 1 - c}
    offsets = [(d, e) for d in range(4) for e in (0, 1) if d or e]

    def plane(axis, index, d, e):
        to, tc = ring(index, d), lax.rem(c + e, 2)
        return {axis: to, "core": tc}, 2 * to + tc

    peers = [plane("batch", y, d, e)[0] for d, e in offsets]
    peers += [plane("z", z, d, e)[0] for d, e in offsets if d]
    peers += [{"x": ring(x, d)} for d in (1, 2, 3)]
    barrier = entry_signal(peers)

    local_sem = s["local_sem"]
    first_loads = [
        pltpu.make_async_copy(hid_hbm, s["hid"], local_sem.at[0]),
        pltpu.make_async_copy(q_hbm, s["q"], local_sem.at[1]),
        pltpu.make_async_copy(g_hbm, s["g"], local_sem.at[2]),
        pltpu.make_async_copy(lg_hbm, s["lg"], local_sem.at[3]),
        pltpu.make_async_copy(segr_hbm, s["segr"], local_sem.at[4]),
        pltpu.make_async_copy(gain_hbm, s["gain"], local_sem.at[5]),
    ]

    def step_at(i):
        return lax.rem(i + 4 - 4 * c, 8)

    def weight_load(hbm, name, i, base):
        cols = rows_of(step_at(i) * 256, 256)
        return pltpu.make_async_copy(hbm.at[:, cols], s[name].at[:, cols], local_sem.at[base + i])

    first_loads[0].start()
    for n in (3, 4, 5):
        first_loads[n].start()
    for i in range(8):
        weight_load(wk_hbm, "wk", i, 8).start()
        weight_load(wv_hbm, "wv", i, 16).start()
        if i == 0:
            first_loads[1].start()
            first_loads[2].start()

    first_loads[0].wait()
    for b in range(8):
        cols = slice(b * TOK, (b + 1) * TOK)
        s["hid_t"][cols, :] = s["hid"][:, cols].astype(F32).T
    pl.semaphore_wait(barrier, len(peers))
    gathers = (("batch", y, s["hy"]), ("z", z, s["hz"]))
    hops = []
    for axis, index, buf in gathers:
        for d in (1, 3):
            hops.append(remote(s["hid_t"], buf.at[index, c], {axis: ring(index, d)}))

    rows_i, cols_i = iota((TOK, TOK), 0), iota((TOK, TOK), 1)
    causal = cols_i <= rows_i
    lower = causal.astype(F32)
    low = cols_i < 64
    low_half = iota((64, PAIR), 1) < 64
    row8 = iota((8, PAIR), 0)
    low_row = iota((1, PAIR), 1) < 64
    for n in (3, 4, 5):
        first_loads[n].wait()
    log_gate = s["lg"][...]
    cum_cols = dot_exact(lower, log_gate, NT)
    s["cumr"][...] = dot_exact(log_gate, lower, NT)
    for pair in range(16):
        s["cumx"][pair] = jnp.where(
            low, cum_cols[:, 2 * pair : 2 * pair + 1], cum_cols[:, 2 * pair + 1 : 2 * pair + 2]
        )
        s["cumr3"][pair, 0:2, :] = s["cumr"][2 * pair : 2 * pair + 2, :]
    seg_row = s["segr"][...].astype(F32)
    s["segc"][...] = jnp.broadcast_to(seg_row, (TOK, TOK)).T
    s["gcross"][...] = jnp.zeros((16, 8, PAIR), F32)

    first_loads[1].wait()
    first_loads[2].wait()

    def project(i, st):
        step = step_at(i)
        weight_load(wk_hbm, "wk", i, 8).wait()
        weight_load(wv_hbm, "wv", i, 16).wait()
        wide = rows_of(step * 256, 256)
        hid = s["hid"][...]
        keys = dot(hid, s["wk"][:, wide], NN).astype(BF16)
        values = dot(hid, s["wv"][:, wide], NN).astype(BF16)
        segc = s["segc"][...]
        for p in range(2):
            pair = 2 * step + p
            k, v = keys[:, p * PAIR : (p + 1) * PAIR], values[:, p * PAIR : (p + 1) * PAIR]
            s["k"][pair] = k
            s["v"][pair] = v
            cum = s["cumx"][pair]
            total = cum[TOK - 1 : TOK, :]
            last_w = jnp.where(segc == segc[TOK - 1 : TOK, :], jnp.exp(total - cum), 0.0)
            first_w = jnp.where(segc == segc[0:1, :], jnp.exp(cum), 0.0)
            s["lw"][pair] = last_w
            s["fw"][pair] = first_w
            cols = rows_of(pair * PAIR, PAIR)
            fwd = dot_left(k.astype(F32) * last_w, v, TN)
            rev = dot_left(s["q"][:, cols].astype(F32) * first_w, s["g"][:, cols], TN)
            pp = 2 * lax.rem(step, 4) + p
            st[rows_of(pp * 64, 64), :] = jnp.where(low_half, fwd[:64], fwd[64:])
            st[rows_of(512 + pp * 64, 64), :] = jnp.where(low_half, rev[:64], rev[64:])
            meta = jnp.where(
                row8 == 0,
                total,
                jnp.where(
                    row8 == 1, segc[0:1, :], jnp.where(row8 == 2, segc[TOK - 1 : TOK, :], 0.0)
                ),
            )
            st[rows_of(1024 + pp * 8, 8), :] = meta

    both = s["both"]
    lax.fori_loop(0, 4, lambda i, carry: project(i, s["st"]), None)
    swap = remote(s["st"], both.at[c], sib)
    down = [remote(s["hid_t"], buf.at[index, c], sib) for _, index, buf in gathers]
    lax.fori_loop(4, 8, lambda i, carry: project(i, both.at[c]), None)

    def inner(pair, carry):
        cols = rows_of(pair * PAIR, PAIR)
        q, g = s["q"][:, cols], s["g"][:, cols]
        k, v = s["k"][pair], s["v"][pair]
        allowed = causal & (s["segc"][...] == seg_row)
        gap = jnp.bitwise_xor(rows_i, cols_i)
        strict = (rows_i < cols_i).astype(BF16)
        zero = jnp.zeros((TOK, PAIR), BF16)
        weighted, scored, queries, keys, grads, gate_rows, gain_rows = [], [], [], [], [], [], []
        for h in range(2):

            def own(a):
                return jnp.where(low, a, zero) if h == 0 else jnp.where(low, zero, a)

            qh, gh, kh = own(q), own(g), own(k)
            score = dot(qh, k, NT)
            dprob = dot(gh, v, NT)
            spread = s["cumx"][pair, :, 64 * h : 64 * h + 1] - s["cumr3"][pair, h : h + 1, :]
            decay = jnp.where(allowed, jnp.exp(jnp.where(allowed, spread, 0.0)), 0.0)
            ds = decay * score
            joint = ds * dprob
            head = 2 * pair + h
            level = jnp.full((TOK, TOK), gain_ref[0, head], F32)
            gain_rows.append(jnp.sum(jnp.where(gap == 0, joint, 0.0), axis=0, keepdims=True))
            for l in range(1, 8):
                above = gap >= 2 ** (l - 1)
                level = jnp.where(above, gain_ref[l, head], level)
                chosen = above & (gap < 2**l)
                gain_rows.append(jnp.sum(jnp.where(chosen, joint, 0.0), axis=0, keepdims=True))
            wd = level * decay * dprob
            weighted.append(wd.astype(BF16))
            scored.append((level * ds).astype(BF16))
            grid = (wd * score).astype(BF16)
            crossing = jnp.where(causal, dot(grid, strict, NN), 0.0)
            gate_rows.append(jnp.sum(crossing, axis=0, keepdims=True))
            queries.append(qh)
            keys.append(kh)
            grads.append(gh)
        s["qacc"][pair] = dot(
            jnp.concatenate(weighted, axis=1), jnp.concatenate(keys, axis=0), NN
        )
        s["kacc"][pair] = dot(
            jnp.concatenate(weighted, axis=0), jnp.concatenate(queries, axis=0), TN
        )
        s["vacc"][pair] = dot(jnp.concatenate(scored, axis=0), jnp.concatenate(grads, axis=0), TN)
        s["gate"][pair] = jnp.concatenate([*gate_rows, jnp.zeros((6, TOK), F32)], axis=0)
        s["gint"][pair] = jnp.concatenate(gain_rows, axis=0)
        return carry

    def inner_two(n, carry):
        inner(2 * n, carry)
        return inner(2 * n + 1, carry)

    swap.wait()

    def meta_rows(total, first, last):
        return jnp.where(
            row8 == 0, total, jnp.where(row8 == 1, first, jnp.where(row8 == 2, last, 0.0))
        )

    chip_send, chip_recv = s["chip_send"], s["chip_recv"]

    def block_pair(pp):
        f0 = both[0, pp * 64 : pp * 64 + 64, :]
        f1 = both[1, pp * 64 : pp * 64 + 64, :]
        r0 = both[0, 512 + pp * 64 : 576 + pp * 64, :]
        r1 = both[1, 512 + pp * 64 : 576 + pp * 64, :]
        m0 = both[0, 1024 + pp * 8 : 1032 + pp * 8, :]
        m1 = both[1, 1024 + pp * 8 : 1032 + pp * 8, :]
        return f0, f1, r0, r1, m0[0:1], m0[1:2], m0[2:3], m1[0:1], m1[1:2], m1[2:3]

    def chip_sums(p):
        for n in range(4):
            f0, f1, r0, r1, t0, first0, last0, t1, first1, last1 = block_pair(2 * n + p)
            chip_send[p, n, 0:64, :] = f1 + linked(last0, last1, t1) * f0
            chip_send[p, n, 64:128, :] = r0 + linked(first0, first1, t0) * r1
            chip_send[p, n, 128:136, :] = meta_rows(t0 + t1, first0, last1)

    def chip_sends(p):
        copies = []
        for d in (2, 1, 3):
            to = ring(x, d)
            copies.append(remote(chip_send.at[p, to], chip_recv.at[p, x], {"x": to}))
        chip_recv[p, pl.ds(x, 1)] = chip_send[p, pl.ds(x, 1)]
        return copies

    xs = []
    for p in range(2):
        chip_sums(p)
        xs.append(chip_sends(p))
    for pp in range(8):
        f0, _, _, r1, _, _, last0, _, first1, _ = block_pair(pp)
        d8 = same(last0, first1) * jnp.sum(f0 * r1, axis=0, keepdims=True)
        s["gcross"][pl.ds(c * 8 + pp, 1)] = jnp.where(row8 == 0, d8, 0.0)[None]
    lax.fori_loop(0, 3, inner_two, 0)

    def chip(j, p):
        return (
            chip_recv[p, j, 0:64, :],
            chip_recv[p, j, 64:128, :],
            chip_recv[p, j, 128:129, :],
            chip_recv[p, j, 129:130, :],
            chip_recv[p, j, 130:131, :],
        )

    def joined(p):
        (f0, r0, t0, a0, l0), (f1, r1, t1, a1, l1), (f2, r2, t2, a2, l2), (f3, r3, t3, a3, l3) = (
            chip(j, p) for j in range(4)
        )
        f01 = f1 + linked(l0, l1, t1) * f0
        r01 = r0 + linked(a0, a1, t0) * r1
        f23 = f3 + linked(l2, l3, t3) * f2
        r23 = r2 + linked(a2, a3, t2) * r3
        return f01, r01, f23, r23

    tot_send, tot_recv = s["tot_send"], s["tot_recv"]
    zs = []
    for p in range(2):
        wait(xs[p])
        f01, r01, f23, r23 = joined(p)
        t0, a0 = chip(0, p)[2:4]
        t1, l1 = chip(1, p)[2], chip(1, p)[4]
        t2, a2 = chip(2, p)[2:4]
        t3, l3 = chip(3, p)[2], chip(3, p)[4]
        tot_send[p, 0, 0:64, :] = f23 + linked(l1, l3, t2 + t3) * f01
        tot_send[p, 1, 0:64, :] = r01 + linked(a0, a2, t0 + t1) * r23
        tot_send[p, 0, 64:72, :] = jnp.broadcast_to(l3, (8, PAIR))
        tot_send[p, 1, 64:72, :] = jnp.broadcast_to(a0, (8, PAIR))
        zs.append(
            [
                remote(tot_send.at[p, n], tot_recv.at[p, n], {"z": ring(z, d)})
                for n, d in ((0, 1), (1, 3))
            ]
        )

    fwd = []
    for n, (axis, index, buf) in enumerate(gathers):
        for m, d in enumerate((1, 3)):
            hops[2 * n + m].wait()
            came = ring(index, 4 - d)
            part = slice(0, 512) if d == 1 else slice(512, 1024)
            fwd.append(
                remote(buf.at[came, c, part], buf.at[came, c, part], {axis: ring(index, d)})
            )
            down.append(remote(buf.at[came, c], buf.at[came, c], sib))

    lax.fori_loop(3, 4, inner_two, 0)

    has_prev = (z > 0).astype(F32)
    has_next = (z < 3).astype(F32)
    prev_top = (z == 2).astype(F32)
    next_top = (z == 1).astype(F32)
    back_send, back_recv = s["back_send"], s["back_recv"]

    def gain_row(pair, level):
        return jnp.where(low_row, gain_ref[level, 2 * pair], gain_ref[level, 2 * pair + 1])

    bs = []
    for p in range(2):
        wait(zs[p])
        (f0, r0, t0, a0, l0), (f1, r1, t1, a1, l1), (f2, r2, t2, a2, l2), (f3, r3, t3, a3, l3) = (
            chip(j, p) for j in range(4)
        )
        f01, r01, f23, r23 = joined(p)
        pair = c * 8 + 2 * x + p
        g9, g10, g11, g12 = (gain_row(pair, level) for level in range(9, 13))
        zf = has_prev * tot_recv[p, 0, 0:64, :]
        zl = tot_recv[p, 0, 64:65, :]
        zr = has_next * tot_recv[p, 1, 0:64, :]
        za = tot_recv[p, 1, 64:65, :]
        gzf = g11 * (1.0 - prev_top) + g12 * prev_top
        gzr = g11 * (1.0 - next_top) + g12 * next_top
        sf = (
            gzf * same(zl, a0) * zf,
            gzf * linked(zl, a1, t0) * zf + g9 * same(l0, a1) * f0,
            gzf * linked(zl, a2, t0 + t1) * zf + g10 * same(l1, a2) * f01,
            gzf * linked(zl, a3, t0 + t1 + t2) * zf
            + g10 * linked(l1, a3, t2) * f01
            + g9 * same(l2, a3) * f2,
        )
        sr = (
            gzr * linked(za, l0, t1 + t2 + t3) * zr
            + g10 * linked(l0, a2, t1) * r23
            + g9 * same(l0, a1) * r1,
            gzr * linked(za, l1, t2 + t3) * zr + g10 * same(l1, a2) * r23,
            gzr * linked(za, l2, t3) * zr + g9 * same(l2, a3) * r3,
            gzr * same(za, l3) * zr,
        )
        for j in range(4):
            back_send[p, j, 0:64, :] = sf[j]
            back_send[p, j, 64:128, :] = sr[j]
        copies = []
        for d in (1, 2, 3):
            to = ring(x, d)
            copies.append(remote(back_send.at[p, to], back_recv.at[p, x], {"x": to}))
        back_recv[p, pl.ds(x, 1)] = back_send[p, pl.ds(x, 1)]
        bs.append(copies)

    for p in range(2):
        (f0, r0, t0, a0, l0), (f1, r1, t1, a1, l1), (f2, r2, t2, a2, l2), (f3, r3, t3, a3, l3) = (
            chip(j, p) for j in range(4)
        )
        f01, r01, f23, r23 = joined(p)
        zf = has_prev * tot_recv[p, 0, 0:64, :]
        zl = tot_recv[p, 0, 64:65, :]
        r_group = r01 + linked(a0, a2, t0 + t1) * r23
        d9 = same(l0, a1) * jnp.sum(f0 * r1, axis=0, keepdims=True) + same(l2, a3) * jnp.sum(
            f2 * r3, axis=0, keepdims=True
        )
        d10 = same(l1, a2) * jnp.sum(f01 * r23, axis=0, keepdims=True)
        dz = same(zl, a0) * jnp.sum(zf * r_group, axis=0, keepdims=True)
        rows = jnp.where(
            row8 == 1,
            d9,
            jnp.where(
                row8 == 2,
                d10,
                jnp.where(
                    row8 == 3, (1.0 - prev_top) * dz, jnp.where(row8 == 4, prev_top * dz, 0.0)
                ),
            ),
        )
        pair = c * 8 + 2 * x + p
        s["gcross"][pl.ds(pair, 1)] = s["gcross"][pl.ds(pair, 1)] + rows[None]
    lax.fori_loop(4, 8, inner_two, 0)
    def rounded(n, block, core):
        buf, out = gathers[n][2], s[("hyb", "hzb")[n]]
        out[:, rows_of((2 * block + core) * TOK, TOK)] = buf[block, core].astype(BF16)

    for n, (_, index, buf) in enumerate(gathers):
        s[("hyb", "hzb")[n]][:, rows_of((2 * index + c) * TOK, TOK)] = s["hid_t"][...].astype(BF16)
        down[n].wait()
        rounded(n, index, 1 - c)
        for m, d in enumerate((1, 3)):
            came = ring(index, 4 - d)
            rounded(n, came, c)
            down[2 + 2 * n + m].wait()
            rounded(n, came, 1 - c)

    own_blocks, s_in = s["own_blocks"], s["s_in"]
    swaps = []
    for p in range(2):
        wait(bs[p])
        for n in range(4):
            pp = 2 * n + p
            f0, _, _, r1, t0, first0, last0, t1, first1, last1 = block_pair(pp)
            sf = back_recv[p, n, 0:64, :]
            sr = back_recv[p, n, 64:128, :]
            link = gain_row(c * 8 + pp, 8) * same(last0, first1)
            at = n * 128
            own_blocks[p, 0, at : at + 64, :] = sf
            own_blocks[p, 1, at : at + 64, :] = linked(first0, first1, t0) * sf + link * f0
            own_blocks[p, 0, at + 64 : at + 128, :] = linked(last0, last1, t1) * sr + link * r1
            own_blocks[p, 1, at + 64 : at + 128, :] = sr
        swaps.append(remote(own_blocks.at[p, 1 - c], s_in.at[p, c], sib))
        s_in[p, pl.ds(c, 1)] = own_blocks[p, pl.ds(c, 1)]

    tail = causal.astype(BF16)
    head_pick = (cols_i[0:8, :] // 64 == row8).astype(BF16)

    def diag(a):
        return jnp.concatenate([jnp.where(low_half, a, 0.0), jnp.where(low_half, 0.0, a)], axis=0)

    def incoming(to, p, part):
        if isinstance(to, int):
            at = to % 4 * 128 + part * 64
            return diag(s_in[p, to // 4, at : at + 64, :])
        at = lax.rem(to, 4) * 128 + part * 64
        return diag(s_in[p, to // 4, rows_of(at, 64), :])

    def key_part(to, p):
        pair = 2 * to + p
        rv = s["lw"][pair] * dot_right(s["v"][pair], incoming(to, p, 1), NT)
        key_sum = (s["kacc"][pair] + rv).astype(BF16)
        s["kacc"][pair] = s["k"][pair].astype(F32) * rv
        s["ksb"][:, rows_of(pair * PAIR, PAIR)] = key_sum
        s["ks"][p, to] = key_sum.astype(F32)

    def value_part(to, p):
        pair = 2 * to + p
        rk = s["lw"][pair] * dot_right(s["k"][pair], incoming(to, p, 1), NN)
        value_sum = (s["vacc"][pair] + rk).astype(BF16)
        s["vsb"][:, rows_of(pair * PAIR, PAIR)] = value_sum
        s["vs"][p, to] = value_sum.astype(F32)

    def query_part(to, p):
        pair = 2 * to + p
        cols = slice(pair * PAIR, (pair + 1) * PAIR)
        sg = s["fw"][pair] * dot_right(s["g"][:, cols], incoming(to, p, 0), NT)
        qg_ref[:, cols] = (s["qacc"][pair] + sg).astype(BF16)
        diff = s["q"][:, cols].astype(F32) * sg - s["kacc"][pair]
        hi, lo = split2(diff)
        diff_rows = dot(head_pick, hi, NT) + dot(head_pick, lo, NT)
        s["gate"][pair] = s["gate"][pair] + dot_left(diff_rows, tail, NN)

    firsts = []
    me_y, me_z = 2 * y + c, 2 * z + c
    far_first = [(2, 0), (2, 1), (1, 0), (3, 0), (1, 1), (3, 1), (0, 1)]
    for n in range(2):
        swaps[n].wait()
        fk, fv = [], []
        for d, e in far_first:
            dev, to = plane("batch", y, d, e)
            key_part(to, n)
            fk.append(remote(s["ks"].at[n, to], s["rk"].at[n, me_y], dev))
            dev, to = plane("z", z, d, e)
            value_part(to, n)
            fv.append(remote(s["vs"].at[n, to], s["rv"].at[n, me_z], dev))
        key_part(me_y, n)
        value_part(me_z, n)
        firsts.append((fk, fv))
    for n, (_, index, buf) in enumerate(gathers):
        wait(fwd[2 * n : 2 * n + 2])
        came = ring(index, 2)
        down.append(remote(buf.at[came, c], buf.at[came, c], sib))
    for n in range(2):
        s["rk"][n, pl.ds(me_y, 1)] = s["ks"][n, pl.ds(me_y, 1)]
        s["rv"][n, pl.ds(me_z, 1)] = s["vs"][n, pl.ds(me_z, 1)]

    for n, (_, index, buf) in enumerate(gathers):
        came = ring(index, 2)
        rounded(n, came, c)
        down[6 + n].wait()
        rounded(n, came, 1 - c)

    def product(left, right, n):
        right = s[right][n].reshape(8 * TOK, PAIR).astype(BF16)
        for b in range(4):
            yield b, dot(s[left][b * 256 : (b + 1) * 256, :], right, NN)

    part1, recv1, part2, recv2 = s["part1"], s["recv1"], s["part2"], s["recv2"]

    def scatter(part, recv, chunk, axis, index):
        out = []
        for d in (1, 2, 3):
            to = ring(index, d)
            out.append(remote(part.at[chunk, to], recv.at[chunk, index], {axis: to}))
        recv[chunk, pl.ds(index, 1)] = part[chunk, pl.ds(index, 1)]
        return out

    wait(firsts[0][0])
    for b, block in product("hyb", "rk", 0):
        for j in range(4):
            part1[0, j, b * 64 : b * 64 + 64, :] = block[j * 64 : j * 64 + 64, :]
    k0 = scatter(part1, recv1, 0, "x", x)
    wait(firsts[0][1])
    for b, block in product("hzb", "rv", 0):
        for j in range(4):
            part1[2, j, b * 64 : b * 64 + 64, :] = block[j * 64 : j * 64 + 64, :]
    v0 = scatter(part1, recv1, 2, "x", x)

    for n in range(2):
        for to in range(8):
            query_part(to, n)
    stores = []

    def store(ref, hbm):
        cp = pltpu.make_async_copy(ref, hbm, local_sem.at[24 + len(stores)])
        cp.start()
        stores.append(cp)

    store(qg_ref, qg_hbm)
    store(s["gate"], gate_hbm)

    ones = jnp.ones((8, PAIR), F32)
    inner_sum = dot_exact(ones, s["gint"][...].reshape(256, PAIR), NT)
    pick = (cols_i[0:8, :] // 64 == row8 - 2).astype(F32)
    outer_sum = dot_exact(pick, s["gcross"][...].reshape(128, PAIR), NT)
    start = (cols_i[0:8, :] == 0).astype(F32)
    own_total = dot_exact(start, s["gate"][...].reshape(128, TOK), NT)
    small, m1, m1s, m2, m2s, m3 = (s[n] for n in ("small", "m1", "m1s", "m2", "m2s", "m3"))
    small[0:8, :] = jnp.where(
        row8 == 0, inner_sum[:, :128], jnp.where(row8 == 1, inner_sum[:, 128:], outer_sum)
    )
    small[8:16, :] = own_total
    smalls = []
    for d, e in offsets:
        smalls.append(remote(small, m1.at[me_z], plane("z", z, d, e)[0]))
    m1[pl.ds(me_z, 1)] = small[...][None]

    def input_grad(n, carry):
        rows = rows_of(n * 256, 256)
        ig_ref[:, rows] = (
            dot(s["ksb"][...], s["wk"][rows, :], NT) + dot(s["vsb"][...], s["wv"][rows, :], NT)
        ).astype(BF16)
        return carry


    wait(firsts[1][0])
    for b, block in product("hyb", "rk", 1):
        part1[1, b] = block
    k1 = scatter(part1, recv1, 1, "z", z)
    wait(firsts[1][1])
    for b, block in product("hzb", "rv", 1):
        for j in range(8):
            for i in range(4):
                at = j * 32 + i * 8
                part1[3, i, b * 64 + j * 8 : b * 64 + j * 8 + 8, :] = block[at : at + 8, :]
    v1 = scatter(part1, recv1, 3, "batch", y)
    lax.fori_loop(0, 4, input_grad, 0)
    store(ig_ref, ig_hbm)

    wait(smalls)
    total = m1[0, 0:8, :]
    for g in range(1, 8):
        total = total + m1[g, 0:8, :]
    m1s[0:8, :] = total
    for g in range(8):
        m1s[8 + g : 9 + g, :] = m1[g, 8:9, :]
    smalls = [remote(m1s, m2.at[x], {"x": ring(x, d)}) for d in (1, 2, 3)]
    m2[pl.ds(x, 1)] = m1s[...][None]

    def summed(recv, chunk):
        return recv[chunk, 0] + recv[chunk, 1] + recv[chunk, 2] + recv[chunk, 3]

    wait(k0)
    total = summed(recv1, 0)
    for j in range(4):
        part2[0, j] = total[j * 64 : j * 64 + 64, :]
    k0 = scatter(part2, recv2, 0, "z", z)
    wait(v0)
    total = summed(recv1, 2)
    for j in range(8):
        for i in range(4):
            at = j * 32 + i * 8
            part2[2, i, j * 8 : j * 8 + 8, :] = total[at : at + 8, :]
    v0 = scatter(part2, recv2, 2, "batch", y)
    wait(k1)
    total = summed(recv1, 1)
    for j in range(4):
        part2[1, j] = total[j * 64 : j * 64 + 64, :]
    k1 = scatter(part2, recv2, 1, "x", x)
    wait(v1)
    total = summed(recv1, 3)
    for j in range(4):
        for i in range(4):
            at = j * 64 + i * 16
            part2[3, i, j * 16 : j * 16 + 16, :] = total[at : at + 16, :]
    v1 = scatter(part2, recv2, 3, "x", x)

    wait(smalls)
    total = m2[0, 0:8, :] + m2[1, 0:8, :] + m2[2, 0:8, :] + m2[3, 0:8, :]
    m2s[...] = total
    smalls = [remote(m2s, m3.at[y], {"batch": ring(y, d)}) for d in (1, 2, 3)]
    m3[pl.ds(y, 1)] = total[None]
    place = z * 8 + x * 2 + c
    later = jnp.zeros((1, PAIR), F32)
    for j in range(4):
        for g in range(8):
            spot = (g // 2) * 8 + j * 2 + g % 2
            later = later + (place < spot).astype(F32) * m2[j, 8 + g : 9 + g, :]
    sout_ref[8:16, :] = jnp.broadcast_to(later, (8, PAIR))

    fins = []
    wait(k0)
    wait(k1)
    for n in range(2):
        total = summed(recv2, n)
        for i in range(4):
            for j in range(2):
                at = j * 32 + i * 8
                s["kown"][2 * i + j, n] = total[at : at + 8, :]
    for d, e in offsets:
        dev, to = plane("batch", y, d, e)
        fins.append(remote(s["kown"].at[to], s["kfin"].at[me_y], dev))
    s["kfin"][pl.ds(me_y, 1)] = s["kown"][pl.ds(me_y, 1)]
    wait(v0)
    wait(v1)
    for n in range(2):
        total = summed(recv2, 2 + n)
        for j in range(8):
            s["vown"][j, n] = total[j * 8 : j * 8 + 8, :]
    for d, e in offsets:
        dev, to = plane("z", z, d, e)
        fins.append(remote(s["vown"].at[to], s["vfin"].at[me_z], dev))
    s["vfin"][pl.ds(me_z, 1)] = s["vown"][pl.ds(me_z, 1)]
    wait(smalls)
    sout_ref[0:8, :] = m3[0] + m3[1] + m3[2] + m3[3]
    store(sout_ref, sout_hbm)
    wait(fins)
    for n in range(2):
        for g in range(8):
            cols = slice((2 * g + n) * PAIR, (2 * g + n + 1) * PAIR)
            kout_ref[:, cols] = s["kfin"][g, n]
            vout_ref[:, cols] = s["vfin"][g, n]
    store(kout_ref, kout_hbm)
    store(vout_ref, vout_hbm)
    wait(stores)


def whole_step(hidden, queries, out_grad, w_key, w_value, log_gate, seg_row, level_gain):
    far = pl.BlockSpec(memory_space=pltpu.HBM)
    return pl.pallas_call(
        step_kernel,
        in_specs=[far] * 8,
        out_specs=[far] * 6,
        out_shape=[
            jax.ShapeDtypeStruct((TOK, 2048), BF16),
            jax.ShapeDtypeStruct((TOK, 1024), BF16),
            jax.ShapeDtypeStruct((16, 8, TOK), F32),
            jax.ShapeDtypeStruct((8, 2048), F32),
            jax.ShapeDtypeStruct((8, 2048), F32),
            jax.ShapeDtypeStruct((16, PAIR), F32),
        ],
        scratch_shapes=list(scratch().values()),
        compiler_params=pltpu.CompilerParams(
            collective_id=0, has_side_effects=True, vmem_limit_bytes=VMEM_LIMIT
        ),
        name="whole_step",
    )(hidden, queries, out_grad, w_key, w_value, log_gate, seg_row, level_gain)


def finish_kernel(
    qg_in, ig_in, gate_in, kw_in, vw_in, small_in, qg_out, ig_out, gate_out, kw_out, vw_out, gains_out,
    qg, ig, gate_ref, kw, vw, small_ref, gate, gains, load_sem, store_sem
):
    loads = [
        pltpu.make_async_copy(a, b, load_sem.at[n])
        for n, (a, b) in enumerate(
            ((gate_in, gate_ref), (small_in, small_ref), (qg_in, qg), (ig_in, ig), (kw_in, kw), (vw_in, vw))
        )
    ]
    for cp in loads:
        cp.start()
    stores = []

    def store(ref, out):
        cp = pltpu.make_async_copy(ref, out, store_sem.at[len(stores)])
        cp.start()
        stores.append(cp)

    loads[0].wait()
    loads[1].wait()
    heads = gate.shape[0]
    lane = iota((heads, PAIR), 1)
    head = iota((heads, PAIR), 0)
    small = small_ref[...]
    later = jnp.broadcast_to(small[8:9, :], (TOK, TOK)).T
    rows = gate_ref[...].reshape(TOK, TOK) + later
    gate[...] = dot_exact((lane == (head // 2) * 8 + head % 2).astype(F32), rows, NN)
    levels = gains.shape[0]
    level, at = iota((levels, PAIR), 0), iota((levels, PAIR), 1) % 8
    first = (level == at).astype(F32)
    second = (level == at + 8).astype(F32)
    pick0 = jnp.where(lane // 8 == head, small[0:1, :], 0.0)
    pick1 = jnp.where(lane // 8 + 16 == head, small[1:2, :], 0.0)
    pair = jnp.where(head % 2 == 0, small[2:3, :], small[3:4, :])
    pick2 = jnp.where(lane // 8 == head // 2, pair, 0.0)
    gains[...] = dot_exact(first, pick0 + pick1, NT) + dot_exact(second, pick2, NT)
    for cp, ref, out in zip(
        loads[2:], (qg, ig, kw, vw), (qg_out, ig_out, kw_out, vw_out)
    ):
        cp.wait()
        store(ref, out)
    store(gate, gate_out)
    store(gains, gains_out)
    for cp in stores:
        cp.wait()


def finish(query_grad, input_grad, gate, key_weight, value_weight, small, heads, levels):
    far = pl.BlockSpec(memory_space=pltpu.HBM)
    parts = (query_grad, input_grad, gate, key_weight, value_weight, small)
    outs = [jax.ShapeDtypeStruct(a.shape, a.dtype) for a in parts]
    outs[2] = jax.ShapeDtypeStruct((heads, TOK), F32)
    outs[5] = jax.ShapeDtypeStruct((levels, heads), F32)
    return pl.pallas_call(
        finish_kernel,
        in_specs=[far] * 6,
        out_specs=[far] * 6,
        out_shape=outs,
        scratch_shapes=[pltpu.VMEM(a.shape, a.dtype) for a in (*parts, outs[2], outs[5])]
        + [pltpu.SemaphoreType.DMA((6,)), pltpu.SemaphoreType.DMA((6,))],
        name="finish",
    )(*parts)


def local(hidden, queries, w_key, w_value, log_gate, level_gain, segment_ids, out_grad):
    heads, levels = level_gain.shape
    parts = whole_step(
        hidden[0], queries[0], out_grad[0], w_key, w_value, log_gate[0], segment_ids, level_gain.T
    )
    query_grad, input_grad, gate_grad, key_weight, value_weight, gains = finish(
        *parts, heads, levels
    )
    return (
        query_grad[None],
        input_grad[None],
        gate_grad[None],
        key_weight,
        value_weight,
        gains.T,
    )


def solution(mesh):
    split = Mesh(
        mesh.devices.reshape(4, 4, 2, mesh.shape["batch"]), ("z", "x", "core", "batch")
    )
    return jax.shard_map(
        local,
        mesh=split,
        in_specs=(
            P("batch", SEQ, None),
            P("batch", SEQ, None),
            P(),
            P(),
            P("batch", None, SEQ),
            P(),
            P("batch", SEQ),
            P("batch", SEQ, None),
        ),
        out_specs=(
            P("batch", SEQ, None),
            P("batch", SEQ, None),
            P("batch", None, SEQ),
            P(SEQ_BATCH, None),
            P(SEQ_BATCH, None),
            P(),
        ),
        check_vma=False,
    )
```
